32 devices in a mesh: data: 1 (over z), inner: 4 (over y), stage: 8 (over x, core).
Axes of the slice: x: 4, y: 4, z: 1, core: 2. Of those that a mesh axis runs over, the one named last changes fastest.
The devices are a block of a 4x4x8 slice.
Arguments:
- x: bfloat16 [8, 256, 1024], P(('data', 'stage'), 'inner')
- g: bfloat16 [8, 256, 1024], P(('data', 'stage'), 'inner')
- w1: bfloat16 [1, 8, 1024, 4096], P(None, 'stage')
- w2: bfloat16 [1, 8, 4096, 1024], P(None, 'stage')
Outputs:
- output 1: bfloat16 [8, 256, 1024], P(('data', 'stage'), 'inner')
- output 2: bfloat16 [8, 256, 1024], P(('data', 'stage'), 'inner')
- output 3: float32 [1, 8, 1024, 4096], P('data', 'stage')
- output 4: float32 [1, 8, 4096, 1024], P('data', 'stage')
All inputs are finite; a program needn't handle non-finite values.
Results may differ from the reference program's by a relative error of at most 0.02.
Values are sent between devices in bfloat16 or wider.
A program may use at most 768 MiB of HBM per device.

```python
import jax
import jax.numpy as jnp
from jax import lax

D = 1024
FF = 4096
V = 1
K = 1
STAGE = 8
MICRO = 8
B = 256

LAYERS = V * STAGE * K


def setup_inputs(seed: int = 0, part: int = 0) -> dict:
    key = jax.random.PRNGKey(seed)
    kbase, kshared = jax.random.split(key)
    kx, kg = jax.random.split(jax.random.fold_in(kbase, part))
    k1, k2 = jax.random.split(kshared)
    x = jax.random.normal(kx, (MICRO, B, D), jnp.float32).astype(jnp.bfloat16)
    g = jax.random.normal(kg, (MICRO, B, D), jnp.float32).astype(jnp.bfloat16)
    w1 = (jax.random.normal(k1, (V, STAGE * K, D, FF), jnp.float32) * D ** -0.5).astype(jnp.bfloat16)
    w2 = (jax.random.normal(k2, (V, STAGE * K, FF, D), jnp.float32) * (2.0 * (FF * LAYERS) ** -0.5)).astype(jnp.bfloat16)
    return {"x": x, "g": g, "w1": w1, "w2": w2}


def _gelu(t):
    return jax.nn.gelu(t, approximate=True)


def _layer_fwd(h, w1, w2):
    z = jnp.dot(h, w1, preferred_element_type=jnp.float32)
    a = _gelu(z).astype(jnp.bfloat16)
    u = jnp.dot(a, w2, preferred_element_type=jnp.float32)
    return (h.astype(jnp.float32) + u).astype(jnp.bfloat16)


def _layer_bwd(h, dh, w1, w2):
    z = jnp.dot(h, w1, preferred_element_type=jnp.float32)
    a32, gelu_vjp = jax.vjp(_gelu, z)
    a = a32.astype(jnp.bfloat16)
    dw2 = jnp.dot(a.T, dh, preferred_element_type=jnp.float32)
    da = jnp.dot(dh, w2.T, preferred_element_type=jnp.float32)
    dz = gelu_vjp(da)[0].astype(jnp.bfloat16)
    dw1 = jnp.dot(h.T, dz, preferred_element_type=jnp.float32)
    dh_prev = (dh.astype(jnp.float32) + jnp.dot(dz, w1.T, preferred_element_type=jnp.float32)).astype(jnp.bfloat16)
    return dh_prev, dw1, dw2


def reference(x, g, w1, w2):
    w1s = w1.reshape(LAYERS, D, FF)
    w2s = w2.reshape(LAYERS, FF, D)

    def one_micro(acc, xg):
        dw1_acc, dw2_acc = acc
        xm, gm = xg

        def fwd(h, w):
            return _layer_fwd(h, w[0], w[1]), h

        y, hs = lax.scan(fwd, xm, (w1s, w2s))

        def bwd(dh, inp):
            h, a, b = inp
            dh_prev, d1, d2 = _layer_bwd(h, dh, a, b)
            return dh_prev, (d1, d2)

        dx, (d1s, d2s) = lax.scan(bwd, gm, (hs, w1s, w2s), reverse=True)
        return (dw1_acc + d1s, dw2_acc + d2s), (y, dx)

    init = (jnp.zeros((LAYERS, D, FF), jnp.float32), jnp.zeros((LAYERS, FF, D), jnp.float32))
    (dw1, dw2), (y, dx) = lax.scan(one_micro, init, (x, g))
    return y, dx, dw1.reshape(w1.shape), dw2.reshape(w2.shape)
```

```python
import functools

import jax
import jax.numpy as jnp
from jax import lax
from jax.experimental import pallas as pl
from jax.experimental.pallas import tpu as pltpu
from jax.sharding import PartitionSpec as P

MESH = pl.DeviceIdType.MESH
F32, BF16 = jnp.float32, jnp.bfloat16
C0, C1 = 0.7978845608028654, 0.044715
VMEM_LIMIT = 62 * 2**20


def _gelu(z):
    return z * (0.5 * (1.0 + jnp.tanh(C0 * (z + C1 * (z * z * z)))))


def _gelu_and_slope(z):
    z2 = z * z
    t = jnp.tanh(C0 * (z + C1 * (z2 * z)))
    half = 0.5 * (1.0 + t)
    return z * half, half + (0.5 * z) * (1.0 - t * t) * (C0 + (3.0 * C0 * C1) * z2)


def _dot(a, b):
    return jnp.dot(a, b, preferred_element_type=F32)


def _chain_kernel(
    n_stage, n_inner, x, g, w1, w2, y, dx, h_all, g_all,
    w1v, w2v, w1t, w2t, hs, gs, ho, go, zb, ab,
    wsem, xsem, h_recv, g_recv, h_send, g_send, out_recv, ring_send, ring_recv,
):
    p, i = lax.axis_index("stage"), lax.axis_index("inner")
    right, left = lax.rem(i + 1, n_inner), lax.rem(i + n_inner - 1, n_inner)
    m_all, rows, d = hs.shape
    f = w1v.shape[1]
    half = rows // 2
    last = n_stage - 1
    cw = min(512, f)

    loads = [
        pltpu.make_async_copy(w1.at[0, 0], w1v, wsem.at[0]),
        pltpu.make_async_copy(w2.at[0, 0], w2v, wsem.at[1]),
    ]
    for c in loads:
        c.start()

    barrier = pltpu.get_barrier_semaphore()
    for q in range(1, n_stage):
        pl.semaphore_signal(barrier, inc=1, device_id={"stage": lax.rem(p + q, n_stage)}, device_id_type=MESH)
    for q in (left, right):
        pl.semaphore_signal(barrier, inc=1, device_id={"inner": q}, device_id_type=MESH)
    pl.semaphore_wait(barrier, n_stage + 1)

    def to_stage(src, dst, send, recv, stage):
        return pltpu.make_async_remote_copy(
            src_ref=src, dst_ref=dst, send_sem=send, recv_sem=recv,
            device_id={"stage": stage}, device_id_type=MESH,
        )

    def to_inner(src, dst, send, recv, inner):
        return pltpu.make_async_remote_copy(
            src_ref=src, dst_ref=dst, send_sem=send, recv_sem=recv,
            device_id={"inner": inner}, device_id_type=MESH,
        )

    def own(src, slots, recv, sem, stage):
        @pl.when(p == stage)
        def _():
            pltpu.make_async_copy(src.at[0], slots.at[p], recv.at[p]).start()

        @pl.when(p != stage)
        def _():
            to_stage(src.at[0], slots.at[p], sem, recv.at[p], stage).start()

    own(x, hs, h_recv, xsem.at[0], 0)
    own(g, gs, g_recv, xsem.at[1], last)

    def ring_first(q, m, slots, whole):
        pltpu.make_async_copy(slots.at[m], whole.at[i, m], ring_send.at[q, m, 4]).start()
        to_inner(slots.at[m], whole.at[i, m], ring_send.at[q, m, 0], ring_recv.at[q, m, 0], right).start()
        to_inner(slots.at[m], whole.at[i, m], ring_send.at[q, m, 1], ring_recv.at[q, m, 1], left).start()

    def ring_forward(q, m, whole):
        a, b = whole.at[left, m], whole.at[right, m]
        to_inner(a, a, ring_send.at[q, m, 0], ring_recv.at[q, m, 0], right).wait_recv()
        a = whole.at[left, m, pl.ds(0, half)]
        to_inner(a, a, ring_send.at[q, m, 2], ring_recv.at[q, m, 2], right).start()
        to_inner(b, b, ring_send.at[q, m, 1], ring_recv.at[q, m, 1], left).wait_recv()
        b = whole.at[right, m, pl.ds(half, half)]
        to_inner(b, b, ring_send.at[q, m, 3], ring_recv.at[q, m, 3], left).start()

    def ring_finish(q, m, slots, whole):
        far = lax.rem(i + 2, n_inner)
        a, b = whole.at[far, m, pl.ds(0, half)], whole.at[far, m, pl.ds(half, half)]
        to_inner(a, a, ring_send.at[q, m, 2], ring_recv.at[q, m, 2], right).wait()
        to_inner(b, b, ring_send.at[q, m, 3], ring_recv.at[q, m, 3], left).wait()
        to_inner(slots.at[m], whole.at[i, m], ring_send.at[q, m, 0], ring_recv.at[q, m, 0], right).wait_send()
        to_inner(slots.at[m], whole.at[i, m], ring_send.at[q, m, 1], ring_recv.at[q, m, 1], left).wait_send()
        pltpu.make_async_copy(slots.at[m], whole.at[i, m], ring_send.at[q, m, 4]).wait()

    def pass_on(m, src, slots, send, recv, end, nxt, out, out_sem):
        @pl.when(p != end)
        def _():
            to_stage(src.at[m], slots.at[m], send.at[m], recv.at[m], nxt).start()

        @pl.when((p == end) & (p != m))
        def _():
            to_stage(src.at[m], out.at[0], send.at[m], out_sem, m).start()

        @pl.when((p == end) & (p == m))
        def _():
            pltpu.make_async_copy(src.at[m], out.at[0], out_sem).start()

    def forward(m):
        pltpu.make_async_copy(hs.at[m], hs.at[m], h_recv.at[m]).wait()
        ring_first(0, m, hs, h_all)
        h = hs[m]
        for c in range(0, f, cw):
            z = _dot(h, w1v[:, c : c + cw])
            zb[m, :, c : c + cw] = z
            ab[:, c : c + cw] = _gelu(z).astype(BF16)
        ho[m] = (h.astype(F32) + _dot(ab[...], w2v[...])).astype(BF16)
        pass_on(m, ho, hs, h_send, h_recv, last, jnp.minimum(p + 1, last), y, out_recv.at[0])

    def backward(m):
        pltpu.make_async_copy(gs.at[m], gs.at[m], g_recv.at[m]).wait()
        ring_first(1, m, gs, g_all)

        @pl.when(p < n_stage - 2)
        def _():
            ring_forward(0, m, h_all)

        dh = gs[m]
        for c in range(0, f, cw):
            da = _dot(dh, w2t[:, c : c + cw])
            _, slope = _gelu_and_slope(zb[m, :, c : c + cw])
            ab[:, c : c + cw] = (da * slope).astype(BF16)
        go[m] = (dh.astype(F32) + _dot(ab[...], w1t[...])).astype(BF16)
        pass_on(m, go, gs, g_send, g_recv, 0, jnp.maximum(p - 1, 0), dx, out_recv.at[1])

    def transpose_weights():
        tw = min(256, d)

        def some(t, carry):
            s = pl.ds(pl.multiple_of(t * tw, tw), tw)
            w1t[s, :] = w1v[:, s].T
            w2t[:, s] = w2v[s, :].T
            return carry

        lax.fori_loop(0, f // tw, some, 0)

    for c in loads:
        c.wait()

    first = jnp.where(p == last, 1, jnp.where(p == last - 1, min(4, m_all), m_all))
    rest = m_all - first
    turn = jnp.where(p < n_stage // 2, first, 0)

    def step(k, carry):
        j = k - first
        alternating = j < 2 * rest
        is_f = (j < 0) | (alternating & (j % 2 == 1))
        m_f = jnp.where(j < 0, k, jnp.minimum(first + j // 2, m_all - 1))
        m_b = jnp.where(j < 0, 0, jnp.where(alternating, j // 2, j - rest))

        @pl.when(k == turn)
        def _():
            transpose_weights()

        @pl.when(is_f)
        def _():
            forward(m_f)

        @pl.when(jnp.logical_not(is_f))
        def _():
            backward(m_b)

        return carry

    lax.fori_loop(0, 2 * m_all, step, 0)

    def each(fn):
        lax.fori_loop(0, m_all, lambda m, c: (fn(m), c)[1], 0)

    @pl.when(p >= n_stage - 2)
    def _():
        each(lambda m: ring_forward(0, m, h_all))

    each(lambda m: ring_forward(1, m, g_all))

    def finish(m):
        ring_finish(0, m, hs, h_all)
        ring_finish(1, m, gs, g_all)

        @pl.when((p != last) | (p != m))
        def _():
            to_stage(ho.at[m], hs.at[m], h_send.at[m], h_recv.at[m], 0).wait_send()

        @pl.when((p != 0) | (p != m))
        def _():
            to_stage(go.at[m], gs.at[m], g_send.at[m], g_recv.at[m], 0).wait_send()

    each(finish)

    @pl.when(p != 0)
    def _():
        to_stage(x.at[0], hs.at[0], xsem.at[0], h_recv.at[0], 0).wait_send()

    @pl.when(p != last)
    def _():
        to_stage(g.at[0], gs.at[0], xsem.at[1], g_recv.at[0], last).wait_send()

    pltpu.make_async_copy(y.at[0], y.at[0], out_recv.at[0]).wait()
    pltpu.make_async_copy(dx.at[0], dx.at[0], out_recv.at[1]).wait()


def _chain(n_stage, n_inner, x, g, w1, w2):
    mb, rows, d = x.shape
    f = w1.shape[-1]
    m_all = mb * n_stage
    hbm = pl.BlockSpec(memory_space=pltpu.HBM)
    whole = jax.ShapeDtypeStruct((n_inner, m_all, rows, d), BF16)
    dma = pltpu.SemaphoreType.DMA
    slots = pltpu.VMEM((m_all, rows, d), BF16)
    return pl.pallas_call(
        functools.partial(_chain_kernel, n_stage, n_inner),
        out_shape=[jax.ShapeDtypeStruct(x.shape, BF16), jax.ShapeDtypeStruct(x.shape, BF16), whole, whole],
        in_specs=[hbm] * 4,
        out_specs=[hbm] * 4,
        scratch_shapes=[
            pltpu.VMEM((d, f), BF16), pltpu.VMEM((f, d), BF16),
            pltpu.VMEM((f, d), BF16), pltpu.VMEM((d, f), BF16),
            slots, slots, slots, slots,
            pltpu.VMEM((m_all, rows, f), F32), pltpu.VMEM((rows, f), BF16),
            dma((2,)), dma((2,)), dma((m_all,)), dma((m_all,)), dma((m_all,)), dma((m_all,)), dma((2,)),
            dma((2, m_all, 5)), dma((2, m_all, 4)),
        ],
        compiler_params=pltpu.CompilerParams(
            collective_id=0, has_side_effects=True, vmem_limit_bytes=VMEM_LIMIT
        ),
        name="chain",
    )(x, g, w1, w2)


def _dw_kernel(tc, h, g, w1, w2, d1, d2, ht, ab, zb):
    t_all, _ = h.shape

    @pl.when(pl.program_id(0) == 0)
    def _():
        tw = min(256, t_all)
        for t in range(0, t_all, tw):
            ht[:, t : t + tw] = h[t : t + tw, :].T

    def some(t, carry):
        s = pl.ds(pl.multiple_of(t * tc, tc), tc)
        z = _dot(h[s, :], w1[...])
        da = lax.dot_general(g[s, :], w2[...], (((1,), (1,)), ((), ())), preferred_element_type=F32)
        a, slope = _gelu_and_slope(z)
        ab[s, :] = a.astype(BF16)
        zb[s, :] = (da * slope).astype(BF16)
        return carry

    lax.fori_loop(0, t_all // tc, some, 0)
    d1[...] = _dot(ht[...], zb[...])
    d2[...] = lax.dot_general(ab[...], g[...], (((0,), (0,)), ((), ())), preferred_element_type=F32)


def _dw(h, g, w1, w2):
    t, d = h.shape
    f = w1.shape[1]
    blk = min(512, f)
    return pl.pallas_call(
        functools.partial(_dw_kernel, min(512, t)),
        grid=(f // blk,),
        in_specs=[
            pl.BlockSpec((t, d), lambda j: (0, 0)), pl.BlockSpec((t, d), lambda j: (0, 0)),
            pl.BlockSpec((d, blk), lambda j: (0, j)), pl.BlockSpec((blk, d), lambda j: (j, 0)),
        ],
        out_specs=[pl.BlockSpec((d, blk), lambda j: (0, j)), pl.BlockSpec((blk, d), lambda j: (j, 0))],
        out_shape=[jax.ShapeDtypeStruct((d, f), F32), jax.ShapeDtypeStruct((f, d), F32)],
        scratch_shapes=[pltpu.VMEM((d, t), BF16), pltpu.VMEM((t, blk), BF16), pltpu.VMEM((t, blk), BF16)],
        compiler_params=pltpu.CompilerParams(vmem_limit_bytes=VMEM_LIMIT),
        cost_estimate=pl.CostEstimate(flops=8 * t * d * f, bytes_accessed=12 * d * f, transcendentals=t * f),
        name="dw",
    )(h, g, w1, w2)


def solution(mesh):
    n_stage, n_inner = mesh.shape["stage"], mesh.shape["inner"]

    def body(x, g, w1, w2):
        d, f = w1.shape[-2:]
        y, dx, h_all, g_all = _chain(n_stage, n_inner, x, g, w1, w2)
        d1, d2 = _dw(h_all.reshape(-1, d), g_all.reshape(-1, d), w1.reshape(d, f), w2.reshape(f, d))
        return y, dx, d1.reshape(w1.shape), d2.reshape(w2.shape)

    tok = P(("data", "stage"), "inner", None)
    wsp = P(None, "stage", None, None)
    dsp = P("data", "stage", None, None)
    return jax.shard_map(body, mesh=mesh, in_specs=(tok, tok, wsp, wsp), out_specs=(tok, tok, dsp, dsp), check_vma=False)
```

```python
import functools

import jax
import jax.numpy as jnp
from jax import lax
from jax.experimental import pallas as pl
from jax.experimental.pallas import tpu as pltpu
from jax.sharding import PartitionSpec as P

MESH = pl.DeviceIdType.MESH
F32, BF16 = jnp.float32, jnp.bfloat16
C0, C1 = 0.7978845608028654, 0.044715
LANES = 128
VMEM_LIMIT = 67043328
SLABS = 4


def _gelu(z):
    return z * (0.5 * jnp.tanh(z * (C0 + (C0 * C1) * (z * z))) + 0.5)


def _gelu_and_slope(z):
    z2 = z * z
    half = 0.5 * jnp.tanh(z * (C0 + (C0 * C1) * z2)) + 0.5
    a = z * half
    return a, half + (a - a * half) * (2.0 * C0 + (6.0 * C0 * C1) * z2)


def _dot(a, b):
    return jnp.dot(a, b, preferred_element_type=F32)


def _wide(slabs):
    return jnp.concatenate(slabs, axis=1)


def _tall(parts):
    return jnp.concatenate(parts, axis=0)


def _cut(value, c):
    return value[:, c * LANES : (c + 1) * LANES]


def _dw_block(rows, hg, gg, groups, group_rows, nd, w1_block, w2_block, w2_transposed, ht, ab, zb, settle, put):
    def some(read, ks):
        return _tall([_wide([read(k, c) for c in range(nd)]) for k in ks])

    step = max(1, rows // group_rows)
    for k in range(0, groups, step):
        ks = range(k, min(k + step, groups))
        s = slice(k * group_rows, (k + len(ks)) * group_rows)
        z = _dot(some(hg, ks), w1_block())
        dims = (((1,), (0,)), ((), ())) if w2_transposed else (((1,), (1,)), ((), ()))
        da = lax.dot_general(some(gg, ks), w2_block(), dims, preferred_element_type=F32)
        a, slope = _gelu_and_slope(z)
        a, dz = a.astype(BF16), (da * slope).astype(BF16)
        for c in range(SLABS):
            ab[c, s, :] = _cut(a, c)
            zb[c, s, :] = _cut(dz, c)
    settle()
    put(
        _dot(_wide([ht[t] for t in range(ht.shape[0])]), _wide([zb[c] for c in range(SLABS)])),
        lax.dot_general(
            _wide([ab[c] for c in range(SLABS)]), some(gg, range(groups)), (((0,), (0,)), ((), ())),
            preferred_element_type=F32,
        ),
    )


def _transposed_rows(hg, groups, group_rows, nd, ht):
    per = LANES // group_rows
    for t in range(groups // per):
        ht[t] = _tall([_wide([hg(t * per + e, c) for c in range(nd)]) for e in range(per)]).T


def _chain_kernel(
    n_stage, n_inner, x, g, w1, w2, y, dx, h_late, g_late, d1_part, d2_part,
    w1v, w2v, w1t, w2t, hw, gw, ho, go, zs, act, ht, ab, zb, d1v, d2v,
    wsem, xsem, h_recv, g_recv, h_send, g_send, out_recv, ring_send, ring_recv, part_sem, late_sem,
):
    p, i = lax.axis_index("stage"), lax.axis_index("inner")
    right, left = lax.rem(i + 1, n_inner), lax.rem(i + n_inner - 1, n_inner)
    _, m_all, nd, rows, _ = hw.shape
    nf = w1v.shape[0]
    units = nf // SLABS
    early = m_all // 2
    last = n_stage - 1
    half = nd // 2

    barrier = pltpu.get_barrier_semaphore()
    for q in range(1, n_stage):
        pl.semaphore_signal(barrier, inc=1, device_id={"stage": lax.rem(p + q, n_stage)}, device_id_type=MESH)
    for q in (left, right):
        pl.semaphore_signal(barrier, inc=1, device_id={"inner": q}, device_id_type=MESH)

    loads = [
        pltpu.make_async_copy(w1.at[0, 0, :, c * LANES : (c + 1) * LANES], w1v.at[c], wsem.at[0]) for c in range(nf)
    ] + [pltpu.make_async_copy(w2.at[0, 0, :, c * LANES : (c + 1) * LANES], w2v.at[c], wsem.at[1]) for c in range(nd)]
    for c in loads:
        c.start()
    with jax.named_scope("barrier"):
        pl.semaphore_wait(barrier, n_stage + 1)

    def to_stage(src, dst, send, recv, stage):
        return pltpu.make_async_remote_copy(
            src_ref=src, dst_ref=dst, send_sem=send, recv_sem=recv,
            device_id={"stage": stage}, device_id_type=MESH,
        )

    def to_inner(src, dst, send, recv, inner):
        return pltpu.make_async_remote_copy(
            src_ref=src, dst_ref=dst, send_sem=send, recv_sem=recv,
            device_id={"inner": inner}, device_id_type=MESH,
        )

    def flat(ref, c):
        return ref.at[0, :, c * LANES : (c + 1) * LANES]

    def own(src, slots, recv, sem, stage):
        @pl.when(p == stage)
        def _():
            for c in range(nd):
                pltpu.make_async_copy(flat(src, c), slots.at[i, p, c], recv.at[p]).start()

        @pl.when(p != stage)
        def _():
            for c in range(nd):
                to_stage(flat(src, c), slots.at[i, p, c], sem, recv.at[p], stage).start()

    own(x, hw, h_recv, xsem.at[0], 0)
    own(g, gw, g_recv, xsem.at[1], last)

    def ring_first(q, m, whole):
        a = whole.at[i, m]
        to_inner(a, a, ring_send.at[q, m, 0], ring_recv.at[q, m, 0], right).start()
        to_inner(a, a, ring_send.at[q, m, 1], ring_recv.at[q, m, 1], left).start()

    def ring_forward(q, m, whole):
        a, b = whole.at[left, m], whole.at[right, m]
        to_inner(a, a, ring_send.at[q, m, 0], ring_recv.at[q, m, 0], right).wait_recv()
        a = whole.at[left, m, pl.ds(0, half)]
        to_inner(a, a, ring_send.at[q, m, 2], ring_recv.at[q, m, 2], right).start()
        to_inner(b, b, ring_send.at[q, m, 1], ring_recv.at[q, m, 1], left).wait_recv()
        b = whole.at[right, m, pl.ds(half, half)]
        to_inner(b, b, ring_send.at[q, m, 3], ring_recv.at[q, m, 3], left).start()

    def ring_far(q, m, whole):
        far = lax.rem(i + 2, n_inner)
        a, b = whole.at[far, m, pl.ds(0, half)], whole.at[far, m, pl.ds(half, half)]
        return (
            to_inner(a, a, ring_send.at[q, m, 2], ring_recv.at[q, m, 2], right),
            to_inner(b, b, ring_send.at[q, m, 3], ring_recv.at[q, m, 3], left),
        )

    def ring_arrived(m):
        for q, whole in ((0, hw), (1, gw)):
            for c in ring_far(q, m, whole):
                c.wait_recv()

    def ring_sent(m):
        for q, whole in ((0, hw), (1, gw)):
            for c in ring_far(q, m, whole):
                c.wait_send()
            a = whole.at[i, m]
            to_inner(a, a, ring_send.at[q, m, 0], ring_recv.at[q, m, 0], right).wait_send()
            to_inner(a, a, ring_send.at[q, m, 1], ring_recv.at[q, m, 1], left).wait_send()

    def pass_on(m, src, slots, send, recv, end, nxt, out, out_sem):
        @pl.when(p != end)
        def _():
            to_stage(src.at[m], slots.at[i, m], send.at[m], recv.at[m], nxt).start()

        @pl.when((p == end) & (p != m))
        def _():
            for c in range(nd):
                to_stage(src.at[m, c], flat(out, c), send.at[m], out_sem, m).start()

        @pl.when((p == end) & (p == m))
        def _():
            for c in range(nd):
                pltpu.make_async_copy(src.at[m, c], flat(out, c), out_sem).start()

    def forward(m):
        with jax.named_scope("wait_h"):
            pltpu.make_async_copy(hw.at[i, m], hw.at[i, m], h_recv.at[m]).wait()
        ring_first(0, m, hw)
        h = _wide([hw[i, m, c] for c in range(nd)])
        for b in range(0, nf, SLABS):
            z = _dot(h, _wide([w1v[b + c] for c in range(SLABS)]))
            a = _gelu(z).astype(BF16)
            for c in range(SLABS):
                zs[m, b + c] = _cut(z, c)
                act[b + c] = _cut(a, c)
        u = _dot(_wide([act[c] for c in range(nf)]), _wide([w2v[c] for c in range(nd)]))
        out = (h.astype(F32) + u).astype(BF16)
        for c in range(nd):
            ho[m, c] = _cut(out, c)
        pass_on(m, ho, hw, h_send, h_recv, last, jnp.minimum(p + 1, last), y, out_recv.at[0])

    def backward(m):
        with jax.named_scope("wait_g"):
            pltpu.make_async_copy(gw.at[i, m], gw.at[i, m], g_recv.at[m]).wait()
        ring_first(1, m, gw)

        @pl.when(p < n_stage - 2)
        def _():
            ring_forward(0, m, hw)

        @pl.when((p < n_stage // 2) & (m > 0))
        def _():
            ring_forward(1, jnp.maximum(m - 1, 0), gw)

        dh = _wide([gw[i, m, c] for c in range(nd)])
        for b in range(0, nf, SLABS):
            da = _dot(dh, _wide([w2t[b + c] for c in range(SLABS)]))
            _, slope = _gelu_and_slope(_wide([zs[m, b + c] for c in range(SLABS)]))
            dz = (da * slope).astype(BF16)
            for c in range(SLABS):
                act[b + c] = _cut(dz, c)
        u = _dot(_wide([act[c] for c in range(nf)]), _wide([w1t[c] for c in range(nd)]))
        out = (dh.astype(F32) + u).astype(BF16)
        for c in range(nd):
            go[m, c] = _cut(out, c)
        pass_on(m, go, gw, g_send, g_recv, 0, jnp.maximum(p - 1, 0), dx, out_recv.at[1])

    def transpose_weights():
        def some(c, carry):
            s = pl.ds(pl.multiple_of(c * LANES, LANES), LANES)
            for e in range(nd):
                w1t[e, s, :] = w1v[c, e * LANES : (e + 1) * LANES, :].T
                w2t[c, e * LANES : (e + 1) * LANES, :] = w2v[e, s, :].T
            return carry

        lax.fori_loop(0, nf, some, 0)

    def each(lo, hi, fn):
        lax.fori_loop(lo, hi, lambda m, c: (fn(m), c)[1], 0)

    def group(whole):
        return lambda k, c: whole[k // early, k % early, c]

    groups = n_inner * early

    def part_copies(j):
        return (
            pltpu.make_async_copy(d1v, d1_part.at[j], part_sem.at[0]),
            pltpu.make_async_copy(d2v, d2_part.at[j], part_sem.at[1]),
        )

    def unit(j):
        @pl.when(j == 0)
        def _():
            @pl.when(p >= n_stage - 2)
            def _():
                each(0, m_all, lambda m: ring_forward(0, m, hw))

            @pl.when(p >= n_stage // 2)
            def _():
                each(0, m_all, lambda m: ring_forward(1, m, gw))

            each(0, early, ring_arrived)
            _transposed_rows(group(hw), groups, rows, nd, ht)

        @pl.when((p < n_stage // 2) & (j == min(units - 1, m_all - early)))
        def _():
            ring_forward(1, m_all - 1, gw)

        def settle():
            @pl.when(j > 0)
            def _():
                for c in part_copies(j):
                    c.wait()

        def put(v1, v2):
            d1v[...] = v1
            d2v[...] = v2

        _dw_block(
            512, group(hw), group(gw), groups, rows, nd,
            lambda: _wide([w1v[j * SLABS + c] for c in range(SLABS)]),
            lambda: _wide([w2t[j * SLABS + c] for c in range(SLABS)]),
            True, ht, ab, zb, settle, put,
        )
        for c in part_copies(j):
            c.start()

    with jax.named_scope("loads"):
        for c in loads:
            c.wait()

    first = jnp.where(p == last, 1, jnp.where(p == last - 1, min(4, m_all), m_all))
    rest = m_all - first
    turn = jnp.where(p < n_stage // 2, first, 0)
    spare = m_all - early - 1

    def step(k, carry):
        j = k - first
        swap = j < 2 * rest
        e = k - (2 * m_all - spare)
        mixed = (p < n_stage // 2) & (e >= 0)
        in_mix = e < 2 * spare
        is_f = (j < 0) | (swap & (j % 2 == 1))
        is_u = jnp.where(p < n_stage // 2, mixed & (jnp.logical_not(in_mix) | (e % 2 == 0)), k >= 2 * m_all)
        is_b = jnp.logical_not(is_f | is_u)
        m_f = jnp.where(j < 0, k, jnp.minimum(first + j // 2, m_all - 1))
        m_b = jnp.where(swap, j // 2, j - rest)
        m_b = jnp.where(mixed, early + 1 + e // 2, m_b)
        m_b = jnp.maximum(jnp.minimum(m_b, m_all - 1), 0)
        u = jnp.where(p < n_stage // 2, jnp.where(in_mix, e // 2, e - spare), k - 2 * m_all)
        u = jnp.maximum(u, 0)

        @pl.when(k == turn)
        def _():
            with jax.named_scope("transp"):
                transpose_weights()

        @pl.when(is_f)
        def _():
            with jax.named_scope("fwd"):
                forward(m_f)

        @pl.when(is_b)
        def _():
            with jax.named_scope("bwd"):
                backward(m_b)

        @pl.when(is_u)
        def _():
            with jax.named_scope("unit"):
                unit(u)

        return carry

    lax.fori_loop(0, 2 * m_all + units, step, 0)

    with jax.named_scope("finish"):
        each(early, m_all, ring_arrived)
        late = [
            pltpu.make_async_copy(whole.at[k, pl.ds(early, m_all - early)], out.at[k], late_sem.at[q, k])
            for q, (whole, out) in enumerate(((hw, h_late), (gw, g_late)))
            for k in range(n_inner)
        ]
        for c in late:
            c.start()

        def finish(m):
            ring_sent(m)

            @pl.when((p != last) | (p != m))
            def _():
                to_stage(ho.at[m], hw.at[i, m], h_send.at[m], h_recv.at[m], 0).wait_send()

            @pl.when((p != 0) | (p != m))
            def _():
                to_stage(go.at[m], gw.at[i, m], g_send.at[m], g_recv.at[m], 0).wait_send()

        each(0, m_all, finish)

        @pl.when(p != 0)
        def _():
            to_stage(x.at[0], x.at[0], xsem.at[0], h_recv.at[0], 0).wait_send()

        @pl.when(p != last)
        def _():
            to_stage(g.at[0], g.at[0], xsem.at[1], g_recv.at[0], last).wait_send()

        for c in (*part_copies(units - 1), *late):
            c.wait()
    with jax.named_scope("outwait"):
        pltpu.make_async_copy(y.at[0], y.at[0], out_recv.at[0]).wait()
        pltpu.make_async_copy(dx.at[0], dx.at[0], out_recv.at[1]).wait()


def _chain(n_stage, n_inner, x, g, w1, w2):
    mb, rows, d = x.shape
    f = w1.shape[-1]
    m_all = mb * n_stage
    early = m_all // 2
    nd, nf = d // LANES, f // LANES
    blk = SLABS * LANES
    tokens = n_inner * early * rows
    hbm = pl.BlockSpec(memory_space=pltpu.HBM)
    whole = (n_inner, m_all, nd, rows, LANES)
    late = jax.ShapeDtypeStruct((n_inner, m_all - early, nd, rows, LANES), BF16)
    dma = pltpu.SemaphoreType.DMA
    vmem = pltpu.VMEM
    return pl.pallas_call(
        functools.partial(_chain_kernel, n_stage, n_inner),
        out_shape=[
            jax.ShapeDtypeStruct(x.shape, BF16), jax.ShapeDtypeStruct(x.shape, BF16), late, late,
            jax.ShapeDtypeStruct((f // blk, d, blk), F32), jax.ShapeDtypeStruct((f // blk, blk, d), F32),
        ],
        in_specs=[hbm] * 4,
        out_specs=[hbm] * 6,
        scratch_shapes=[
            vmem((nf, d, LANES), BF16), vmem((nd, f, LANES), BF16),
            vmem((nd, f, LANES), BF16), vmem((nf, d, LANES), BF16),
            vmem(whole, BF16), vmem(whole, BF16),
            vmem((m_all, nd, rows, LANES), BF16), vmem((m_all, nd, rows, LANES), BF16),
            vmem((m_all, nf, rows, LANES), F32), vmem((nf, rows, LANES), BF16),
            vmem((tokens // LANES, d, LANES), BF16),
            vmem((SLABS, tokens, LANES), BF16), vmem((SLABS, tokens, LANES), BF16),
            vmem((d, blk), F32), vmem((blk, d), F32),
            dma((2,)), dma((2,)), dma((m_all,)), dma((m_all,)), dma((m_all,)), dma((m_all,)), dma((2,)),
            dma((2, m_all, 4)), dma((2, m_all, 4)), dma((2,)), dma((2, n_inner)),
        ],
        compiler_params=pltpu.CompilerParams(
            collective_id=0, has_side_effects=True, vmem_limit_bytes=VMEM_LIMIT
        ),
        name="chain",
    )(x, g, w1, w2)


def _late_kernel(h, g, w1_0, w1_1, w1_2, w1_3, *rest):
    nd = h.shape[1]
    w1 = (w1_0, w1_1, w1_2, w1_3)
    w2, (p1, p2, d1, d2, ht, ab, zb) = rest[:nd], rest[nd:]
    groups, _, rows, _ = h.shape

    @pl.when(pl.program_id(0) == 0)
    def _():
        _transposed_rows(lambda k, c: h[k, c], groups, rows, nd, ht)

    def put(v1, v2):
        d1[...] = p1[0] + v1
        d2[...] = p2[0] + v2

    _dw_block(
        512, lambda k, c: h[k, c], lambda k, c: g[k, c], groups, rows, nd,
        lambda: _wide([w[...] for w in w1]), lambda: _wide([w[...] for w in w2]),
        False, ht, ab, zb, lambda: None, put,
    )


def _late(h, g, w1, w2, p1, p2):
    groups, nd, rows, _ = h.shape
    d, f = w1.shape
    blk = SLABS * LANES
    t = groups * rows
    whole = pl.BlockSpec(h.shape, lambda j: (0, 0, 0, 0))
    return pl.pallas_call(
        _late_kernel,
        grid=(f // blk,),
        in_specs=[whole, whole]
        + [pl.BlockSpec((d, LANES), functools.partial(lambda c, j: (0, j * SLABS + c), c)) for c in range(SLABS)]
        + [pl.BlockSpec((blk, LANES), functools.partial(lambda c, j: (j, c), c)) for c in range(nd)]
        + [pl.BlockSpec((1, d, blk), lambda j: (j, 0, 0)), pl.BlockSpec((1, blk, d), lambda j: (j, 0, 0))],
        out_specs=[pl.BlockSpec((d, blk), lambda j: (0, j)), pl.BlockSpec((blk, d), lambda j: (j, 0))],
        out_shape=[jax.ShapeDtypeStruct((d, f), F32), jax.ShapeDtypeStruct((f, d), F32)],
        scratch_shapes=[
            pltpu.VMEM((t // LANES, d, LANES), BF16),
            pltpu.VMEM((SLABS, t, LANES), BF16), pltpu.VMEM((SLABS, t, LANES), BF16),
        ],
        compiler_params=pltpu.CompilerParams(vmem_limit_bytes=VMEM_LIMIT),
        cost_estimate=pl.CostEstimate(flops=8 * t * d * f, bytes_accessed=20 * d * f, transcendentals=t * f),
        name="late",
    )(h, g, *([w1] * SLABS), *([w2] * nd), p1, p2)


def solution(mesh):
    n_stage, n_inner = mesh.shape["stage"], mesh.shape["inner"]

    def body(x, g, w1, w2):
        d, f = w1.shape[-2:]
        y, dx, h, gg, p1, p2 = _chain(n_stage, n_inner, x, g, w1, w2)
        flat = (-1, *h.shape[2:])
        d1, d2 = _late(h.reshape(flat), gg.reshape(flat), w1.reshape(d, f), w2.reshape(f, d), p1, p2)
        return y, dx, d1.reshape(w1.shape), d2.reshape(w2.shape)

    tok = P(("data", "stage"), "inner", None)
    wsp = P(None, "stage", None, None)
    dsp = P("data", "stage", None, None)
    return jax.shard_map(body, mesh=mesh, in_specs=(tok, tok, wsp, wsp), out_specs=(tok, tok, dsp, dsp), check_vma=False)
```

```python
import functools

import jax
import jax.numpy as jnp
from jax import lax
from jax.experimental import pallas as pl
from jax.experimental.pallas import tpu as pltpu
from jax.sharding import PartitionSpec as P

MESH = pl.DeviceIdType.MESH
F32, BF16 = jnp.float32, jnp.bfloat16
C0, C1 = 0.7978845608028654, 0.044715
LANES = 128
VMEM_LIMIT = 67043328
SLABS = 4
MERGE = 2
EARLY = 1


def _gelu(z):
    return z * (0.5 * jnp.tanh(z * (C0 + (C0 * C1) * (z * z))) + 0.5)


def _gelu_and_slope(z):
    z2 = z * z
    half = 0.5 * jnp.tanh(z * (C0 + (C0 * C1) * z2)) + 0.5
    a = z * half
    return a, half + (a - a * half) * (2.0 * C0 + (6.0 * C0 * C1) * z2)


def _dot(a, b):
    return jnp.dot(a, b, preferred_element_type=F32)


def _wide(slabs):
    return jnp.concatenate(slabs, axis=1)


def _tall(parts):
    return jnp.concatenate(parts, axis=0)


def _cut(value, c):
    return value[:, c * LANES : (c + 1) * LANES]


def _dw_block(rows, hg, gg, groups, group_rows, nd, w1_block, w2_block, w2_transposed, ht, ab, zb, settle, put):
    def some(read, ks):
        return _tall([_wide([read(k, c) for c in range(nd)]) for k in ks])

    step = max(1, rows // group_rows)
    for k in range(0, groups, step):
        ks = range(k, min(k + step, groups))
        s = slice(k * group_rows, (k + len(ks)) * group_rows)
        z = _dot(some(hg, ks), w1_block())
        dims = (((1,), (0,)), ((), ())) if w2_transposed else (((1,), (1,)), ((), ()))
        da = lax.dot_general(some(gg, ks), w2_block(), dims, preferred_element_type=F32)
        a, slope = _gelu_and_slope(z)
        a, dz = a.astype(BF16), (da * slope).astype(BF16)
        for c in range(SLABS):
            ab[c, s, :] = _cut(a, c)
            zb[c, s, :] = _cut(dz, c)
    settle()
    put(
        _dot(_wide([ht[t] for t in range(ht.shape[0])]), _wide([zb[c] for c in range(SLABS)])),
        lax.dot_general(
            _wide([ab[c] for c in range(SLABS)]), some(gg, range(groups)), (((0,), (0,)), ((), ())),
            preferred_element_type=F32,
        ),
    )


def _transposed_rows(hg, groups, group_rows, nd, ht):
    per = LANES // group_rows
    for t in range(groups // per):
        ht[t] = _tall([_wide([hg(t * per + e, c) for c in range(nd)]) for e in range(per)]).T


def _chain_kernel(
    n_stage, n_inner, x, g, w1, w2, y, dx, h_late, g_late, d1_part, d2_part,
    w1v, w2v, w1t, w2t, hw, gw, ho, go, zs, act, ht, ab, zb, d1v, d2v,
    wsem, xsem, h_recv, g_recv, h_send, g_send, out_recv, ring_send, ring_recv, part_sem, late_sem,
):
    p, i = lax.axis_index("stage"), lax.axis_index("inner")
    right, left = lax.rem(i + 1, n_inner), lax.rem(i + n_inner - 1, n_inner)
    _, m_all, nd, rows, _ = hw.shape
    nf = w1v.shape[0]
    units = nf // SLABS
    early = EARLY
    last = n_stage - 1
    half = nd // 2
    part = rows // MERGE

    barrier = pltpu.get_barrier_semaphore()
    for q in range(1, n_stage):
        pl.semaphore_signal(barrier, inc=1, device_id={"stage": lax.rem(p + q, n_stage)}, device_id_type=MESH)
    for q in (left, right):
        pl.semaphore_signal(barrier, inc=1, device_id={"inner": q}, device_id_type=MESH)

    loads = [
        pltpu.make_async_copy(w1.at[0, 0, :, c * LANES : (c + 1) * LANES], w1v.at[c], wsem.at[0]) for c in range(nf)
    ] + [pltpu.make_async_copy(w2.at[0, 0, :, c * LANES : (c + 1) * LANES], w2v.at[c], wsem.at[1]) for c in range(nd)]
    for c in loads:
        c.start()
    with jax.named_scope("barrier"):
        pl.semaphore_wait(barrier, n_stage + 1)

    def to_stage(src, dst, send, recv, stage):
        return pltpu.make_async_remote_copy(
            src_ref=src, dst_ref=dst, send_sem=send, recv_sem=recv,
            device_id={"stage": stage}, device_id_type=MESH,
        )

    def to_inner(src, dst, send, recv, inner):
        return pltpu.make_async_remote_copy(
            src_ref=src, dst_ref=dst, send_sem=send, recv_sem=recv,
            device_id={"inner": inner}, device_id_type=MESH,
        )

    def flat(ref, c):
        return ref.at[0, :, c * LANES : (c + 1) * LANES]

    def piece(e):
        return pl.ds(pl.multiple_of(e * part, part), part)

    def own(src, slots, recv, sem, stage):
        def to(c):
            return slots.at[i, p // MERGE, c, piece(p % MERGE)]

        @pl.when(p == stage)
        def _():
            for c in range(nd):
                pltpu.make_async_copy(flat(src, c), to(c), recv.at[p // MERGE]).start()

        @pl.when(p != stage)
        def _():
            for c in range(nd):
                to_stage(flat(src, c), to(c), sem, recv.at[p // MERGE], stage).start()

    own(x, hw, h_recv, xsem.at[0], 0)
    own(g, gw, g_recv, xsem.at[1], last)

    def ring_first(q, m, whole):
        a = whole.at[i, m]
        to_inner(a, a, ring_send.at[q, m, 0], ring_recv.at[q, m, 0], right).start()
        to_inner(a, a, ring_send.at[q, m, 1], ring_recv.at[q, m, 1], left).start()

    def ring_forward(q, m, whole):
        a, b = whole.at[left, m], whole.at[right, m]
        to_inner(a, a, ring_send.at[q, m, 0], ring_recv.at[q, m, 0], right).wait_recv()
        a = whole.at[left, m, pl.ds(0, half)]
        to_inner(a, a, ring_send.at[q, m, 2], ring_recv.at[q, m, 2], right).start()
        to_inner(b, b, ring_send.at[q, m, 1], ring_recv.at[q, m, 1], left).wait_recv()
        b = whole.at[right, m, pl.ds(half, half)]
        to_inner(b, b, ring_send.at[q, m, 3], ring_recv.at[q, m, 3], left).start()

    def ring_far(q, m, whole):
        far = lax.rem(i + 2, n_inner)
        a, b = whole.at[far, m, pl.ds(0, half)], whole.at[far, m, pl.ds(half, half)]
        return (
            to_inner(a, a, ring_send.at[q, m, 2], ring_recv.at[q, m, 2], right),
            to_inner(b, b, ring_send.at[q, m, 3], ring_recv.at[q, m, 3], left),
        )

    def ring_arrived(m):
        for q, whole in ((0, hw), (1, gw)):
            for c in ring_far(q, m, whole):
                c.wait_recv()

    def ring_sent(m):
        for q, whole in ((0, hw), (1, gw)):
            for c in ring_far(q, m, whole):
                c.wait_send()
            a = whole.at[i, m]
            to_inner(a, a, ring_send.at[q, m, 0], ring_recv.at[q, m, 0], right).wait_send()
            to_inner(a, a, ring_send.at[q, m, 1], ring_recv.at[q, m, 1], left).wait_send()

    def pass_on(m, lo, hi, src, slots, send, recv, end, nxt, out, out_sem):
        @pl.when(p != end)
        def _():
            some = pl.ds(lo, hi - lo)
            to_stage(src.at[m, some], slots.at[i, m, some], send.at[m], recv.at[m], nxt).start()

        for e in range(MERGE):
            home = m * MERGE + e

            @pl.when((p == end) & (p != home))
            def _():
                for c in range(lo, hi):
                    to_stage(src.at[m, c, piece(e)], flat(out, c), send.at[m], out_sem, home).start()

            @pl.when((p == end) & (p == home))
            def _():
                for c in range(lo, hi):
                    pltpu.make_async_copy(src.at[m, c, piece(e)], flat(out, c), out_sem).start()

    def project(m, res, w, src, *rest):
        full = _wide([act[c] for c in range(nf)])
        for lo in range(0, nd, half):
            u = _dot(full, _wide([w[lo + c] for c in range(half)]))
            out = (res[:, lo * LANES : (lo + half) * LANES].astype(F32) + u).astype(BF16)
            for c in range(half):
                src[m, lo + c] = _cut(out, c)
            pass_on(m, lo, lo + half, src, *rest)

    def forward(m):
        with jax.named_scope("wait_h"):
            pltpu.make_async_copy(hw.at[i, m], hw.at[i, m], h_recv.at[m]).wait()
        ring_first(0, m, hw)
        h = _wide([hw[i, m, c] for c in range(nd)])
        for b in range(0, nf, SLABS):
            z = _dot(h, _wide([w1v[b + c] for c in range(SLABS)]))
            a = _gelu(z).astype(BF16)
            for c in range(SLABS):
                zs[m, b + c] = _cut(z, c)
                act[b + c] = _cut(a, c)

        @pl.when((m == 0) & (p < n_stage // 2))
        def _():
            for c in loads[nf:]:
                c.wait()

        project(m, h, w2v, ho, hw, h_send, h_recv, last, jnp.minimum(p + 1, last), y, out_recv.at[0])

    def backward(m):
        @pl.when((p < n_stage // 2) & (m > 0))
        def _():
            ring_forward(1, jnp.maximum(m - 1, 0), gw)

        with jax.named_scope("wait_g"):
            pltpu.make_async_copy(gw.at[i, m], gw.at[i, m], g_recv.at[m]).wait()
        ring_first(1, m, gw)

        @pl.when(p < n_stage - 2)
        def _():
            ring_forward(0, m, hw)

        dh = _wide([gw[i, m, c] for c in range(nd)])
        for b in range(0, nf, SLABS):
            da = _dot(dh, _wide([w2t[b + c] for c in range(SLABS)]))
            _, slope = _gelu_and_slope(_wide([zs[m, b + c] for c in range(SLABS)]))
            dz = (da * slope).astype(BF16)
            for c in range(SLABS):
                act[b + c] = _cut(dz, c)
        project(m, dh, w1t, go, gw, g_send, g_recv, 0, jnp.maximum(p - 1, 0), dx, out_recv.at[1])

    def transpose_weights():
        def some(c, carry):
            s = pl.ds(pl.multiple_of(c * LANES, LANES), LANES)
            for e in range(nd):
                w1t[e, s, :] = w1v[c, e * LANES : (e + 1) * LANES, :].T
                w2t[c, e * LANES : (e + 1) * LANES, :] = w2v[e, s, :].T
            return carry

        lax.fori_loop(0, nf, some, 0)

    def each(lo, hi, fn):
        lax.fori_loop(lo, hi, lambda m, c: (fn(m), c)[1], 0)

    def group(whole):
        return lambda k, c: whole[k // early, k % early, c]

    groups = n_inner * early

    def part_copies(j):
        return (
            pltpu.make_async_copy(d1v, d1_part.at[j], part_sem.at[0]),
            pltpu.make_async_copy(d2v, d2_part.at[j], part_sem.at[1]),
        )

    def unit(j):
        @pl.when(j == 0)
        def _():
            @pl.when(p >= n_stage - 2)
            def _():
                each(0, m_all, lambda m: ring_forward(0, m, hw))

            @pl.when(p >= n_stage // 2)
            def _():
                each(0, m_all, lambda m: ring_forward(1, m, gw))

            each(0, early, ring_arrived)
            _transposed_rows(group(hw), groups, rows, nd, ht)

        @pl.when((p < n_stage // 2) & (j == min(units - 1, m_all - early)))
        def _():
            ring_forward(1, m_all - 1, gw)

        def settle():
            @pl.when(j > 0)
            def _():
                for c in part_copies(j):
                    c.wait()

        def put(v1, v2):
            d1v[...] = v1
            d2v[...] = v2

        _dw_block(
            512, group(hw), group(gw), groups, rows, nd,
            lambda: _wide([w1v[j * SLABS + c] for c in range(SLABS)]),
            lambda: _wide([w2t[j * SLABS + c] for c in range(SLABS)]),
            True, ht, ab, zb, settle, put,
        )
        for c in part_copies(j):
            c.start()

    with jax.named_scope("loads"):
        for c in loads[:nf]:
            c.wait()

    first = jnp.where(p == last, 1, m_all)
    rest = m_all - first
    turn = jnp.where(p < n_stage // 2, first, 0)
    spare = m_all - early - 1

    def step(k, carry):
        j = k - first
        swap = j < 2 * rest
        e = k - (2 * m_all - spare)
        mixed = (p < n_stage // 2) & (e >= 0)
        in_mix = e < 2 * spare
        is_f = (j < 0) | (swap & (j % 2 == 1))
        is_u = jnp.where(p < n_stage // 2, mixed & (jnp.logical_not(in_mix) | (e % 2 == 0)), k >= 2 * m_all)
        is_b = jnp.logical_not(is_f | is_u)
        m_f = jnp.where(j < 0, k, jnp.minimum(first + j // 2, m_all - 1))
        m_b = jnp.where(swap, j // 2, j - rest)
        m_b = jnp.where(mixed, early + 1 + e // 2, m_b)
        m_b = jnp.maximum(jnp.minimum(m_b, m_all - 1), 0)
        u = jnp.where(p < n_stage // 2, jnp.where(in_mix, e // 2, e - spare), k - 2 * m_all)
        u = jnp.maximum(u, 0)

        @pl.when(k == turn)
        def _():
            with jax.named_scope("transp"):
                @pl.when(p >= n_stage // 2)
                def _():
                    for c in loads[nf:]:
                        c.wait()

                transpose_weights()

        @pl.when(is_f)
        def _():
            with jax.named_scope("fwd"):
                forward(m_f)

        @pl.when(is_b)
        def _():
            with jax.named_scope("bwd"):
                backward(m_b)

        @pl.when(is_u)
        def _():
            with jax.named_scope("unit"):
                unit(u)

        return carry

    lax.fori_loop(0, 2 * m_all + units, step, 0)

    with jax.named_scope("finish"):
        each(early, m_all, ring_arrived)
        late = [
            pltpu.make_async_copy(whole.at[k, pl.ds(early, m_all - early)], out.at[k], late_sem.at[q, k])
            for q, (whole, out) in enumerate(((hw, h_late), (gw, g_late)))
            for k in range(n_inner)
        ]
        for c in late:
            c.start()

        def finish(m):
            ring_sent(m)

            for src, slots, send, recv, end in ((ho, hw, h_send, h_recv, last), (go, gw, g_send, g_recv, 0)):
                for e in range(MERGE):
                    a = src.at[m, :, piece(e)]

                    @pl.when((p != end) | (p != m * MERGE + e))
                    def _():
                        to_stage(a, a, send.at[m], recv.at[m], 0).wait_send()

        each(0, m_all, finish)

        @pl.when(p != 0)
        def _():
            to_stage(x.at[0], x.at[0], xsem.at[0], h_recv.at[0], 0).wait_send()

        @pl.when(p != last)
        def _():
            to_stage(g.at[0], g.at[0], xsem.at[1], g_recv.at[0], last).wait_send()

        for c in (*part_copies(units - 1), *late):
            c.wait()
    with jax.named_scope("outwait"):
        pltpu.make_async_copy(y.at[0], y.at[0], out_recv.at[0]).wait()
        pltpu.make_async_copy(dx.at[0], dx.at[0], out_recv.at[1]).wait()


def _chain(n_stage, n_inner, x, g, w1, w2):
    mb, rows, d = x.shape
    f = w1.shape[-1]
    rows = rows * MERGE
    m_all = mb * n_stage // MERGE
    early = EARLY
    nd, nf = d // LANES, f // LANES
    blk = SLABS * LANES
    tokens = n_inner * early * rows
    hbm = pl.BlockSpec(memory_space=pltpu.HBM)
    whole = (n_inner, m_all, nd, rows, LANES)
    late = jax.ShapeDtypeStruct((n_inner, m_all - early, nd, rows, LANES), BF16)
    dma = pltpu.SemaphoreType.DMA
    vmem = pltpu.VMEM
    return pl.pallas_call(
        functools.partial(_chain_kernel, n_stage, n_inner),
        out_shape=[
            jax.ShapeDtypeStruct(x.shape, BF16), jax.ShapeDtypeStruct(x.shape, BF16), late, late,
            jax.ShapeDtypeStruct((f // blk, d, blk), F32), jax.ShapeDtypeStruct((f // blk, blk, d), F32),
        ],
        in_specs=[hbm] * 4,
        out_specs=[hbm] * 6,
        scratch_shapes=[
            vmem((nf, d, LANES), BF16), vmem((nd, f, LANES), BF16),
            vmem((nd, f, LANES), BF16), vmem((nf, d, LANES), BF16),
            vmem(whole, BF16), vmem(whole, BF16),
            vmem((m_all, nd, rows, LANES), BF16), vmem((m_all, nd, rows, LANES), BF16),
            vmem((m_all, nf, rows, LANES), F32), vmem((nf, rows, LANES), BF16),
            vmem((tokens // LANES, d, LANES), BF16),
            vmem((SLABS, tokens, LANES), BF16), vmem((SLABS, tokens, LANES), BF16),
            vmem((d, blk), F32), vmem((blk, d), F32),
            dma((2,)), dma((2,)), dma((m_all,)), dma((m_all,)), dma((m_all,)), dma((m_all,)), dma((2,)),
            dma((2, m_all, 4)), dma((2, m_all, 4)), dma((2,)), dma((2, n_inner)),
        ],
        compiler_params=pltpu.CompilerParams(
            collective_id=0, has_side_effects=True, vmem_limit_bytes=VMEM_LIMIT
        ),
        name="chain",
    )(x, g, w1, w2)


def _late_kernel(h, g, y_in, dx_in, w1_0, w1_1, w1_2, w1_3, *rest):
    nd = h.shape[1]
    w1 = (w1_0, w1_1, w1_2, w1_3)
    w2, (p1, p2, d1, d2, y, dx, ht, ab, zb) = rest[:nd], rest[nd:]
    groups, _, rows, _ = h.shape

    @pl.when(pl.program_id(0) == 0)
    def _():
        y[...] = y_in[...]
        dx[...] = dx_in[...]
        _transposed_rows(lambda k, c: h[k, c], groups, rows, nd, ht)

    def put(v1, v2):
        d1[...] = p1[0] + v1
        d2[...] = p2[0] + v2

    _dw_block(
        512, lambda k, c: h[k, c], lambda k, c: g[k, c], groups, rows, nd,
        lambda: _wide([w[...] for w in w1]), lambda: _wide([w[...] for w in w2]),
        False, ht, ab, zb, lambda: None, put,
    )


def _late(h, g, y, dx, w1, w2, p1, p2):
    groups, nd, rows, _ = h.shape
    d, f = w1.shape
    blk = SLABS * LANES
    t = groups * rows
    whole = pl.BlockSpec(h.shape, lambda j: (0, 0, 0, 0))
    mine = pl.BlockSpec(y.shape, lambda j: (0, 0, 0))
    return pl.pallas_call(
        _late_kernel,
        grid=(f // blk,),
        in_specs=[whole, whole, mine, mine]
        + [pl.BlockSpec((d, LANES), functools.partial(lambda c, j: (0, j * SLABS + c), c)) for c in range(SLABS)]
        + [pl.BlockSpec((blk, LANES), functools.partial(lambda c, j: (j, c), c)) for c in range(nd)]
        + [pl.BlockSpec((1, d, blk), lambda j: (j, 0, 0)), pl.BlockSpec((1, blk, d), lambda j: (j, 0, 0))],
        out_specs=[pl.BlockSpec((d, blk), lambda j: (0, j)), pl.BlockSpec((blk, d), lambda j: (j, 0)), mine, mine],
        out_shape=[
            jax.ShapeDtypeStruct((d, f), F32), jax.ShapeDtypeStruct((f, d), F32),
            jax.ShapeDtypeStruct(y.shape, BF16), jax.ShapeDtypeStruct(dx.shape, BF16),
        ],
        scratch_shapes=[
            pltpu.VMEM((t // LANES, d, LANES), BF16),
            pltpu.VMEM((SLABS, t, LANES), BF16), pltpu.VMEM((SLABS, t, LANES), BF16),
        ],
        compiler_params=pltpu.CompilerParams(vmem_limit_bytes=VMEM_LIMIT),
        cost_estimate=pl.CostEstimate(flops=8 * t * d * f, bytes_accessed=20 * d * f, transcendentals=t * f),
        name="late",
    )(h, g, y, dx, *([w1] * SLABS), *([w2] * nd), p1, p2)


def solution(mesh):
    n_stage, n_inner = mesh.shape["stage"], mesh.shape["inner"]

    def body(x, g, w1, w2):
        d, f = w1.shape[-2:]
        y, dx, h, gg, p1, p2 = _chain(n_stage, n_inner, x, g, w1, w2)
        flat = (-1, *h.shape[2:])
        d1, d2, y, dx = _late(h.reshape(flat), gg.reshape(flat), y, dx, w1.reshape(d, f), w2.reshape(f, d), p1, p2)
        return y, dx, d1.reshape(w1.shape), d2.reshape(w2.shape)

    tok = P(("data", "stage"), "inner", None)
    wsp = P(None, "stage", None, None)
    dsp = P("data", "stage", None, None)
    return jax.shard_map(body, mesh=mesh, in_specs=(tok, tok, wsp, wsp), out_specs=(tok, tok, dsp, dsp), check_vma=False)
```

```python
import functools

import jax
import jax.numpy as jnp
from jax import lax
from jax.experimental import pallas as pl
from jax.experimental.pallas import tpu as pltpu
from jax.sharding import PartitionSpec as P

MESH = pl.DeviceIdType.MESH
F32, BF16 = jnp.float32, jnp.bfloat16
C0, C1 = 0.7978845608028654, 0.044715
LANES = 128
VMEM_LIMIT = 67043328
SLABS = 4
MERGE = 2
EARLY = 2


def _gelu_and_slope(z):
    z2 = z * z
    half = 0.5 * jnp.tanh(z * (C0 + (C0 * C1) * z2)) + 0.5
    a = z * half
    return a, half + (a - a * half) * (2.0 * C0 + (6.0 * C0 * C1) * z2)


def _dot(a, b):
    return jnp.dot(a, b, preferred_element_type=F32)


def _wide(slabs):
    return jnp.concatenate(slabs, axis=1)


def _tall(parts):
    return jnp.concatenate(parts, axis=0)


def _cut(value, c):
    return value[:, c * LANES : (c + 1) * LANES]


def _dw_block(rows, hg, gg, groups, group_rows, nd, w1_block, w2_block, w2_transposed, ht, ab, zb, settle, put):
    def some(read, ks):
        return _tall([_wide([read(k, c) for c in range(nd)]) for k in ks])

    step = max(1, rows // group_rows)
    for k in range(0, groups, step):
        ks = range(k, min(k + step, groups))
        if k + step >= groups:
            settle()
        s = slice(k * group_rows, (k + len(ks)) * group_rows)
        z = _dot(some(hg, ks), w1_block())
        dims = (((1,), (0,)), ((), ())) if w2_transposed else (((1,), (1,)), ((), ()))
        da = lax.dot_general(some(gg, ks), w2_block(), dims, preferred_element_type=F32)
        a, slope = _gelu_and_slope(z)
        a, dz = a.astype(BF16), (da * slope).astype(BF16)
        for c in range(SLABS):
            ab[c, s, :] = _cut(a, c)
            zb[c, s, :] = _cut(dz, c)
    v2 = lax.dot_general(
        _wide([ab[c] for c in range(SLABS)]), some(gg, range(groups)), (((0,), (0,)), ((), ())),
        preferred_element_type=F32,
    )
    put(_dot(_wide([ht[t] for t in range(ht.shape[0])]), _wide([zb[c] for c in range(SLABS)])), v2)


def _transposed_rows(hg, groups, group_rows, nd, ht):
    per = LANES // group_rows
    for t in range(groups // per):
        ht[t] = _tall([_wide([hg(t * per + e, c) for c in range(nd)]) for e in range(per)]).T


def _chain_kernel(
    n_stage, n_inner, x, g, w1, w2, y, dx, h_late, g_late, d1_part, d2_part,
    w1v, w2v, w1t, w2t, hw, gw, ho, go, zs, act, ht, ab, zb, d1v, d2v,
    wsem, xsem, h_recv, g_recv, h_send, g_send, out_recv, ring_send, ring_recv, part_sem, late_sem,
):
    p, i = lax.axis_index("stage"), lax.axis_index("inner")
    right, left = lax.rem(i + 1, n_inner), lax.rem(i + n_inner - 1, n_inner)
    _, m_all, nd, rows, _ = hw.shape
    nf = w1v.shape[0]
    units = nf // SLABS
    early = EARLY
    last = n_stage - 1
    half = nd // 2
    part = rows // MERGE

    barrier = pltpu.get_barrier_semaphore()
    for q in range(1, n_stage):
        pl.semaphore_signal(barrier, inc=1, device_id={"stage": lax.rem(p + q, n_stage)}, device_id_type=MESH)
    for q in (left, right):
        pl.semaphore_signal(barrier, inc=1, device_id={"inner": q}, device_id_type=MESH)

    loads = [
        pltpu.make_async_copy(w1.at[0, 0, :, c * LANES : (c + 1) * LANES], w1v.at[c], wsem.at[0]) for c in range(nf)
    ] + [pltpu.make_async_copy(w2.at[0, 0, :, c * LANES : (c + 1) * LANES], w2v.at[c], wsem.at[1]) for c in range(nd)]
    for c in loads:
        c.start()
    with jax.named_scope("barrier"):
        pl.semaphore_wait(barrier, n_stage + 1)

    def to_stage(src, dst, send, recv, stage):
        return pltpu.make_async_remote_copy(
            src_ref=src, dst_ref=dst, send_sem=send, recv_sem=recv,
            device_id={"stage": stage}, device_id_type=MESH,
        )

    def to_inner(src, dst, send, recv, inner):
        return pltpu.make_async_remote_copy(
            src_ref=src, dst_ref=dst, send_sem=send, recv_sem=recv,
            device_id={"inner": inner}, device_id_type=MESH,
        )

    def flat(ref, c):
        return ref.at[0, :, c * LANES : (c + 1) * LANES]

    def piece(e):
        return pl.ds(pl.multiple_of(e * part, part), part)

    def own(src, slots, recv, sem, stage):
        def to(c):
            return slots.at[i, p // MERGE, c, piece(p % MERGE)]

        @pl.when(p == stage)
        def _():
            for c in range(nd):
                pltpu.make_async_copy(flat(src, c), to(c), recv.at[p // MERGE]).start()

        @pl.when(p != stage)
        def _():
            for c in range(nd):
                to_stage(flat(src, c), to(c), sem, recv.at[p // MERGE], stage).start()

    own(x, hw, h_recv, xsem.at[0], 0)
    own(g, gw, g_recv, xsem.at[1], last)

    def ring_first(q, m, whole):
        a = whole.at[i, m]
        to_inner(a, a, ring_send.at[q, m, 0], ring_recv.at[q, m, 0], right).start()
        to_inner(a, a, ring_send.at[q, m, 1], ring_recv.at[q, m, 1], left).start()

    def ring_forward(q, m, whole):
        a, b = whole.at[left, m], whole.at[right, m]
        to_inner(a, a, ring_send.at[q, m, 0], ring_recv.at[q, m, 0], right).wait_recv()
        a = whole.at[left, m, pl.ds(0, half)]
        to_inner(a, a, ring_send.at[q, m, 2], ring_recv.at[q, m, 2], right).start()
        to_inner(b, b, ring_send.at[q, m, 1], ring_recv.at[q, m, 1], left).wait_recv()
        b = whole.at[right, m, pl.ds(half, half)]
        to_inner(b, b, ring_send.at[q, m, 3], ring_recv.at[q, m, 3], left).start()

    def ring_far(q, m, whole):
        far = lax.rem(i + 2, n_inner)
        a, b = whole.at[far, m, pl.ds(0, half)], whole.at[far, m, pl.ds(half, half)]
        return (
            to_inner(a, a, ring_send.at[q, m, 2], ring_recv.at[q, m, 2], right),
            to_inner(b, b, ring_send.at[q, m, 3], ring_recv.at[q, m, 3], left),
        )

    def ring_arrived(m):
        for q, whole in ((0, hw), (1, gw)):
            for c in ring_far(q, m, whole):
                c.wait_recv()

    def ring_sent(m):
        for q, whole in ((0, hw), (1, gw)):
            for c in ring_far(q, m, whole):
                c.wait_send()
            a = whole.at[i, m]
            to_inner(a, a, ring_send.at[q, m, 0], ring_recv.at[q, m, 0], right).wait_send()
            to_inner(a, a, ring_send.at[q, m, 1], ring_recv.at[q, m, 1], left).wait_send()

    def pass_on(m, src, slots, send, recv, end, nxt, out, out_sem):
        @pl.when(p != end)
        def _():
            to_stage(src.at[m], slots.at[i, m], send.at[m], recv.at[m], nxt).start()

        @pl.when(p == end)
        def _():
            for e in range(MERGE):
                home = m * MERGE + e

                @pl.when(p != home)
                def _():
                    for c in range(nd):
                        to_stage(src.at[m, c, piece(e)], flat(out, c), send.at[m], out_sem, home).start()

                @pl.when(p == home)
                def _():
                    for c in range(nd):
                        pltpu.make_async_copy(src.at[m, c, piece(e)], flat(out, c), out_sem).start()

    def project(m, res, w, src, *rest):
        u = _dot(_wide([act[c] for c in range(nf)]), _wide([w[c] for c in range(nd)]))
        out = (res.astype(F32) + u).astype(BF16)
        for c in range(nd):
            src[m, c] = _cut(out, c)
        pass_on(m, src, *rest)

    def forward(m):
        with jax.named_scope("wait_h"):
            pltpu.make_async_copy(hw.at[i, m], hw.at[i, m], h_recv.at[m]).wait()
        h = _wide([hw[i, m, c] for c in range(nd)])
        for b in range(0, nf, SLABS):
            z = _dot(h, _wide([w1v[b + c] for c in range(SLABS)]))
            a, slope = _gelu_and_slope(z)
            a = a.astype(BF16)
            for c in range(SLABS):
                zs[m, b + c] = _cut(slope, c)
                act[b + c] = _cut(a, c)

        @pl.when((m == 0) & (p < n_stage // 2))
        def _():
            for c in loads[nf:]:
                c.wait()

        project(m, h, w2v, ho, hw, h_send, h_recv, last, jnp.minimum(p + 1, last), y, out_recv.at[0])

        @pl.when((p < n_stage - 2) | (m < early))
        def _():
            ring_first(0, m, hw)

    def backward(m):
        @pl.when((p < n_stage // 2) & (m > 0))
        def _():
            ring_forward(1, jnp.maximum(m - 1, 0), gw)

        with jax.named_scope("wait_g"):
            pltpu.make_async_copy(gw.at[i, m], gw.at[i, m], g_recv.at[m]).wait()

        @pl.when((p < n_stage - 2) | (m < early))
        def _():
            ring_first(1, m, gw)

        @pl.when(p < n_stage - 2)
        def _():
            ring_forward(0, m, hw)

        dh = _wide([gw[i, m, c] for c in range(nd)])
        for b in range(0, nf, SLABS):
            da = _dot(dh, _wide([w2t[b + c] for c in range(SLABS)]))
            dz = (da * _wide([zs[m, b + c] for c in range(SLABS)])).astype(BF16)
            for c in range(SLABS):
                act[b + c] = _cut(dz, c)
        project(m, dh, w1t, go, gw, g_send, g_recv, 0, jnp.maximum(p - 1, 0), dx, out_recv.at[1])

    def transpose_weights():
        def some(c, carry):
            s = pl.ds(pl.multiple_of(c * LANES, LANES), LANES)
            for e in range(nd):
                w1t[e, s, :] = w1v[c, e * LANES : (e + 1) * LANES, :].T
                w2t[c, e * LANES : (e + 1) * LANES, :] = w2v[e, s, :].T
            return carry

        lax.fori_loop(0, nf, some, 0)

    def each(lo, hi, fn):
        lax.fori_loop(lo, hi, lambda m, c: (fn(m), c)[1], 0)

    def group(whole):
        return lambda k, c: whole[k // early, k % early, c]

    groups = n_inner * early

    def part_copies(j):
        return (
            pltpu.make_async_copy(d1v, d1_part.at[j], part_sem.at[0]),
            pltpu.make_async_copy(d2v, d2_part.at[j], part_sem.at[1]),
        )

    def unit(j):
        def forwards(m):
            @pl.when(p >= n_stage - 2)
            def _():
                ring_forward(0, m, hw)

            ring_forward(1, m, gw)

        def firsts(m):
            ring_first(0, m, hw)
            ring_first(1, m, gw)

        @pl.when(j == 0)
        def _():
            @pl.when(p >= n_stage // 2)
            def _():
                each(0, early, forwards)

            @pl.when(p >= n_stage - 2)
            def _():
                each(early, m_all, firsts)

            each(0, early, ring_arrived)
            _transposed_rows(group(hw), groups, rows, nd, ht)

        for m in range(early, m_all):
            @pl.when((p >= n_stage // 2) & (j == min(units - 1, 3 * (m - early + 1))))
            def _():
                forwards(m)

        @pl.when((p < n_stage // 2) & (j == min(units - 1, m_all - early)))
        def _():
            ring_forward(1, m_all - 1, gw)

        def settle():
            @pl.when(j > 0)
            def _():
                for c in part_copies(j):
                    c.wait()

        def put(v1, v2):
            d1v[...] = v1
            d2v[...] = v2

        _dw_block(
            256, group(hw), group(gw), groups, rows, nd,
            lambda: _wide([w1v[j * SLABS + c] for c in range(SLABS)]),
            lambda: _wide([w2t[j * SLABS + c] for c in range(SLABS)]),
            True, ht, ab, zb, settle, put,
        )
        for c in part_copies(j):
            c.start()

    with jax.named_scope("loads"):
        for c in loads[:nf]:
            c.wait()

    first = jnp.where(p == last, 1, m_all)
    rest = m_all - first
    turn = jnp.where(p < n_stage // 2, first, 0)
    spare = m_all - early - 1

    def step(k, carry):
        j = k - first
        swap = j < 2 * rest
        e = k - (2 * m_all - spare)
        mixed = (p < n_stage // 2) & (e >= 0)
        in_mix = e < 2 * spare
        is_f = (j < 0) | (swap & (j % 2 == 1))
        is_u = jnp.where(p < n_stage // 2, mixed & (jnp.logical_not(in_mix) | (e % 2 == 0)), k >= 2 * m_all)
        is_b = jnp.logical_not(is_f | is_u)
        m_f = jnp.where(j < 0, k, jnp.minimum(first + j // 2, m_all - 1))
        m_b = jnp.where(swap, j // 2, j - rest)
        m_b = jnp.where(mixed, early + 1 + e // 2, m_b)
        m_b = jnp.maximum(jnp.minimum(m_b, m_all - 1), 0)
        u = jnp.where(p < n_stage // 2, jnp.where(in_mix, e // 2, e - spare), k - 2 * m_all)
        u = jnp.maximum(u, 0)

        @pl.when(k == turn)
        def _():
            with jax.named_scope("transp"):
                @pl.when(p >= n_stage // 2)
                def _():
                    for c in loads[nf:]:
                        c.wait()

                transpose_weights()

        @pl.when(is_f)
        def _():
            with jax.named_scope("fwd"):
                forward(m_f)

        @pl.when(is_b)
        def _():
            with jax.named_scope("bwd"):
                backward(m_b)

        @pl.when(is_u)
        def _():
            with jax.named_scope("unit"):
                unit(u)

        return carry

    lax.fori_loop(0, 2 * m_all + units, step, 0)

    with jax.named_scope("finish"):
        each(early, m_all, ring_arrived)
        late = [
            pltpu.make_async_copy(whole.at[k, pl.ds(early, m_all - early)], out.at[k], late_sem.at[q, k])
            for q, (whole, out) in enumerate(((hw, h_late), (gw, g_late)))
            for k in range(n_inner)
        ]
        for c in late:
            c.start()

        def finish(m):
            ring_sent(m)

            for src, slots, send, recv, end in ((ho, hw, h_send, h_recv, last), (go, gw, g_send, g_recv, 0)):
                for e in range(MERGE):
                    a = src.at[m, :, piece(e)]

                    @pl.when((p != end) | (p != m * MERGE + e))
                    def _():
                        to_stage(a, a, send.at[m], recv.at[m], 0).wait_send()

        each(0, m_all, finish)

        @pl.when(p != 0)
        def _():
            to_stage(x.at[0], x.at[0], xsem.at[0], h_recv.at[0], 0).wait_send()

        @pl.when(p != last)
        def _():
            to_stage(g.at[0], g.at[0], xsem.at[1], g_recv.at[0], last).wait_send()

        for c in (*part_copies(units - 1), *late):
            c.wait()
    with jax.named_scope("outwait"):
        pltpu.make_async_copy(y.at[0], y.at[0], out_recv.at[0]).wait()
        pltpu.make_async_copy(dx.at[0], dx.at[0], out_recv.at[1]).wait()


def _chain(n_stage, n_inner, x, g, w1, w2):
    mb, rows, d = x.shape
    f = w1.shape[-1]
    rows = rows * MERGE
    m_all = mb * n_stage // MERGE
    early = EARLY
    nd, nf = d // LANES, f // LANES
    blk = SLABS * LANES
    tokens = n_inner * early * rows
    hbm = pl.BlockSpec(memory_space=pltpu.HBM)
    whole = (n_inner, m_all, nd, rows, LANES)
    late = jax.ShapeDtypeStruct((n_inner, m_all - early, nd, rows, LANES), BF16)
    dma = pltpu.SemaphoreType.DMA
    vmem = pltpu.VMEM
    return pl.pallas_call(
        functools.partial(_chain_kernel, n_stage, n_inner),
        out_shape=[
            jax.ShapeDtypeStruct(x.shape, BF16), jax.ShapeDtypeStruct(x.shape, BF16), late, late,
            jax.ShapeDtypeStruct((f // blk, d, blk), F32), jax.ShapeDtypeStruct((f // blk, blk, d), F32),
        ],
        in_specs=[hbm] * 4,
        out_specs=[hbm] * 6,
        scratch_shapes=[
            vmem((nf, d, LANES), BF16), vmem((nd, f, LANES), BF16),
            vmem((nd, f, LANES), BF16), vmem((nf, d, LANES), BF16),
            vmem(whole, BF16), vmem(whole, BF16),
            vmem((m_all, nd, rows, LANES), BF16), vmem((m_all, nd, rows, LANES), BF16),
            vmem((m_all, nf, rows, LANES), F32), vmem((nf, rows, LANES), BF16),
            vmem((tokens // LANES, d, LANES), BF16),
            vmem((SLABS, tokens, LANES), BF16), vmem((SLABS, tokens, LANES), BF16),
            vmem((d, blk), F32), vmem((blk, d), F32),
            dma((2,)), dma((2,)), dma((m_all,)), dma((m_all,)), dma((m_all,)), dma((m_all,)), dma((2,)),
            dma((2, m_all, 4)), dma((2, m_all, 4)), dma((2,)), dma((2, n_inner)),
        ],
        compiler_params=pltpu.CompilerParams(
            collective_id=0, has_side_effects=True, vmem_limit_bytes=VMEM_LIMIT
        ),
        name="chain",
    )(x, g, w1, w2)


def _late_kernel(h, g, y_in, dx_in, w1_0, w1_1, w1_2, w1_3, *rest):
    nd = h.shape[1]
    w1 = (w1_0, w1_1, w1_2, w1_3)
    w2, (p1, p2, d1, d2, y, dx, ht, ab, zb) = rest[:nd], rest[nd:]
    groups, _, rows, _ = h.shape

    @pl.when(pl.program_id(0) == 0)
    def _():
        y[...] = y_in[...]
        dx[...] = dx_in[...]
        _transposed_rows(lambda k, c: h[k, c], groups, rows, nd, ht)

    def put(v1, v2):
        d1[...] = p1[0] + v1
        d2[...] = p2[0] + v2

    _dw_block(
        512, lambda k, c: h[k, c], lambda k, c: g[k, c], groups, rows, nd,
        lambda: _wide([w[...] for w in w1]), lambda: _wide([w[...] for w in w2]),
        False, ht, ab, zb, lambda: None, put,
    )


def _late(h, g, y, dx, w1, w2, p1, p2):
    groups, nd, rows, _ = h.shape
    d, f = w1.shape
    blk = SLABS * LANES
    t = groups * rows
    whole = pl.BlockSpec(h.shape, lambda j: (0, 0, 0, 0))
    mine = pl.BlockSpec(y.shape, lambda j: (0, 0, 0))
    return pl.pallas_call(
        _late_kernel,
        grid=(f // blk,),
        in_specs=[whole, whole, mine, mine]
        + [pl.BlockSpec((d, LANES), functools.partial(lambda c, j: (0, j * SLABS + c), c)) for c in range(SLABS)]
        + [pl.BlockSpec((blk, LANES), functools.partial(lambda c, j: (j, c), c)) for c in range(nd)]
        + [pl.BlockSpec((1, d, blk), lambda j: (j, 0, 0)), pl.BlockSpec((1, blk, d), lambda j: (j, 0, 0))],
        out_specs=[pl.BlockSpec((d, blk), lambda j: (0, j)), pl.BlockSpec((blk, d), lambda j: (j, 0)), mine, mine],
        out_shape=[
            jax.ShapeDtypeStruct((d, f), F32), jax.ShapeDtypeStruct((f, d), F32),
            jax.ShapeDtypeStruct(y.shape, BF16), jax.ShapeDtypeStruct(dx.shape, BF16),
        ],
        scratch_shapes=[
            pltpu.VMEM((t // LANES, d, LANES), BF16),
            pltpu.VMEM((SLABS, t, LANES), BF16), pltpu.VMEM((SLABS, t, LANES), BF16),
        ],
        compiler_params=pltpu.CompilerParams(vmem_limit_bytes=VMEM_LIMIT),
        cost_estimate=pl.CostEstimate(flops=8 * t * d * f, bytes_accessed=20 * d * f, transcendentals=t * f),
        name="late",
    )(h, g, y, dx, *([w1] * SLABS), *([w2] * nd), p1, p2)


def solution(mesh):
    n_stage, n_inner = mesh.shape["stage"], mesh.shape["inner"]

    def body(x, g, w1, w2):
        d, f = w1.shape[-2:]
        y, dx, h, gg, p1, p2 = _chain(n_stage, n_inner, x, g, w1, w2)
        flat = (-1, *h.shape[2:])
        d1, d2, y, dx = _late(h.reshape(flat), gg.reshape(flat), y, dx, w1.reshape(d, f), w2.reshape(f, d), p1, p2)
        return y, dx, d1.reshape(w1.shape), d2.reshape(w2.shape)

    tok = P(("data", "stage"), "inner", None)
    wsp = P(None, "stage", None, None)
    dsp = P("data", "stage", None, None)
    return jax.shard_map(body, mesh=mesh, in_specs=(tok, tok, wsp, wsp), out_specs=(tok, tok, dsp, dsp), check_vma=False)
```

```python
import functools

import jax
import jax.numpy as jnp
from jax import lax
from jax.experimental import pallas as pl
from jax.experimental.pallas import tpu as pltpu
from jax.sharding import PartitionSpec as P

MESH = pl.DeviceIdType.MESH
F32, BF16 = jnp.float32, jnp.bfloat16
C0, C1 = 0.7978845608028654, 0.044715
LANES = 128
VMEM_LIMIT = 67043328
SLABS = 4
MERGE = 2
EARLY = 2


def _gelu_and_slope(z):
    z2 = z * z
    half = 0.5 * jnp.tanh(z * (C0 + (C0 * C1) * z2)) + 0.5
    a = z * half
    return a, half + (a - a * half) * (2.0 * C0 + (6.0 * C0 * C1) * z2)


def _dot(a, b):
    return jnp.dot(a, b, preferred_element_type=F32)


def _wide(slabs):
    return jnp.concatenate(slabs, axis=1)


def _tall(parts):
    return jnp.concatenate(parts, axis=0)


def _cut(value, c):
    return value[:, c * LANES : (c + 1) * LANES]


def _dw_block(rows, hg, gg, groups, group_rows, nd, w1_block, w2_block, w2_transposed, ht, ab, zb, settle, put):
    def some(read, ks):
        return _tall([_wide([read(k, c) for c in range(nd)]) for k in ks])

    step = max(1, rows // group_rows)
    for k in range(0, groups, step):
        ks = range(k, min(k + step, groups))
        if k + step >= groups:
            settle()
        s = slice(k * group_rows, (k + len(ks)) * group_rows)
        z = _dot(some(hg, ks), w1_block())
        dims = (((1,), (0,)), ((), ())) if w2_transposed else (((1,), (1,)), ((), ()))
        da = lax.dot_general(some(gg, ks), w2_block(), dims, preferred_element_type=F32)
        a, slope = _gelu_and_slope(z)
        a, dz = a.astype(BF16), (da * slope).astype(BF16)
        for c in range(SLABS):
            ab[c, s, :] = _cut(a, c)
            zb[c, s, :] = _cut(dz, c)
    v2 = lax.dot_general(
        _wide([ab[c] for c in range(SLABS)]), some(gg, range(groups)), (((0,), (0,)), ((), ())),
        preferred_element_type=F32,
    )
    put(_dot(_wide([ht[t] for t in range(ht.shape[0])]), _wide([zb[c] for c in range(SLABS)])), v2)


def _transposed_rows(hg, groups, group_rows, nd, ht):
    per = LANES // group_rows
    for t in range(groups // per):
        ht[t] = _tall([_wide([hg(t * per + e, c) for c in range(nd)]) for e in range(per)]).T


def _chain_kernel(
    n_stage, n_inner, x, g, w1, w2, y, dx, h_late, g_late, d1_part, d2_part,
    w1v, w2v, w1t, w2t, hw, gw, ho, go, zs, act, ht, ab, zb, d1v, d2v,
    wsem, xsem, h_recv, g_recv, h_send, g_send, out_recv, ring_send, ring_recv, part_sem, late_sem,
):
    p, i = lax.axis_index("stage"), lax.axis_index("inner")
    right, left = lax.rem(i + 1, n_inner), lax.rem(i + n_inner - 1, n_inner)
    _, m_all, nd, rows, _ = hw.shape
    nf = w1v.shape[0]
    units = nf // SLABS
    early = EARLY
    last = n_stage - 1
    half = nd // 2
    part = rows // MERGE

    barrier = pltpu.get_barrier_semaphore()
    for q in range(1, n_stage):
        pl.semaphore_signal(barrier, inc=1, device_id={"stage": lax.rem(p + q, n_stage)}, device_id_type=MESH)
    for q in (left, right):
        pl.semaphore_signal(barrier, inc=1, device_id={"inner": q}, device_id_type=MESH)

    loads = [
        pltpu.make_async_copy(w1.at[0, 0, :, c * LANES : (c + 1) * LANES], w1v.at[c], wsem.at[0]) for c in range(nf)
    ] + [pltpu.make_async_copy(w2.at[0, 0, :, c * LANES : (c + 1) * LANES], w2v.at[c], wsem.at[1]) for c in range(nd)]
    for c in loads:
        c.start()
    with jax.named_scope("barrier"):
        pl.semaphore_wait(barrier, n_stage + 1)

    def to_stage(src, dst, send, recv, stage):
        return pltpu.make_async_remote_copy(
            src_ref=src, dst_ref=dst, send_sem=send, recv_sem=recv,
            device_id={"stage": stage}, device_id_type=MESH,
        )

    def to_inner(src, dst, send, recv, inner):
        return pltpu.make_async_remote_copy(
            src_ref=src, dst_ref=dst, send_sem=send, recv_sem=recv,
            device_id={"inner": inner}, device_id_type=MESH,
        )

    def flat(ref, c):
        return ref.at[0, :, c * LANES : (c + 1) * LANES]

    def piece(e):
        return pl.ds(pl.multiple_of(e * part, part), part)

    def own(src, slots, recv, sem, stage):
        def to(c):
            return slots.at[i, p // MERGE, c, piece(p % MERGE)]

        @pl.when(p == stage)
        def _():
            for c in range(nd):
                pltpu.make_async_copy(flat(src, c), to(c), recv.at[p // MERGE]).start()

        @pl.when(p != stage)
        def _():
            for c in range(nd):
                to_stage(flat(src, c), to(c), sem, recv.at[p // MERGE], stage).start()

    own(x, hw, h_recv, xsem.at[0], 0)
    own(g, gw, g_recv, xsem.at[1], last)

    def ring_first(q, m, whole):
        a = whole.at[i, m]
        to_inner(a, a, ring_send.at[q, m, 0], ring_recv.at[q, m, 0], right).start()
        to_inner(a, a, ring_send.at[q, m, 1], ring_recv.at[q, m, 1], left).start()

    def ring_forward(q, m, whole):
        a, b = whole.at[left, m], whole.at[right, m]
        to_inner(a, a, ring_send.at[q, m, 0], ring_recv.at[q, m, 0], right).wait_recv()
        a = whole.at[left, m, pl.ds(0, half)]
        to_inner(a, a, ring_send.at[q, m, 2], ring_recv.at[q, m, 2], right).start()
        to_inner(b, b, ring_send.at[q, m, 1], ring_recv.at[q, m, 1], left).wait_recv()
        b = whole.at[right, m, pl.ds(half, half)]
        to_inner(b, b, ring_send.at[q, m, 3], ring_recv.at[q, m, 3], left).start()

    def ring_far(q, m, whole):
        far = lax.rem(i + 2, n_inner)
        a, b = whole.at[far, m, pl.ds(0, half)], whole.at[far, m, pl.ds(half, half)]
        return (
            to_inner(a, a, ring_send.at[q, m, 2], ring_recv.at[q, m, 2], right),
            to_inner(b, b, ring_send.at[q, m, 3], ring_recv.at[q, m, 3], left),
        )

    def ring_arrived(m):
        for q, whole in ((0, hw), (1, gw)):
            for c in ring_far(q, m, whole):
                c.wait_recv()

    def ring_sent(m):
        for q, whole in ((0, hw), (1, gw)):
            for c in ring_far(q, m, whole):
                c.wait_send()
            a = whole.at[i, m]
            to_inner(a, a, ring_send.at[q, m, 0], ring_recv.at[q, m, 0], right).wait_send()
            to_inner(a, a, ring_send.at[q, m, 1], ring_recv.at[q, m, 1], left).wait_send()

    def pass_on(m, src, slots, send, recv, end, nxt, out, out_sem):
        @pl.when(p != end)
        def _():
            to_stage(src.at[m], slots.at[i, m], send.at[m], recv.at[m], nxt).start()

        @pl.when(p == end)
        def _():
            for e in range(MERGE):
                home = m * MERGE + e

                @pl.when(p != home)
                def _():
                    for c in range(nd):
                        to_stage(src.at[m, c, piece(e)], flat(out, c), send.at[m], out_sem, home).start()

                @pl.when(p == home)
                def _():
                    for c in range(nd):
                        pltpu.make_async_copy(src.at[m, c, piece(e)], flat(out, c), out_sem).start()

    def project(m, res, w, src, *rest):
        u = _dot(_wide([act[c] for c in range(nf)]), _wide([w[c] for c in range(nd)]))
        out = (res.astype(F32) + u).astype(BF16)
        for c in range(nd):
            src[m, c] = _cut(out, c)
        pass_on(m, src, *rest)

    def forward(m, sloped):
        with jax.named_scope("wait_h"):
            pltpu.make_async_copy(hw.at[i, m], hw.at[i, m], h_recv.at[m]).wait()
        h = _wide([hw[i, m, c] for c in range(nd)])
        for b in range(0, nf, SLABS):
            z = _dot(h, _wide([w1v[b + c] for c in range(SLABS)]))
            a, slope = _gelu_and_slope(z)
            a, kept = a.astype(BF16), slope if sloped else z
            for c in range(SLABS):
                zs[m, b + c] = _cut(kept, c)
                act[b + c] = _cut(a, c)

        @pl.when((m == 0) & (p < n_stage // 2))
        def _():
            for c in loads[nf:]:
                c.wait()

        project(m, h, w2v, ho, hw, h_send, h_recv, last, jnp.minimum(p + 1, last), y, out_recv.at[0])

        @pl.when((p < n_stage - 2) | (m < early))
        def _():
            ring_first(0, m, hw)

    def backward(m):
        with jax.named_scope("wait_g"):
            pltpu.make_async_copy(gw.at[i, m], gw.at[i, m], g_recv.at[m]).wait()

        @pl.when((m < early) | ((p < n_stage - 2) & (m > early)))
        def _():
            ring_first(1, m, gw)

        dh = _wide([gw[i, m, c] for c in range(nd)])
        for b in range(0, nf, SLABS):
            da = _dot(dh, _wide([w2t[b + c] for c in range(SLABS)]))
            dz = (da * _wide([zs[m, b + c] for c in range(SLABS)])).astype(BF16)
            for c in range(SLABS):
                act[b + c] = _cut(dz, c)
        project(m, dh, w1t, go, gw, g_send, g_recv, 0, jnp.maximum(p - 1, 0), dx, out_recv.at[1])

        @pl.when(p < n_stage - 2)
        def _():
            ring_forward(0, m, hw)

            @pl.when(m == early)
            def _():
                each(0, early, lambda e: ring_forward(1, e, gw))
                ring_first(1, m, gw)

    def transpose_weights():
        def some(c, carry):
            s = pl.ds(pl.multiple_of(c * LANES, LANES), LANES)
            for e in range(nd):
                w1t[e, s, :] = w1v[c, e * LANES : (e + 1) * LANES, :].T
                w2t[c, e * LANES : (e + 1) * LANES, :] = w2v[e, s, :].T
            return carry

        lax.fori_loop(0, nf, some, 0)

    def slopes():
        def some(t, carry):
            m, b = t // (nf // SLABS), t % (nf // SLABS) * SLABS
            for c in range(SLABS):
                zs[m, b + c] = _gelu_and_slope(zs[m, b + c])[1]
            return carry

        lax.fori_loop(0, m_all * (nf // SLABS), some, 0)

    def each(lo, hi, fn):
        lax.fori_loop(lo, hi, lambda m, c: (fn(m), c)[1], 0)

    def group(whole):
        return lambda k, c: whole[k // early, k % early, c]

    groups = n_inner * early

    def part_copies(j):
        return (
            pltpu.make_async_copy(d1v, d1_part.at[j], part_sem.at[0]),
            pltpu.make_async_copy(d2v, d2_part.at[j], part_sem.at[1]),
        )

    def late_copies():
        return [
            pltpu.make_async_copy(whole.at[k, pl.ds(early, m_all - early)], out.at[k], late_sem.at[q, k])
            for q, (whole, out) in enumerate(((hw, h_late), (gw, g_late)))
            for k in range(n_inner)
        ]

    def sent(m):
        ring_sent(m)
        for src, slots, send, recv, end in ((ho, hw, h_send, h_recv, last), (go, gw, g_send, g_recv, 0)):
            for e in range(MERGE):
                a = src.at[m, :, piece(e)]

                @pl.when((p != end) | (p != m * MERGE + e))
                def _():
                    to_stage(a, a, send.at[m], recv.at[m], 0).wait_send()

        @pl.when((m == 0) & (p != 0))
        def _():
            to_stage(x.at[0], x.at[0], xsem.at[0], h_recv.at[0], 0).wait_send()

        @pl.when((m == 0) & (p != last))
        def _():
            to_stage(g.at[0], g.at[0], xsem.at[1], g_recv.at[0], last).wait_send()

    def unit(j):
        def forwards(m):
            @pl.when(p >= n_stage - 2)
            def _():
                ring_forward(0, m, hw)

            ring_forward(1, m, gw)

        def firsts(m):
            ring_first(0, m, hw)
            ring_first(1, m, gw)

        @pl.when(j == 0)
        def _():
            @pl.when(p >= n_stage - 2)
            def _():
                each(0, early, forwards)
                each(early, m_all, firsts)

            each(0, early, ring_arrived)
            _transposed_rows(group(hw), groups, rows, nd, ht)

        for m in range(early, m_all):
            @pl.when(j == min(units - 1, 2 * (m - early + 1)))
            def _():
                forwards(m)

        @pl.when(j == units - 1)
        def _():
            each(early, m_all, ring_arrived)
            for c in late_copies():
                c.start()
            each(0, m_all, sent)

        def settle():
            @pl.when(j > 0)
            def _():
                for c in part_copies(j):
                    c.wait()

        def put(v1, v2):
            d1v[...] = v1
            d2v[...] = v2

        _dw_block(
            256, group(hw), group(gw), groups, rows, nd,
            lambda: _wide([w1v[j * SLABS + c] for c in range(SLABS)]),
            lambda: _wide([w2t[j * SLABS + c] for c in range(SLABS)]),
            True, ht, ab, zb, settle, put,
        )
        for c in part_copies(j):
            c.start()

    with jax.named_scope("loads"):
        for c in loads[:nf]:
            c.wait()

    first = jnp.where(p == last, 1, m_all)
    rest = m_all - first
    turn = jnp.where(p < n_stage // 2, first, 0)

    def step(k, carry):
        j = k - first
        swap = j < 2 * rest
        is_u = k >= 2 * m_all
        is_f = (j < 0) | (swap & (j % 2 == 1))
        is_b = jnp.logical_not(is_f | is_u)
        m_f = jnp.where(j < 0, k, jnp.minimum(first + j // 2, m_all - 1))
        m_b = jnp.maximum(jnp.minimum(jnp.where(swap, j // 2, j - rest), m_all - 1), 0)
        u = jnp.maximum(k - 2 * m_all, 0)

        @pl.when(k == turn)
        def _():
            with jax.named_scope("transp"):
                @pl.when(p >= n_stage // 2)
                def _():
                    for c in loads[nf:]:
                        c.wait()

                transpose_weights()

        @pl.when((k == first) & (p < n_stage - 2))
        def _():
            with jax.named_scope("slopes"):
                slopes()

        @pl.when(is_f & (p < n_stage - 2))
        def _():
            with jax.named_scope("fwd"):
                forward(m_f, False)

        @pl.when(is_f & (p >= n_stage - 2))
        def _():
            with jax.named_scope("fwd"):
                forward(m_f, True)

        @pl.when(is_b)
        def _():
            with jax.named_scope("bwd"):
                backward(m_b)

        @pl.when(is_u)
        def _():
            with jax.named_scope("unit"):
                unit(u)

        return carry

    lax.fori_loop(0, 2 * m_all + units, step, 0)

    with jax.named_scope("finish"):
        for c in (*part_copies(units - 1), *late_copies()):
            c.wait()
    with jax.named_scope("outwait"):
        pltpu.make_async_copy(y.at[0], y.at[0], out_recv.at[0]).wait()
        pltpu.make_async_copy(dx.at[0], dx.at[0], out_recv.at[1]).wait()


def _chain(n_stage, n_inner, x, g, w1, w2):
    mb, rows, d = x.shape
    f = w1.shape[-1]
    rows = rows * MERGE
    m_all = mb * n_stage // MERGE
    early = EARLY
    nd, nf = d // LANES, f // LANES
    blk = SLABS * LANES
    tokens = n_inner * early * rows
    hbm = pl.BlockSpec(memory_space=pltpu.HBM)
    whole = (n_inner, m_all, nd, rows, LANES)
    late = jax.ShapeDtypeStruct((n_inner, m_all - early, nd, rows, LANES), BF16)
    dma = pltpu.SemaphoreType.DMA
    vmem = pltpu.VMEM
    return pl.pallas_call(
        functools.partial(_chain_kernel, n_stage, n_inner),
        out_shape=[
            jax.ShapeDtypeStruct(x.shape, BF16), jax.ShapeDtypeStruct(x.shape, BF16), late, late,
            jax.ShapeDtypeStruct((f // blk, d, blk), F32), jax.ShapeDtypeStruct((f // blk, blk, d), F32),
        ],
        in_specs=[hbm] * 4,
        out_specs=[hbm] * 6,
        scratch_shapes=[
            vmem((nf, d, LANES), BF16), vmem((nd, f, LANES), BF16),
            vmem((nd, f, LANES), BF16), vmem((nf, d, LANES), BF16),
            vmem(whole, BF16), vmem(whole, BF16),
            vmem((m_all, nd, rows, LANES), BF16), vmem((m_all, nd, rows, LANES), BF16),
            vmem((m_all, nf, rows, LANES), F32), vmem((nf, rows, LANES), BF16),
            vmem((tokens // LANES, d, LANES), BF16),
            vmem((SLABS, tokens, LANES), BF16), vmem((SLABS, tokens, LANES), BF16),
            vmem((d, blk), F32), vmem((blk, d), F32),
            dma((2,)), dma((2,)), dma((m_all,)), dma((m_all,)), dma((m_all,)), dma((m_all,)), dma((2,)),
            dma((2, m_all, 4)), dma((2, m_all, 4)), dma((2,)), dma((2, n_inner)),
        ],
        compiler_params=pltpu.CompilerParams(
            collective_id=0, has_side_effects=True, vmem_limit_bytes=VMEM_LIMIT
        ),
        name="chain",
    )(x, g, w1, w2)


def _late_kernel(h, g, y_in, dx_in, w1_0, w1_1, w1_2, w1_3, *rest):
    nd = h.shape[1]
    w1 = (w1_0, w1_1, w1_2, w1_3)
    w2, (p1, p2, d1, d2, y, dx, ht, ab, zb) = rest[:nd], rest[nd:]
    groups, _, rows, _ = h.shape

    @pl.when(pl.program_id(0) == 0)
    def _():
        y[...] = y_in[...]
        dx[...] = dx_in[...]
        _transposed_rows(lambda k, c: h[k, c], groups, rows, nd, ht)

    def put(v1, v2):
        d1[...] = p1[0] + v1
        d2[...] = p2[0] + v2

    _dw_block(
        512, lambda k, c: h[k, c], lambda k, c: g[k, c], groups, rows, nd,
        lambda: _wide([w[...] for w in w1]), lambda: _wide([w[...] for w in w2]),
        False, ht, ab, zb, lambda: None, put,
    )


def _late(h, g, y, dx, w1, w2, p1, p2):
    groups, nd, rows, _ = h.shape
    d, f = w1.shape
    blk = SLABS * LANES
    t = groups * rows
    whole = pl.BlockSpec(h.shape, lambda j: (0, 0, 0, 0))
    mine = pl.BlockSpec(y.shape, lambda j: (0, 0, 0))
    return pl.pallas_call(
        _late_kernel,
        grid=(f // blk,),
        in_specs=[whole, whole, mine, mine]
        + [pl.BlockSpec((d, LANES), functools.partial(lambda c, j: (0, j * SLABS + c), c)) for c in range(SLABS)]
        + [pl.BlockSpec((blk, LANES), functools.partial(lambda c, j: (j, c), c)) for c in range(nd)]
        + [pl.BlockSpec((1, d, blk), lambda j: (j, 0, 0)), pl.BlockSpec((1, blk, d), lambda j: (j, 0, 0))],
        out_specs=[pl.BlockSpec((d, blk), lambda j: (0, j)), pl.BlockSpec((blk, d), lambda j: (j, 0)), mine, mine],
        out_shape=[
            jax.ShapeDtypeStruct((d, f), F32), jax.ShapeDtypeStruct((f, d), F32),
            jax.ShapeDtypeStruct(y.shape, BF16), jax.ShapeDtypeStruct(dx.shape, BF16),
        ],
        scratch_shapes=[
            pltpu.VMEM((t // LANES, d, LANES), BF16),
            pltpu.VMEM((SLABS, t, LANES), BF16), pltpu.VMEM((SLABS, t, LANES), BF16),
        ],
        compiler_params=pltpu.CompilerParams(vmem_limit_bytes=VMEM_LIMIT),
        cost_estimate=pl.CostEstimate(flops=8 * t * d * f, bytes_accessed=20 * d * f, transcendentals=t * f),
        name="late",
    )(h, g, y, dx, *([w1] * SLABS), *([w2] * nd), p1, p2)


def solution(mesh):
    n_stage, n_inner = mesh.shape["stage"], mesh.shape["inner"]

    def body(x, g, w1, w2):
        d, f = w1.shape[-2:]
        y, dx, h, gg, p1, p2 = _chain(n_stage, n_inner, x, g, w1, w2)
        flat = (-1, *h.shape[2:])
        d1, d2, y, dx = _late(h.reshape(flat), gg.reshape(flat), y, dx, w1.reshape(d, f), w2.reshape(f, d), p1, p2)
        return y, dx, d1.reshape(w1.shape), d2.reshape(w2.shape)

    tok = P(("data", "stage"), "inner", None)
    wsp = P(None, "stage", None, None)
    dsp = P("data", "stage", None, None)
    return jax.shard_map(body, mesh=mesh, in_specs=(tok, tok, wsp, wsp), out_specs=(tok, tok, dsp, dsp), check_vma=False)
```

```python
import functools

import jax
import jax.numpy as jnp
from jax import lax
from jax.experimental import pallas as pl
from jax.experimental.pallas import tpu as pltpu
from jax.sharding import PartitionSpec as P

MESH = pl.DeviceIdType.MESH
F32, BF16 = jnp.float32, jnp.bfloat16
C0, C1 = 0.7978845608028654, 0.044715
LANES = 128
VMEM_LIMIT = 67043328
SLABS = 4
MERGE = 2
EARLY = 2


def _gelu_and_slope(z):
    z2 = z * z
    half = 0.5 * jnp.tanh(z * (C0 + (C0 * C1) * z2)) + 0.5
    a = z * half
    return a, half + (a - a * half) * (2.0 * C0 + (6.0 * C0 * C1) * z2)


def _dot(a, b):
    return jnp.dot(a, b, preferred_element_type=F32)


def _wide(slabs):
    return jnp.concatenate(slabs, axis=1)


def _tall(parts):
    return jnp.concatenate(parts, axis=0)


def _cut(value, c):
    return value[:, c * LANES : (c + 1) * LANES]


def _rows_of(read, ks, n):
    return _tall([_wide([read(k, c) for c in range(n)]) for k in ks])


def _chunks(rows, groups, group_rows):
    step = max(1, rows // group_rows)
    for k in range(0, groups, step):
        ks = range(k, min(k + step, groups))
        yield ks, slice(k * group_rows, (k + len(ks)) * group_rows)


def _dw_block(
    rows, hg, gg, groups, group_rows, nd, w1_block, w2_block, w2_transposed, ht, ab, zb, settle, put, ready=None
):
    for ks, s in _chunks(rows, groups, group_rows):
        if ks.stop == groups:
            settle()
        if ready is None:
            z = _dot(_rows_of(hg, ks, nd), w1_block())
        dims = (((1,), (0,)), ((), ())) if w2_transposed else (((1,), (1,)), ((), ()))
        da = lax.dot_general(_rows_of(gg, ks, nd), w2_block(), dims, preferred_element_type=F32)
        if ready is None:
            a, slope = _gelu_and_slope(z)
            a = a.astype(BF16)
            for c in range(SLABS):
                ab[c, s, :] = _cut(a, c)
        else:
            slope = _rows_of(ready[1], ks, SLABS)
        dz = (da * slope).astype(BF16)
        for c in range(SLABS):
            zb[c, s, :] = _cut(dz, c)
    a = _wide([ab[c] for c in range(SLABS)] if ready is None else [ready[0](c) for c in range(SLABS)])
    v2 = lax.dot_general(
        a, _rows_of(gg, range(groups), nd), (((0,), (0,)), ((), ())), preferred_element_type=F32
    )
    put(_dot(_wide([ht[t] for t in range(ht.shape[0])]), _wide([zb[c] for c in range(SLABS)])), v2)


def _transposed_rows(hg, groups, group_rows, nd, ht):
    per = LANES // group_rows
    for t in range(groups // per):
        ht[t] = _tall([_wide([hg(t * per + e, c) for c in range(nd)]) for e in range(per)]).T


def _chain_kernel(
    n_stage, n_inner, x, g, w1, w2, y, dx, h_late, g_late, d1_part, d2_part, a_pre, s_pre,
    w1v, w2v, w1t, w2t, hw, gw, ho, go, zs, act, ht, narrow, full, d2v,
    wsem, xsem, h_recv, g_recv, h_send, g_send, out_recv, ring_send, ring_recv, part_sem, late_sem, pre_sem,
):
    p, i = lax.axis_index("stage"), lax.axis_index("inner")
    right, left = lax.rem(i + 1, n_inner), lax.rem(i + n_inner - 1, n_inner)
    _, m_all, nd, rows, _ = hw.shape
    nf = w1v.shape[0]
    units = nf // SLABS
    early = EARLY
    last = n_stage - 1
    half = nd // 2
    part = rows // MERGE
    groups = n_inner * early
    tokens = groups * rows
    ab, zb = narrow.at[0], narrow.at[1]
    d1v = full.at[1]

    barrier = pltpu.get_barrier_semaphore()
    for q in range(1, n_stage):
        pl.semaphore_signal(barrier, inc=1, device_id={"stage": lax.rem(p + q, n_stage)}, device_id_type=MESH)
    for q in (left, right):
        pl.semaphore_signal(barrier, inc=1, device_id={"inner": q}, device_id_type=MESH)

    loads = [
        pltpu.make_async_copy(w1.at[0, 0, :, c * LANES : (c + 1) * LANES], w1v.at[c], wsem.at[0]) for c in range(nf)
    ] + [pltpu.make_async_copy(w2.at[0, 0, :, c * LANES : (c + 1) * LANES], w2v.at[c], wsem.at[1]) for c in range(nd)]
    for c in loads:
        c.start()
    with jax.named_scope("barrier"):
        pl.semaphore_wait(barrier, n_stage + 1)

    def to_stage(src, dst, send, recv, stage):
        return pltpu.make_async_remote_copy(
            src_ref=src, dst_ref=dst, send_sem=send, recv_sem=recv,
            device_id={"stage": stage}, device_id_type=MESH,
        )

    def to_inner(src, dst, send, recv, inner):
        return pltpu.make_async_remote_copy(
            src_ref=src, dst_ref=dst, send_sem=send, recv_sem=recv,
            device_id={"inner": inner}, device_id_type=MESH,
        )

    def flat(ref, c):
        return ref.at[0, :, c * LANES : (c + 1) * LANES]

    def piece(e):
        return pl.ds(pl.multiple_of(e * part, part), part)

    def own(src, slots, recv, sem, stage):
        def to(c):
            return slots.at[i, p // MERGE, c, piece(p % MERGE)]

        @pl.when(p == stage)
        def _():
            for c in range(nd):
                pltpu.make_async_copy(flat(src, c), to(c), recv.at[p // MERGE]).start()

        @pl.when(p != stage)
        def _():
            for c in range(nd):
                to_stage(flat(src, c), to(c), sem, recv.at[p // MERGE], stage).start()

    own(x, hw, h_recv, xsem.at[0], 0)
    own(g, gw, g_recv, xsem.at[1], last)

    def ring_first(q, m, whole):
        a = whole.at[i, m]
        to_inner(a, a, ring_send.at[q, m, 0], ring_recv.at[q, m, 0], right).start()
        to_inner(a, a, ring_send.at[q, m, 1], ring_recv.at[q, m, 1], left).start()

    def ring_forward(q, m, whole):
        a, b = whole.at[left, m], whole.at[right, m]
        to_inner(a, a, ring_send.at[q, m, 0], ring_recv.at[q, m, 0], right).wait_recv()
        a = whole.at[left, m, pl.ds(0, half)]
        to_inner(a, a, ring_send.at[q, m, 2], ring_recv.at[q, m, 2], right).start()
        to_inner(b, b, ring_send.at[q, m, 1], ring_recv.at[q, m, 1], left).wait_recv()
        b = whole.at[right, m, pl.ds(half, half)]
        to_inner(b, b, ring_send.at[q, m, 3], ring_recv.at[q, m, 3], left).start()

    def ring_far(q, m, whole):
        far = lax.rem(i + 2, n_inner)
        a, b = whole.at[far, m, pl.ds(0, half)], whole.at[far, m, pl.ds(half, half)]
        return (
            to_inner(a, a, ring_send.at[q, m, 2], ring_recv.at[q, m, 2], right),
            to_inner(b, b, ring_send.at[q, m, 3], ring_recv.at[q, m, 3], left),
        )

    def ring_arrived(m, q):
        for c in ring_far(q, m, (hw, gw)[q]):
            c.wait_recv()

    def ring_sent(m):
        for q, whole in ((0, hw), (1, gw)):
            for c in ring_far(q, m, whole):
                c.wait_send()
            a = whole.at[i, m]
            to_inner(a, a, ring_send.at[q, m, 0], ring_recv.at[q, m, 0], right).wait_send()
            to_inner(a, a, ring_send.at[q, m, 1], ring_recv.at[q, m, 1], left).wait_send()

    def pass_on(m, src, slots, send, recv, end, nxt, out, out_sem):
        @pl.when(p != end)
        def _():
            to_stage(src.at[m], slots.at[i, m], send.at[m], recv.at[m], nxt).start()

        @pl.when(p == end)
        def _():
            for e in range(MERGE):
                home = m * MERGE + e

                @pl.when(p != home)
                def _():
                    for c in range(nd):
                        to_stage(src.at[m, c, piece(e)], flat(out, c), send.at[m], out_sem, home).start()

                @pl.when(p == home)
                def _():
                    for c in range(nd):
                        pltpu.make_async_copy(src.at[m, c, piece(e)], flat(out, c), out_sem).start()

    def project(m, res, w, src, *rest):
        u = _dot(_wide([act[c] for c in range(nf)]), _wide([w[c] for c in range(nd)]))
        out = (res.astype(F32) + u).astype(BF16)
        for c in range(nd):
            src[m, c] = _cut(out, c)
        pass_on(m, src, *rest)

    def forward(m, sloped):
        with jax.named_scope("wait_h"):
            pltpu.make_async_copy(hw.at[i, m], hw.at[i, m], h_recv.at[m]).wait()
        h = _wide([hw[i, m, c] for c in range(nd)])
        for b in range(0, nf, SLABS):
            z = _dot(h, _wide([w1v[b + c] for c in range(SLABS)]))
            a, slope = _gelu_and_slope(z)
            a, kept = a.astype(BF16), slope if sloped else z
            for c in range(SLABS):
                zs[m, b + c] = _cut(kept, c)
                act[b + c] = _cut(a, c)

        @pl.when((m == 0) & (p < n_stage // 2))
        def _():
            for c in loads[nf:]:
                c.wait()

        project(m, h, w2v, ho, hw, h_send, h_recv, last, jnp.minimum(p + 1, last), y, out_recv.at[0])

        @pl.when((p < n_stage - 2) | (m < early))
        def _():
            ring_first(0, m, hw)

    def backward(m):
        with jax.named_scope("wait_g"):
            pltpu.make_async_copy(gw.at[i, m], gw.at[i, m], g_recv.at[m]).wait()

        @pl.when((m < early) | ((p < n_stage - 2) & (m > early)))
        def _():
            ring_first(1, m, gw)

        dh = _wide([gw[i, m, c] for c in range(nd)])
        for b in range(0, nf, SLABS):
            da = _dot(dh, _wide([w2t[b + c] for c in range(SLABS)]))
            dz = (da * _wide([zs[m, b + c] for c in range(SLABS)])).astype(BF16)
            for c in range(SLABS):
                act[b + c] = _cut(dz, c)
        project(m, dh, w1t, go, gw, g_send, g_recv, 0, jnp.maximum(p - 1, 0), dx, out_recv.at[1])

        @pl.when((p < n_stage - 2) & (m == early))
        def _():
            each(0, early, lambda e: ring_forward(1, e, gw))
            ring_first(1, m, gw)

    def transpose_weights():
        def some(c, carry):
            s = pl.ds(pl.multiple_of(c * LANES, LANES), LANES)
            for e in range(nd):
                w1t[e, s, :] = w1v[c, e * LANES : (e + 1) * LANES, :].T
                w2t[c, e * LANES : (e + 1) * LANES, :] = w2v[e, s, :].T
            return carry

        lax.fori_loop(0, nf, some, 0)

    def slopes():
        def some(t, carry):
            m, b = t // (nf // SLABS), t % (nf // SLABS) * SLABS
            for c in range(SLABS):
                zs[m, b + c] = _gelu_and_slope(zs[m, b + c])[1]
            return carry

        lax.fori_loop(0, m_all * (nf // SLABS), some, 0)

    def each(lo, hi, fn):
        lax.fori_loop(lo, hi, lambda m, c: (fn(m), c)[1], 0)

    def group(whole):
        return lambda k, c: whole[k // early, k % early, c]

    def pre_stores(j):
        b = j % 2
        return (
            pltpu.make_async_copy(narrow.at[b], a_pre.at[j], pre_sem.at[0, b]),
            pltpu.make_async_copy(full.at[b, pl.ds(0, SLABS * groups)], s_pre.at[j], pre_sem.at[1, b]),
        )

    def pre_loads(j):
        b = j % 2
        return (
            pltpu.make_async_copy(
                a_pre.at[j], w2v.at[pl.ds(b * SLABS, SLABS), pl.ds(0, tokens)], pre_sem.at[0, b]
            ),
            pltpu.make_async_copy(s_pre.at[j], zs.at[b, pl.ds(0, SLABS * groups)], pre_sem.at[1, b]),
        )

    def pre_unit(j):
        b = j % 2

        @pl.when(j > 1)
        def _():
            for c in pre_stores(j):
                c.wait()

        for ks, s in _chunks(512, groups, rows):
            z = _dot(_rows_of(group(hw), ks, nd), _wide([w1v[j * SLABS + c] for c in range(SLABS)]))
            a, slope = _gelu_and_slope(z)
            a = a.astype(BF16)
            for c in range(SLABS):
                narrow[b, c, s, :] = _cut(a, c)
                for n, k in enumerate(ks):
                    full[b, c * groups + k] = _cut(slope[n * rows : (n + 1) * rows], c)
        for c in pre_stores(j):
            c.start()

    def part_copies(j):
        return (
            pltpu.make_async_copy(d1v.at[pl.ds(0, SLABS * nd)], d1_part.at[j], part_sem.at[0]),
            pltpu.make_async_copy(d2v, d2_part.at[j], part_sem.at[1]),
        )

    def late_copies():
        return [
            pltpu.make_async_copy(whole.at[k, pl.ds(early, m_all - early)], out.at[k], late_sem.at[q, k])
            for q, (whole, out) in enumerate(((hw, h_late), (gw, g_late)))
            for k in range(n_inner)
        ]

    def sent(m):
        ring_sent(m)
        for src, slots, send, recv, end in ((ho, hw, h_send, h_recv, last), (go, gw, g_send, g_recv, 0)):
            for e in range(MERGE):
                a = src.at[m, :, piece(e)]

                @pl.when((p != end) | (p != m * MERGE + e))
                def _():
                    to_stage(a, a, send.at[m], recv.at[m], 0).wait_send()

        @pl.when((m == 0) & (p != 0))
        def _():
            to_stage(x.at[0], x.at[0], xsem.at[0], h_recv.at[0], 0).wait_send()

        @pl.when((m == 0) & (p != last))
        def _():
            to_stage(g.at[0], g.at[0], xsem.at[1], g_recv.at[0], last).wait_send()

    def unit(j):
        def forwards(m):
            @pl.when(p >= n_stage - 2)
            def _():
                ring_forward(0, m, hw)

            ring_forward(1, m, gw)

        def firsts(m):
            ring_first(0, m, hw)
            ring_first(1, m, gw)

        @pl.when(j == 0)
        def _():
            @pl.when(p >= n_stage - 2)
            def _():
                each(0, early, forwards)
                each(early, m_all, firsts)

            @pl.when(p < n_stage // 2)
            def _():
                for c in pre_loads(0):
                    c.start()

            each(0, early, lambda m: ring_arrived(m, 1))

            @pl.when(p >= n_stage // 2)
            def _():
                each(0, early, lambda m: ring_arrived(m, 0))

            _transposed_rows(group(hw), groups, rows, nd, ht)

        for m in range(early, m_all):
            @pl.when(j == min(units - 1, 2 * (m - early + 1)))
            def _():
                forwards(m)

        @pl.when(j == units - 1)
        def _():
            each(early, m_all, lambda m: ring_arrived(m, 0))
            each(early, m_all, lambda m: ring_arrived(m, 1))
            for c in late_copies():
                c.start()
            each(0, m_all, sent)

        def settle():
            @pl.when(j > 0)
            def _():
                for c in part_copies(j):
                    c.wait()

        def put(v1, v2):
            d2v[...] = v2
            for c in range(SLABS):
                for e in range(nd):
                    d1v[c * nd + e] = _cut(v1[e * LANES : (e + 1) * LANES], c)

        def block(ready):
            _dw_block(
                256, group(hw), group(gw), groups, rows, nd,
                lambda: _wide([w1v[j * SLABS + c] for c in range(SLABS)]),
                lambda: _wide([w2t[j * SLABS + c] for c in range(SLABS)]),
                True, ht, ab, zb, settle, put, ready,
            )

        @pl.when(p < n_stage // 2)
        def _():
            b = j % 2
            for c in pre_loads(j):
                c.wait()

            @pl.when(j + 1 < units)
            def _():
                for c in pre_loads(j + 1):
                    c.start()

            block((
                lambda c: w2v[b * SLABS + c, 0:tokens, :],
                lambda k, c: zs[b, c * groups + k],
            ))

        @pl.when(p >= n_stage // 2)
        def _():
            block(None)

        for c in part_copies(j):
            c.start()

    with jax.named_scope("loads"):
        for c in loads[:nf]:
            c.wait()

    first = jnp.where(p == last, 1, m_all)
    rest = m_all - first
    turn = jnp.where(p < n_stage // 2, first, 0)

    def step(k, carry):
        j = k - first
        swap = j < 2 * rest
        is_u = k >= 2 * m_all
        is_f = (j < 0) | (swap & (j % 2 == 1))
        is_b = jnp.logical_not(is_f | is_u)
        m_f = jnp.where(j < 0, k, jnp.minimum(first + j // 2, m_all - 1))
        m_b = jnp.maximum(jnp.minimum(jnp.where(swap, j // 2, j - rest), m_all - 1), 0)
        u = jnp.maximum(k - 2 * m_all, 0)

        @pl.when(k == turn)
        def _():
            with jax.named_scope("transp"):
                @pl.when(p >= n_stage // 2)
                def _():
                    for c in loads[nf:]:
                        c.wait()

                transpose_weights()

        @pl.when((k == first) & (p < n_stage - 2))
        def _():
            with jax.named_scope("slopes"):
                slopes()
            with jax.named_scope("hring"):
                each(0, m_all, lambda m: ring_forward(0, m, hw))

        @pl.when((k == first) & (p < n_stage // 2))
        def _():
            with jax.named_scope("pre"):
                each(0, early, lambda m: ring_arrived(m, 0))
                each(0, units, pre_unit)
                for c in (*pre_stores(units - 2), *pre_stores(units - 1)):
                    c.wait()

        @pl.when(is_f & (p < n_stage - 2))
        def _():
            with jax.named_scope("fwd"):
                forward(m_f, False)

        @pl.when(is_f & (p >= n_stage - 2))
        def _():
            with jax.named_scope("fwd"):
                forward(m_f, True)

        @pl.when(is_b)
        def _():
            with jax.named_scope("bwd"):
                backward(m_b)

        @pl.when(is_u)
        def _():
            with jax.named_scope("unit"):
                unit(u)

        return carry

    lax.fori_loop(0, 2 * m_all + units, step, 0)

    with jax.named_scope("finish"):
        for c in (*part_copies(units - 1), *late_copies()):
            c.wait()
    with jax.named_scope("outwait"):
        pltpu.make_async_copy(y.at[0], y.at[0], out_recv.at[0]).wait()
        pltpu.make_async_copy(dx.at[0], dx.at[0], out_recv.at[1]).wait()


def _chain(n_stage, n_inner, x, g, w1, w2):
    mb, rows, d = x.shape
    f = w1.shape[-1]
    rows = rows * MERGE
    m_all = mb * n_stage // MERGE
    early = EARLY
    nd, nf = d // LANES, f // LANES
    blk = SLABS * LANES
    groups = n_inner * early
    tokens = groups * rows
    tiles = SLABS * max(nd, groups)
    hbm = pl.BlockSpec(memory_space=pltpu.HBM)
    whole = (n_inner, m_all, nd, rows, LANES)
    late = jax.ShapeDtypeStruct((n_inner, m_all - early, nd, rows, LANES), BF16)
    dma = pltpu.SemaphoreType.DMA
    vmem = pltpu.VMEM
    return pl.pallas_call(
        functools.partial(_chain_kernel, n_stage, n_inner),
        out_shape=[
            jax.ShapeDtypeStruct(x.shape, BF16), jax.ShapeDtypeStruct(x.shape, BF16), late, late,
            jax.ShapeDtypeStruct((f // blk, SLABS * nd, LANES, LANES), F32),
            jax.ShapeDtypeStruct((f // blk, blk, d), F32),
            jax.ShapeDtypeStruct((f // blk, SLABS, tokens, LANES), BF16),
            jax.ShapeDtypeStruct((f // blk, SLABS * groups, rows, LANES), F32),
        ],
        in_specs=[hbm] * 4,
        out_specs=[hbm] * 8,
        scratch_shapes=[
            vmem((nf, d, LANES), BF16), vmem((nd, f, LANES), BF16),
            vmem((nd, f, LANES), BF16), vmem((nf, d, LANES), BF16),
            vmem(whole, BF16), vmem(whole, BF16),
            vmem((m_all, nd, rows, LANES), BF16), vmem((m_all, nd, rows, LANES), BF16),
            vmem((m_all, nf, rows, LANES), F32), vmem((nf, rows, LANES), BF16),
            vmem((tokens // LANES, d, LANES), BF16),
            vmem((2, SLABS, tokens, LANES), BF16), vmem((2, tiles, LANES, LANES), F32), vmem((blk, d), F32),
            dma((2,)), dma((2,)), dma((m_all,)), dma((m_all,)), dma((m_all,)), dma((m_all,)), dma((2,)),
            dma((2, m_all, 4)), dma((2, m_all, 4)), dma((2,)), dma((2, n_inner)), dma((2, 2)),
        ],
        compiler_params=pltpu.CompilerParams(
            collective_id=0, has_side_effects=True, vmem_limit_bytes=VMEM_LIMIT
        ),
        name="chain",
    )(x, g, w1, w2)


def _late_kernel(h, g, y_in, dx_in, w1_0, w1_1, w1_2, w1_3, *rest):
    nd = h.shape[1]
    w1 = (w1_0, w1_1, w1_2, w1_3)
    w2, (p1, p2, d1, d2, y, dx, ht, ab, zb) = rest[:nd], rest[nd:]
    groups, _, rows, _ = h.shape

    @pl.when(pl.program_id(0) == 0)
    def _():
        y[...] = y_in[...]
        dx[...] = dx_in[...]
        _transposed_rows(lambda k, c: h[k, c], groups, rows, nd, ht)

    def put(v1, v2):
        d2[...] = p2[0] + v2
        for c in range(SLABS):
            for e in range(nd):
                r, s = slice(e * LANES, (e + 1) * LANES), slice(c * LANES, (c + 1) * LANES)
                d1[r, s] = p1[0, c * nd + e] + v1[r, s]

    _dw_block(
        512, lambda k, c: h[k, c], lambda k, c: g[k, c], groups, rows, nd,
        lambda: _wide([w[...] for w in w1]), lambda: _wide([w[...] for w in w2]),
        False, ht, ab, zb, lambda: None, put,
    )


def _late(h, g, y, dx, w1, w2, p1, p2):
    groups, nd, rows, _ = h.shape
    d, f = w1.shape
    blk = SLABS * LANES
    t = groups * rows
    whole = pl.BlockSpec(h.shape, lambda j: (0, 0, 0, 0))
    mine = pl.BlockSpec(y.shape, lambda j: (0, 0, 0))
    return pl.pallas_call(
        _late_kernel,
        grid=(f // blk,),
        in_specs=[whole, whole, mine, mine]
        + [pl.BlockSpec((d, LANES), functools.partial(lambda c, j: (0, j * SLABS + c), c)) for c in range(SLABS)]
        + [pl.BlockSpec((blk, LANES), functools.partial(lambda c, j: (j, c), c)) for c in range(nd)]
        + [pl.BlockSpec((1, SLABS * nd, LANES, LANES), lambda j: (j, 0, 0, 0)), pl.BlockSpec((1, blk, d), lambda j: (j, 0, 0))],
        out_specs=[pl.BlockSpec((d, blk), lambda j: (0, j)), pl.BlockSpec((blk, d), lambda j: (j, 0)), mine, mine],
        out_shape=[
            jax.ShapeDtypeStruct((d, f), F32), jax.ShapeDtypeStruct((f, d), F32),
            jax.ShapeDtypeStruct(y.shape, BF16), jax.ShapeDtypeStruct(dx.shape, BF16),
        ],
        scratch_shapes=[
            pltpu.VMEM((t // LANES, d, LANES), BF16),
            pltpu.VMEM((SLABS, t, LANES), BF16), pltpu.VMEM((SLABS, t, LANES), BF16),
        ],
        compiler_params=pltpu.CompilerParams(vmem_limit_bytes=VMEM_LIMIT),
        cost_estimate=pl.CostEstimate(flops=8 * t * d * f, bytes_accessed=20 * d * f, transcendentals=t * f),
        name="late",
    )(h, g, y, dx, *([w1] * SLABS), *([w2] * nd), p1, p2)


def solution(mesh):
    n_stage, n_inner = mesh.shape["stage"], mesh.shape["inner"]

    def body(x, g, w1, w2):
        d, f = w1.shape[-2:]
        y, dx, h, gg, p1, p2, _, _ = _chain(n_stage, n_inner, x, g, w1, w2)
        flat = (-1, *h.shape[2:])
        d1, d2, y, dx = _late(h.reshape(flat), gg.reshape(flat), y, dx, w1.reshape(d, f), w2.reshape(f, d), p1, p2)
        return y, dx, d1.reshape(w1.shape), d2.reshape(w2.shape)

    tok = P(("data", "stage"), "inner", None)
    wsp = P(None, "stage", None, None)
    dsp = P("data", "stage", None, None)
    return jax.shard_map(body, mesh=mesh, in_specs=(tok, tok, wsp, wsp), out_specs=(tok, tok, dsp, dsp), check_vma=False)
```

```python
import functools

import jax
import jax.numpy as jnp
from jax import lax
from jax.experimental import pallas as pl
from jax.experimental.pallas import tpu as pltpu
from jax.sharding import PartitionSpec as P

MESH = pl.DeviceIdType.MESH
F32, BF16 = jnp.float32, jnp.bfloat16
C0, C1 = 0.7978845608028654, 0.044715
LANES = 128
VMEM_LIMIT = 67043328
SLABS = 4
MERGE = 2
EARLY = 2
PRE_LATE = 2


def _gelu_and_slope(z):
    z2 = z * z
    half = 0.5 * jnp.tanh(z * (C0 + (C0 * C1) * z2)) + 0.5
    a = z * half
    return a, half + (a - a * half) * (2.0 * C0 + (6.0 * C0 * C1) * z2)


def _dot(a, b):
    return jnp.dot(a, b, preferred_element_type=F32)


def _wide(slabs):
    return jnp.concatenate(slabs, axis=1)


def _tall(parts):
    return jnp.concatenate(parts, axis=0)


def _cut(value, c):
    return value[:, c * LANES : (c + 1) * LANES]


def _rows_of(read, ks, n):
    return _tall([_wide([read(k, c) for c in range(n)]) for k in ks])


def _chunks(rows, groups, group_rows):
    step = max(1, rows // group_rows)
    for k in range(0, groups, step):
        ks = range(k, min(k + step, groups))
        yield ks, slice(k * group_rows, (k + len(ks)) * group_rows)


def _dw_block(
    rows, hg, gg, groups, group_rows, nd, w1_block, w2_block, w2_transposed, ht, ab, zb, settle, put, ready=None
):
    for ks, s in _chunks(rows, groups, group_rows):
        if ks.stop == groups:
            settle()
        if ready is None:
            z = _dot(_rows_of(hg, ks, nd), w1_block())
        dims = (((1,), (0,)), ((), ())) if w2_transposed else (((1,), (1,)), ((), ()))
        da = lax.dot_general(_rows_of(gg, ks, nd), w2_block(), dims, preferred_element_type=F32)
        if ready is None:
            a, slope = _gelu_and_slope(z)
            a = a.astype(BF16)
            for c in range(SLABS):
                ab[c, s, :] = _cut(a, c)
        else:
            slope = _rows_of(ready[1], ks, SLABS)
        dz = (da * slope).astype(BF16)
        for c in range(SLABS):
            zb[c, s, :] = _cut(dz, c)
    a = _wide([ab[c] for c in range(SLABS)] if ready is None else [ready[0](c) for c in range(SLABS)])
    v2 = lax.dot_general(
        a, _rows_of(gg, range(groups), nd), (((0,), (0,)), ((), ())), preferred_element_type=F32
    )
    put(_dot(_wide([ht[t] for t in range(ht.shape[0])]), _wide([zb[c] for c in range(SLABS)])), v2)


def _transposed_rows(hg, groups, group_rows, nd, ht):
    per = LANES // group_rows
    for t in range(groups // per):
        ht[t] = _tall([_wide([hg(t * per + e, c) for c in range(nd)]) for e in range(per)]).T


def _chain_kernel(
    n_stage, n_inner, x, g, w1, w2, y, dx, h_late, g_late, d1_part, d2_part, a_pre, s_pre,
    w1v, w2v, w1t, w2t, hw, gw, ho, go, zs, act, ht, narrow, full,
    wsem, xsem, h_recv, g_recv, h_send, g_send, out_recv, ring_send, ring_recv, part_sem, late_sem, pre_sem,
):
    p, i = lax.axis_index("stage"), lax.axis_index("inner")
    right, left = lax.rem(i + 1, n_inner), lax.rem(i + n_inner - 1, n_inner)
    _, m_all, nd, rows, _ = hw.shape
    nf = w1v.shape[0]
    units = nf // SLABS
    early = EARLY
    last = n_stage - 1
    half = nd // 2
    part = rows // MERGE
    groups = n_inner * early
    tokens = groups * rows
    ab, zb = narrow.at[0], narrow.at[1]

    barrier = pltpu.get_barrier_semaphore()
    for q in range(1, n_stage):
        pl.semaphore_signal(barrier, inc=1, device_id={"stage": lax.rem(p + q, n_stage)}, device_id_type=MESH)
    for q in (left, right):
        pl.semaphore_signal(barrier, inc=1, device_id={"inner": q}, device_id_type=MESH)

    loads = [
        pltpu.make_async_copy(w1.at[0, 0, :, c * LANES : (c + 1) * LANES], w1v.at[c], wsem.at[0]) for c in range(nf)
    ] + [pltpu.make_async_copy(w2.at[0, 0, :, c * LANES : (c + 1) * LANES], w2v.at[c], wsem.at[1]) for c in range(nd)]
    for c in loads:
        c.start()
    with jax.named_scope("barrier"):
        pl.semaphore_wait(barrier, n_stage + 1)

    def to_stage(src, dst, send, recv, stage):
        return pltpu.make_async_remote_copy(
            src_ref=src, dst_ref=dst, send_sem=send, recv_sem=recv,
            device_id={"stage": stage}, device_id_type=MESH,
        )

    def to_inner(src, dst, send, recv, inner):
        return pltpu.make_async_remote_copy(
            src_ref=src, dst_ref=dst, send_sem=send, recv_sem=recv,
            device_id={"inner": inner}, device_id_type=MESH,
        )

    def flat(ref, c):
        return ref.at[0, :, c * LANES : (c + 1) * LANES]

    def piece(e):
        return pl.ds(pl.multiple_of(e * part, part), part)

    def own(src, slots, recv, sem, stage):
        def to(c):
            return slots.at[i, p // MERGE, c, piece(p % MERGE)]

        @pl.when(p == stage)
        def _():
            for c in range(nd):
                pltpu.make_async_copy(flat(src, c), to(c), recv.at[p // MERGE]).start()

        @pl.when(p != stage)
        def _():
            for c in range(nd):
                to_stage(flat(src, c), to(c), sem, recv.at[p // MERGE], stage).start()

    own(x, hw, h_recv, xsem.at[0], 0)
    own(g, gw, g_recv, xsem.at[1], last)

    def ring_first(q, m, whole):
        a = whole.at[i, m]
        to_inner(a, a, ring_send.at[q, m, 0], ring_recv.at[q, m, 0], right).start()
        to_inner(a, a, ring_send.at[q, m, 1], ring_recv.at[q, m, 1], left).start()

    def ring_forward(q, m, whole):
        a, b = whole.at[left, m], whole.at[right, m]
        to_inner(a, a, ring_send.at[q, m, 0], ring_recv.at[q, m, 0], right).wait_recv()
        a = whole.at[left, m, pl.ds(0, half)]
        to_inner(a, a, ring_send.at[q, m, 2], ring_recv.at[q, m, 2], right).start()
        to_inner(b, b, ring_send.at[q, m, 1], ring_recv.at[q, m, 1], left).wait_recv()
        b = whole.at[right, m, pl.ds(half, half)]
        to_inner(b, b, ring_send.at[q, m, 3], ring_recv.at[q, m, 3], left).start()

    def ring_far(q, m, whole):
        far = lax.rem(i + 2, n_inner)
        a, b = whole.at[far, m, pl.ds(0, half)], whole.at[far, m, pl.ds(half, half)]
        return (
            to_inner(a, a, ring_send.at[q, m, 2], ring_recv.at[q, m, 2], right),
            to_inner(b, b, ring_send.at[q, m, 3], ring_recv.at[q, m, 3], left),
        )

    def ring_arrived(m, q):
        for c in ring_far(q, m, (hw, gw)[q]):
            c.wait_recv()

    def ring_sent(m):
        for q, whole in ((0, hw), (1, gw)):
            for c in ring_far(q, m, whole):
                c.wait_send()
            a = whole.at[i, m]
            to_inner(a, a, ring_send.at[q, m, 0], ring_recv.at[q, m, 0], right).wait_send()
            to_inner(a, a, ring_send.at[q, m, 1], ring_recv.at[q, m, 1], left).wait_send()

    def pass_on(m, src, slots, send, recv, end, nxt, out, out_sem):
        @pl.when(p != end)
        def _():
            to_stage(src.at[m], slots.at[i, m], send.at[m], recv.at[m], nxt).start()

        @pl.when(p == end)
        def _():
            for e in range(MERGE):
                home = m * MERGE + e

                @pl.when(p != home)
                def _():
                    for c in range(nd):
                        to_stage(src.at[m, c, piece(e)], flat(out, c), send.at[m], out_sem, home).start()

                @pl.when(p == home)
                def _():
                    for c in range(nd):
                        pltpu.make_async_copy(src.at[m, c, piece(e)], flat(out, c), out_sem).start()

    def project(m, res, w, src, *rest):
        u = _dot(_wide([act[c] for c in range(nf)]), _wide([w[c] for c in range(nd)]))
        out = (res.astype(F32) + u).astype(BF16)
        for c in range(nd):
            src[m, c] = _cut(out, c)
        pass_on(m, src, *rest)

    def forward(m, sloped):
        with jax.named_scope("wait_h"):
            pltpu.make_async_copy(hw.at[i, m], hw.at[i, m], h_recv.at[m]).wait()
        h = _wide([hw[i, m, c] for c in range(nd)])
        for b in range(0, nf, SLABS):
            z = _dot(h, _wide([w1v[b + c] for c in range(SLABS)]))
            a, slope = _gelu_and_slope(z)
            a, kept = a.astype(BF16), slope if sloped else z
            for c in range(SLABS):
                zs[m, b + c] = _cut(kept, c)
                act[b + c] = _cut(a, c)

        @pl.when((m == 0) & (p < n_stage // 2))
        def _():
            for c in loads[nf:]:
                c.wait()

        project(m, h, w2v, ho, hw, h_send, h_recv, last, jnp.minimum(p + 1, last), y, out_recv.at[0])

        @pl.when((p < n_stage - 2) | (m < early))
        def _():
            ring_first(0, m, hw)

    def backward(m):
        with jax.named_scope("wait_g"):
            pltpu.make_async_copy(gw.at[i, m], gw.at[i, m], g_recv.at[m]).wait()

        @pl.when(m < early)
        def _():
            ring_first(1, m, gw)

        dh = _wide([gw[i, m, c] for c in range(nd)])
        for b in range(0, nf, SLABS):
            da = _dot(dh, _wide([w2t[b + c] for c in range(SLABS)]))
            dz = (da * _wide([zs[m, b + c] for c in range(SLABS)])).astype(BF16)
            for c in range(SLABS):
                act[b + c] = _cut(dz, c)
        project(m, dh, w1t, go, gw, g_send, g_recv, 0, jnp.maximum(p - 1, 0), dx, out_recv.at[1])

        @pl.when((p >= n_stage - 2) & (m == early - 1))
        def _():
            ring_forward(0, 0, hw)

        @pl.when(m == early)
        def _():
            @pl.when(p >= n_stage - 2)
            def _():
                each(1, early, lambda e: ring_forward(0, e, hw))

            each(0, early - 1, lambda e: ring_forward(1, e, gw))

    def transpose_weights():
        def some(c, carry):
            s = pl.ds(pl.multiple_of(c * LANES, LANES), LANES)
            for e in range(nd):
                w1t[e, s, :] = w1v[c, e * LANES : (e + 1) * LANES, :].T
                w2t[c, e * LANES : (e + 1) * LANES, :] = w2v[e, s, :].T
            return carry

        lax.fori_loop(0, nf, some, 0)

    def slopes():
        def some(t, carry):
            m, b = t // (nf // SLABS), t % (nf // SLABS) * SLABS
            for c in range(SLABS):
                zs[m, b + c] = _gelu_and_slope(zs[m, b + c])[1]
            return carry

        lax.fori_loop(0, m_all * (nf // SLABS), some, 0)

    def each(lo, hi, fn):
        lax.fori_loop(lo, hi, lambda m, c: (fn(m), c)[1], 0)

    def group(whole, part=0):
        return lambda k, c: whole[k // early, part * early + k % early, c]

    def pre_stores(j):
        b = j % 2
        return (
            pltpu.make_async_copy(narrow.at[b], a_pre.at[j], pre_sem.at[0, b]),
            pltpu.make_async_copy(full.at[b, pl.ds(0, SLABS * groups)], s_pre.at[j], pre_sem.at[1, b]),
        )

    def pre_loads(j):
        b = j % 2
        return (
            pltpu.make_async_copy(
                a_pre.at[j], w2v.at[pl.ds(b * SLABS, SLABS), pl.ds(0, tokens)], pre_sem.at[0, b]
            ),
            pltpu.make_async_copy(s_pre.at[j], zs.at[b, pl.ds(0, SLABS * groups)], pre_sem.at[1, b]),
        )

    def pre_unit(j):
        b = j % 2

        @pl.when(j > 1)
        def _():
            for c in pre_stores(j):
                c.wait()

        for ks, s in _chunks(512, groups, rows):
            z = _dot(_rows_of(group(hw, j // units), ks, nd), _wide([w1v[j % units * SLABS + c] for c in range(SLABS)]))
            a, slope = _gelu_and_slope(z)
            a = a.astype(BF16)
            for c in range(SLABS):
                narrow[b, c, s, :] = _cut(a, c)
                for n, k in enumerate(ks):
                    full[b, c * groups + k] = _cut(slope[n * rows : (n + 1) * rows], c)
        for c in pre_stores(j):
            c.start()

    def part_copies(j):
        b, some = j % 2, pl.ds(0, SLABS * nd)
        return (
            pltpu.make_async_copy(full.at[b, some], d1_part.at[j], part_sem.at[0, b]),
            pltpu.make_async_copy(zs.at[m_all - 2 + b, some], d2_part.at[j], part_sem.at[1, b]),
        )

    def late_copies():
        return [
            pltpu.make_async_copy(whole.at[k, pl.ds(early, m_all - early)], out.at[k], late_sem.at[q, k])
            for q, (whole, out) in enumerate(((hw, h_late), (gw, g_late)))
            for k in range(n_inner)
        ]

    def sent(m):
        ring_sent(m)
        for src, slots, send, recv, end in ((ho, hw, h_send, h_recv, last), (go, gw, g_send, g_recv, 0)):
            for e in range(MERGE):
                a = src.at[m, :, piece(e)]

                @pl.when((p != end) | (p != m * MERGE + e))
                def _():
                    to_stage(a, a, send.at[m], recv.at[m], 0).wait_send()

        @pl.when((m == 0) & (p != 0))
        def _():
            to_stage(x.at[0], x.at[0], xsem.at[0], h_recv.at[0], 0).wait_send()

        @pl.when((m == 0) & (p != last))
        def _():
            to_stage(g.at[0], g.at[0], xsem.at[1], g_recv.at[0], last).wait_send()

    def unit(j):
        def forwards(m):
            @pl.when(p >= n_stage - 2)
            def _():
                ring_forward(0, m, hw)

            ring_forward(1, m, gw)

        def firsts(m):
            @pl.when(p >= n_stage - 2)
            def _():
                ring_first(0, m, hw)

            ring_first(1, m, gw)

        @pl.when(j == 0)
        def _():
            ring_forward(1, early - 1, gw)
            each(early, m_all, firsts)

            @pl.when(p < n_stage // 2)
            def _():
                for c in pre_loads(0):
                    c.start()

            each(0, early, lambda m: ring_arrived(m, 1))

            @pl.when(p >= n_stage // 2)
            def _():
                each(0, early, lambda m: ring_arrived(m, 0))

            _transposed_rows(group(hw), groups, rows, nd, ht)

        for m in range(early, m_all):
            @pl.when(j == min(units - 1, 2 * (m - early + 1)))
            def _():
                forwards(m)

        @pl.when(j == units - 1)
        def _():
            each(early, m_all, lambda m: ring_arrived(m, 1))

            @pl.when(p >= n_stage // 2)
            def _():
                each(early, m_all, lambda m: ring_arrived(m, 0))

            for c in late_copies():
                c.start()
            each(0, m_all, sent)

        def settle():
            @pl.when(j > 1)
            def _():
                for c in part_copies(j):
                    c.wait()

        def put(v1, v2):
            for c in range(SLABS):
                for e in range(nd):
                    zs[m_all - 2 + j % 2, c * nd + e] = _cut(v2[c * LANES : (c + 1) * LANES], e)
                    full[j % 2, c * nd + e] = _cut(v1[e * LANES : (e + 1) * LANES], c)

        def block(ready):
            _dw_block(
                256, group(hw), group(gw), groups, rows, nd,
                lambda: _wide([w1v[j * SLABS + c] for c in range(SLABS)]),
                lambda: _wide([w2t[j * SLABS + c] for c in range(SLABS)]),
                True, ht, ab, zb, settle, put, ready,
            )

        @pl.when(p < n_stage // 2)
        def _():
            b = j % 2
            for c in pre_loads(j):
                c.wait()

            @pl.when(j + 1 < units)
            def _():
                for c in pre_loads(j + 1):
                    c.start()

            block((
                lambda c: w2v[b * SLABS + c, 0:tokens, :],
                lambda k, c: zs[b, c * groups + k],
            ))

        @pl.when(p >= n_stage // 2)
        def _():
            block(None)

        for c in part_copies(j):
            c.start()

    with jax.named_scope("loads"):
        for c in loads[:nf]:
            c.wait()

    first = jnp.where(p == last, 1, m_all)
    rest = m_all - first
    turn = jnp.where(p < n_stage // 2, first, 0)

    def step(k, carry):
        j = k - first
        swap = j < 2 * rest
        is_u = k >= 2 * m_all
        is_f = (j < 0) | (swap & (j % 2 == 1))
        is_b = jnp.logical_not(is_f | is_u)
        m_f = jnp.where(j < 0, k, jnp.minimum(first + j // 2, m_all - 1))
        m_b = jnp.maximum(jnp.minimum(jnp.where(swap, j // 2, j - rest), m_all - 1), 0)
        u = jnp.maximum(k - 2 * m_all, 0)

        @pl.when(k == turn)
        def _():
            with jax.named_scope("transp"):
                @pl.when(p >= n_stage // 2)
                def _():
                    for c in loads[nf:]:
                        c.wait()

                transpose_weights()

        @pl.when((k == first) & (p < n_stage - 2))
        def _():
            with jax.named_scope("slopes"):
                slopes()
            with jax.named_scope("hring"):
                each(0, m_all, lambda m: ring_forward(0, m, hw))

        @pl.when((k == first) & (p < n_stage // 2))
        def _():
            with jax.named_scope("pre"):
                each(0, m_all, lambda m: ring_arrived(m, 0))
                each(0, jnp.where(p < PRE_LATE, 2, 1) * units, pre_unit)
                for c in (*pre_stores(units - 2), *pre_stores(units - 1)):
                    c.wait()

        @pl.when(is_f & (p < n_stage - 2))
        def _():
            with jax.named_scope("fwd"):
                forward(m_f, False)

        @pl.when(is_f & (p >= n_stage - 2))
        def _():
            with jax.named_scope("fwd"):
                forward(m_f, True)

        @pl.when(is_b)
        def _():
            with jax.named_scope("bwd"):
                backward(m_b)

        @pl.when(is_u)
        def _():
            with jax.named_scope("unit"):
                unit(u)

        return carry

    lax.fori_loop(0, 2 * m_all + units, step, 0)

    with jax.named_scope("finish"):
        for c in (*part_copies(units - 2), *part_copies(units - 1), *late_copies()):
            c.wait()
    with jax.named_scope("outwait"):
        pltpu.make_async_copy(y.at[0], y.at[0], out_recv.at[0]).wait()
        pltpu.make_async_copy(dx.at[0], dx.at[0], out_recv.at[1]).wait()


def _chain(n_stage, n_inner, x, g, w1, w2):
    mb, rows, d = x.shape
    f = w1.shape[-1]
    rows = rows * MERGE
    m_all = mb * n_stage // MERGE
    early = EARLY
    nd, nf = d // LANES, f // LANES
    blk = SLABS * LANES
    groups = n_inner * early
    tokens = groups * rows
    tiles = SLABS * max(nd, groups)
    hbm = pl.BlockSpec(memory_space=pltpu.HBM)
    whole = (n_inner, m_all, nd, rows, LANES)
    late = jax.ShapeDtypeStruct((n_inner, m_all - early, nd, rows, LANES), BF16)
    dma = pltpu.SemaphoreType.DMA
    vmem = pltpu.VMEM
    return pl.pallas_call(
        functools.partial(_chain_kernel, n_stage, n_inner),
        out_shape=[
            jax.ShapeDtypeStruct(x.shape, BF16), jax.ShapeDtypeStruct(x.shape, BF16), late, late,
            jax.ShapeDtypeStruct((f // blk, SLABS * nd, LANES, LANES), F32),
            jax.ShapeDtypeStruct((f // blk, SLABS * nd, LANES, LANES), F32),
            jax.ShapeDtypeStruct((2 * f // blk, SLABS, tokens, LANES), BF16),
            jax.ShapeDtypeStruct((2 * f // blk, SLABS * groups, rows, LANES), F32),
        ],
        in_specs=[hbm] * 4,
        out_specs=[hbm] * 8,
        scratch_shapes=[
            vmem((nf, d, LANES), BF16), vmem((nd, f, LANES), BF16),
            vmem((nd, f, LANES), BF16), vmem((nf, d, LANES), BF16),
            vmem(whole, BF16), vmem(whole, BF16),
            vmem((m_all, nd, rows, LANES), BF16), vmem((m_all, nd, rows, LANES), BF16),
            vmem((m_all, nf, rows, LANES), F32), vmem((nf, rows, LANES), BF16),
            vmem((tokens // LANES, d, LANES), BF16),
            vmem((2, SLABS, tokens, LANES), BF16), vmem((2, tiles, LANES, LANES), F32),
            dma((2,)), dma((2,)), dma((m_all,)), dma((m_all,)), dma((m_all,)), dma((m_all,)), dma((2,)),
            dma((2, m_all, 4)), dma((2, m_all, 4)), dma((2, 2)), dma((2, n_inner)), dma((2, 2)),
        ],
        compiler_params=pltpu.CompilerParams(
            collective_id=0, has_side_effects=True, vmem_limit_bytes=VMEM_LIMIT
        ),
        name="chain",
    )(x, g, w1, w2)


def _late_kernel(h, g, y_in, dx_in, w1_0, w1_1, w1_2, w1_3, *rest):
    nd = h.shape[1]
    w1 = (w1_0, w1_1, w1_2, w1_3)
    w2, (p1, p2, ap, sp, d1, d2, y, dx, ht, ab, zb) = rest[:nd], rest[nd:]
    groups, _, rows, _ = h.shape

    @pl.when(pl.program_id(0) == 0)
    def _():
        y[...] = y_in[...]
        dx[...] = dx_in[...]
        _transposed_rows(lambda k, c: h[k, c], groups, rows, nd, ht)

    def put(v1, v2):
        for c in range(SLABS):
            for e in range(nd):
                r, s = slice(e * LANES, (e + 1) * LANES), slice(c * LANES, (c + 1) * LANES)
                d1[r, s] = p1[0, c * nd + e] + v1[r, s]
                d2[s, r] = p2[0, c * nd + e] + v2[s, r]

    def block(ready):
        _dw_block(
            512, lambda k, c: h[k, c], lambda k, c: g[k, c], groups, rows, nd,
            lambda: _wide([w[...] for w in w1]), lambda: _wide([w[...] for w in w2]),
            False, ht, ab, zb, lambda: None, put, ready,
        )

    @pl.when(lax.axis_index("stage") < PRE_LATE)
    def _():
        block((lambda c: ap[0, c], lambda k, c: sp[0, c * groups + k]))

    @pl.when(lax.axis_index("stage") >= PRE_LATE)
    def _():
        block(None)


def _late(h, g, y, dx, w1, w2, p1, p2, ap, sp):
    groups, nd, rows, _ = h.shape
    d, f = w1.shape
    blk = SLABS * LANES
    t = groups * rows
    whole = pl.BlockSpec(h.shape, lambda j: (0, 0, 0, 0))
    mine = pl.BlockSpec(y.shape, lambda j: (0, 0, 0))
    return pl.pallas_call(
        _late_kernel,
        grid=(f // blk,),
        in_specs=[whole, whole, mine, mine]
        + [pl.BlockSpec((d, LANES), functools.partial(lambda c, j: (0, j * SLABS + c), c)) for c in range(SLABS)]
        + [pl.BlockSpec((blk, LANES), functools.partial(lambda c, j: (j, c), c)) for c in range(nd)]
        + [pl.BlockSpec((1, SLABS * nd, LANES, LANES), lambda j: (j, 0, 0, 0))] * 2
        + [pl.BlockSpec((1, *a.shape[1:]), lambda j: (j + f // blk, 0, 0, 0)) for a in (ap, sp)],
        out_specs=[pl.BlockSpec((d, blk), lambda j: (0, j)), pl.BlockSpec((blk, d), lambda j: (j, 0)), mine, mine],
        out_shape=[
            jax.ShapeDtypeStruct((d, f), F32), jax.ShapeDtypeStruct((f, d), F32),
            jax.ShapeDtypeStruct(y.shape, BF16), jax.ShapeDtypeStruct(dx.shape, BF16),
        ],
        scratch_shapes=[
            pltpu.VMEM((t // LANES, d, LANES), BF16),
            pltpu.VMEM((SLABS, t, LANES), BF16), pltpu.VMEM((SLABS, t, LANES), BF16),
        ],
        compiler_params=pltpu.CompilerParams(vmem_limit_bytes=VMEM_LIMIT),
        cost_estimate=pl.CostEstimate(flops=8 * t * d * f, bytes_accessed=20 * d * f, transcendentals=t * f),
        name="late",
    )(h, g, y, dx, *([w1] * SLABS), *([w2] * nd), p1, p2, ap, sp)


def solution(mesh):
    n_stage, n_inner = mesh.shape["stage"], mesh.shape["inner"]

    def body(x, g, w1, w2):
        d, f = w1.shape[-2:]
        y, dx, h, gg, *parts = _chain(n_stage, n_inner, x, g, w1, w2)
        flat = (-1, *h.shape[2:])
        d1, d2, y, dx = _late(h.reshape(flat), gg.reshape(flat), y, dx, w1.reshape(d, f), w2.reshape(f, d), *parts)
        return y, dx, d1.reshape(w1.shape), d2.reshape(w2.shape)

    tok = P(("data", "stage"), "inner", None)
    wsp = P(None, "stage", None, None)
    dsp = P("data", "stage", None, None)
    return jax.shard_map(body, mesh=mesh, in_specs=(tok, tok, wsp, wsp), out_specs=(tok, tok, dsp, dsp), check_vma=False)
```

```python
import functools

import jax
import jax.numpy as jnp
from jax import lax
from jax.experimental import pallas as pl
from jax.experimental.pallas import tpu as pltpu
from jax.sharding import PartitionSpec as P

MESH = pl.DeviceIdType.MESH
F32, BF16 = jnp.float32, jnp.bfloat16
C0, C1 = 0.7978845608028654, 0.044715
LANES = 128
VMEM_LIMIT = 67043328
SLABS = 4
MERGE = 2
EARLY = 2
PRE_LATE = 2


def _gelu_and_slope(z):
    z2 = z * z
    half = 0.5 * jnp.tanh(z * (C0 + (C0 * C1) * z2)) + 0.5
    a = z * half
    return a, half + (a - a * half) * (2.0 * C0 + (6.0 * C0 * C1) * z2)


def _dot(a, b):
    return jnp.dot(a, b, preferred_element_type=F32)


def _wide(slabs):
    return jnp.concatenate(slabs, axis=1)


def _tall(parts):
    return jnp.concatenate(parts, axis=0)


def _cut(value, c):
    return value[:, c * LANES : (c + 1) * LANES]


def _rows_of(read, ks, n):
    return _tall([_wide([read(k, c) for c in range(n)]) for k in ks])


def _chunks(rows, groups, group_rows):
    step = max(1, rows // group_rows)
    for k in range(0, groups, step):
        ks = range(k, min(k + step, groups))
        yield ks, slice(k * group_rows, (k + len(ks)) * group_rows)


def _dw_block(
    rows, hg, gg, groups, group_rows, nd, w1_block, w2t_block, ht, ab, zb, put, ready=None
):
    for ks, s in _chunks(rows, groups, group_rows):
        if ready is None:
            z = _dot(_rows_of(hg, ks, nd), w1_block())
        da = _dot(_rows_of(gg, ks, nd), w2t_block())
        if ready is None:
            a, slope = _gelu_and_slope(z)
            a = a.astype(BF16)
            for c in range(SLABS):
                ab[c, s, :] = _cut(a, c)
        else:
            slope = _rows_of(ready[1], ks, SLABS)
        dz = (da * slope).astype(BF16)
        for c in range(SLABS):
            zb[c, s, :] = _cut(dz, c)
    a = _wide([ab[c] for c in range(SLABS)] if ready is None else [ready[0](c) for c in range(SLABS)])
    v2 = lax.dot_general(
        a, _rows_of(gg, range(groups), nd), (((0,), (0,)), ((), ())), preferred_element_type=F32
    )
    put(_dot(_wide([ht[t] for t in range(ht.shape[0])]), _wide([zb[c] for c in range(SLABS)])), v2)


def _transposed_rows(hg, groups, group_rows, nd, ht):
    per = LANES // group_rows
    for t in range(groups // per):
        ht[t] = _tall([_wide([hg(t * per + e, c) for c in range(nd)]) for e in range(per)]).T


def _chain_kernel(
    n_stage, n_inner, x, g, w1, w2, y, dx, h_late, g_late, w1_out, w2_out, d1_part, d2_part, a_pre, s_pre,
    w1v, w2v, w1t, w2t, hw, gw, ho, go, zs, act, ht, narrow, full,
    wsem, xsem, h_recv, g_recv, h_send, g_send, out_recv, ring_send, ring_recv, part_sem, late_sem, pre_sem, keep_sem,
):
    p, i = lax.axis_index("stage"), lax.axis_index("inner")
    right, left = lax.rem(i + 1, n_inner), lax.rem(i + n_inner - 1, n_inner)
    _, m_all, nd, rows, _ = hw.shape
    nf = w1v.shape[0]
    units = nf // SLABS
    early = EARLY
    last = n_stage - 1
    half = nd // 2
    part = rows // MERGE
    groups = n_inner * early
    tokens = groups * rows
    ab, zb = narrow.at[0], narrow.at[1]

    barrier = pltpu.get_barrier_semaphore()
    for q in range(1, n_stage):
        pl.semaphore_signal(barrier, inc=1, device_id={"stage": lax.rem(p + q, n_stage)}, device_id_type=MESH)
    for q in (left, right):
        pl.semaphore_signal(barrier, inc=1, device_id={"inner": q}, device_id_type=MESH)

    loads = [
        pltpu.make_async_copy(w1.at[0, 0, :, c * LANES : (c + 1) * LANES], w1v.at[c], wsem.at[0]) for c in range(nf)
    ] + [pltpu.make_async_copy(w2.at[0, 0, :, c * LANES : (c + 1) * LANES], w2v.at[c], wsem.at[1]) for c in range(nd)]
    for c in loads:
        c.start()
    with jax.named_scope("barrier"):
        pl.semaphore_wait(barrier, n_stage + 1)

    def to_stage(src, dst, send, recv, stage):
        return pltpu.make_async_remote_copy(
            src_ref=src, dst_ref=dst, send_sem=send, recv_sem=recv,
            device_id={"stage": stage}, device_id_type=MESH,
        )

    def to_inner(src, dst, send, recv, inner):
        return pltpu.make_async_remote_copy(
            src_ref=src, dst_ref=dst, send_sem=send, recv_sem=recv,
            device_id={"inner": inner}, device_id_type=MESH,
        )

    def flat(ref, c):
        return ref.at[0, :, c * LANES : (c + 1) * LANES]

    def piece(e):
        return pl.ds(pl.multiple_of(e * part, part), part)

    def own(src, slots, recv, sem, stage):
        def to(c):
            return slots.at[i, p // MERGE, c, piece(p % MERGE)]

        @pl.when(p == stage)
        def _():
            for c in range(nd):
                pltpu.make_async_copy(flat(src, c), to(c), recv.at[p // MERGE]).start()

        @pl.when(p != stage)
        def _():
            for c in range(nd):
                to_stage(flat(src, c), to(c), sem, recv.at[p // MERGE], stage).start()

    own(x, hw, h_recv, xsem.at[0], 0)
    own(g, gw, g_recv, xsem.at[1], last)

    def ring_first(q, m, whole):
        a = whole.at[i, m]
        to_inner(a, a, ring_send.at[q, m, 0], ring_recv.at[q, m, 0], right).start()
        to_inner(a, a, ring_send.at[q, m, 1], ring_recv.at[q, m, 1], left).start()

    def ring_forward(q, m, whole):
        a, b = whole.at[left, m], whole.at[right, m]
        to_inner(a, a, ring_send.at[q, m, 0], ring_recv.at[q, m, 0], right).wait_recv()
        a = whole.at[left, m, pl.ds(0, half)]
        to_inner(a, a, ring_send.at[q, m, 2], ring_recv.at[q, m, 2], right).start()
        to_inner(b, b, ring_send.at[q, m, 1], ring_recv.at[q, m, 1], left).wait_recv()
        b = whole.at[right, m, pl.ds(half, half)]
        to_inner(b, b, ring_send.at[q, m, 3], ring_recv.at[q, m, 3], left).start()

    def ring_far(q, m, whole):
        far = lax.rem(i + 2, n_inner)
        a, b = whole.at[far, m, pl.ds(0, half)], whole.at[far, m, pl.ds(half, half)]
        return (
            to_inner(a, a, ring_send.at[q, m, 2], ring_recv.at[q, m, 2], right),
            to_inner(b, b, ring_send.at[q, m, 3], ring_recv.at[q, m, 3], left),
        )

    def ring_arrived(m, q):
        for c in ring_far(q, m, (hw, gw)[q]):
            c.wait_recv()

    def ring_sent(m):
        for q, whole in ((0, hw), (1, gw)):
            for c in ring_far(q, m, whole):
                c.wait_send()
            a = whole.at[i, m]
            to_inner(a, a, ring_send.at[q, m, 0], ring_recv.at[q, m, 0], right).wait_send()
            to_inner(a, a, ring_send.at[q, m, 1], ring_recv.at[q, m, 1], left).wait_send()

    def pass_on(m, src, slots, send, recv, end, nxt, out, out_sem):
        @pl.when(p != end)
        def _():
            to_stage(src.at[m], slots.at[i, m], send.at[m], recv.at[m], nxt).start()

        @pl.when(p == end)
        def _():
            for e in range(MERGE):
                home = m * MERGE + e

                @pl.when(p != home)
                def _():
                    for c in range(nd):
                        to_stage(src.at[m, c, piece(e)], flat(out, c), send.at[m], out_sem, home).start()

                @pl.when(p == home)
                def _():
                    for c in range(nd):
                        pltpu.make_async_copy(src.at[m, c, piece(e)], flat(out, c), out_sem).start()

    def project(m, res, w, src, *rest):
        u = _dot(_wide([act[c] for c in range(nf)]), _wide([w[c] for c in range(nd)]))
        out = (res.astype(F32) + u).astype(BF16)
        for c in range(nd):
            src[m, c] = _cut(out, c)
        pass_on(m, src, *rest)

    def forward(m, sloped):
        with jax.named_scope("wait_h"):
            pltpu.make_async_copy(hw.at[i, m], hw.at[i, m], h_recv.at[m]).wait()
        h = _wide([hw[i, m, c] for c in range(nd)])
        for b in range(0, nf, SLABS):
            z = _dot(h, _wide([w1v[b + c] for c in range(SLABS)]))
            a, slope = _gelu_and_slope(z)
            a, kept = a.astype(BF16), slope if sloped else z
            for c in range(SLABS):
                zs[m, b + c] = _cut(kept, c)
                act[b + c] = _cut(a, c)

        @pl.when((m == 0) & (p < n_stage // 2))
        def _():
            for c in loads[nf:]:
                c.wait()

        project(m, h, w2v, ho, hw, h_send, h_recv, last, jnp.minimum(p + 1, last), y, out_recv.at[0])

        @pl.when((p < n_stage - 2) | (m < early))
        def _():
            ring_first(0, m, hw)

    def backward(m):
        with jax.named_scope("wait_g"):
            pltpu.make_async_copy(gw.at[i, m], gw.at[i, m], g_recv.at[m]).wait()

        @pl.when(m < early)
        def _():
            ring_first(1, m, gw)

        dh = _wide([gw[i, m, c] for c in range(nd)])
        for b in range(0, nf, SLABS):
            da = _dot(dh, _wide([w2t[b + c] for c in range(SLABS)]))
            dz = (da * _wide([zs[m, b + c] for c in range(SLABS)])).astype(BF16)
            for c in range(SLABS):
                act[b + c] = _cut(dz, c)
        project(m, dh, w1t, go, gw, g_send, g_recv, 0, jnp.maximum(p - 1, 0), dx, out_recv.at[1])

        @pl.when(m == early)
        def _():
            @pl.when(p >= n_stage - 2)
            def _():
                ring_forward(0, 0, hw)

            @pl.when(p < n_stage - 2)
            def _():
                each(0, early - 1, lambda e: ring_forward(1, e, gw))

    def transpose_weights():
        def some(c, carry):
            s = pl.ds(pl.multiple_of(c * LANES, LANES), LANES)
            for e in range(nd):
                w1t[e, s, :] = w1v[c, e * LANES : (e + 1) * LANES, :].T
                w2t[c, e * LANES : (e + 1) * LANES, :] = w2v[e, s, :].T
            return carry

        lax.fori_loop(0, nf, some, 0)

    def slopes():
        def some(t, carry):
            m, b = t // (nf // SLABS), t % (nf // SLABS) * SLABS
            for c in range(SLABS):
                zs[m, b + c] = _gelu_and_slope(zs[m, b + c])[1]
            return carry

        lax.fori_loop(0, m_all * (nf // SLABS), some, 0)

    def each(lo, hi, fn):
        lax.fori_loop(lo, hi, lambda m, c: (fn(m), c)[1], 0)

    def group(whole, part=0):
        return lambda k, c: whole[k // early, part * early + k % early, c]

    def pre_stores(j):
        b = j % 2
        return (
            pltpu.make_async_copy(narrow.at[b], a_pre.at[j], pre_sem.at[0, b]),
            pltpu.make_async_copy(full.at[b, pl.ds(0, SLABS * groups)], s_pre.at[j], pre_sem.at[1, b]),
        )

    def pre_loads(j):
        b = j % 2
        return (
            pltpu.make_async_copy(
                a_pre.at[j], w2v.at[pl.ds(b * SLABS, SLABS), pl.ds(0, tokens)], pre_sem.at[0, b]
            ),
            pltpu.make_async_copy(s_pre.at[j], zs.at[b, pl.ds(0, SLABS * groups)], pre_sem.at[1, b]),
        )

    def pre_unit(j):
        b = j % 2

        @pl.when(j > 1)
        def _():
            for c in pre_stores(j):
                c.wait()

        for ks, s in _chunks(256, groups, rows):
            z = _dot(_rows_of(group(hw, j // units), ks, nd), _wide([w1v[j % units * SLABS + c] for c in range(SLABS)]))
            a, slope = _gelu_and_slope(z)
            a = a.astype(BF16)
            for c in range(SLABS):
                narrow[b, c, s, :] = _cut(a, c)
                for n, k in enumerate(ks):
                    full[b, c * groups + k] = _cut(slope[n * rows : (n + 1) * rows], c)
        for c in pre_stores(j):
            c.start()

    def part_copies(j):
        b, some = j % 2, pl.ds(0, SLABS * nd)
        return (
            pltpu.make_async_copy(full.at[b, some], d1_part.at[j], part_sem.at[0, b]),
            pltpu.make_async_copy(zs.at[m_all - 2 + b, some], d2_part.at[j], part_sem.at[1, b]),
        )

    def late_copies():
        return [
            pltpu.make_async_copy(whole.at[k, pl.ds(early, m_all - early)], out.at[k], late_sem.at[q, k])
            for q, (whole, out) in enumerate(((hw, h_late), (gw, g_late)))
            for k in range(n_inner)
        ]

    def sent(m):
        ring_sent(m)
        for src, slots, send, recv, end in ((ho, hw, h_send, h_recv, last), (go, gw, g_send, g_recv, 0)):
            for e in range(MERGE):
                a = src.at[m, :, piece(e)]

                @pl.when((p != end) | (p != m * MERGE + e))
                def _():
                    to_stage(a, a, send.at[m], recv.at[m], 0).wait_send()

        @pl.when((m == 0) & (p != 0))
        def _():
            to_stage(x.at[0], x.at[0], xsem.at[0], h_recv.at[0], 0).wait_send()

        @pl.when((m == 0) & (p != last))
        def _():
            to_stage(g.at[0], g.at[0], xsem.at[1], g_recv.at[0], last).wait_send()

    def unit(j):
        def forwards(m):
            @pl.when(p >= n_stage - 2)
            def _():
                ring_forward(0, m, hw)

            ring_forward(1, m, gw)

        def firsts(m):
            @pl.when(p >= n_stage - 2)
            def _():
                ring_first(0, m, hw)

            ring_first(1, m, gw)

        @pl.when(j == 0)
        def _():
            @pl.when(p >= n_stage - 2)
            def _():
                each(0, early - 1, lambda e: ring_forward(1, e, gw))
                each(1, early, lambda e: ring_forward(0, e, hw))

            ring_forward(1, early - 1, gw)
            each(early, m_all, firsts)

            @pl.when(p < n_stage // 2)
            def _():
                for c in pre_loads(0):
                    c.start()

            each(0, early, lambda m: ring_arrived(m, 1))

            @pl.when(p >= n_stage // 2)
            def _():
                each(0, early, lambda m: ring_arrived(m, 0))

            _transposed_rows(group(hw), groups, rows, nd, ht)

        for m in range(early, m_all):
            @pl.when(j == min(units - 1, 2 * (m - early + 1)))
            def _():
                forwards(m)

        @pl.when(j == units - 1)
        def _():
            each(early, m_all, lambda m: ring_arrived(m, 1))

            @pl.when(p >= n_stage // 2)
            def _():
                each(early, m_all, lambda m: ring_arrived(m, 0))

            for c in late_copies():
                c.start()
            each(0, m_all, sent)

        @pl.when(j > 1)
        def _():
            for c in part_copies(j):
                c.wait()

        def put(v1, v2):
            for c in range(SLABS):
                for e in range(nd):
                    zs[m_all - 2 + j % 2, c * nd + e] = _cut(v2[c * LANES : (c + 1) * LANES], e)
                    full[j % 2, c * nd + e] = _cut(v1[e * LANES : (e + 1) * LANES], c)

        def block(ready):
            _dw_block(
                512, group(hw), group(gw), groups, rows, nd,
                lambda: _wide([w1v[j * SLABS + c] for c in range(SLABS)]),
                lambda: _wide([w2t[j * SLABS + c] for c in range(SLABS)]),
                ht, ab, zb, put, ready,
            )

        @pl.when(p < n_stage // 2)
        def _():
            b = j % 2
            for c in pre_loads(j):
                c.wait()

            @pl.when(j + 1 < units)
            def _():
                for c in pre_loads(j + 1):
                    c.start()

            block((
                lambda c: w2v[b * SLABS + c, 0:tokens, :],
                lambda k, c: zs[b, c * groups + k],
            ))

        @pl.when(p >= n_stage // 2)
        def _():
            block(None)

        for c in part_copies(j):
            c.start()

    kept = (
        pltpu.make_async_copy(w1v, w1_out, keep_sem.at[0]), pltpu.make_async_copy(w2t, w2_out, keep_sem.at[1])
    )
    with jax.named_scope("loads"):
        for c in loads[:nf]:
            c.wait()

    first = jnp.where(p == last, 1, m_all)
    rest = m_all - first
    turn = jnp.where(p < n_stage // 2, first, 0)

    def step(k, carry):
        j = k - first
        swap = j < 2 * rest
        is_u = k >= 2 * m_all
        is_f = (j < 0) | (swap & (j % 2 == 1))
        is_b = jnp.logical_not(is_f | is_u)
        m_f = jnp.where(j < 0, k, jnp.minimum(first + j // 2, m_all - 1))
        m_b = jnp.maximum(jnp.minimum(jnp.where(swap, j // 2, j - rest), m_all - 1), 0)
        u = jnp.maximum(k - 2 * m_all, 0)

        @pl.when(k == turn)
        def _():
            with jax.named_scope("transp"):
                @pl.when(p >= n_stage // 2)
                def _():
                    for c in loads[nf:]:
                        c.wait()

                transpose_weights()
                for c in kept:
                    c.start()

        @pl.when((k == first) & (p < n_stage - 2))
        def _():
            with jax.named_scope("slopes"):
                slopes()
            with jax.named_scope("hring"):
                each(0, m_all, lambda m: ring_forward(0, m, hw))

        @pl.when((k == first) & (p < n_stage // 2))
        def _():
            with jax.named_scope("pre"):
                each(0, m_all, lambda m: ring_arrived(m, 0))
                each(0, jnp.where(p < PRE_LATE, 2, 1) * units, pre_unit)
                for c in (*pre_stores(units - 2), *pre_stores(units - 1)):
                    c.wait()

        @pl.when(is_f & (p < n_stage - 2))
        def _():
            with jax.named_scope("fwd"):
                forward(m_f, False)

        @pl.when(is_f & (p >= n_stage - 2))
        def _():
            with jax.named_scope("fwd"):
                forward(m_f, True)

        @pl.when(is_b)
        def _():
            with jax.named_scope("bwd"):
                backward(m_b)

        @pl.when(is_u)
        def _():
            with jax.named_scope("unit"):
                unit(u)

        return carry

    lax.fori_loop(0, 2 * m_all + units, step, 0)

    with jax.named_scope("finish"):
        for c in (*kept, *part_copies(units - 2), *part_copies(units - 1), *late_copies()):
            c.wait()
    with jax.named_scope("outwait"):
        pltpu.make_async_copy(y.at[0], y.at[0], out_recv.at[0]).wait()
        pltpu.make_async_copy(dx.at[0], dx.at[0], out_recv.at[1]).wait()


def _chain(n_stage, n_inner, x, g, w1, w2):
    mb, rows, d = x.shape
    f = w1.shape[-1]
    rows = rows * MERGE
    m_all = mb * n_stage // MERGE
    early = EARLY
    nd, nf = d // LANES, f // LANES
    blk = SLABS * LANES
    groups = n_inner * early
    tokens = groups * rows
    tiles = SLABS * max(nd, groups)
    hbm = pl.BlockSpec(memory_space=pltpu.HBM)
    whole = (n_inner, m_all, nd, rows, LANES)
    late = jax.ShapeDtypeStruct((n_inner, m_all - early, nd, rows, LANES), BF16)
    dma = pltpu.SemaphoreType.DMA
    vmem = pltpu.VMEM
    return pl.pallas_call(
        functools.partial(_chain_kernel, n_stage, n_inner),
        out_shape=[
            jax.ShapeDtypeStruct(x.shape, BF16), jax.ShapeDtypeStruct(x.shape, BF16), late, late,
            jax.ShapeDtypeStruct((nf, d, LANES), BF16), jax.ShapeDtypeStruct((nf, d, LANES), BF16),
            jax.ShapeDtypeStruct((f // blk, SLABS * nd, LANES, LANES), F32),
            jax.ShapeDtypeStruct((f // blk, SLABS * nd, LANES, LANES), F32),
            jax.ShapeDtypeStruct((2 * f // blk, SLABS, tokens, LANES), BF16),
            jax.ShapeDtypeStruct((2 * f // blk, SLABS * groups, rows, LANES), F32),
        ],
        in_specs=[hbm] * 4,
        out_specs=[hbm] * 10,
        scratch_shapes=[
            vmem((nf, d, LANES), BF16), vmem((nd, f, LANES), BF16),
            vmem((nd, f, LANES), BF16), vmem((nf, d, LANES), BF16),
            vmem(whole, BF16), vmem(whole, BF16),
            vmem((m_all, nd, rows, LANES), BF16), vmem((m_all, nd, rows, LANES), BF16),
            vmem((m_all, nf, rows, LANES), F32), vmem((nf, rows, LANES), BF16),
            vmem((tokens // LANES, d, LANES), BF16),
            vmem((2, SLABS, tokens, LANES), BF16), vmem((2, tiles, LANES, LANES), F32),
            dma((2,)), dma((2,)), dma((m_all,)), dma((m_all,)), dma((m_all,)), dma((m_all,)), dma((2,)),
            dma((2, m_all, 4)), dma((2, m_all, 4)), dma((2, 2)), dma((2, n_inner)), dma((2, 2)), dma((2,)),
        ],
        compiler_params=pltpu.CompilerParams(
            collective_id=0, has_side_effects=True, vmem_limit_bytes=VMEM_LIMIT
        ),
        name="chain",
    )(x, g, w1, w2)


def _late_kernel(
    h, g, y_in, dx_in, w1, w2t, p1, p2, ap, sp, d1, d2, y, dx,
    hv, gv, w1v, w2v, p1v, p2v, av, sv, d1v, d2v, ht, ab, zb, yv, first_sem, load_sem, store_sem, pass_sem,
):
    groups, nd, rows, _ = h.shape
    units = w1.shape[0] // SLABS
    d, blk = d1v.shape[1:]
    pre = lax.axis_index("stage") < PRE_LATE

    def weights(j):
        b, some = j % 2, pl.ds(j * SLABS, SLABS)
        return (pltpu.make_async_copy(w2t.at[some], w2v.at[b], load_sem.at[0, b]),)

    def own(j):
        b, some = j % 2, pl.ds(j * SLABS, SLABS)
        return (pltpu.make_async_copy(w1.at[some], w1v.at[b], load_sem.at[1, b]),)

    def ready(j):
        b = j % 2
        return (
            pltpu.make_async_copy(ap.at[units + j], av.at[b], load_sem.at[1, b]),
            pltpu.make_async_copy(sp.at[units + j], sv.at[b], load_sem.at[2, b]),
        )

    def parts(j):
        b = j % 2
        return (
            pltpu.make_async_copy(p1.at[j], p1v.at[b], load_sem.at[3, b]),
            pltpu.make_async_copy(p2.at[j], p2v.at[b], load_sem.at[4, b]),
        )

    def stores(j):
        b, some = j % 2, pl.ds(pl.multiple_of(j * blk, blk), blk)
        return (
            pltpu.make_async_copy(d1v.at[b], d1.at[:, some], store_sem.at[0, b]),
            pltpu.make_async_copy(d2v.at[b], d2.at[some, :], store_sem.at[1, b]),
        )

    def do(copies, how):
        for c in copies:
            getattr(c, how)()

    def inputs(j, how):
        @pl.when(pre)
        def _():
            do(ready(j), how)

        @pl.when(jnp.logical_not(pre))
        def _():
            do(own(j), how)

        do(weights(j), how)

    firsts = (pltpu.make_async_copy(h, hv, first_sem.at[0]), pltpu.make_async_copy(g, gv, first_sem.at[1]))
    firsts[0].start()
    inputs(0, "start")
    firsts[1].start()
    do(parts(0), "start")
    into = [pltpu.make_async_copy(a, yv.at[n], pass_sem.at[n]) for n, a in enumerate((y_in, dx_in))]
    out_of = [pltpu.make_async_copy(yv.at[n], a, pass_sem.at[n]) for n, a in enumerate((y, dx))]
    do(into, "start")
    firsts[0].wait()
    _transposed_rows(lambda k, c: hv[k, c], groups, rows, nd, ht)
    do(into, "wait")
    do(out_of, "start")

    def unit(j, carry):
        b = j % 2
        inputs(j, "wait")

        @pl.when(j == 0)
        def _():
            firsts[1].wait()

        @pl.when(j + 1 < units)
        def _():
            inputs(j + 1, "start")
            do(parts(j + 1), "start")

        do(parts(j), "wait")

        @pl.when(j > 1)
        def _():
            do(stores(j), "wait")

        def put(v1, v2):
            for c in range(SLABS):
                for e in range(nd):
                    r, s = slice(e * LANES, (e + 1) * LANES), slice(c * LANES, (c + 1) * LANES)
                    d2v[b, s, r] = p2v[b, c * nd + e] + v2[s, r]
                    d1v[b, r, s] = p1v[b, c * nd + e] + v1[r, s]

        def block(ready):
            _dw_block(
                512, lambda k, c: hv[k, c], lambda k, c: gv[k, c], groups, rows, nd,
                lambda: _wide([w1v[b, c] for c in range(SLABS)]), lambda: _wide([w2v[b, c] for c in range(SLABS)]),
                ht, ab, zb, put, ready,
            )

        @pl.when(pre)
        def _():
            block((lambda c: av[b, c], lambda k, c: sv[b, c * groups + k]))

        @pl.when(jnp.logical_not(pre))
        def _():
            block(None)

        do(stores(j), "start")
        return carry

    lax.fori_loop(0, units, unit, 0)
    do(stores(units - 2), "wait")
    do(stores(units - 1), "wait")
    do(out_of, "wait")


def _late(h, g, y, dx, w1, w2t, p1, p2, ap, sp):
    groups, nd, rows, _ = h.shape
    nf, d, _ = w1.shape
    f, blk, t = nf * LANES, SLABS * LANES, groups * rows
    hbm = pl.BlockSpec(memory_space=pltpu.HBM)
    vmem, dma = pltpu.VMEM, pltpu.SemaphoreType.DMA
    return pl.pallas_call(
        _late_kernel,
        in_specs=[hbm] * 10,
        out_specs=[hbm] * 4,
        out_shape=[
            jax.ShapeDtypeStruct((d, f), F32), jax.ShapeDtypeStruct((f, d), F32),
            jax.ShapeDtypeStruct(y.shape, BF16), jax.ShapeDtypeStruct(dx.shape, BF16),
        ],
        scratch_shapes=[
            vmem(h.shape, BF16), vmem(g.shape, BF16),
            vmem((2, SLABS, d, LANES), BF16), vmem((2, SLABS, d, LANES), BF16),
            vmem((2, *p1.shape[1:]), F32), vmem((2, *p2.shape[1:]), F32),
            vmem((2, *ap.shape[1:]), BF16), vmem((2, *sp.shape[1:]), F32),
            vmem((2, d, blk), F32), vmem((2, blk, d), F32),
            vmem((t // LANES, d, LANES), BF16), vmem((SLABS, t, LANES), BF16), vmem((SLABS, t, LANES), BF16),
            vmem((2, *y.shape), BF16),
            dma((2,)), dma((5, 2)), dma((2, 2)), dma((2,)),
        ],
        compiler_params=pltpu.CompilerParams(vmem_limit_bytes=VMEM_LIMIT),
        cost_estimate=pl.CostEstimate(flops=8 * t * d * f, bytes_accessed=20 * d * f, transcendentals=t * f),
        name="late",
    )(h, g, y, dx, w1, w2t, p1, p2, ap, sp)


def solution(mesh):
    n_stage, n_inner = mesh.shape["stage"], mesh.shape["inner"]

    def body(x, g, w1, w2):
        y, dx, h, gg, w1s, w2s, *parts = _chain(n_stage, n_inner, x, g, w1, w2)
        flat = (-1, *h.shape[2:])
        d1, d2, y, dx = _late(h.reshape(flat), gg.reshape(flat), y, dx, w1s, w2s, *parts)
        return y, dx, d1.reshape(w1.shape), d2.reshape(w2.shape)

    tok = P(("data", "stage"), "inner", None)
    wsp = P(None, "stage", None, None)
    dsp = P("data", "stage", None, None)
    return jax.shard_map(body, mesh=mesh, in_specs=(tok, tok, wsp, wsp), out_specs=(tok, tok, dsp, dsp), check_vma=False)
```

```python
import functools

import jax
import jax.numpy as jnp
from jax import lax
from jax.experimental import pallas as pl
from jax.experimental.pallas import tpu as pltpu
from jax.sharding import PartitionSpec as P

MESH = pl.DeviceIdType.MESH
F32, BF16 = jnp.float32, jnp.bfloat16
C0, C1 = 0.7978845608028654, 0.044715
LANES = 128
VMEM_LIMIT = 67043328
SLABS = 4
MERGE = 2
EARLY = 2
PRE_LATE = 2


def _gelu_and_slope(z):
    z2 = z * z
    half = 0.5 * jnp.tanh(z * (C0 + (C0 * C1) * z2)) + 0.5
    a = z * half
    return a, half + (a - a * half) * (2.0 * C0 + (6.0 * C0 * C1) * z2)


def _dot(a, b):
    return jnp.dot(a, b, preferred_element_type=F32)


def _wide(slabs):
    return jnp.concatenate(slabs, axis=1)


def _tall(parts):
    return jnp.concatenate(parts, axis=0)


def _cut(value, c):
    return value[:, c * LANES : (c + 1) * LANES]


def _rows_of(read, ks, n):
    return _tall([_wide([read(k, c) for c in range(n)]) for k in ks])


def _chunks(rows, groups, group_rows):
    step = max(1, rows // group_rows)
    for k in range(0, groups, step):
        ks = range(k, min(k + step, groups))
        yield ks, slice(k * group_rows, (k + len(ks)) * group_rows)


def _dw_block(
    rows, hg, gg, groups, group_rows, nd, w1_block, w2t_block, ht, ab, zb, put, ready=None
):
    for ks, s in _chunks(rows, groups, group_rows):
        if ready is None:
            z = _dot(_rows_of(hg, ks, nd), w1_block())
        da = _dot(_rows_of(gg, ks, nd), w2t_block())
        if ready is None:
            a, slope = _gelu_and_slope(z)
            a = a.astype(BF16)
            for c in range(SLABS):
                ab[c, s, :] = _cut(a, c)
        else:
            slope = _rows_of(ready[1], ks, SLABS)
        dz = (da * slope).astype(BF16)
        for c in range(SLABS):
            zb[c, s, :] = _cut(dz, c)
    a = _wide([ab[c] for c in range(SLABS)] if ready is None else [ready[0](c) for c in range(SLABS)])
    v2 = lax.dot_general(
        a, _rows_of(gg, range(groups), nd), (((0,), (0,)), ((), ())), preferred_element_type=F32
    )
    put(_dot(_wide([ht[t] for t in range(ht.shape[0])]), _wide([zb[c] for c in range(SLABS)])), v2)


def _transposed_rows(hg, groups, group_rows, nd, ht):
    per = LANES // group_rows
    for t in range(groups // per):
        ht[t] = _tall([_wide([hg(t * per + e, c) for c in range(nd)]) for e in range(per)]).T


def _chain_kernel(
    n_stage, n_inner, x, g, w1, w2, y, dx, h_late, g_late, w1_out, w2_out, d1_part, d2_part, a_pre, s_pre,
    w1v, w2v, w1t, w2t, hw, gw, ho, go, zs, act, ht, narrow, full,
    wsem, xsem, h_recv, g_recv, h_send, g_send, out_recv, ring_send, ring_recv, part_sem, late_sem, pre_sem, keep_sem,
):
    p, i = lax.axis_index("stage"), lax.axis_index("inner")
    right, left = lax.rem(i + 1, n_inner), lax.rem(i + n_inner - 1, n_inner)
    _, m_all, nd, rows, _ = hw.shape
    nf = w1v.shape[0]
    units = nf // SLABS
    early = EARLY
    last = n_stage - 1
    half = nd // 2
    part = rows // MERGE
    groups = n_inner * early
    tokens = groups * rows
    ab, zb = narrow.at[0], narrow.at[1]

    barrier = pltpu.get_barrier_semaphore()
    for q in range(1, n_stage):
        pl.semaphore_signal(barrier, inc=1, device_id={"stage": lax.rem(p + q, n_stage)}, device_id_type=MESH)
    for q in (left, right):
        pl.semaphore_signal(barrier, inc=1, device_id={"inner": q}, device_id_type=MESH)

    loads = [
        pltpu.make_async_copy(w1.at[0, 0, :, c * LANES : (c + 1) * LANES], w1v.at[c], wsem.at[0]) for c in range(nf)
    ] + [pltpu.make_async_copy(w2.at[0, 0, :, c * LANES : (c + 1) * LANES], w2v.at[c], wsem.at[1]) for c in range(nd)]
    for c in loads:
        c.start()
    with jax.named_scope("barrier"):
        pl.semaphore_wait(barrier, n_stage + 1)

    def to_stage(src, dst, send, recv, stage):
        return pltpu.make_async_remote_copy(
            src_ref=src, dst_ref=dst, send_sem=send, recv_sem=recv,
            device_id={"stage": stage}, device_id_type=MESH,
        )

    def to_inner(src, dst, send, recv, inner):
        return pltpu.make_async_remote_copy(
            src_ref=src, dst_ref=dst, send_sem=send, recv_sem=recv,
            device_id={"inner": inner}, device_id_type=MESH,
        )

    def flat(ref, c):
        return ref.at[0, :, c * LANES : (c + 1) * LANES]

    def piece(e):
        return pl.ds(pl.multiple_of(e * part, part), part)

    def own(src, slots, recv, sem, stage):
        def to(c):
            return slots.at[i, p // MERGE, c, piece(p % MERGE)]

        @pl.when(p == stage)
        def _():
            for c in range(nd):
                pltpu.make_async_copy(flat(src, c), to(c), recv.at[p // MERGE]).start()

        @pl.when(p != stage)
        def _():
            for c in range(nd):
                to_stage(flat(src, c), to(c), sem, recv.at[p // MERGE], stage).start()

    own(x, hw, h_recv, xsem.at[0], 0)
    own(g, gw, g_recv, xsem.at[1], last)

    def ring_first(q, m, whole):
        a = whole.at[i, m]
        to_inner(a, a, ring_send.at[q, m, 0], ring_recv.at[q, m, 0], right).start()
        to_inner(a, a, ring_send.at[q, m, 1], ring_recv.at[q, m, 1], left).start()

    def ring_forward(q, m, whole):
        a, b = whole.at[left, m], whole.at[right, m]
        to_inner(a, a, ring_send.at[q, m, 0], ring_recv.at[q, m, 0], right).wait_recv()
        a = whole.at[left, m, pl.ds(0, half)]
        to_inner(a, a, ring_send.at[q, m, 2], ring_recv.at[q, m, 2], right).start()
        to_inner(b, b, ring_send.at[q, m, 1], ring_recv.at[q, m, 1], left).wait_recv()
        b = whole.at[right, m, pl.ds(half, half)]
        to_inner(b, b, ring_send.at[q, m, 3], ring_recv.at[q, m, 3], left).start()

    def ring_far(q, m, whole):
        far = lax.rem(i + 2, n_inner)
        a, b = whole.at[far, m, pl.ds(0, half)], whole.at[far, m, pl.ds(half, half)]
        return (
            to_inner(a, a, ring_send.at[q, m, 2], ring_recv.at[q, m, 2], right),
            to_inner(b, b, ring_send.at[q, m, 3], ring_recv.at[q, m, 3], left),
        )

    def ring_arrived(m, q):
        for c in ring_far(q, m, (hw, gw)[q]):
            c.wait_recv()

    def ring_sent(m):
        for q, whole in ((0, hw), (1, gw)):
            for c in ring_far(q, m, whole):
                c.wait_send()
            a = whole.at[i, m]
            to_inner(a, a, ring_send.at[q, m, 0], ring_recv.at[q, m, 0], right).wait_send()
            to_inner(a, a, ring_send.at[q, m, 1], ring_recv.at[q, m, 1], left).wait_send()

    def pass_on(m, lo, hi, src, slots, send, recv, end, nxt, out, out_sem):
        @pl.when(p != end)
        def _():
            some = pl.ds(lo, hi - lo)
            to_stage(src.at[m, some], slots.at[i, m, some], send.at[m], recv.at[m], nxt).start()

        if hi - lo < nd:
            return

        @pl.when(p == end)
        def _():
            for e in range(MERGE):
                home = m * MERGE + e

                @pl.when(p != home)
                def _():
                    for c in range(nd):
                        to_stage(src.at[m, c, piece(e)], flat(out, c), send.at[m], out_sem, home).start()

                @pl.when(p == home)
                def _():
                    for c in range(nd):
                        pltpu.make_async_copy(src.at[m, c, piece(e)], flat(out, c), out_sem).start()

    def project(m, split, res, w, src, *rest):
        whole = _wide([act[c] for c in range(nf)])
        count = half if split else nd
        for lo in range(0, nd, count):
            u = _dot(whole, _wide([w[lo + c] for c in range(count)]))
            out = (res[:, lo * LANES : (lo + count) * LANES].astype(F32) + u).astype(BF16)
            for c in range(count):
                src[m, lo + c] = _cut(out, c)
            pass_on(m, lo, lo + count, src, *rest)

    def forward(m, sloped, split):
        with jax.named_scope("wait_h"):
            pltpu.make_async_copy(hw.at[i, m], hw.at[i, m], h_recv.at[m]).wait()
        h = _wide([hw[i, m, c] for c in range(nd)])
        for b in range(0, nf, SLABS):
            z = _dot(h, _wide([w1v[b + c] for c in range(SLABS)]))
            a, slope = _gelu_and_slope(z)
            a, kept = a.astype(BF16), slope if sloped else z
            for c in range(SLABS):
                zs[m, b + c] = _cut(kept, c)
                act[b + c] = _cut(a, c)

        @pl.when((m == 0) & (p < n_stage // 2))
        def _():
            for c in loads[nf:]:
                c.wait()

        project(m, split, h, w2v, ho, hw, h_send, h_recv, last, jnp.minimum(p + 1, last), y, out_recv.at[0])

        @pl.when((p < n_stage - 2) | (m < early))
        def _():
            ring_first(0, m, hw)

    def backward(m, split):
        @pl.when((p < n_stage - 2) & (m == early + 1))
        def _():
            ring_forward(1, early - 1, gw)

        with jax.named_scope("wait_g"):
            pltpu.make_async_copy(gw.at[i, m], gw.at[i, m], g_recv.at[m]).wait()

        @pl.when(m < early)
        def _():
            ring_first(1, m, gw)

        dh = _wide([gw[i, m, c] for c in range(nd)])
        for b in range(0, nf, SLABS):
            da = _dot(dh, _wide([w2t[b + c] for c in range(SLABS)]))
            dz = (da * _wide([zs[m, b + c] for c in range(SLABS)])).astype(BF16)
            for c in range(SLABS):
                act[b + c] = _cut(dz, c)
        project(m, split, dh, w1t, go, gw, g_send, g_recv, 0, jnp.maximum(p - 1, 0), dx, out_recv.at[1])

        @pl.when(m == early)
        def _():
            @pl.when(p >= n_stage - 2)
            def _():
                ring_forward(0, 0, hw)

            @pl.when(p < n_stage - 2)
            def _():
                each(0, early - 1, lambda e: ring_forward(1, e, gw))

    def transpose_weights():
        def some(c, carry):
            s = pl.ds(pl.multiple_of(c * LANES, LANES), LANES)
            for e in range(nd):
                w1t[e, s, :] = w1v[c, e * LANES : (e + 1) * LANES, :].T
                w2t[c, e * LANES : (e + 1) * LANES, :] = w2v[e, s, :].T
            return carry

        lax.fori_loop(0, nf, some, 0)

    def slopes():
        def some(t, carry):
            m, b = t // (nf // SLABS), t % (nf // SLABS) * SLABS
            for c in range(SLABS):
                zs[m, b + c] = _gelu_and_slope(zs[m, b + c])[1]
            return carry

        lax.fori_loop(0, m_all * (nf // SLABS), some, 0)

    def each(lo, hi, fn):
        lax.fori_loop(lo, hi, lambda m, c: (fn(m), c)[1], 0)

    def group(whole, part=0):
        return lambda k, c: whole[k // early, part * early + k % early, c]

    def pre_stores(j):
        b = j % 2
        return (
            pltpu.make_async_copy(narrow.at[b], a_pre.at[j], pre_sem.at[0, b]),
            pltpu.make_async_copy(full.at[b, pl.ds(0, SLABS * groups)], s_pre.at[j], pre_sem.at[1, b]),
        )

    def pre_loads(j):
        b = j % 2
        return (
            pltpu.make_async_copy(
                a_pre.at[j], w2v.at[pl.ds(b * SLABS, SLABS), pl.ds(0, tokens)], pre_sem.at[0, b]
            ),
            pltpu.make_async_copy(s_pre.at[j], zs.at[b, pl.ds(0, SLABS * groups)], pre_sem.at[1, b]),
        )

    def pre_unit(j):
        b = j % 2

        @pl.when(j > 1)
        def _():
            for c in pre_stores(j):
                c.wait()

        for ks, s in _chunks(256, groups, rows):
            z = _dot(_rows_of(group(hw, j // units), ks, nd), _wide([w1v[j % units * SLABS + c] for c in range(SLABS)]))
            a, slope = _gelu_and_slope(z)
            a = a.astype(BF16)
            for c in range(SLABS):
                narrow[b, c, s, :] = _cut(a, c)
                for n, k in enumerate(ks):
                    full[b, c * groups + k] = _cut(slope[n * rows : (n + 1) * rows], c)
        for c in pre_stores(j):
            c.start()

    def part_copies(j):
        b, some = j % 2, pl.ds(0, SLABS * nd)
        return (
            pltpu.make_async_copy(full.at[b, some], d1_part.at[j], part_sem.at[0, b]),
            pltpu.make_async_copy(zs.at[m_all - 2 + b, some], d2_part.at[j], part_sem.at[1, b]),
        )

    def late_copies():
        return [
            pltpu.make_async_copy(whole.at[k, pl.ds(early, m_all - early)], out.at[k], late_sem.at[q, k])
            for q, (whole, out) in enumerate(((hw, h_late), (gw, g_late)))
            for k in range(n_inner)
        ]

    def sent(m):
        ring_sent(m)
        for src, slots, send, recv, end in ((ho, hw, h_send, h_recv, last), (go, gw, g_send, g_recv, 0)):
            for e in range(MERGE):
                a = src.at[m, :, piece(e)]

                @pl.when((p != end) | (p != m * MERGE + e))
                def _():
                    to_stage(a, a, send.at[m], recv.at[m], 0).wait_send()

        @pl.when((m == 0) & (p != 0))
        def _():
            to_stage(x.at[0], x.at[0], xsem.at[0], h_recv.at[0], 0).wait_send()

        @pl.when((m == 0) & (p != last))
        def _():
            to_stage(g.at[0], g.at[0], xsem.at[1], g_recv.at[0], last).wait_send()

    def unit(j):
        def forwards(m):
            @pl.when(p >= n_stage - 2)
            def _():
                ring_forward(0, m, hw)

            ring_forward(1, m, gw)

        def firsts(m):
            @pl.when(p >= n_stage - 2)
            def _():
                ring_first(0, m, hw)

            ring_first(1, m, gw)

        @pl.when(j == 0)
        def _():
            @pl.when(p >= n_stage - 2)
            def _():
                each(0, early, lambda e: ring_forward(1, e, gw))
                each(1, early, lambda e: ring_forward(0, e, hw))


            @pl.when(p < n_stage // 2)
            def _():
                for c in pre_loads(0):
                    c.start()

            each(0, early, lambda m: ring_arrived(m, 1))

            @pl.when(p >= n_stage // 2)
            def _():
                each(0, early, lambda m: ring_arrived(m, 0))

            each(early, m_all, firsts)
            _transposed_rows(group(hw), groups, rows, nd, ht)

        for m in range(early, m_all):
            @pl.when(j == jnp.where(p < n_stage - 2, 2, 3) * (m - early + 1))
            def _():
                forwards(m)

        @pl.when(j == units - 1)
        def _():
            each(early, m_all, lambda m: ring_arrived(m, 1))

            @pl.when(p >= n_stage // 2)
            def _():
                each(early, m_all, lambda m: ring_arrived(m, 0))

            for c in late_copies():
                c.start()
            each(0, m_all, sent)

        @pl.when(j > 1)
        def _():
            for c in part_copies(j):
                c.wait()

        def put(v1, v2):
            for c in range(SLABS):
                for e in range(nd):
                    zs[m_all - 2 + j % 2, c * nd + e] = _cut(v2[c * LANES : (c + 1) * LANES], e)
                    full[j % 2, c * nd + e] = _cut(v1[e * LANES : (e + 1) * LANES], c)

        def block(ready):
            _dw_block(
                512, group(hw), group(gw), groups, rows, nd,
                lambda: _wide([w1v[j * SLABS + c] for c in range(SLABS)]),
                lambda: _wide([w2t[j * SLABS + c] for c in range(SLABS)]),
                ht, ab, zb, put, ready,
            )

        @pl.when(p < n_stage // 2)
        def _():
            b = j % 2
            for c in pre_loads(j):
                c.wait()

            @pl.when(j + 1 < units)
            def _():
                for c in pre_loads(j + 1):
                    c.start()

            block((
                lambda c: w2v[b * SLABS + c, 0:tokens, :],
                lambda k, c: zs[b, c * groups + k],
            ))

        @pl.when(p >= n_stage // 2)
        def _():
            block(None)

        for c in part_copies(j):
            c.start()

    kept = (
        pltpu.make_async_copy(w1v, w1_out, keep_sem.at[0]), pltpu.make_async_copy(w2t, w2_out, keep_sem.at[1])
    )
    with jax.named_scope("loads"):
        for c in loads[:nf]:
            c.wait()

    first = jnp.where(p == last, 1, m_all)
    rest = m_all - first
    turn = jnp.where(p < n_stage // 2, first, 0)

    def step(k, carry):
        j = k - first
        swap = j < 2 * rest
        is_u = k >= 2 * m_all
        is_f = (j < 0) | (swap & (j % 2 == 1))
        is_b = jnp.logical_not(is_f | is_u)
        m_f = jnp.where(j < 0, k, jnp.minimum(first + j // 2, m_all - 1))
        m_b = jnp.maximum(jnp.minimum(jnp.where(swap, j // 2, j - rest), m_all - 1), 0)
        u = jnp.maximum(k - 2 * m_all, 0)

        @pl.when(k == turn)
        def _():
            with jax.named_scope("transp"):
                @pl.when(p >= n_stage // 2)
                def _():
                    for c in loads[nf:]:
                        c.wait()

                transpose_weights()
                for c in kept:
                    c.start()

        @pl.when((k == first) & (p < n_stage - 2))
        def _():
            with jax.named_scope("slopes"):
                slopes()
            with jax.named_scope("hring"):
                each(0, m_all, lambda m: ring_forward(0, m, hw))

        @pl.when((k == first) & (p < n_stage // 2))
        def _():
            with jax.named_scope("pre"):
                each(0, m_all, lambda m: ring_arrived(m, 0))
                each(0, jnp.where(p < PRE_LATE, 2, 1) * units, pre_unit)
                for c in (*pre_stores(units - 2), *pre_stores(units - 1)):
                    c.wait()

        early_f, odd = is_f & (p < n_stage - 2), p % 2 == 1
        for when, sloped, split in (
            (early_f & jnp.logical_not(odd), False, False),
            (early_f & odd, False, True),
            (is_f & (p >= n_stage - 2), True, False),
        ):
            @pl.when(when)
            def _():
                with jax.named_scope("fwd"):
                    forward(m_f, sloped, split)

        leaves = (p > 0) & jnp.logical_not(odd)
        for when, split in ((is_b & leaves, True), (is_b & jnp.logical_not(leaves), False)):
            @pl.when(when)
            def _():
                with jax.named_scope("bwd"):
                    backward(m_b, split)

        @pl.when(is_u)
        def _():
            with jax.named_scope("unit"):
                unit(u)

        return carry

    lax.fori_loop(0, 2 * m_all + units, step, 0)

    with jax.named_scope("finish"):
        for c in (*kept, *part_copies(units - 2), *part_copies(units - 1), *late_copies()):
            c.wait()
    with jax.named_scope("outwait"):
        pltpu.make_async_copy(y.at[0], y.at[0], out_recv.at[0]).wait()
        pltpu.make_async_copy(dx.at[0], dx.at[0], out_recv.at[1]).wait()


def _chain(n_stage, n_inner, x, g, w1, w2):
    mb, rows, d = x.shape
    f = w1.shape[-1]
    rows = rows * MERGE
    m_all = mb * n_stage // MERGE
    early = EARLY
    nd, nf = d // LANES, f // LANES
    blk = SLABS * LANES
    groups = n_inner * early
    tokens = groups * rows
    tiles = SLABS * max(nd, groups)
    hbm = pl.BlockSpec(memory_space=pltpu.HBM)
    whole = (n_inner, m_all, nd, rows, LANES)
    late = jax.ShapeDtypeStruct((n_inner, m_all - early, nd, rows, LANES), BF16)
    dma = pltpu.SemaphoreType.DMA
    vmem = pltpu.VMEM
    return pl.pallas_call(
        functools.partial(_chain_kernel, n_stage, n_inner),
        out_shape=[
            jax.ShapeDtypeStruct(x.shape, BF16), jax.ShapeDtypeStruct(x.shape, BF16), late, late,
            jax.ShapeDtypeStruct((nf, d, LANES), BF16), jax.ShapeDtypeStruct((nf, d, LANES), BF16),
            jax.ShapeDtypeStruct((f // blk, SLABS * nd, LANES, LANES), F32),
            jax.ShapeDtypeStruct((f // blk, SLABS * nd, LANES, LANES), F32),
            jax.ShapeDtypeStruct((2 * f // blk, SLABS, tokens, LANES), BF16),
            jax.ShapeDtypeStruct((2 * f // blk, SLABS * groups, rows, LANES), F32),
        ],
        in_specs=[hbm] * 4,
        out_specs=[hbm] * 10,
        scratch_shapes=[
            vmem((nf, d, LANES), BF16), vmem((nd, f, LANES), BF16),
            vmem((nd, f, LANES), BF16), vmem((nf, d, LANES), BF16),
            vmem(whole, BF16), vmem(whole, BF16),
            vmem((m_all, nd, rows, LANES), BF16), vmem((m_all, nd, rows, LANES), BF16),
            vmem((m_all, nf, rows, LANES), F32), vmem((nf, rows, LANES), BF16),
            vmem((tokens // LANES, d, LANES), BF16),
            vmem((2, SLABS, tokens, LANES), BF16), vmem((2, tiles, LANES, LANES), F32),
            dma((2,)), dma((2,)), dma((m_all,)), dma((m_all,)), dma((m_all,)), dma((m_all,)), dma((2,)),
            dma((2, m_all, 4)), dma((2, m_all, 4)), dma((2, 2)), dma((2, n_inner)), dma((2, 2)), dma((2,)),
        ],
        compiler_params=pltpu.CompilerParams(
            collective_id=0, has_side_effects=True, vmem_limit_bytes=VMEM_LIMIT
        ),
        name="chain",
    )(x, g, w1, w2)


def _late_kernel(
    h, g, y_in, dx_in, w1, w2t, p1, p2, ap, sp, d1, d2, y, dx,
    hv, gv, w1v, w2v, p1v, p2v, av, sv, d1v, d2v, ht, ab, zb, yv, first_sem, load_sem, store_sem, pass_sem,
):
    groups, nd, rows, _ = h.shape
    units = w1.shape[0] // SLABS
    d, blk = d1v.shape[1:]

    def pre(j):
        return (lax.axis_index("stage") < PRE_LATE) & (j % 2 == 0)

    def weights(j):
        b, some = j % 2, pl.ds(j * SLABS, SLABS)
        return (pltpu.make_async_copy(w2t.at[some], w2v.at[b], load_sem.at[0, b]),)

    def own(j):
        b, some = j % 2, pl.ds(j * SLABS, SLABS)
        return (pltpu.make_async_copy(w1.at[some], w1v.at[b], load_sem.at[1, b]),)

    def ready(j):
        b = j % 2
        return (
            pltpu.make_async_copy(ap.at[units + j], av.at[b], load_sem.at[1, b]),
            pltpu.make_async_copy(sp.at[units + j], sv.at[b], load_sem.at[2, b]),
        )

    def parts(j):
        b = j % 2
        return (
            pltpu.make_async_copy(p1.at[j], p1v.at[b], load_sem.at[3, b]),
            pltpu.make_async_copy(p2.at[j], p2v.at[b], load_sem.at[4, b]),
        )

    def stores(j):
        b, some = j % 2, pl.ds(pl.multiple_of(j * blk, blk), blk)
        return (
            pltpu.make_async_copy(d1v.at[b], d1.at[:, some], store_sem.at[0, b]),
            pltpu.make_async_copy(d2v.at[b], d2.at[some, :], store_sem.at[1, b]),
        )

    def do(copies, how):
        for c in copies:
            getattr(c, how)()

    def inputs(j, how):
        @pl.when(pre(j))
        def _():
            do(ready(j), how)

        @pl.when(jnp.logical_not(pre(j)))
        def _():
            do(own(j), how)

        do(weights(j), how)

    firsts = (pltpu.make_async_copy(h, hv, first_sem.at[0]), pltpu.make_async_copy(g, gv, first_sem.at[1]))
    firsts[0].start()
    inputs(0, "start")
    firsts[1].start()
    do(parts(0), "start")
    into = [pltpu.make_async_copy(a, yv.at[n], pass_sem.at[n]) for n, a in enumerate((y_in, dx_in))]
    out_of = [pltpu.make_async_copy(yv.at[n], a, pass_sem.at[n]) for n, a in enumerate((y, dx))]
    do(into, "start")
    firsts[0].wait()
    _transposed_rows(lambda k, c: hv[k, c], groups, rows, nd, ht)
    do(into, "wait")
    do(out_of, "start")

    def unit(j, carry):
        b = j % 2
        inputs(j, "wait")

        @pl.when(j == 0)
        def _():
            firsts[1].wait()

        @pl.when(j + 1 < units)
        def _():
            inputs(j + 1, "start")
            do(parts(j + 1), "start")

        do(parts(j), "wait")

        @pl.when(j > 1)
        def _():
            do(stores(j), "wait")

        def put(v1, v2):
            for c in range(SLABS):
                for e in range(nd):
                    r, s = slice(e * LANES, (e + 1) * LANES), slice(c * LANES, (c + 1) * LANES)
                    d2v[b, s, r] = p2v[b, c * nd + e] + v2[s, r]
                    d1v[b, r, s] = p1v[b, c * nd + e] + v1[r, s]

        def block(ready):
            _dw_block(
                512, lambda k, c: hv[k, c], lambda k, c: gv[k, c], groups, rows, nd,
                lambda: _wide([w1v[b, c] for c in range(SLABS)]), lambda: _wide([w2v[b, c] for c in range(SLABS)]),
                ht, ab, zb, put, ready,
            )

        @pl.when(pre(j))
        def _():
            block((lambda c: av[b, c], lambda k, c: sv[b, c * groups + k]))

        @pl.when(jnp.logical_not(pre(j)))
        def _():
            block(None)

        do(stores(j), "start")
        return carry

    lax.fori_loop(0, units, unit, 0)
    do(stores(units - 2), "wait")
    do(stores(units - 1), "wait")
    do(out_of, "wait")


def _late(h, g, y, dx, w1, w2t, p1, p2, ap, sp):
    groups, nd, rows, _ = h.shape
    nf, d, _ = w1.shape
    f, blk, t = nf * LANES, SLABS * LANES, groups * rows
    hbm = pl.BlockSpec(memory_space=pltpu.HBM)
    vmem, dma = pltpu.VMEM, pltpu.SemaphoreType.DMA
    return pl.pallas_call(
        _late_kernel,
        in_specs=[hbm] * 10,
        out_specs=[hbm] * 4,
        out_shape=[
            jax.ShapeDtypeStruct((d, f), F32), jax.ShapeDtypeStruct((f, d), F32),
            jax.ShapeDtypeStruct(y.shape, BF16), jax.ShapeDtypeStruct(dx.shape, BF16),
        ],
        scratch_shapes=[
            vmem(h.shape, BF16), vmem(g.shape, BF16),
            vmem((2, SLABS, d, LANES), BF16), vmem((2, SLABS, d, LANES), BF16),
            vmem((2, *p1.shape[1:]), F32), vmem((2, *p2.shape[1:]), F32),
            vmem((2, *ap.shape[1:]), BF16), vmem((2, *sp.shape[1:]), F32),
            vmem((2, d, blk), F32), vmem((2, blk, d), F32),
            vmem((t // LANES, d, LANES), BF16), vmem((SLABS, t, LANES), BF16), vmem((SLABS, t, LANES), BF16),
            vmem((2, *y.shape), BF16),
            dma((2,)), dma((5, 2)), dma((2, 2)), dma((2,)),
        ],
        compiler_params=pltpu.CompilerParams(vmem_limit_bytes=VMEM_LIMIT),
        cost_estimate=pl.CostEstimate(flops=8 * t * d * f, bytes_accessed=20 * d * f, transcendentals=t * f),
        name="late",
    )(h, g, y, dx, w1, w2t, p1, p2, ap, sp)


def solution(mesh):
    n_stage, n_inner = mesh.shape["stage"], mesh.shape["inner"]

    def body(x, g, w1, w2):
        y, dx, h, gg, w1s, w2s, *parts = _chain(n_stage, n_inner, x, g, w1, w2)
        flat = (-1, *h.shape[2:])
        d1, d2, y, dx = _late(h.reshape(flat), gg.reshape(flat), y, dx, w1s, w2s, *parts)
        return y, dx, d1.reshape(w1.shape), d2.reshape(w2.shape)

    tok = P(("data", "stage"), "inner", None)
    wsp = P(None, "stage", None, None)
    dsp = P("data", "stage", None, None)
    return jax.shard_map(body, mesh=mesh, in_specs=(tok, tok, wsp, wsp), out_specs=(tok, tok, dsp, dsp), check_vma=False)
```

```python
import functools

import jax
import jax.numpy as jnp
from jax import lax
from jax.experimental import pallas as pl
from jax.experimental.pallas import tpu as pltpu
from jax.sharding import PartitionSpec as P

MESH = pl.DeviceIdType.MESH
F32, BF16 = jnp.float32, jnp.bfloat16
C0, C1 = 0.7978845608028654, 0.044715
LANES = 128
VMEM_LIMIT = 67043328
SLABS = 4
MERGE = 2
EARLY = 2
PRE_LATE = 2


def _gelu_and_slope(z):
    z2 = z * z
    half = 0.5 * jnp.tanh(z * (C0 + (C0 * C1) * z2)) + 0.5
    a = z * half
    return a, half + (a - a * half) * (2.0 * C0 + (6.0 * C0 * C1) * z2)


def _dot(a, b):
    return jnp.dot(a, b, preferred_element_type=F32)


def _wide(slabs):
    return jnp.concatenate(slabs, axis=1)


def _tall(parts):
    return jnp.concatenate(parts, axis=0)


def _cut(value, c):
    return value[:, c * LANES : (c + 1) * LANES]


def _rows_of(read, ks, n):
    return _tall([_wide([read(k, c) for c in range(n)]) for k in ks])


def _chunks(rows, groups, group_rows):
    step = max(1, rows // group_rows)
    for k in range(0, groups, step):
        ks = range(k, min(k + step, groups))
        yield ks, slice(k * group_rows, (k + len(ks)) * group_rows)


def _dw_block(
    rows, hg, gg, groups, group_rows, nd, w1_block, w2t_block, ht, ab, zb, put, ready=None
):
    for ks, s in _chunks(rows, groups, group_rows):
        if ready is None:
            z = _dot(_rows_of(hg, ks, nd), w1_block())
        da = _dot(_rows_of(gg, ks, nd), w2t_block())
        if ready is None:
            a, slope = _gelu_and_slope(z)
            a = a.astype(BF16)
            for c in range(SLABS):
                ab[c, s, :] = _cut(a, c)
        else:
            slope = _rows_of(ready[1], ks, SLABS)
        dz = (da * slope).astype(BF16)
        for c in range(SLABS):
            zb[c, s, :] = _cut(dz, c)
    a = _wide([ab[c] for c in range(SLABS)] if ready is None else [ready[0](c) for c in range(SLABS)])
    v2 = lax.dot_general(
        a, _rows_of(gg, range(groups), nd), (((0,), (0,)), ((), ())), preferred_element_type=F32
    )
    put(_dot(_wide([ht[t] for t in range(ht.shape[0])]), _wide([zb[c] for c in range(SLABS)])), v2)


def _transposed_rows(hg, groups, group_rows, nd, ht):
    per = LANES // group_rows
    for t in range(groups // per):
        ht[t] = _tall([_wide([hg(t * per + e, c) for c in range(nd)]) for e in range(per)]).T


def _chain_kernel(
    n_stage, n_inner, x, g, w1, w2, y, dx, h_late, g_late, w1_out, w2_out, d1_part, d2_part, a_pre, s_pre,
    w1v, w2v, w1t, w2t, hw, gw, ho, go, zs, act, ht, narrow, full, own_v,
    wsem, xsem, h_recv, g_recv, h_send, g_send, out_recv, ring_send, ring_recv, part_sem, late_sem, pre_sem, keep_sem, own_sem,
):
    p, i = lax.axis_index("stage"), lax.axis_index("inner")
    right, left = lax.rem(i + 1, n_inner), lax.rem(i + n_inner - 1, n_inner)
    _, m_all, nd, rows, _ = hw.shape
    nf = w1v.shape[0]
    units = nf // SLABS
    early = EARLY
    last = n_stage - 1
    half = nd // 2
    part = rows // MERGE
    groups = n_inner * early
    tokens = groups * rows
    ab, zb = narrow.at[0], narrow.at[1]

    def flat(ref, c):
        return ref.at[0, :, c * LANES : (c + 1) * LANES]

    mine = [
        pltpu.make_async_copy(flat(src, c), own_v.at[n, c], own_sem.at[n]) for n, src in enumerate((x, g)) for c in range(nd)
    ]
    for c in mine:
        c.start()

    barrier = pltpu.get_barrier_semaphore()
    for q in range(1, n_stage):
        pl.semaphore_signal(barrier, inc=1, device_id={"stage": lax.rem(p + q, n_stage)}, device_id_type=MESH)
    for q in (left, right):
        pl.semaphore_signal(barrier, inc=1, device_id={"inner": q}, device_id_type=MESH)

    loads = [
        pltpu.make_async_copy(w1.at[0, 0, :, c * LANES : (c + 1) * LANES], w1v.at[c], wsem.at[0]) for c in range(nf)
    ] + [pltpu.make_async_copy(w2.at[0, 0, :, c * LANES : (c + 1) * LANES], w2v.at[c], wsem.at[1]) for c in range(nd)]
    for c in loads:
        c.start()

    def to_stage(src, dst, send, recv, stage):
        return pltpu.make_async_remote_copy(
            src_ref=src, dst_ref=dst, send_sem=send, recv_sem=recv,
            device_id={"stage": stage}, device_id_type=MESH,
        )

    def to_inner(src, dst, send, recv, inner):
        return pltpu.make_async_remote_copy(
            src_ref=src, dst_ref=dst, send_sem=send, recv_sem=recv,
            device_id={"inner": inner}, device_id_type=MESH,
        )

    def piece(e):
        return pl.ds(pl.multiple_of(e * part, part), part)

    with jax.named_scope("barrier"):
        pl.semaphore_wait(barrier, n_stage + 1)
    for c in mine:
        c.wait()

    def own(mine_v, slots, recv, sem, stage):
        there = slots.at[i, p // MERGE, :, piece(p % MERGE)]

        @pl.when(p == stage)
        def _():
            pltpu.make_async_copy(mine_v, there, recv.at[p // MERGE]).start()

        @pl.when(p != stage)
        def _():
            to_stage(mine_v, there, sem, recv.at[p // MERGE], stage).start()

    own(own_v.at[0], hw, h_recv, xsem.at[0], 0)
    own(own_v.at[1], gw, g_recv, xsem.at[1], last)

    def ring_first(q, m, whole):
        a = whole.at[i, m]
        to_inner(a, a, ring_send.at[q, m, 0], ring_recv.at[q, m, 0], right).start()
        to_inner(a, a, ring_send.at[q, m, 1], ring_recv.at[q, m, 1], left).start()

    def ring_forward(q, m, whole):
        a, b = whole.at[left, m], whole.at[right, m]
        to_inner(a, a, ring_send.at[q, m, 0], ring_recv.at[q, m, 0], right).wait_recv()
        a = whole.at[left, m, pl.ds(0, half)]
        to_inner(a, a, ring_send.at[q, m, 2], ring_recv.at[q, m, 2], right).start()
        to_inner(b, b, ring_send.at[q, m, 1], ring_recv.at[q, m, 1], left).wait_recv()
        b = whole.at[right, m, pl.ds(half, half)]
        to_inner(b, b, ring_send.at[q, m, 3], ring_recv.at[q, m, 3], left).start()

    def ring_far(q, m, whole):
        far = lax.rem(i + 2, n_inner)
        a, b = whole.at[far, m, pl.ds(0, half)], whole.at[far, m, pl.ds(half, half)]
        return (
            to_inner(a, a, ring_send.at[q, m, 2], ring_recv.at[q, m, 2], right),
            to_inner(b, b, ring_send.at[q, m, 3], ring_recv.at[q, m, 3], left),
        )

    def ring_arrived(m, q):
        for c in ring_far(q, m, (hw, gw)[q]):
            c.wait_recv()

    def ring_sent(m):
        for q, whole in ((0, hw), (1, gw)):
            for c in ring_far(q, m, whole):
                c.wait_send()
            a = whole.at[i, m]
            to_inner(a, a, ring_send.at[q, m, 0], ring_recv.at[q, m, 0], right).wait_send()
            to_inner(a, a, ring_send.at[q, m, 1], ring_recv.at[q, m, 1], left).wait_send()

    def pass_on(m, lo, hi, src, slots, send, recv, end, nxt, out, out_sem):
        @pl.when(p != end)
        def _():
            some = pl.ds(lo, hi - lo)
            to_stage(src.at[m, some], slots.at[i, m, some], send.at[m], recv.at[m], nxt).start()

        if hi - lo < nd:
            return

        @pl.when(p == end)
        def _():
            for e in range(MERGE):
                home = m * MERGE + e

                @pl.when(p != home)
                def _():
                    for c in range(nd):
                        to_stage(src.at[m, c, piece(e)], flat(out, c), send.at[m], out_sem, home).start()

                @pl.when(p == home)
                def _():
                    for c in range(nd):
                        pltpu.make_async_copy(src.at[m, c, piece(e)], flat(out, c), out_sem).start()

    def project(m, split, res, w, src, *rest):
        whole = _wide([act[c] for c in range(nf)])
        count = half if split else nd
        for lo in range(0, nd, count):
            u = _dot(whole, _wide([w[lo + c] for c in range(count)]))
            out = (res[:, lo * LANES : (lo + count) * LANES].astype(F32) + u).astype(BF16)
            for c in range(count):
                src[m, lo + c] = _cut(out, c)
            pass_on(m, lo, lo + count, src, *rest)

    def forward(m, sloped, split):
        with jax.named_scope("wait_h"):
            pltpu.make_async_copy(hw.at[i, m], hw.at[i, m], h_recv.at[m]).wait()
        h = _wide([hw[i, m, c] for c in range(nd)])
        for b in range(0, nf, SLABS):
            z = _dot(h, _wide([w1v[b + c] for c in range(SLABS)]))
            a, slope = _gelu_and_slope(z)
            a, kept = a.astype(BF16), slope if sloped else z
            for c in range(SLABS):
                zs[m, b + c] = _cut(kept, c)
                act[b + c] = _cut(a, c)

        @pl.when((m == 0) & (p < n_stage // 2))
        def _():
            for c in loads[nf:]:
                c.wait()

        project(m, split, h, w2v, ho, hw, h_send, h_recv, last, jnp.minimum(p + 1, last), y, out_recv.at[0])

        @pl.when((p < n_stage - 2) | (m < early))
        def _():
            ring_first(0, m, hw)

    def backward(m, split):
        @pl.when((p < n_stage // 2) & (m == early + 1))
        def _():
            ring_forward(1, early - 1, gw)

        with jax.named_scope("wait_g"):
            pltpu.make_async_copy(gw.at[i, m], gw.at[i, m], g_recv.at[m]).wait()

        @pl.when(m < early)
        def _():
            ring_first(1, m, gw)

        dh = _wide([gw[i, m, c] for c in range(nd)])
        for b in range(0, nf, SLABS):
            da = _dot(dh, _wide([w2t[b + c] for c in range(SLABS)]))
            dz = (da * _wide([zs[m, b + c] for c in range(SLABS)])).astype(BF16)
            for c in range(SLABS):
                act[b + c] = _cut(dz, c)
        project(m, split, dh, w1t, go, gw, g_send, g_recv, 0, jnp.maximum(p - 1, 0), dx, out_recv.at[1])

        @pl.when(m == early)
        def _():
            @pl.when(p >= n_stage - 2)
            def _():
                ring_forward(0, 0, hw)

            @pl.when(p < n_stage - 2)
            def _():
                each(0, early - 1, lambda e: ring_forward(1, e, gw))

    def transpose_weights():
        def some(c, carry):
            s = pl.ds(pl.multiple_of(c * LANES, LANES), LANES)
            for e in range(nd):
                w1t[e, s, :] = w1v[c, e * LANES : (e + 1) * LANES, :].T
                w2t[c, e * LANES : (e + 1) * LANES, :] = w2v[e, s, :].T
            return carry

        lax.fori_loop(0, nf, some, 0)

    def slopes():
        def some(t, carry):
            m, b = t // (nf // SLABS), t % (nf // SLABS) * SLABS
            for c in range(SLABS):
                zs[m, b + c] = _gelu_and_slope(zs[m, b + c])[1]
            return carry

        lax.fori_loop(0, m_all * (nf // SLABS), some, 0)

    def each(lo, hi, fn):
        lax.fori_loop(lo, hi, lambda m, c: (fn(m), c)[1], 0)

    def group(whole, part=0):
        return lambda k, c: whole[k // early, part * early + k % early, c]

    def pre_stores(j):
        b = j % 2
        return (
            pltpu.make_async_copy(narrow.at[b], a_pre.at[j], pre_sem.at[0, b]),
            pltpu.make_async_copy(full.at[b, pl.ds(0, SLABS * groups)], s_pre.at[j], pre_sem.at[1, b]),
        )

    def pre_loads(j):
        b = j % 2
        return (
            pltpu.make_async_copy(
                a_pre.at[j], w2v.at[pl.ds(b * SLABS, SLABS), pl.ds(0, tokens)], pre_sem.at[0, b]
            ),
            pltpu.make_async_copy(s_pre.at[j], zs.at[b, pl.ds(0, SLABS * groups)], pre_sem.at[1, b]),
        )

    def pre_unit(j):
        b = j % 2

        @pl.when(j > 1)
        def _():
            for c in pre_stores(j):
                c.wait()

        for ks, s in _chunks(256, groups, rows):
            z = _dot(_rows_of(group(hw, j // units), ks, nd), _wide([w1v[j % units * SLABS + c] for c in range(SLABS)]))
            a, slope = _gelu_and_slope(z)
            a = a.astype(BF16)
            for c in range(SLABS):
                narrow[b, c, s, :] = _cut(a, c)
                for n, k in enumerate(ks):
                    full[b, c * groups + k] = _cut(slope[n * rows : (n + 1) * rows], c)
        for c in pre_stores(j):
            c.start()

    mid = n_stage // 2
    formed = jnp.where(
        p < PRE_LATE, 2 * units, jnp.where(p < mid - 1, units, jnp.where(p == mid - 1, units // 2, 0))
    )

    def part_copies(j):
        b, some = j % 2, pl.ds(0, SLABS * nd)
        return (
            pltpu.make_async_copy(full.at[b, some], d1_part.at[j], part_sem.at[0, b]),
            pltpu.make_async_copy(zs.at[m_all - 2 + b, some], d2_part.at[j], part_sem.at[1, b]),
        )

    def late_copies():
        return [
            pltpu.make_async_copy(whole.at[k, pl.ds(early, m_all - early)], out.at[k], late_sem.at[q, k])
            for q, (whole, out) in enumerate(((hw, h_late), (gw, g_late)))
            for k in range(n_inner)
        ]

    def sent(m):
        ring_sent(m)
        for src, slots, send, recv, end in ((ho, hw, h_send, h_recv, last), (go, gw, g_send, g_recv, 0)):
            for e in range(MERGE):
                a = src.at[m, :, piece(e)]

                @pl.when((p != end) | (p != m * MERGE + e))
                def _():
                    to_stage(a, a, send.at[m], recv.at[m], 0).wait_send()

        @pl.when((m == 0) & (p != 0))
        def _():
            to_stage(own_v.at[0], own_v.at[0], xsem.at[0], h_recv.at[0], 0).wait_send()

        @pl.when((m == 0) & (p != last))
        def _():
            to_stage(own_v.at[1], own_v.at[1], xsem.at[1], g_recv.at[0], last).wait_send()

    def unit(j):
        def forwards(m):
            @pl.when(p >= n_stage - 2)
            def _():
                ring_forward(0, m, hw)

            ring_forward(1, m, gw)

        def firsts(m):
            @pl.when(p >= n_stage - 2)
            def _():
                ring_first(0, m, hw)

            ring_first(1, m, gw)

        @pl.when(j == 0)
        def _():
            @pl.when(p >= n_stage - 2)
            def _():
                each(0, early - 1, lambda e: ring_forward(1, e, gw))
                each(1, early, lambda e: ring_forward(0, e, hw))

            @pl.when(p >= n_stage // 2)
            def _():
                ring_forward(1, early - 1, gw)


            @pl.when(p < n_stage // 2)
            def _():
                for c in pre_loads(0):
                    c.start()

            each(0, early, lambda m: ring_arrived(m, 1))

            @pl.when(p >= n_stage // 2)
            def _():
                each(0, early, lambda m: ring_arrived(m, 0))

            each(early, m_all, firsts)
            _transposed_rows(group(hw), groups, rows, nd, ht)

        for m in range(early, m_all):
            @pl.when(j == jnp.where(p < n_stage - 2, 2, 3) * (m - early + 1))
            def _():
                forwards(m)

        @pl.when(j == units - 1)
        def _():
            each(early, m_all, lambda m: ring_arrived(m, 1))

            @pl.when(p >= PRE_LATE)
            def _():
                each(early, m_all, lambda m: ring_arrived(m, 0))

            for c in late_copies():
                c.start()
            each(0, m_all, sent)

        @pl.when(j > 1)
        def _():
            for c in part_copies(j):
                c.wait()

        def put(v1, v2):
            for c in range(SLABS):
                for e in range(nd):
                    zs[m_all - 2 + j % 2, c * nd + e] = _cut(v2[c * LANES : (c + 1) * LANES], e)
                    full[j % 2, c * nd + e] = _cut(v1[e * LANES : (e + 1) * LANES], c)

        def block(ready):
            _dw_block(
                512, group(hw), group(gw), groups, rows, nd,
                lambda: _wide([w1v[j * SLABS + c] for c in range(SLABS)]),
                lambda: _wide([w2t[j * SLABS + c] for c in range(SLABS)]),
                ht, ab, zb, put, ready,
            )

        @pl.when(j < formed)
        def _():
            b = j % 2
            for c in pre_loads(j):
                c.wait()

            @pl.when(j + 1 < jnp.minimum(formed, units))
            def _():
                for c in pre_loads(j + 1):
                    c.start()

            block((
                lambda c: w2v[b * SLABS + c, 0:tokens, :],
                lambda k, c: zs[b, c * groups + k],
            ))

        @pl.when(j >= formed)
        def _():
            block(None)

        for c in part_copies(j):
            c.start()

    kept = (
        pltpu.make_async_copy(w1v, w1_out, keep_sem.at[0]), pltpu.make_async_copy(w2t, w2_out, keep_sem.at[1])
    )
    with jax.named_scope("loads"):
        for c in loads[:nf]:
            c.wait()

    first = jnp.where(p == last, 1, m_all)
    rest = m_all - first
    turn = jnp.where(p < n_stage // 2, first, 0)

    def step(k, carry):
        j = k - first
        swap = j < 2 * rest
        is_u = k >= 2 * m_all
        is_f = (j < 0) | (swap & (j % 2 == 1))
        is_b = jnp.logical_not(is_f | is_u)
        m_f = jnp.where(j < 0, k, jnp.minimum(first + j // 2, m_all - 1))
        m_b = jnp.maximum(jnp.minimum(jnp.where(swap, j // 2, j - rest), m_all - 1), 0)
        u = jnp.maximum(k - 2 * m_all, 0)

        @pl.when(k == turn)
        def _():
            with jax.named_scope("transp"):
                @pl.when(p >= n_stage // 2)
                def _():
                    for c in loads[nf:]:
                        c.wait()

                transpose_weights()
                for c in kept:
                    c.start()

        @pl.when((k == first) & (p < n_stage - 2))
        def _():
            with jax.named_scope("slopes"):
                slopes()
            with jax.named_scope("hring"):
                each(0, m_all, lambda m: ring_forward(0, m, hw))

        @pl.when((k == first) & (p < n_stage // 2))
        def _():
            with jax.named_scope("pre"):
                each(0, early, lambda m: ring_arrived(m, 0))

                @pl.when(p < PRE_LATE)
                def _():
                    each(early, m_all, lambda m: ring_arrived(m, 0))

                each(0, formed, pre_unit)
                for c in (*pre_stores(0), *pre_stores(1)):
                    c.wait()

        early_f, odd = is_f & (p < n_stage - 2), p % 2 == 1
        for when, sloped, split in (
            (early_f & jnp.logical_not(odd), False, False),
            (early_f & odd, False, True),
            (is_f & (p >= n_stage - 2), True, False),
        ):
            @pl.when(when)
            def _():
                with jax.named_scope("fwd"):
                    forward(m_f, sloped, split)

        leaves = (p > 0) & jnp.logical_not(odd)
        for when, split in ((is_b & leaves, True), (is_b & jnp.logical_not(leaves), False)):
            @pl.when(when)
            def _():
                with jax.named_scope("bwd"):
                    backward(m_b, split)

        @pl.when(is_u)
        def _():
            with jax.named_scope("unit"):
                unit(u)

        return carry

    lax.fori_loop(0, 2 * m_all + units, step, 0)

    with jax.named_scope("finish"):
        for c in (*kept, *part_copies(units - 2), *part_copies(units - 1), *late_copies()):
            c.wait()
    with jax.named_scope("outwait"):
        pltpu.make_async_copy(y.at[0], y.at[0], out_recv.at[0]).wait()
        pltpu.make_async_copy(dx.at[0], dx.at[0], out_recv.at[1]).wait()


def _chain(n_stage, n_inner, x, g, w1, w2):
    mb, rows, d = x.shape
    f = w1.shape[-1]
    rows = rows * MERGE
    m_all = mb * n_stage // MERGE
    early = EARLY
    nd, nf = d // LANES, f // LANES
    blk = SLABS * LANES
    groups = n_inner * early
    tokens = groups * rows
    tiles = SLABS * max(nd, groups)
    hbm = pl.BlockSpec(memory_space=pltpu.HBM)
    whole = (n_inner, m_all, nd, rows, LANES)
    late = jax.ShapeDtypeStruct((n_inner, m_all - early, nd, rows, LANES), BF16)
    dma = pltpu.SemaphoreType.DMA
    vmem = pltpu.VMEM
    return pl.pallas_call(
        functools.partial(_chain_kernel, n_stage, n_inner),
        out_shape=[
            jax.ShapeDtypeStruct(x.shape, BF16), jax.ShapeDtypeStruct(x.shape, BF16), late, late,
            jax.ShapeDtypeStruct((nf, d, LANES), BF16), jax.ShapeDtypeStruct((nf, d, LANES), BF16),
            jax.ShapeDtypeStruct((f // blk, SLABS * nd, LANES, LANES), F32),
            jax.ShapeDtypeStruct((f // blk, SLABS * nd, LANES, LANES), F32),
            jax.ShapeDtypeStruct((2 * f // blk, SLABS, tokens, LANES), BF16),
            jax.ShapeDtypeStruct((2 * f // blk, SLABS * groups, rows, LANES), F32),
        ],
        in_specs=[hbm] * 4,
        out_specs=[hbm] * 10,
        scratch_shapes=[
            vmem((nf, d, LANES), BF16), vmem((nd, f, LANES), BF16),
            vmem((nd, f, LANES), BF16), vmem((nf, d, LANES), BF16),
            vmem(whole, BF16), vmem(whole, BF16),
            vmem((m_all, nd, rows, LANES), BF16), vmem((m_all, nd, rows, LANES), BF16),
            vmem((m_all, nf, rows, LANES), F32), vmem((nf, rows, LANES), BF16),
            vmem((tokens // LANES, d, LANES), BF16),
            vmem((2, SLABS, tokens, LANES), BF16), vmem((2, tiles, LANES, LANES), F32),
            vmem((2, nd, rows // MERGE, LANES), BF16),
            dma((2,)), dma((2,)), dma((m_all,)), dma((m_all,)), dma((m_all,)), dma((m_all,)), dma((2,)),
            dma((2, m_all, 4)), dma((2, m_all, 4)), dma((2, 2)), dma((2, n_inner)), dma((2, 2)), dma((2,)), dma((2,)),
        ],
        compiler_params=pltpu.CompilerParams(
            collective_id=0, has_side_effects=True, vmem_limit_bytes=VMEM_LIMIT
        ),
        name="chain",
    )(x, g, w1, w2)


def _late_kernel(
    h, g, y_in, dx_in, w1, w2t, p1, p2, ap, sp, d1, d2, y, dx,
    hv, gv, w1v, w2v, p1v, p2v, av, sv, d1v, d2v, ht, ab, zb, yv, first_sem, load_sem, store_sem, pass_sem,
):
    groups, nd, rows, _ = h.shape
    units = w1.shape[0] // SLABS
    d, blk = d1v.shape[1:]

    def pre(j):
        return (lax.axis_index("stage") < PRE_LATE) & (j % 2 == 0)

    def weights(j):
        b, some = j % 2, pl.ds(j * SLABS, SLABS)
        return (pltpu.make_async_copy(w2t.at[some], w2v.at[b], load_sem.at[0, b]),)

    def own(j):
        b, some = j % 2, pl.ds(j * SLABS, SLABS)
        return (pltpu.make_async_copy(w1.at[some], w1v.at[b], load_sem.at[1, b]),)

    def ready(j):
        b = j % 2
        return (
            pltpu.make_async_copy(ap.at[units + j], av.at[b], load_sem.at[1, b]),
            pltpu.make_async_copy(sp.at[units + j], sv.at[b], load_sem.at[2, b]),
        )

    def parts(j):
        b = j % 2
        return (
            pltpu.make_async_copy(p1.at[j], p1v.at[b], load_sem.at[3, b]),
            pltpu.make_async_copy(p2.at[j], p2v.at[b], load_sem.at[4, b]),
        )

    def stores(j):
        b, some = j % 2, pl.ds(pl.multiple_of(j * blk, blk), blk)
        return (
            pltpu.make_async_copy(d1v.at[b], d1.at[:, some], store_sem.at[0, b]),
            pltpu.make_async_copy(d2v.at[b], d2.at[some, :], store_sem.at[1, b]),
        )

    def do(copies, how):
        for c in copies:
            getattr(c, how)()

    def inputs(j, how):
        @pl.when(pre(j))
        def _():
            do(ready(j), how)

        @pl.when(jnp.logical_not(pre(j)))
        def _():
            do(own(j), how)

        do(weights(j), how)

    firsts = (pltpu.make_async_copy(h, hv, first_sem.at[0]), pltpu.make_async_copy(g, gv, first_sem.at[1]))
    firsts[0].start()
    inputs(0, "start")
    firsts[1].start()
    do(parts(0), "start")
    into = [pltpu.make_async_copy(a, yv.at[n], pass_sem.at[n]) for n, a in enumerate((y_in, dx_in))]
    out_of = [pltpu.make_async_copy(yv.at[n], a, pass_sem.at[n]) for n, a in enumerate((y, dx))]
    do(into, "start")
    firsts[0].wait()
    _transposed_rows(lambda k, c: hv[k, c], groups, rows, nd, ht)
    do(into, "wait")
    do(out_of, "start")

    def unit(j, carry):
        b = j % 2
        inputs(j, "wait")

        @pl.when(j == 0)
        def _():
            firsts[1].wait()

        @pl.when(j + 1 < units)
        def _():
            inputs(j + 1, "start")
            do(parts(j + 1), "start")

        do(parts(j), "wait")

        @pl.when(j > 1)
        def _():
            do(stores(j), "wait")

        def put(v1, v2):
            for c in range(SLABS):
                for e in range(nd):
                    r, s = slice(e * LANES, (e + 1) * LANES), slice(c * LANES, (c + 1) * LANES)
                    d2v[b, s, r] = p2v[b, c * nd + e] + v2[s, r]
                    d1v[b, r, s] = p1v[b, c * nd + e] + v1[r, s]

        def block(ready):
            _dw_block(
                512, lambda k, c: hv[k, c], lambda k, c: gv[k, c], groups, rows, nd,
                lambda: _wide([w1v[b, c] for c in range(SLABS)]), lambda: _wide([w2v[b, c] for c in range(SLABS)]),
                ht, ab, zb, put, ready,
            )

        @pl.when(pre(j))
        def _():
            block((lambda c: av[b, c], lambda k, c: sv[b, c * groups + k]))

        @pl.when(jnp.logical_not(pre(j)))
        def _():
            block(None)

        do(stores(j), "start")
        return carry

    lax.fori_loop(0, units, unit, 0)
    do(stores(units - 2), "wait")
    do(stores(units - 1), "wait")
    do(out_of, "wait")


def _late(h, g, y, dx, w1, w2t, p1, p2, ap, sp):
    groups, nd, rows, _ = h.shape
    nf, d, _ = w1.shape
    f, blk, t = nf * LANES, SLABS * LANES, groups * rows
    hbm = pl.BlockSpec(memory_space=pltpu.HBM)
    vmem, dma = pltpu.VMEM, pltpu.SemaphoreType.DMA
    return pl.pallas_call(
        _late_kernel,
        in_specs=[hbm] * 10,
        out_specs=[hbm] * 4,
        out_shape=[
            jax.ShapeDtypeStruct((d, f), F32), jax.ShapeDtypeStruct((f, d), F32),
            jax.ShapeDtypeStruct(y.shape, BF16), jax.ShapeDtypeStruct(dx.shape, BF16),
        ],
        scratch_shapes=[
            vmem(h.shape, BF16), vmem(g.shape, BF16),
            vmem((2, SLABS, d, LANES), BF16), vmem((2, SLABS, d, LANES), BF16),
            vmem((2, *p1.shape[1:]), F32), vmem((2, *p2.shape[1:]), F32),
            vmem((2, *ap.shape[1:]), BF16), vmem((2, *sp.shape[1:]), F32),
            vmem((2, d, blk), F32), vmem((2, blk, d), F32),
            vmem((t // LANES, d, LANES), BF16), vmem((SLABS, t, LANES), BF16), vmem((SLABS, t, LANES), BF16),
            vmem((2, *y.shape), BF16),
            dma((2,)), dma((5, 2)), dma((2, 2)), dma((2,)),
        ],
        compiler_params=pltpu.CompilerParams(vmem_limit_bytes=VMEM_LIMIT),
        cost_estimate=pl.CostEstimate(flops=8 * t * d * f, bytes_accessed=20 * d * f, transcendentals=t * f),
        name="late",
    )(h, g, y, dx, w1, w2t, p1, p2, ap, sp)


def solution(mesh):
    n_stage, n_inner = mesh.shape["stage"], mesh.shape["inner"]

    def body(x, g, w1, w2):
        y, dx, h, gg, w1s, w2s, *parts = _chain(n_stage, n_inner, x, g, w1, w2)
        flat = (-1, *h.shape[2:])
        d1, d2, y, dx = _late(h.reshape(flat), gg.reshape(flat), y, dx, w1s, w2s, *parts)
        return y, dx, d1.reshape(w1.shape), d2.reshape(w2.shape)

    tok = P(("data", "stage"), "inner", None)
    wsp = P(None, "stage", None, None)
    dsp = P("data", "stage", None, None)
    return jax.shard_map(body, mesh=mesh, in_specs=(tok, tok, wsp, wsp), out_specs=(tok, tok, dsp, dsp), check_vma=False)
```

```python
import functools

import jax
import jax.numpy as jnp
from jax import lax
from jax.experimental import pallas as pl
from jax.experimental.pallas import tpu as pltpu
from jax.sharding import PartitionSpec as P

MESH = pl.DeviceIdType.MESH
F32, BF16 = jnp.float32, jnp.bfloat16
C0, C1 = 0.7978845608028654, 0.044715
LANES = 128
VMEM_LIMIT = 67043328
SLABS = 4
MERGE = 2
EARLY = 2
DEEP = 3
PRE_LATE = 2


def _gelu_and_slope(z):
    z2 = z * z
    half = 0.5 * jnp.tanh(z * (C0 + (C0 * C1) * z2)) + 0.5
    a = z * half
    return a, half + (a - a * half) * (2.0 * C0 + (6.0 * C0 * C1) * z2)


def _dot(a, b):
    return jnp.dot(a, b, preferred_element_type=F32)


def _wide(slabs):
    return jnp.concatenate(slabs, axis=1)


def _tall(parts):
    return jnp.concatenate(parts, axis=0)


def _cut(value, c):
    return value[:, c * LANES : (c + 1) * LANES]


def _rows_of(read, ks, n):
    return _tall([_wide([read(k, c) for c in range(n)]) for k in ks])


def _chunks(rows, groups, group_rows):
    step = max(1, rows // group_rows)
    for k in range(0, groups, step):
        ks = range(k, min(k + step, groups))
        yield ks, slice(k * group_rows, (k + len(ks)) * group_rows)


def _dw_block(
    rows, hg, gg, groups, group_rows, nd, w1_block, w2t_block, ht, ab, zb, put, ready=None
):
    for ks, s in _chunks(rows, groups, group_rows):
        if ready is None:
            z = _dot(_rows_of(hg, ks, nd), w1_block())
        da = _dot(_rows_of(gg, ks, nd), w2t_block())
        if ready is None:
            a, slope = _gelu_and_slope(z)
            a = a.astype(BF16)
            for c in range(SLABS):
                ab[c, s, :] = _cut(a, c)
        else:
            slope = _rows_of(ready[1], ks, SLABS)
        dz = (da * slope).astype(BF16)
        for c in range(SLABS):
            zb[c, s, :] = _cut(dz, c)
    a = _wide([ab[c] for c in range(SLABS)] if ready is None else [ready[0](c) for c in range(SLABS)])
    v2 = lax.dot_general(
        a, _rows_of(gg, range(groups), nd), (((0,), (0,)), ((), ())), preferred_element_type=F32
    )
    put(_dot(_wide([ht[t] for t in range(ht.shape[0])]), _wide([zb[c] for c in range(SLABS)])), v2)


def _transposed_rows(hg, groups, group_rows, nd, ht):
    per = LANES // group_rows
    for t in range(groups // per):
        ht[t] = _tall([_wide([hg(t * per + e, c) for c in range(nd)]) for e in range(per)]).T


def _chain_kernel(
    n_stage, n_inner, x, g, w1, w2, y, dx, h_late, g_late, w1_out, w2_out, d1_part, d2_part, a_pre, s_pre,
    w1v, w2v, w1t, w2t, hw, gw, ho, go, zs, act, ht, narrow, full, own_v,
    wsem, xsem, h_recv, g_recv, h_send, g_send, out_recv, ring_send, ring_recv, part_sem, late_sem, pre_sem, keep_sem, own_sem,
):
    p, i = lax.axis_index("stage"), lax.axis_index("inner")
    right, left = lax.rem(i + 1, n_inner), lax.rem(i + n_inner - 1, n_inner)
    _, m_all, nd, rows, _ = hw.shape
    nf = w1v.shape[0]
    units = nf // SLABS
    early = EARLY
    last = n_stage - 1
    half = nd // 2
    part = rows // MERGE
    groups = n_inner * early
    tokens = groups * rows
    ab, zb = narrow.at[0], narrow.at[1]

    def flat(ref, c):
        return ref.at[0, :, c * LANES : (c + 1) * LANES]

    mine = [
        pltpu.make_async_copy(flat(src, c), own_v.at[n, c], own_sem.at[n]) for n, src in enumerate((x, g)) for c in range(nd)
    ]
    for c in mine:
        c.start()

    barrier = pltpu.get_barrier_semaphore()
    for q in range(1, n_stage):
        pl.semaphore_signal(barrier, inc=1, device_id={"stage": lax.rem(p + q, n_stage)}, device_id_type=MESH)
    for q in (left, right):
        pl.semaphore_signal(barrier, inc=1, device_id={"inner": q}, device_id_type=MESH)

    loads = [
        pltpu.make_async_copy(w1.at[0, 0, :, c * LANES : (c + 1) * LANES], w1v.at[c], wsem.at[0]) for c in range(nf)
    ] + [pltpu.make_async_copy(w2.at[0, 0, :, c * LANES : (c + 1) * LANES], w2v.at[c], wsem.at[1]) for c in range(nd)]
    for c in loads:
        c.start()

    def to_stage(src, dst, send, recv, stage):
        return pltpu.make_async_remote_copy(
            src_ref=src, dst_ref=dst, send_sem=send, recv_sem=recv,
            device_id={"stage": stage}, device_id_type=MESH,
        )

    def to_inner(src, dst, send, recv, inner):
        return pltpu.make_async_remote_copy(
            src_ref=src, dst_ref=dst, send_sem=send, recv_sem=recv,
            device_id={"inner": inner}, device_id_type=MESH,
        )

    def piece(e):
        return pl.ds(pl.multiple_of(e * part, part), part)

    with jax.named_scope("barrier"):
        pl.semaphore_wait(barrier, n_stage + 1)
    for c in mine:
        c.wait()

    def own(mine_v, slots, recv, sem, stage):
        there = slots.at[i, p // MERGE, :, piece(p % MERGE)]

        @pl.when(p == stage)
        def _():
            pltpu.make_async_copy(mine_v, there, recv.at[p // MERGE]).start()

        @pl.when(p != stage)
        def _():
            to_stage(mine_v, there, sem, recv.at[p // MERGE], stage).start()

    own(own_v.at[0], hw, h_recv, xsem.at[0], 0)
    own(own_v.at[1], gw, g_recv, xsem.at[1], last)

    def ring_first(q, m, whole):
        a = whole.at[i, m]
        to_inner(a, a, ring_send.at[q, m, 0], ring_recv.at[q, m, 0], right).start()
        to_inner(a, a, ring_send.at[q, m, 1], ring_recv.at[q, m, 1], left).start()

    def ring_forward(q, m, whole):
        a, b = whole.at[left, m], whole.at[right, m]
        to_inner(a, a, ring_send.at[q, m, 0], ring_recv.at[q, m, 0], right).wait_recv()
        a = whole.at[left, m, pl.ds(0, half)]
        to_inner(a, a, ring_send.at[q, m, 2], ring_recv.at[q, m, 2], right).start()
        to_inner(b, b, ring_send.at[q, m, 1], ring_recv.at[q, m, 1], left).wait_recv()
        b = whole.at[right, m, pl.ds(half, half)]
        to_inner(b, b, ring_send.at[q, m, 3], ring_recv.at[q, m, 3], left).start()

    def ring_far(q, m, whole):
        far = lax.rem(i + 2, n_inner)
        a, b = whole.at[far, m, pl.ds(0, half)], whole.at[far, m, pl.ds(half, half)]
        return (
            to_inner(a, a, ring_send.at[q, m, 2], ring_recv.at[q, m, 2], right),
            to_inner(b, b, ring_send.at[q, m, 3], ring_recv.at[q, m, 3], left),
        )

    def ring_arrived(m, q):
        for c in ring_far(q, m, (hw, gw)[q]):
            c.wait_recv()

    def ring_sent(m):
        for q, whole in ((0, hw), (1, gw)):
            for c in ring_far(q, m, whole):
                c.wait_send()
            a = whole.at[i, m]
            to_inner(a, a, ring_send.at[q, m, 0], ring_recv.at[q, m, 0], right).wait_send()
            to_inner(a, a, ring_send.at[q, m, 1], ring_recv.at[q, m, 1], left).wait_send()

    def pass_on(m, lo, hi, src, slots, send, recv, end, nxt, out, out_sem):
        @pl.when(p != end)
        def _():
            some = pl.ds(lo, hi - lo)
            to_stage(src.at[m, some], slots.at[i, m, some], send.at[m], recv.at[m], nxt).start()

        if hi - lo < nd:
            return

        @pl.when(p == end)
        def _():
            for e in range(MERGE):
                home = m * MERGE + e

                @pl.when(p != home)
                def _():
                    for c in range(nd):
                        to_stage(src.at[m, c, piece(e)], flat(out, c), send.at[m], out_sem, home).start()

                @pl.when(p == home)
                def _():
                    for c in range(nd):
                        pltpu.make_async_copy(src.at[m, c, piece(e)], flat(out, c), out_sem).start()

    def project(m, split, res, w, src, *rest):
        whole = _wide([act[c] for c in range(nf)])
        count = half if split else nd
        for lo in range(0, nd, count):
            u = _dot(whole, _wide([w[lo + c] for c in range(count)]))
            out = (res[:, lo * LANES : (lo + count) * LANES].astype(F32) + u).astype(BF16)
            for c in range(count):
                src[m, lo + c] = _cut(out, c)
            pass_on(m, lo, lo + count, src, *rest)

    def forward(m, sloped, split):
        with jax.named_scope("wait_h"):
            pltpu.make_async_copy(hw.at[i, m], hw.at[i, m], h_recv.at[m]).wait()
        h = _wide([hw[i, m, c] for c in range(nd)])
        for b in range(0, nf, SLABS):
            z = _dot(h, _wide([w1v[b + c] for c in range(SLABS)]))
            a, slope = _gelu_and_slope(z)
            a, kept = a.astype(BF16), slope if sloped else z
            for c in range(SLABS):
                zs[m, b + c] = _cut(kept, c)
                act[b + c] = _cut(a, c)

        @pl.when((m == 0) & (p < n_stage // 2))
        def _():
            for c in loads[nf:]:
                c.wait()

        project(m, split, h, w2v, ho, hw, h_send, h_recv, last, jnp.minimum(p + 1, last), y, out_recv.at[0])

        @pl.when((p < n_stage - 2) | (m < early))
        def _():
            ring_first(0, m, hw)

    def backward(m, split):
        with jax.named_scope("wait_g"):
            pltpu.make_async_copy(gw.at[i, m], gw.at[i, m], g_recv.at[m]).wait()

        @pl.when(m < early)
        def _():
            ring_first(1, m, gw)

        dh = _wide([gw[i, m, c] for c in range(nd)])
        for b in range(0, nf, SLABS):
            da = _dot(dh, _wide([w2t[b + c] for c in range(SLABS)]))
            dz = (da * _wide([zs[m, b + c] for c in range(SLABS)])).astype(BF16)
            for c in range(SLABS):
                act[b + c] = _cut(dz, c)
        project(m, split, dh, w1t, go, gw, g_send, g_recv, 0, jnp.maximum(p - 1, 0), dx, out_recv.at[1])

        @pl.when((p >= n_stage - 2) & (m == early))
        def _():
            ring_forward(0, 0, hw)

        @pl.when((p < n_stage - 2) & (m > 0) & (m <= early))
        def _():
            ring_forward(1, jnp.maximum(m - 1, 0), gw)

    def transpose_weights():
        def some(c, carry):
            s = pl.ds(pl.multiple_of(c * LANES, LANES), LANES)
            for e in range(nd):
                w1t[e, s, :] = w1v[c, e * LANES : (e + 1) * LANES, :].T
                w2t[c, e * LANES : (e + 1) * LANES, :] = w2v[e, s, :].T
            return carry

        lax.fori_loop(0, nf, some, 0)

    def slopes():
        def some(t, carry):
            m, b = t // (nf // SLABS), t % (nf // SLABS) * SLABS
            for c in range(SLABS):
                zs[m, b + c] = _gelu_and_slope(zs[m, b + c])[1]
            return carry

        lax.fori_loop(0, m_all * (nf // SLABS), some, 0)

    def each(lo, hi, fn):
        lax.fori_loop(lo, hi, lambda m, c: (fn(m), c)[1], 0)

    def group(whole, part=0):
        return lambda k, c: whole[k // early, part * early + k % early, c]

    def pre_stores(j):
        b = j % 2
        return (
            pltpu.make_async_copy(narrow.at[b], a_pre.at[j], pre_sem.at[0, b]),
            pltpu.make_async_copy(full.at[b, pl.ds(0, SLABS * groups)], s_pre.at[j], pre_sem.at[1, b]),
        )

    def pre_loads(j):
        b = j % 2
        return (
            pltpu.make_async_copy(
                a_pre.at[j], w2v.at[pl.ds(b * SLABS, SLABS), pl.ds(0, tokens)], pre_sem.at[0, b]
            ),
            pltpu.make_async_copy(s_pre.at[j], zs.at[b, pl.ds(0, SLABS * groups)], pre_sem.at[1, b]),
        )

    def pre_unit(j):
        b = j % 2

        @pl.when(j > 1)
        def _():
            for c in pre_stores(j):
                c.wait()

        for ks, s in _chunks(256, groups, rows):
            z = _dot(_rows_of(group(hw, j // units), ks, nd), _wide([w1v[j % units * SLABS + c] for c in range(SLABS)]))
            a, slope = _gelu_and_slope(z)
            a = a.astype(BF16)
            for c in range(SLABS):
                narrow[b, c, s, :] = _cut(a, c)
                for n, k in enumerate(ks):
                    full[b, c * groups + k] = _cut(slope[n * rows : (n + 1) * rows], c)
        for c in pre_stores(j):
            c.start()

    mid = n_stage // 2
    formed = jnp.where(
        p < PRE_LATE, 2 * units, jnp.where(p < mid - 1, units, jnp.where(p == mid - 1, units // 2, 0))
    )

    def part_copies(j):
        b, some = j % 2, pl.ds(0, SLABS * nd)
        return (
            pltpu.make_async_copy(full.at[b, some], d1_part.at[j], part_sem.at[0, b]),
            pltpu.make_async_copy(zs.at[m_all - 2 + b, some], d2_part.at[j], part_sem.at[1, b]),
        )

    def late_copies():
        return [
            pltpu.make_async_copy(whole.at[k, pl.ds(early, m_all - early)], out.at[k], late_sem.at[q, k])
            for q, (whole, out) in enumerate(((hw, h_late), (gw, g_late)))
            for k in range(n_inner)
        ]

    def sent(m):
        ring_sent(m)
        for src, slots, send, recv, end in ((ho, hw, h_send, h_recv, last), (go, gw, g_send, g_recv, 0)):
            for e in range(MERGE):
                a = src.at[m, :, piece(e)]

                @pl.when((p != end) | (p != m * MERGE + e))
                def _():
                    to_stage(a, a, send.at[m], recv.at[m], 0).wait_send()

        @pl.when((m == 0) & (p != 0))
        def _():
            to_stage(own_v.at[0], own_v.at[0], xsem.at[0], h_recv.at[0], 0).wait_send()

        @pl.when((m == 0) & (p != last))
        def _():
            to_stage(own_v.at[1], own_v.at[1], xsem.at[1], g_recv.at[0], last).wait_send()

    def unit(j):
        def forwards(m):
            @pl.when(p >= n_stage - 2)
            def _():
                ring_forward(0, m, hw)

            ring_forward(1, m, gw)

        def firsts(m):
            @pl.when(p >= n_stage - 2)
            def _():
                ring_first(0, m, hw)

            ring_first(1, m, gw)

        @pl.when(j == 0)
        def _():
            @pl.when(p >= n_stage - 2)
            def _():
                ring_forward(1, 0, gw)
                each(1, early, lambda e: (ring_forward(0, e, hw), ring_forward(1, e, gw)))


            @pl.when(p < n_stage // 2)
            def _():
                for c in pre_loads(0):
                    c.start()

            each(0, early, lambda m: ring_arrived(m, 1))

            @pl.when(p >= n_stage // 2)
            def _():
                each(0, early, lambda m: ring_arrived(m, 0))

            each(early, m_all, firsts)

            @pl.when(p >= mid)
            def _():
                _transposed_rows(group(hw), groups, rows, nd, ht)

        for m in range(early, m_all):
            @pl.when(j == jnp.where(p < n_stage - 2, 2, 3) * (m - early + 1))
            def _():
                forwards(m)

        @pl.when(j == units - 1)
        def _():
            each(early, m_all, lambda m: ring_arrived(m, 1))

            @pl.when(p >= PRE_LATE)
            def _():
                each(early, m_all, lambda m: ring_arrived(m, 0))

            for c in late_copies():
                c.start()
            each(0, m_all, sent)

        @pl.when(j > 1)
        def _():
            for c in part_copies(j):
                c.wait()

        def put(v1, v2):
            for c in range(SLABS):
                for e in range(nd):
                    zs[m_all - 2 + j % 2, c * nd + e] = _cut(v2[c * LANES : (c + 1) * LANES], e)
                    full[j % 2, c * nd + e] = _cut(v1[e * LANES : (e + 1) * LANES], c)

        def block(ready):
            _dw_block(
                512, group(hw), group(gw), groups, rows, nd,
                lambda: _wide([w1v[j * SLABS + c] for c in range(SLABS)]),
                lambda: _wide([w2t[j * SLABS + c] for c in range(SLABS)]),
                ht, ab, zb, put, ready,
            )

        @pl.when(j < formed)
        def _():
            b = j % 2
            for c in pre_loads(j):
                c.wait()

            @pl.when(j + 1 < jnp.minimum(formed, units))
            def _():
                for c in pre_loads(j + 1):
                    c.start()

            block((
                lambda c: w2v[b * SLABS + c, 0:tokens, :],
                lambda k, c: zs[b, c * groups + k],
            ))

        @pl.when(j >= formed)
        def _():
            block(None)

        for c in part_copies(j):
            c.start()

    kept = (
        pltpu.make_async_copy(w1v, w1_out, keep_sem.at[0]), pltpu.make_async_copy(w2t, w2_out, keep_sem.at[1])
    )
    with jax.named_scope("loads"):
        for c in loads[:nf]:
            c.wait()

    first = jnp.where(p == last, 1, m_all)
    rest = m_all - first
    turn = jnp.where(p < n_stage // 2, first, 0)

    def step(k, carry):
        j = k - first
        swap = j < 2 * rest
        is_u = k >= 2 * m_all
        is_f = (j < 0) | (swap & (j % 2 == 1))
        is_b = jnp.logical_not(is_f | is_u)
        m_f = jnp.where(j < 0, k, jnp.minimum(first + j // 2, m_all - 1))
        m_b = jnp.maximum(jnp.minimum(jnp.where(swap, j // 2, j - rest), m_all - 1), 0)
        u = jnp.maximum(k - 2 * m_all, 0)

        @pl.when(k == turn)
        def _():
            with jax.named_scope("transp"):
                @pl.when(p >= n_stage // 2)
                def _():
                    for c in loads[nf:]:
                        c.wait()

                transpose_weights()
                for c in kept:
                    c.start()

        @pl.when((k == first) & (p < n_stage - 2))
        def _():
            with jax.named_scope("slopes"):
                slopes()
            with jax.named_scope("hring"):
                each(0, m_all, lambda m: ring_forward(0, m, hw))

        @pl.when((k == first) & (p < n_stage // 2))
        def _():
            with jax.named_scope("pre"):
                each(0, early, lambda m: ring_arrived(m, 0))

                @pl.when(p < PRE_LATE)
                def _():
                    each(early, m_all, lambda m: ring_arrived(m, 0))

                _transposed_rows(group(hw), groups, rows, nd, ht)
                each(0, formed, pre_unit)
                for c in (*pre_stores(0), *pre_stores(1)):
                    c.wait()

        early_f, odd = is_f & (p < n_stage - 2), p % 2 == 1
        for when, sloped, split in (
            (early_f & jnp.logical_not(odd), False, False),
            (early_f & odd, False, True),
            (is_f & (p >= n_stage - 2), True, False),
        ):
            @pl.when(when)
            def _():
                with jax.named_scope("fwd"):
                    forward(m_f, sloped, split)

        leaves = (p > 0) & jnp.logical_not(odd)
        for when, split in ((is_b & leaves, True), (is_b & jnp.logical_not(leaves), False)):
            @pl.when(when)
            def _():
                with jax.named_scope("bwd"):
                    backward(m_b, split)

        @pl.when(is_u)
        def _():
            with jax.named_scope("unit"):
                unit(u)

        return carry

    lax.fori_loop(0, 2 * m_all + units, step, 0)

    with jax.named_scope("finish"):
        for c in (*kept, *part_copies(units - 2), *part_copies(units - 1), *late_copies()):
            c.wait()
    with jax.named_scope("outwait"):
        pltpu.make_async_copy(y.at[0], y.at[0], out_recv.at[0]).wait()
        pltpu.make_async_copy(dx.at[0], dx.at[0], out_recv.at[1]).wait()


def _chain(n_stage, n_inner, x, g, w1, w2):
    mb, rows, d = x.shape
    f = w1.shape[-1]
    rows = rows * MERGE
    m_all = mb * n_stage // MERGE
    early = EARLY
    nd, nf = d // LANES, f // LANES
    blk = SLABS * LANES
    groups = n_inner * early
    tokens = groups * rows
    tiles = SLABS * max(nd, groups)
    hbm = pl.BlockSpec(memory_space=pltpu.HBM)
    whole = (n_inner, m_all, nd, rows, LANES)
    late = jax.ShapeDtypeStruct((n_inner, m_all - early, nd, rows, LANES), BF16)
    dma = pltpu.SemaphoreType.DMA
    vmem = pltpu.VMEM
    return pl.pallas_call(
        functools.partial(_chain_kernel, n_stage, n_inner),
        out_shape=[
            jax.ShapeDtypeStruct(x.shape, BF16), jax.ShapeDtypeStruct(x.shape, BF16), late, late,
            jax.ShapeDtypeStruct((nf, d, LANES), BF16), jax.ShapeDtypeStruct((nf, d, LANES), BF16),
            jax.ShapeDtypeStruct((f // blk, SLABS * nd, LANES, LANES), F32),
            jax.ShapeDtypeStruct((f // blk, SLABS * nd, LANES, LANES), F32),
            jax.ShapeDtypeStruct((2 * f // blk, SLABS, tokens, LANES), BF16),
            jax.ShapeDtypeStruct((2 * f // blk, SLABS * groups, rows, LANES), F32),
        ],
        in_specs=[hbm] * 4,
        out_specs=[hbm] * 10,
        scratch_shapes=[
            vmem((nf, d, LANES), BF16), vmem((nd, f, LANES), BF16),
            vmem((nd, f, LANES), BF16), vmem((nf, d, LANES), BF16),
            vmem(whole, BF16), vmem(whole, BF16),
            vmem((m_all, nd, rows, LANES), BF16), vmem((m_all, nd, rows, LANES), BF16),
            vmem((m_all, nf, rows, LANES), F32), vmem((nf, rows, LANES), BF16),
            vmem((tokens // LANES, d, LANES), BF16),
            vmem((2, SLABS, tokens, LANES), BF16), vmem((2, tiles, LANES, LANES), F32),
            vmem((2, nd, rows // MERGE, LANES), BF16),
            dma((2,)), dma((2,)), dma((m_all,)), dma((m_all,)), dma((m_all,)), dma((m_all,)), dma((2,)),
            dma((2, m_all, 4)), dma((2, m_all, 4)), dma((2, 2)), dma((2, n_inner)), dma((2, 2)), dma((2,)), dma((2,)),
        ],
        compiler_params=pltpu.CompilerParams(
            collective_id=0, has_side_effects=True, vmem_limit_bytes=VMEM_LIMIT
        ),
        name="chain",
    )(x, g, w1, w2)


def _late_kernel(
    h, g, y_in, dx_in, w1, w2t, p1, p2, ap, sp, d1, d2, y, dx,
    hv, gv, w1v, w2v, p1v, p2v, av, sv, d1v, d2v, ht, ab, zb, yv, first_sem, load_sem, store_sem, pass_sem,
):
    groups, nd, rows, _ = h.shape
    units = w1.shape[0] // SLABS
    d, blk = d1v.shape[1:]

    def pre(j):
        return (lax.axis_index("stage") < PRE_LATE) & (j % 2 == 1)

    def weights(j):
        b, some = j % DEEP, pl.ds(j * SLABS, SLABS)
        return (pltpu.make_async_copy(w2t.at[some], w2v.at[b], load_sem.at[0, b]),)

    def own(j):
        b, some = j % DEEP, pl.ds(j * SLABS, SLABS)
        return (pltpu.make_async_copy(w1.at[some], w1v.at[b], load_sem.at[1, b]),)

    def ready(j):
        b = j % DEEP
        return (
            pltpu.make_async_copy(ap.at[units + j], av.at[b], load_sem.at[1, b]),
            pltpu.make_async_copy(sp.at[units + j], sv.at[b], load_sem.at[2, b]),
        )

    def parts(j):
        b = j % DEEP
        return (
            pltpu.make_async_copy(p1.at[j], p1v.at[b], load_sem.at[3, b]),
            pltpu.make_async_copy(p2.at[j], p2v.at[b], load_sem.at[4, b]),
        )

    def stores(j):
        b, some = j % 2, pl.ds(pl.multiple_of(j * blk, blk), blk)
        return (
            pltpu.make_async_copy(d1v.at[b], d1.at[:, some], store_sem.at[0, b]),
            pltpu.make_async_copy(d2v.at[b], d2.at[some, :], store_sem.at[1, b]),
        )

    def do(copies, how):
        for c in copies:
            getattr(c, how)()

    def inputs(j, how):
        @pl.when(pre(j))
        def _():
            do(ready(j), how)

        @pl.when(jnp.logical_not(pre(j)))
        def _():
            do(own(j), how)

        do(weights(j), how)

    firsts = (pltpu.make_async_copy(h, hv, first_sem.at[0]), pltpu.make_async_copy(g, gv, first_sem.at[1]))
    firsts[0].start()
    inputs(0, "start")
    firsts[1].start()
    do(parts(0), "start")
    for n in range(1, DEEP - 1):
        inputs(n, "start")
        do(parts(n), "start")
    into = [pltpu.make_async_copy(a, yv.at[n], pass_sem.at[n]) for n, a in enumerate((y_in, dx_in))]
    out_of = [pltpu.make_async_copy(yv.at[n], a, pass_sem.at[n]) for n, a in enumerate((y, dx))]
    do(into, "start")
    firsts[0].wait()
    _transposed_rows(lambda k, c: hv[k, c], groups, rows, nd, ht)
    do(into, "wait")
    do(out_of, "start")

    def unit(j, carry):
        b, n = j % 2, j % DEEP
        inputs(j, "wait")

        @pl.when(j == 0)
        def _():
            firsts[1].wait()

        @pl.when(j + DEEP - 1 < units)
        def _():
            inputs(j + DEEP - 1, "start")
            do(parts(j + DEEP - 1), "start")

        do(parts(j), "wait")

        @pl.when(j > 1)
        def _():
            do(stores(j), "wait")

        def put(v1, v2):
            for c in range(SLABS):
                for e in range(nd):
                    r, s = slice(e * LANES, (e + 1) * LANES), slice(c * LANES, (c + 1) * LANES)
                    d2v[b, s, r] = p2v[n, c * nd + e] + v2[s, r]
                    d1v[b, r, s] = p1v[n, c * nd + e] + v1[r, s]

        def block(ready):
            _dw_block(
                512, lambda k, c: hv[k, c], lambda k, c: gv[k, c], groups, rows, nd,
                lambda: _wide([w1v[n, c] for c in range(SLABS)]), lambda: _wide([w2v[n, c] for c in range(SLABS)]),
                ht, ab, zb, put, ready,
            )

        @pl.when(pre(j))
        def _():
            block((lambda c: av[n, c], lambda k, c: sv[n, c * groups + k]))

        @pl.when(jnp.logical_not(pre(j)))
        def _():
            block(None)

        do(stores(j), "start")
        return carry

    lax.fori_loop(0, units, unit, 0)
    do(stores(units - 2), "wait")
    do(stores(units - 1), "wait")
    do(out_of, "wait")


def _late(h, g, y, dx, w1, w2t, p1, p2, ap, sp):
    groups, nd, rows, _ = h.shape
    nf, d, _ = w1.shape
    f, blk, t = nf * LANES, SLABS * LANES, groups * rows
    hbm = pl.BlockSpec(memory_space=pltpu.HBM)
    vmem, dma = pltpu.VMEM, pltpu.SemaphoreType.DMA
    return pl.pallas_call(
        _late_kernel,
        in_specs=[hbm] * 10,
        out_specs=[hbm] * 4,
        out_shape=[
            jax.ShapeDtypeStruct((d, f), F32), jax.ShapeDtypeStruct((f, d), F32),
            jax.ShapeDtypeStruct(y.shape, BF16), jax.ShapeDtypeStruct(dx.shape, BF16),
        ],
        scratch_shapes=[
            vmem(h.shape, BF16), vmem(g.shape, BF16),
            vmem((DEEP, SLABS, d, LANES), BF16), vmem((DEEP, SLABS, d, LANES), BF16),
            vmem((DEEP, *p1.shape[1:]), F32), vmem((DEEP, *p2.shape[1:]), F32),
            vmem((DEEP, *ap.shape[1:]), BF16), vmem((DEEP, *sp.shape[1:]), F32),
            vmem((2, d, blk), F32), vmem((2, blk, d), F32),
            vmem((t // LANES, d, LANES), BF16), vmem((SLABS, t, LANES), BF16), vmem((SLABS, t, LANES), BF16),
            vmem((2, *y.shape), BF16),
            dma((2,)), dma((5, DEEP)), dma((2, 2)), dma((2,)),
        ],
        compiler_params=pltpu.CompilerParams(vmem_limit_bytes=VMEM_LIMIT),
        cost_estimate=pl.CostEstimate(flops=8 * t * d * f, bytes_accessed=20 * d * f, transcendentals=t * f),
        name="late",
    )(h, g, y, dx, w1, w2t, p1, p2, ap, sp)


def solution(mesh):
    n_stage, n_inner = mesh.shape["stage"], mesh.shape["inner"]

    def body(x, g, w1, w2):
        y, dx, h, gg, w1s, w2s, *parts = _chain(n_stage, n_inner, x, g, w1, w2)
        flat = (-1, *h.shape[2:])
        d1, d2, y, dx = _late(h.reshape(flat), gg.reshape(flat), y, dx, w1s, w2s, *parts)
        return y, dx, d1.reshape(w1.shape), d2.reshape(w2.shape)

    tok = P(("data", "stage"), "inner", None)
    wsp = P(None, "stage", None, None)
    dsp = P("data", "stage", None, None)
    return jax.shard_map(body, mesh=mesh, in_specs=(tok, tok, wsp, wsp), out_specs=(tok, tok, dsp, dsp), check_vma=False)
```

```python
import functools

import jax
import jax.numpy as jnp
from jax import lax
from jax.experimental import pallas as pl
from jax.experimental.pallas import tpu as pltpu
from jax.sharding import PartitionSpec as P

MESH = pl.DeviceIdType.MESH
F32, BF16 = jnp.float32, jnp.bfloat16
C0, C1 = 0.7978845608028654, 0.044715
LANES = 128
VMEM_LIMIT = 67043328
SLABS = 4
MERGE = 2
EARLY = 2
DEEP = 3
PRE_LATE = 2


def _gelu_and_slope(z):
    z2 = z * z
    half = 0.5 * jnp.tanh(z * (C0 + (C0 * C1) * z2)) + 0.5
    a = z * half
    return a, half + (a - a * half) * (2.0 * C0 + (6.0 * C0 * C1) * z2)


def _dot(a, b):
    return jnp.dot(a, b, preferred_element_type=F32)


def _wide(slabs):
    return jnp.concatenate(slabs, axis=1)


def _tall(parts):
    return jnp.concatenate(parts, axis=0)


def _cut(value, c):
    return value[:, c * LANES : (c + 1) * LANES]


def _rows_of(read, ks, n):
    return _tall([_wide([read(k, c) for c in range(n)]) for k in ks])


def _chunks(rows, groups, group_rows):
    step = max(1, rows // group_rows)
    for k in range(0, groups, step):
        ks = range(k, min(k + step, groups))
        yield ks, slice(k * group_rows, (k + len(ks)) * group_rows)


def _dw_block(
    rows, hg, gg, groups, group_rows, nd, w1_block, w2t_block, ht, ab, zb, put, ready=None
):
    for ks, s in _chunks(rows, groups, group_rows):
        if ready is None:
            z = _dot(_rows_of(hg, ks, nd), w1_block())
        da = _dot(_rows_of(gg, ks, nd), w2t_block())
        if ready is None:
            a, slope = _gelu_and_slope(z)
            a = a.astype(BF16)
            for c in range(SLABS):
                ab[c, s, :] = _cut(a, c)
        else:
            slope = _rows_of(ready[1], ks, SLABS)
        dz = (da * slope).astype(BF16)
        for c in range(SLABS):
            zb[c, s, :] = _cut(dz, c)
    a = _wide([ab[c] for c in range(SLABS)] if ready is None else [ready[0](c) for c in range(SLABS)])
    v2 = lax.dot_general(
        a, _rows_of(gg, range(groups), nd), (((0,), (0,)), ((), ())), preferred_element_type=F32
    )
    put(_dot(_wide([ht[t] for t in range(ht.shape[0])]), _wide([zb[c] for c in range(SLABS)])), v2)


def _transposed_rows(hg, groups, group_rows, nd, ht):
    per = LANES // group_rows
    for t in range(groups // per):
        ht[t] = _tall([_wide([hg(t * per + e, c) for c in range(nd)]) for e in range(per)]).T


def _chain_kernel(
    n_stage, n_inner, x, g, w1, w2, y, dx, h_late, g_late, w1_out, w2_out, d1_part, d2_part, a_pre, s_pre,
    w1v, w2v, w1t, w2t, hw, gw, ho, go, zs, act, ht, narrow, full, own_v,
    wsem, xsem, h_recv, g_recv, h_send, g_send, out_recv, ring_send, ring_recv, part_sem, late_sem, pre_sem, keep_sem, own_sem,
):
    p, i = lax.axis_index("stage"), lax.axis_index("inner")
    right, left = lax.rem(i + 1, n_inner), lax.rem(i + n_inner - 1, n_inner)
    _, m_all, nd, rows, _ = hw.shape
    nf = w1v.shape[0]
    units = nf // SLABS
    early = EARLY
    last = n_stage - 1
    half = nd // 2
    part = rows // MERGE
    mid = n_stage // 2
    groups = n_inner * early
    tokens = groups * rows
    ab, zb = narrow.at[0], narrow.at[1]

    def flat(ref, c):
        return ref.at[0, :, c * LANES : (c + 1) * LANES]

    mine = [
        pltpu.make_async_copy(flat(src, c), own_v.at[n, c], own_sem.at[n]) for n, src in enumerate((x, g)) for c in range(nd)
    ]
    for c in mine:
        c.start()

    barrier = pltpu.get_barrier_semaphore()
    for q in range(1, n_stage):
        pl.semaphore_signal(barrier, inc=1, device_id={"stage": lax.rem(p + q, n_stage)}, device_id_type=MESH)
    for q in (left, right):
        pl.semaphore_signal(barrier, inc=1, device_id={"inner": q}, device_id_type=MESH)

    loads = [
        pltpu.make_async_copy(w1.at[0, 0, :, c * LANES : (c + 1) * LANES], w1v.at[c], wsem.at[0]) for c in range(nf)
    ] + [pltpu.make_async_copy(w2.at[0, 0, :, c * LANES : (c + 1) * LANES], w2v.at[c], wsem.at[1]) for c in range(nd)]
    for c in loads:
        c.start()

    def to_stage(src, dst, send, recv, stage):
        return pltpu.make_async_remote_copy(
            src_ref=src, dst_ref=dst, send_sem=send, recv_sem=recv,
            device_id={"stage": stage}, device_id_type=MESH,
        )

    def to_inner(src, dst, send, recv, inner):
        return pltpu.make_async_remote_copy(
            src_ref=src, dst_ref=dst, send_sem=send, recv_sem=recv,
            device_id={"inner": inner}, device_id_type=MESH,
        )

    def piece(e):
        return pl.ds(pl.multiple_of(e * part, part), part)

    with jax.named_scope("barrier"):
        pl.semaphore_wait(barrier, n_stage + 1)
    for c in mine:
        c.wait()

    def own(mine_v, slots, recv, sem, stage):
        there = slots.at[i, p // MERGE, :, piece(p % MERGE)]

        @pl.when(p == stage)
        def _():
            pltpu.make_async_copy(mine_v, there, recv.at[p // MERGE]).start()

        @pl.when(p != stage)
        def _():
            to_stage(mine_v, there, sem, recv.at[p // MERGE], stage).start()

    own(own_v.at[0], hw, h_recv, xsem.at[0], 0)
    own(own_v.at[1], gw, g_recv, xsem.at[1], last)

    def ring_first(q, m, whole):
        a = whole.at[i, m]
        to_inner(a, a, ring_send.at[q, m, 0], ring_recv.at[q, m, 0], right).start()
        to_inner(a, a, ring_send.at[q, m, 1], ring_recv.at[q, m, 1], left).start()

    def ring_forward(q, m, whole):
        a, b = whole.at[left, m], whole.at[right, m]
        to_inner(a, a, ring_send.at[q, m, 0], ring_recv.at[q, m, 0], right).wait_recv()
        a = whole.at[left, m, pl.ds(0, half)]
        to_inner(a, a, ring_send.at[q, m, 2], ring_recv.at[q, m, 2], right).start()
        to_inner(b, b, ring_send.at[q, m, 1], ring_recv.at[q, m, 1], left).wait_recv()
        b = whole.at[right, m, pl.ds(half, half)]
        to_inner(b, b, ring_send.at[q, m, 3], ring_recv.at[q, m, 3], left).start()

    def ring_far(q, m, whole):
        far = lax.rem(i + 2, n_inner)
        a, b = whole.at[far, m, pl.ds(0, half)], whole.at[far, m, pl.ds(half, half)]
        return (
            to_inner(a, a, ring_send.at[q, m, 2], ring_recv.at[q, m, 2], right),
            to_inner(b, b, ring_send.at[q, m, 3], ring_recv.at[q, m, 3], left),
        )

    def ring_arrived(m, q):
        for c in ring_far(q, m, (hw, gw)[q]):
            c.wait_recv()

    def ring_sent(m):
        for q, whole in ((0, hw), (1, gw)):
            for c in ring_far(q, m, whole):
                c.wait_send()
            a = whole.at[i, m]
            to_inner(a, a, ring_send.at[q, m, 0], ring_recv.at[q, m, 0], right).wait_send()
            to_inner(a, a, ring_send.at[q, m, 1], ring_recv.at[q, m, 1], left).wait_send()

    def pass_on(m, lo, hi, src, slots, send, recv, end, nxt, out, out_sem):
        @pl.when(p != end)
        def _():
            some = pl.ds(lo, hi - lo)
            to_stage(src.at[m, some], slots.at[i, m, some], send.at[m], recv.at[m], nxt).start()

        if hi - lo < nd:
            return

        @pl.when(p == end)
        def _():
            for e in range(MERGE):
                home = m * MERGE + e

                @pl.when(p != home)
                def _():
                    for c in range(nd):
                        to_stage(src.at[m, c, piece(e)], flat(out, c), send.at[m], out_sem, home).start()

                @pl.when(p == home)
                def _():
                    for c in range(nd):
                        pltpu.make_async_copy(src.at[m, c, piece(e)], flat(out, c), out_sem).start()

    def project(m, split, res, w, src, *rest):
        whole = _wide([act[c] for c in range(nf)])
        count = half if split else nd
        for lo in range(0, nd, count):
            u = _dot(whole, _wide([w[lo + c] for c in range(count)]))
            out = (res[:, lo * LANES : (lo + count) * LANES].astype(F32) + u).astype(BF16)
            for c in range(count):
                src[m, lo + c] = _cut(out, c)
            pass_on(m, lo, lo + count, src, *rest)

    def forward(m, sloped, split):
        with jax.named_scope("wait_h"):
            pltpu.make_async_copy(hw.at[i, m], hw.at[i, m], h_recv.at[m]).wait()
        h = _wide([hw[i, m, c] for c in range(nd)])
        for b in range(0, nf, SLABS):
            z = _dot(h, _wide([w1v[b + c] for c in range(SLABS)]))
            a, slope = _gelu_and_slope(z)
            a, kept = a.astype(BF16), slope if sloped else z
            for c in range(SLABS):
                zs[m, b + c] = _cut(kept, c)
                act[b + c] = _cut(a, c)

        @pl.when((m == 0) & (p < n_stage // 2))
        def _():
            for c in loads[nf:]:
                c.wait()

        project(m, split, h, w2v, ho, hw, h_send, h_recv, last, jnp.minimum(p + 1, last), y, out_recv.at[0])

        @pl.when((p < mid) | (m < early))
        def _():
            ring_first(0, m, hw)

    def backward(m, split):
        with jax.named_scope("wait_g"):
            pltpu.make_async_copy(gw.at[i, m], gw.at[i, m], g_recv.at[m]).wait()

        @pl.when(m < early)
        def _():
            ring_first(1, m, gw)

        dh = _wide([gw[i, m, c] for c in range(nd)])
        for b in range(0, nf, SLABS):
            da = _dot(dh, _wide([w2t[b + c] for c in range(SLABS)]))
            dz = (da * _wide([zs[m, b + c] for c in range(SLABS)])).astype(BF16)
            for c in range(SLABS):
                act[b + c] = _cut(dz, c)
        project(m, split, dh, w1t, go, gw, g_send, g_recv, 0, jnp.maximum(p - 1, 0), dx, out_recv.at[1])

        @pl.when((p >= n_stage - 2) & (m == early))
        def _():
            ring_forward(0, 0, hw)

        @pl.when((p < mid) & (m > 0) & (m <= early))
        def _():
            ring_forward(1, jnp.maximum(m - 1, 0), gw)

        @pl.when((p >= mid) & (p < n_stage - 2) & (m == early))
        def _():
            ring_forward(1, 0, gw)

    def transpose_weights():
        def some(c, carry):
            s = pl.ds(pl.multiple_of(c * LANES, LANES), LANES)
            for e in range(nd):
                w1t[e, s, :] = w1v[c, e * LANES : (e + 1) * LANES, :].T
                w2t[c, e * LANES : (e + 1) * LANES, :] = w2v[e, s, :].T
            return carry

        lax.fori_loop(0, nf, some, 0)

    def slopes():
        def some(t, carry):
            m, b = t // (nf // SLABS), t % (nf // SLABS) * SLABS
            for c in range(SLABS):
                zs[m, b + c] = _gelu_and_slope(zs[m, b + c])[1]
            return carry

        lax.fori_loop(0, m_all * (nf // SLABS), some, 0)

    def each(lo, hi, fn):
        lax.fori_loop(lo, hi, lambda m, c: (fn(m), c)[1], 0)

    def group(whole, part=0):
        return lambda k, c: whole[k // early, part * early + k % early, c]

    def pre_stores(j):
        b = j % 2
        return (
            pltpu.make_async_copy(narrow.at[b], a_pre.at[j], pre_sem.at[0, b]),
            pltpu.make_async_copy(full.at[b, pl.ds(0, SLABS * groups)], s_pre.at[j], pre_sem.at[1, b]),
        )

    def pre_loads(j):
        b = j % 2
        return (
            pltpu.make_async_copy(
                a_pre.at[j], w2v.at[pl.ds(b * SLABS, SLABS), pl.ds(0, tokens)], pre_sem.at[0, b]
            ),
            pltpu.make_async_copy(s_pre.at[j], zs.at[b, pl.ds(0, SLABS * groups)], pre_sem.at[1, b]),
        )

    def pre_unit(j):
        b = j % 2

        @pl.when(j > 1)
        def _():
            for c in pre_stores(j):
                c.wait()

        for ks, s in _chunks(256, groups, rows):
            z = _dot(_rows_of(group(hw, j // units), ks, nd), _wide([w1v[j % units * SLABS + c] for c in range(SLABS)]))
            a, slope = _gelu_and_slope(z)
            a = a.astype(BF16)
            for c in range(SLABS):
                narrow[b, c, s, :] = _cut(a, c)
                for n, k in enumerate(ks):
                    full[b, c * groups + k] = _cut(slope[n * rows : (n + 1) * rows], c)
        for c in pre_stores(j):
            c.start()

    formed = jnp.where(
        p < PRE_LATE, 2 * units, jnp.where(p < mid - 1, units, jnp.where(p == mid - 1, units // 2, 0))
    )

    def part_copies(j):
        b, some = j % 2, pl.ds(0, SLABS * nd)
        return (
            pltpu.make_async_copy(full.at[b, some], d1_part.at[j], part_sem.at[0, b]),
            pltpu.make_async_copy(zs.at[m_all - 2 + b, some], d2_part.at[j], part_sem.at[1, b]),
        )

    def late_copies():
        return [
            pltpu.make_async_copy(whole.at[k, pl.ds(early, m_all - early)], out.at[k], late_sem.at[q, k])
            for q, (whole, out) in enumerate(((hw, h_late), (gw, g_late)))
            for k in range(n_inner)
        ]

    def sent(m):
        ring_sent(m)
        for src, slots, send, recv, end in ((ho, hw, h_send, h_recv, last), (go, gw, g_send, g_recv, 0)):
            for e in range(MERGE):
                a = src.at[m, :, piece(e)]

                @pl.when((p != end) | (p != m * MERGE + e))
                def _():
                    to_stage(a, a, send.at[m], recv.at[m], 0).wait_send()

        @pl.when((m == 0) & (p != 0))
        def _():
            to_stage(own_v.at[0], own_v.at[0], xsem.at[0], h_recv.at[0], 0).wait_send()

        @pl.when((m == 0) & (p != last))
        def _():
            to_stage(own_v.at[1], own_v.at[1], xsem.at[1], g_recv.at[0], last).wait_send()

    def unit(j):
        def forwards(m):
            @pl.when(p >= mid)
            def _():
                ring_forward(0, m, hw)

            ring_forward(1, m, gw)

        def firsts(m):
            @pl.when(p >= mid)
            def _():
                ring_first(0, m, hw)

            ring_first(1, m, gw)

        @pl.when(j == 0)
        def _():
            @pl.when(p >= n_stage - 2)
            def _():
                ring_forward(1, 0, gw)
                each(1, early, lambda e: (ring_forward(0, e, hw), ring_forward(1, e, gw)))

            @pl.when((p >= mid) & (p < n_stage - 2))
            def _():
                each(1, early, lambda e: ring_forward(1, e, gw))


            @pl.when(p < n_stage // 2)
            def _():
                for c in pre_loads(0):
                    c.start()

            each(0, early, lambda m: ring_arrived(m, 1))

            @pl.when(p >= n_stage // 2)
            def _():
                each(0, early, lambda m: ring_arrived(m, 0))

            each(early, m_all, firsts)

            @pl.when(p >= mid)
            def _():
                _transposed_rows(group(hw), groups, rows, nd, ht)

        for m in range(early, m_all):
            @pl.when(j == 2 * (m - early + 1) + jnp.where(p < mid, 0, 1))
            def _():
                forwards(m)

        @pl.when(j == units - 1)
        def _():
            each(early, m_all, lambda m: ring_arrived(m, 1))

            @pl.when(p >= PRE_LATE)
            def _():
                each(early, m_all, lambda m: ring_arrived(m, 0))

            for c in late_copies():
                c.start()
            each(0, m_all, sent)

        @pl.when(j > 1)
        def _():
            for c in part_copies(j):
                c.wait()

        def put(v1, v2):
            for c in range(SLABS):
                for e in range(nd):
                    zs[m_all - 2 + j % 2, c * nd + e] = _cut(v2[c * LANES : (c + 1) * LANES], e)
                    full[j % 2, c * nd + e] = _cut(v1[e * LANES : (e + 1) * LANES], c)

        def block(ready):
            _dw_block(
                512, group(hw), group(gw), groups, rows, nd,
                lambda: _wide([w1v[j * SLABS + c] for c in range(SLABS)]),
                lambda: _wide([w2t[j * SLABS + c] for c in range(SLABS)]),
                ht, ab, zb, put, ready,
            )

        @pl.when(j < formed)
        def _():
            b = j % 2
            for c in pre_loads(j):
                c.wait()

            @pl.when(j + 1 < jnp.minimum(formed, units))
            def _():
                for c in pre_loads(j + 1):
                    c.start()

            block((
                lambda c: w2v[b * SLABS + c, 0:tokens, :],
                lambda k, c: zs[b, c * groups + k],
            ))

        @pl.when(j >= formed)
        def _():
            block(None)

        for c in part_copies(j):
            c.start()

    kept = (
        pltpu.make_async_copy(w1v, w1_out, keep_sem.at[0]), pltpu.make_async_copy(w2t, w2_out, keep_sem.at[1])
    )
    with jax.named_scope("loads"):
        for c in loads[:nf]:
            c.wait()

    first = jnp.where(p == last, 1, m_all)
    rest = m_all - first
    turn = jnp.where(p < n_stage // 2, first, 0)

    def step(k, carry):
        j = k - first
        swap = j < 2 * rest
        is_u = k >= 2 * m_all
        is_f = (j < 0) | (swap & (j % 2 == 1))
        is_b = jnp.logical_not(is_f | is_u)
        m_f = jnp.where(j < 0, k, jnp.minimum(first + j // 2, m_all - 1))
        m_b = jnp.maximum(jnp.minimum(jnp.where(swap, j // 2, j - rest), m_all - 1), 0)
        u = jnp.maximum(k - 2 * m_all, 0)

        @pl.when(k == turn)
        def _():
            with jax.named_scope("transp"):
                @pl.when(p >= n_stage // 2)
                def _():
                    for c in loads[nf:]:
                        c.wait()

                transpose_weights()
                for c in kept:
                    c.start()

        @pl.when((k == first) & (p < n_stage - 2))
        def _():
            with jax.named_scope("slopes"):
                slopes()
            with jax.named_scope("hring"):
                each(0, jnp.where(p < mid, m_all, early), lambda m: ring_forward(0, m, hw))

        @pl.when((k == first) & (p < n_stage // 2))
        def _():
            with jax.named_scope("pre"):
                each(0, early, lambda m: ring_arrived(m, 0))

                @pl.when(p < PRE_LATE)
                def _():
                    each(early, m_all, lambda m: ring_arrived(m, 0))

                _transposed_rows(group(hw), groups, rows, nd, ht)
                each(0, formed, pre_unit)
                for c in (*pre_stores(0), *pre_stores(1)):
                    c.wait()

        early_f, odd = is_f & (p < n_stage - 2), p % 2 == 1
        for when, sloped, split in (
            (early_f & jnp.logical_not(odd), False, False),
            (early_f & odd, False, True),
            (is_f & (p >= n_stage - 2), True, False),
        ):
            @pl.when(when)
            def _():
                with jax.named_scope("fwd"):
                    forward(m_f, sloped, split)

        leaves = (p > 0) & jnp.logical_not(odd)
        for when, split in ((is_b & leaves, True), (is_b & jnp.logical_not(leaves), False)):
            @pl.when(when)
            def _():
                with jax.named_scope("bwd"):
                    backward(m_b, split)

        @pl.when(is_u)
        def _():
            with jax.named_scope("unit"):
                unit(u)

        return carry

    lax.fori_loop(0, 2 * m_all + units, step, 0)

    with jax.named_scope("finish"):
        for c in (*kept, *part_copies(units - 2), *part_copies(units - 1), *late_copies()):
            c.wait()
    with jax.named_scope("outwait"):
        pltpu.make_async_copy(y.at[0], y.at[0], out_recv.at[0]).wait()
        pltpu.make_async_copy(dx.at[0], dx.at[0], out_recv.at[1]).wait()


def _chain(n_stage, n_inner, x, g, w1, w2):
    mb, rows, d = x.shape
    f = w1.shape[-1]
    rows = rows * MERGE
    m_all = mb * n_stage // MERGE
    early = EARLY
    nd, nf = d // LANES, f // LANES
    blk = SLABS * LANES
    groups = n_inner * early
    tokens = groups * rows
    tiles = SLABS * max(nd, groups)
    hbm = pl.BlockSpec(memory_space=pltpu.HBM)
    whole = (n_inner, m_all, nd, rows, LANES)
    late = jax.ShapeDtypeStruct((n_inner, m_all - early, nd, rows, LANES), BF16)
    dma = pltpu.SemaphoreType.DMA
    vmem = pltpu.VMEM
    return pl.pallas_call(
        functools.partial(_chain_kernel, n_stage, n_inner),
        out_shape=[
            jax.ShapeDtypeStruct(x.shape, BF16), jax.ShapeDtypeStruct(x.shape, BF16), late, late,
            jax.ShapeDtypeStruct((nf, d, LANES), BF16), jax.ShapeDtypeStruct((nf, d, LANES), BF16),
            jax.ShapeDtypeStruct((f // blk, SLABS * nd, LANES, LANES), F32),
            jax.ShapeDtypeStruct((f // blk, SLABS * nd, LANES, LANES), F32),
            jax.ShapeDtypeStruct((2 * f // blk, SLABS, tokens, LANES), BF16),
            jax.ShapeDtypeStruct((2 * f // blk, SLABS * groups, rows, LANES), F32),
        ],
        in_specs=[hbm] * 4,
        out_specs=[hbm] * 10,
        scratch_shapes=[
            vmem((nf, d, LANES), BF16), vmem((nd, f, LANES), BF16),
            vmem((nd, f, LANES), BF16), vmem((nf, d, LANES), BF16),
            vmem(whole, BF16), vmem(whole, BF16),
            vmem((m_all, nd, rows, LANES), BF16), vmem((m_all, nd, rows, LANES), BF16),
            vmem((m_all, nf, rows, LANES), F32), vmem((nf, rows, LANES), BF16),
            vmem((tokens // LANES, d, LANES), BF16),
            vmem((2, SLABS, tokens, LANES), BF16), vmem((2, tiles, LANES, LANES), F32),
            vmem((2, nd, rows // MERGE, LANES), BF16),
            dma((2,)), dma((2,)), dma((m_all,)), dma((m_all,)), dma((m_all,)), dma((m_all,)), dma((2,)),
            dma((2, m_all, 4)), dma((2, m_all, 4)), dma((2, 2)), dma((2, n_inner)), dma((2, 2)), dma((2,)), dma((2,)),
        ],
        compiler_params=pltpu.CompilerParams(
            collective_id=0, has_side_effects=True, vmem_limit_bytes=VMEM_LIMIT
        ),
        name="chain",
    )(x, g, w1, w2)


def _late_kernel(
    h, g, y_in, dx_in, w1, w2t, p1, p2, ap, sp, d1, d2, y, dx,
    hv, gv, w1v, w2v, p1v, p2v, av, sv, d1v, d2v, ht, ab, zb, yv, first_sem, load_sem, store_sem, pass_sem,
):
    groups, nd, rows, _ = h.shape
    units = w1.shape[0] // SLABS
    d, blk = d1v.shape[1:]

    def pre(j):
        return (lax.axis_index("stage") < PRE_LATE) & (j % 2 == 1)

    def weights(j):
        b, some = j % DEEP, pl.ds(j * SLABS, SLABS)
        return (pltpu.make_async_copy(w2t.at[some], w2v.at[b], load_sem.at[0, b]),)

    def own(j):
        b, some = j % DEEP, pl.ds(j * SLABS, SLABS)
        return (pltpu.make_async_copy(w1.at[some], w1v.at[b], load_sem.at[1, b]),)

    def ready(j):
        b = j % DEEP
        return (
            pltpu.make_async_copy(ap.at[units + j], av.at[b], load_sem.at[1, b]),
            pltpu.make_async_copy(sp.at[units + j], sv.at[b], load_sem.at[2, b]),
        )

    def parts(j):
        b = j % DEEP
        return (
            pltpu.make_async_copy(p1.at[j], p1v.at[b], load_sem.at[3, b]),
            pltpu.make_async_copy(p2.at[j], p2v.at[b], load_sem.at[4, b]),
        )

    def stores(j):
        b, some = j % 2, pl.ds(pl.multiple_of(j * blk, blk), blk)
        return (
            pltpu.make_async_copy(d1v.at[b], d1.at[:, some], store_sem.at[0, b]),
            pltpu.make_async_copy(d2v.at[b], d2.at[some, :], store_sem.at[1, b]),
        )

    def do(copies, how):
        for c in copies:
            getattr(c, how)()

    def inputs(j, how):
        @pl.when(pre(j))
        def _():
            do(ready(j), how)

        @pl.when(jnp.logical_not(pre(j)))
        def _():
            do(own(j), how)

        do(weights(j), how)

    firsts = (pltpu.make_async_copy(h, hv, first_sem.at[0]), pltpu.make_async_copy(g, gv, first_sem.at[1]))
    firsts[0].start()
    inputs(0, "start")
    firsts[1].start()
    do(parts(0), "start")
    into = [pltpu.make_async_copy(a, yv.at[n], pass_sem.at[n]) for n, a in enumerate((y_in, dx_in))]
    out_of = [pltpu.make_async_copy(yv.at[n], a, pass_sem.at[n]) for n, a in enumerate((y, dx))]
    do(into, "start")
    firsts[0].wait()
    _transposed_rows(lambda k, c: hv[k, c], groups, rows, nd, ht)
    do(into, "wait")
    do(out_of, "start")

    def unit(j, carry):
        b, n = j % 2, j % DEEP
        inputs(j, "wait")
        do(parts(j), "wait")

        @pl.when(j == 0)
        def _():
            firsts[1].wait()
            for e in range(1, DEEP - 1):
                inputs(e, "start")
                do(parts(e), "start")

        @pl.when(j + DEEP - 1 < units)
        def _():
            inputs(j + DEEP - 1, "start")
            do(parts(j + DEEP - 1), "start")

        @pl.when(j > 1)
        def _():
            do(stores(j), "wait")

        def put(v1, v2):
            for c in range(SLABS):
                for e in range(nd):
                    r, s = slice(e * LANES, (e + 1) * LANES), slice(c * LANES, (c + 1) * LANES)
                    d2v[b, s, r] = p2v[n, c * nd + e] + v2[s, r]
                    d1v[b, r, s] = p1v[n, c * nd + e] + v1[r, s]

        def block(ready):
            _dw_block(
                512, lambda k, c: hv[k, c], lambda k, c: gv[k, c], groups, rows, nd,
                lambda: _wide([w1v[n, c] for c in range(SLABS)]), lambda: _wide([w2v[n, c] for c in range(SLABS)]),
                ht, ab, zb, put, ready,
            )

        @pl.when(pre(j))
        def _():
            block((lambda c: av[n, c], lambda k, c: sv[n, c * groups + k]))

        @pl.when(jnp.logical_not(pre(j)))
        def _():
            block(None)

        do(stores(j), "start")
        return carry

    lax.fori_loop(0, units, unit, 0)
    do(stores(units - 2), "wait")
    do(stores(units - 1), "wait")
    do(out_of, "wait")


def _late(h, g, y, dx, w1, w2t, p1, p2, ap, sp):
    groups, nd, rows, _ = h.shape
    nf, d, _ = w1.shape
    f, blk, t = nf * LANES, SLABS * LANES, groups * rows
    hbm = pl.BlockSpec(memory_space=pltpu.HBM)
    vmem, dma = pltpu.VMEM, pltpu.SemaphoreType.DMA
    return pl.pallas_call(
        _late_kernel,
        in_specs=[hbm] * 10,
        out_specs=[hbm] * 4,
        out_shape=[
            jax.ShapeDtypeStruct((d, f), F32), jax.ShapeDtypeStruct((f, d), F32),
            jax.ShapeDtypeStruct(y.shape, BF16), jax.ShapeDtypeStruct(dx.shape, BF16),
        ],
        scratch_shapes=[
            vmem(h.shape, BF16), vmem(g.shape, BF16),
            vmem((DEEP, SLABS, d, LANES), BF16), vmem((DEEP, SLABS, d, LANES), BF16),
            vmem((DEEP, *p1.shape[1:]), F32), vmem((DEEP, *p2.shape[1:]), F32),
            vmem((DEEP, *ap.shape[1:]), BF16), vmem((DEEP, *sp.shape[1:]), F32),
            vmem((2, d, blk), F32), vmem((2, blk, d), F32),
            vmem((t // LANES, d, LANES), BF16), vmem((SLABS, t, LANES), BF16), vmem((SLABS, t, LANES), BF16),
            vmem((2, *y.shape), BF16),
            dma((2,)), dma((5, DEEP)), dma((2, 2)), dma((2,)),
        ],
        compiler_params=pltpu.CompilerParams(vmem_limit_bytes=VMEM_LIMIT),
        cost_estimate=pl.CostEstimate(flops=8 * t * d * f, bytes_accessed=20 * d * f, transcendentals=t * f),
        name="late",
    )(h, g, y, dx, w1, w2t, p1, p2, ap, sp)


def solution(mesh):
    n_stage, n_inner = mesh.shape["stage"], mesh.shape["inner"]

    def body(x, g, w1, w2):
        y, dx, h, gg, w1s, w2s, *parts = _chain(n_stage, n_inner, x, g, w1, w2)
        flat = (-1, *h.shape[2:])
        d1, d2, y, dx = _late(h.reshape(flat), gg.reshape(flat), y, dx, w1s, w2s, *parts)
        return y, dx, d1.reshape(w1.shape), d2.reshape(w2.shape)

    tok = P(("data", "stage"), "inner", None)
    wsp = P(None, "stage", None, None)
    dsp = P("data", "stage", None, None)
    return jax.shard_map(body, mesh=mesh, in_specs=(tok, tok, wsp, wsp), out_specs=(tok, tok, dsp, dsp), check_vma=False)
```

```python
import functools

import jax
import jax.numpy as jnp
from jax import lax
from jax.experimental import pallas as pl
from jax.experimental.pallas import tpu as pltpu
from jax.sharding import PartitionSpec as P

MESH = pl.DeviceIdType.MESH
F32, BF16 = jnp.float32, jnp.bfloat16
C0, C1 = 0.7978845608028654, 0.044715
LANES = 128
VMEM_LIMIT = 67043328
SLABS = 4
MERGE = 2
EARLY = 2
DEEP = 3
PRE_LATE = 2


def _gelu_and_slope(z):
    z2 = z * z
    half = 0.5 * jnp.tanh(z * (C0 + (C0 * C1) * z2)) + 0.5
    a = z * half
    return a, half + (a - a * half) * (2.0 * C0 + (6.0 * C0 * C1) * z2)


def _dot(a, b):
    return jnp.dot(a, b, preferred_element_type=F32)


def _wide(slabs):
    return jnp.concatenate(slabs, axis=1)


def _tall(parts):
    return jnp.concatenate(parts, axis=0)


def _cut(value, c):
    return value[:, c * LANES : (c + 1) * LANES]


def _rows_of(read, ks, n):
    return _tall([_wide([read(k, c) for c in range(n)]) for k in ks])


def _chunks(rows, groups, group_rows):
    step = max(1, rows // group_rows)
    for k in range(0, groups, step):
        ks = range(k, min(k + step, groups))
        yield ks, slice(k * group_rows, (k + len(ks)) * group_rows)


def _dw_block(
    rows, hg, gg, groups, group_rows, nd, w1_block, w2t_block, ht, ab, zb, put, ready=None
):
    for ks, s in _chunks(rows, groups, group_rows):
        if ready is None:
            z = _dot(_rows_of(hg, ks, nd), w1_block())
        da = _dot(_rows_of(gg, ks, nd), w2t_block())
        if ready is None:
            a, slope = _gelu_and_slope(z)
            a = a.astype(BF16)
            for c in range(SLABS):
                ab[c, s, :] = _cut(a, c)
        else:
            slope = _rows_of(ready[1], ks, SLABS)
        dz = (da * slope).astype(BF16)
        for c in range(SLABS):
            zb[c, s, :] = _cut(dz, c)
    a = _wide([ab[c] for c in range(SLABS)] if ready is None else [ready[0](c) for c in range(SLABS)])
    v2 = lax.dot_general(
        a, _rows_of(gg, range(groups), nd), (((0,), (0,)), ((), ())), preferred_element_type=F32
    )
    put(_dot(_wide([ht[t] for t in range(ht.shape[0])]), _wide([zb[c] for c in range(SLABS)])), v2)


def _transposed_rows(hg, groups, group_rows, nd, ht):
    per = LANES // group_rows
    for t in range(groups // per):
        ht[t] = _tall([_wide([hg(t * per + e, c) for c in range(nd)]) for e in range(per)]).T


def _chain_kernel(
    n_stage, n_inner, x, g, w1, w2, y, dx, h_late, g_late, w1_out, w2_out, d1_part, d2_part, a_pre, s_pre,
    w1v, w2v, w1t, w2t, hw, gw, ho, go, zs, act, ht, narrow, full, own_v,
    wsem, xsem, h_recv, g_recv, h_send, g_send, out_recv, ring_send, ring_recv, part_sem, late_sem, pre_sem, keep_sem, own_sem,
):
    p, i = lax.axis_index("stage"), lax.axis_index("inner")
    right, left = lax.rem(i + 1, n_inner), lax.rem(i + n_inner - 1, n_inner)
    _, m_all, nd, rows, _ = hw.shape
    nf = w1v.shape[0]
    units = nf // SLABS
    early = EARLY
    last = n_stage - 1
    half = nd // 2
    part = rows // MERGE
    mid = n_stage // 2
    groups = n_inner * early
    tokens = groups * rows
    ab, zb = narrow.at[0], narrow.at[1]

    def flat(ref, c):
        return ref.at[0, :, c * LANES : (c + 1) * LANES]

    mine = [
        pltpu.make_async_copy(flat(src, c), own_v.at[n, c], own_sem.at[n]) for n, src in enumerate((x, g)) for c in range(nd)
    ]
    for c in mine:
        c.start()

    barrier = pltpu.get_barrier_semaphore()
    for q in range(1, n_stage):
        pl.semaphore_signal(barrier, inc=1, device_id={"stage": lax.rem(p + q, n_stage)}, device_id_type=MESH)
    for q in (left, right):
        pl.semaphore_signal(barrier, inc=1, device_id={"inner": q}, device_id_type=MESH)

    loads = [
        pltpu.make_async_copy(w1.at[0, 0, :, c * LANES : (c + 1) * LANES], w1v.at[c], wsem.at[0]) for c in range(nf)
    ] + [pltpu.make_async_copy(w2.at[0, 0, :, c * LANES : (c + 1) * LANES], w2v.at[c], wsem.at[1]) for c in range(nd)]
    for c in loads:
        c.start()

    def to_stage(src, dst, send, recv, stage):
        return pltpu.make_async_remote_copy(
            src_ref=src, dst_ref=dst, send_sem=send, recv_sem=recv,
            device_id={"stage": stage}, device_id_type=MESH,
        )

    def to_inner(src, dst, send, recv, inner):
        return pltpu.make_async_remote_copy(
            src_ref=src, dst_ref=dst, send_sem=send, recv_sem=recv,
            device_id={"inner": inner}, device_id_type=MESH,
        )

    def piece(e):
        return pl.ds(pl.multiple_of(e * part, part), part)

    with jax.named_scope("barrier"):
        pl.semaphore_wait(barrier, n_stage + 1)
    for c in mine:
        c.wait()

    def own(mine_v, slots, recv, sem, stage):
        there = slots.at[i, p // MERGE, :, piece(p % MERGE)]

        @pl.when(p == stage)
        def _():
            pltpu.make_async_copy(mine_v, there, recv.at[p // MERGE]).start()

        @pl.when(p != stage)
        def _():
            to_stage(mine_v, there, sem, recv.at[p // MERGE], stage).start()

    own(own_v.at[0], hw, h_recv, xsem.at[0], 0)
    own(own_v.at[1], gw, g_recv, xsem.at[1], last)

    def ring_first(q, m, whole):
        a = whole.at[i, m]
        to_inner(a, a, ring_send.at[q, m, 0], ring_recv.at[q, m, 0], right).start()
        to_inner(a, a, ring_send.at[q, m, 1], ring_recv.at[q, m, 1], left).start()

    def ring_forward(q, m, whole):
        a, b = whole.at[left, m], whole.at[right, m]
        to_inner(a, a, ring_send.at[q, m, 0], ring_recv.at[q, m, 0], right).wait_recv()
        a = whole.at[left, m, pl.ds(0, half)]
        to_inner(a, a, ring_send.at[q, m, 2], ring_recv.at[q, m, 2], right).start()
        to_inner(b, b, ring_send.at[q, m, 1], ring_recv.at[q, m, 1], left).wait_recv()
        b = whole.at[right, m, pl.ds(half, half)]
        to_inner(b, b, ring_send.at[q, m, 3], ring_recv.at[q, m, 3], left).start()

    def ring_far(q, m, whole):
        far = lax.rem(i + 2, n_inner)
        a, b = whole.at[far, m, pl.ds(0, half)], whole.at[far, m, pl.ds(half, half)]
        return (
            to_inner(a, a, ring_send.at[q, m, 2], ring_recv.at[q, m, 2], right),
            to_inner(b, b, ring_send.at[q, m, 3], ring_recv.at[q, m, 3], left),
        )

    def ring_arrived(m, q):
        for c in ring_far(q, m, (hw, gw)[q]):
            c.wait_recv()

    def ring_sent(m):
        for q, whole in ((0, hw), (1, gw)):
            for c in ring_far(q, m, whole):
                c.wait_send()
            a = whole.at[i, m]
            to_inner(a, a, ring_send.at[q, m, 0], ring_recv.at[q, m, 0], right).wait_send()
            to_inner(a, a, ring_send.at[q, m, 1], ring_recv.at[q, m, 1], left).wait_send()

    def pass_on(m, lo, hi, src, slots, send, recv, end, nxt, out, out_sem):
        @pl.when(p != end)
        def _():
            some = pl.ds(lo, hi - lo)
            to_stage(src.at[m, some], slots.at[i, m, some], send.at[m], recv.at[m], nxt).start()

        if hi - lo < nd:
            return

        @pl.when(p == end)
        def _():
            for e in range(MERGE):
                home = m * MERGE + e

                @pl.when(p != home)
                def _():
                    for c in range(nd):
                        to_stage(src.at[m, c, piece(e)], flat(out, c), send.at[m], out_sem, home).start()

                @pl.when(p == home)
                def _():
                    for c in range(nd):
                        pltpu.make_async_copy(src.at[m, c, piece(e)], flat(out, c), out_sem).start()

    def project(m, split, res, w, src, *rest):
        whole = _wide([act[c] for c in range(nf)])
        count = half if split else nd
        for lo in range(0, nd, count):
            u = _dot(whole, _wide([w[lo + c] for c in range(count)]))
            out = (res[:, lo * LANES : (lo + count) * LANES].astype(F32) + u).astype(BF16)
            for c in range(count):
                src[m, lo + c] = _cut(out, c)
            pass_on(m, lo, lo + count, src, *rest)

    def forward(m, sloped, split):
        with jax.named_scope("wait_h"):
            pltpu.make_async_copy(hw.at[i, m], hw.at[i, m], h_recv.at[m]).wait()
        h = _wide([hw[i, m, c] for c in range(nd)])
        for b in range(0, nf, SLABS):
            z = _dot(h, _wide([w1v[b + c] for c in range(SLABS)]))
            a, slope = _gelu_and_slope(z)
            a, kept = a.astype(BF16), slope if sloped else z
            for c in range(SLABS):
                zs[m, b + c] = _cut(kept, c)
                act[b + c] = _cut(a, c)

        @pl.when((m == 0) & (p < n_stage // 2))
        def _():
            for c in loads[nf:]:
                c.wait()

        project(m, split, h, w2v, ho, hw, h_send, h_recv, last, jnp.minimum(p + 1, last), y, out_recv.at[0])

        @pl.when((p < mid) | (m < early))
        def _():
            ring_first(0, m, hw)

    def backward(m, split):
        @pl.when((p >= mid) & (p < n_stage - 2) & (m == early + 1))
        def _():
            ring_forward(1, early - 1, gw)

        with jax.named_scope("wait_g"):
            pltpu.make_async_copy(gw.at[i, m], gw.at[i, m], g_recv.at[m]).wait()

        @pl.when(m < early)
        def _():
            ring_first(1, m, gw)

        dh = _wide([gw[i, m, c] for c in range(nd)])
        for b in range(0, nf, SLABS):
            da = _dot(dh, _wide([w2t[b + c] for c in range(SLABS)]))
            dz = (da * _wide([zs[m, b + c] for c in range(SLABS)])).astype(BF16)
            for c in range(SLABS):
                act[b + c] = _cut(dz, c)
        project(m, split, dh, w1t, go, gw, g_send, g_recv, 0, jnp.maximum(p - 1, 0), dx, out_recv.at[1])

        @pl.when((p >= n_stage - 2) & (m == early))
        def _():
            ring_forward(0, 0, hw)

        @pl.when((p < mid) & (m > 0) & (m <= early))
        def _():
            ring_forward(1, jnp.maximum(m - 1, 0), gw)

        @pl.when((p >= mid) & (p < n_stage - 2) & (m == early))
        def _():
            ring_forward(1, 0, gw)

    def transpose_weights():
        def some(c, carry):
            s = pl.ds(pl.multiple_of(c * LANES, LANES), LANES)
            for e in range(nd):
                w1t[e, s, :] = w1v[c, e * LANES : (e + 1) * LANES, :].T
                w2t[c, e * LANES : (e + 1) * LANES, :] = w2v[e, s, :].T
            return carry

        lax.fori_loop(0, nf, some, 0)

    def slopes():
        def some(t, carry):
            m, b = t // (nf // SLABS), t % (nf // SLABS) * SLABS
            for c in range(SLABS):
                zs[m, b + c] = _gelu_and_slope(zs[m, b + c])[1]
            return carry

        lax.fori_loop(0, m_all * (nf // SLABS), some, 0)

    def each(lo, hi, fn):
        lax.fori_loop(lo, hi, lambda m, c: (fn(m), c)[1], 0)

    def group(whole, part=0):
        return lambda k, c: whole[k // early, part * early + k % early, c]

    def pre_stores(j):
        b = j % 2
        return (
            pltpu.make_async_copy(narrow.at[b], a_pre.at[j], pre_sem.at[0, b]),
            pltpu.make_async_copy(full.at[b, pl.ds(0, SLABS * groups)], s_pre.at[j], pre_sem.at[1, b]),
        )

    def pre_loads(j):
        b = j % 2
        return (
            pltpu.make_async_copy(
                a_pre.at[j], w2v.at[pl.ds(b * SLABS, SLABS), pl.ds(0, tokens)], pre_sem.at[0, b]
            ),
            pltpu.make_async_copy(s_pre.at[j], zs.at[b, pl.ds(0, SLABS * groups)], pre_sem.at[1, b]),
        )

    def pre_unit(j):
        b = j % 2

        @pl.when(j > 1)
        def _():
            for c in pre_stores(j):
                c.wait()

        for ks, s in _chunks(256, groups, rows):
            z = _dot(_rows_of(group(hw, j // units), ks, nd), _wide([w1v[j % units * SLABS + c] for c in range(SLABS)]))
            a, slope = _gelu_and_slope(z)
            a = a.astype(BF16)
            for c in range(SLABS):
                narrow[b, c, s, :] = _cut(a, c)
                for n, k in enumerate(ks):
                    full[b, c * groups + k] = _cut(slope[n * rows : (n + 1) * rows], c)
        for c in pre_stores(j):
            c.start()

    formed = jnp.where(
        p < PRE_LATE, 2 * units, jnp.where(p < mid - 1, units, jnp.where(p == mid - 1, units // 2, 0))
    )

    def part_copies(j):
        b, some = j % 2, pl.ds(0, SLABS * nd)
        return (
            pltpu.make_async_copy(full.at[b, some], d1_part.at[j], part_sem.at[0, b]),
            pltpu.make_async_copy(zs.at[m_all - 2 + b, some], d2_part.at[j], part_sem.at[1, b]),
        )

    def late_copies():
        return [
            pltpu.make_async_copy(whole.at[k, pl.ds(early, m_all - early)], out.at[k], late_sem.at[q, k])
            for q, (whole, out) in enumerate(((hw, h_late), (gw, g_late)))
            for k in range(n_inner)
        ]

    def sent(m):
        ring_sent(m)
        for src, slots, send, recv, end in ((ho, hw, h_send, h_recv, last), (go, gw, g_send, g_recv, 0)):
            for e in range(MERGE):
                a = src.at[m, :, piece(e)]

                @pl.when((p != end) | (p != m * MERGE + e))
                def _():
                    to_stage(a, a, send.at[m], recv.at[m], 0).wait_send()

        @pl.when((m == 0) & (p != 0))
        def _():
            to_stage(own_v.at[0], own_v.at[0], xsem.at[0], h_recv.at[0], 0).wait_send()

        @pl.when((m == 0) & (p != last))
        def _():
            to_stage(own_v.at[1], own_v.at[1], xsem.at[1], g_recv.at[0], last).wait_send()

    def unit(j):
        def forwards(m):
            @pl.when(p >= mid)
            def _():
                ring_forward(0, m, hw)

            ring_forward(1, m, gw)

        def firsts(m):
            @pl.when(p >= mid)
            def _():
                ring_first(0, m, hw)

            ring_first(1, m, gw)

        @pl.when(j == 0)
        def _():
            @pl.when(p >= n_stage - 2)
            def _():
                ring_forward(1, 0, gw)
                each(1, early, lambda e: (ring_forward(0, e, hw), ring_forward(1, e, gw)))


            @pl.when(p < n_stage // 2)
            def _():
                for c in pre_loads(0):
                    c.start()

            each(0, early, lambda m: ring_arrived(m, 1))

            @pl.when(p >= n_stage // 2)
            def _():
                each(0, early, lambda m: ring_arrived(m, 0))

            each(early, m_all, firsts)

            @pl.when(p >= mid)
            def _():
                _transposed_rows(group(hw), groups, rows, nd, ht)

        for m in range(early, m_all):
            @pl.when(j == 2 * (m - early + 1) + jnp.where(p < mid, 0, 1))
            def _():
                forwards(m)

        @pl.when(j == units - 1)
        def _():
            each(early, m_all, lambda m: ring_arrived(m, 1))

            @pl.when(p >= PRE_LATE)
            def _():
                each(early, m_all, lambda m: ring_arrived(m, 0))

            for c in late_copies():
                c.start()
            each(0, m_all, sent)

        @pl.when(j > 1)
        def _():
            for c in part_copies(j):
                c.wait()

        def put(v1, v2):
            for c in range(SLABS):
                for e in range(nd):
                    zs[m_all - 2 + j % 2, c * nd + e] = _cut(v2[c * LANES : (c + 1) * LANES], e)
                    full[j % 2, c * nd + e] = _cut(v1[e * LANES : (e + 1) * LANES], c)

        def block(ready):
            _dw_block(
                512, group(hw), group(gw), groups, rows, nd,
                lambda: _wide([w1v[j * SLABS + c] for c in range(SLABS)]),
                lambda: _wide([w2t[j * SLABS + c] for c in range(SLABS)]),
                ht, ab, zb, put, ready,
            )

        @pl.when(j < formed)
        def _():
            b = j % 2
            for c in pre_loads(j):
                c.wait()

            @pl.when(j + 1 < jnp.minimum(formed, units))
            def _():
                for c in pre_loads(j + 1):
                    c.start()

            block((
                lambda c: w2v[b * SLABS + c, 0:tokens, :],
                lambda k, c: zs[b, c * groups + k],
            ))

        @pl.when(j >= formed)
        def _():
            block(None)

        for c in part_copies(j):
            c.start()

    kept = (
        pltpu.make_async_copy(w1v, w1_out, keep_sem.at[0]), pltpu.make_async_copy(w2t, w2_out, keep_sem.at[1])
    )
    with jax.named_scope("loads"):
        for c in loads[:nf]:
            c.wait()

    first = jnp.where(p == last, 1, m_all)
    rest = m_all - first
    turn = jnp.where(p < n_stage // 2, first, 0)

    def step(k, carry):
        j = k - first
        swap = j < 2 * rest
        is_u = k >= 2 * m_all
        is_f = (j < 0) | (swap & (j % 2 == 1))
        is_b = jnp.logical_not(is_f | is_u)
        m_f = jnp.where(j < 0, k, jnp.minimum(first + j // 2, m_all - 1))
        m_b = jnp.maximum(jnp.minimum(jnp.where(swap, j // 2, j - rest), m_all - 1), 0)
        u = jnp.maximum(k - 2 * m_all, 0)

        @pl.when(k == turn)
        def _():
            with jax.named_scope("transp"):
                @pl.when(p >= n_stage // 2)
                def _():
                    for c in loads[nf:]:
                        c.wait()

                transpose_weights()
                for c in kept:
                    c.start()

        @pl.when((k == first) & (p < n_stage - 2))
        def _():
            with jax.named_scope("slopes"):
                slopes()
            with jax.named_scope("hring"):
                each(0, jnp.where(p < mid, m_all, early), lambda m: ring_forward(0, m, hw))

        @pl.when((k == first) & (p < n_stage // 2))
        def _():
            with jax.named_scope("pre"):
                each(0, early, lambda m: ring_arrived(m, 0))

                @pl.when(p < PRE_LATE)
                def _():
                    each(early, m_all, lambda m: ring_arrived(m, 0))

                _transposed_rows(group(hw), groups, rows, nd, ht)
                each(0, formed, pre_unit)
                for c in (*pre_stores(0), *pre_stores(1)):
                    c.wait()

        early_f, odd = is_f & (p < n_stage - 2), p % 2 == 1
        for when, sloped, split in (
            (early_f & jnp.logical_not(odd), False, False),
            (early_f & odd, False, True),
            (is_f & (p >= n_stage - 2), True, False),
        ):
            @pl.when(when)
            def _():
                with jax.named_scope("fwd"):
                    forward(m_f, sloped, split)

        leaves = (p > 0) & jnp.logical_not(odd)
        for when, split in ((is_b & leaves, True), (is_b & jnp.logical_not(leaves), False)):
            @pl.when(when)
            def _():
                with jax.named_scope("bwd"):
                    backward(m_b, split)

        @pl.when(is_u)
        def _():
            with jax.named_scope("unit"):
                unit(u)

        return carry

    lax.fori_loop(0, 2 * m_all + units, step, 0)

    with jax.named_scope("finish"):
        for c in (*kept, *part_copies(units - 2), *part_copies(units - 1), *late_copies()):
            c.wait()
    with jax.named_scope("outwait"):
        pltpu.make_async_copy(y.at[0], y.at[0], out_recv.at[0]).wait()
        pltpu.make_async_copy(dx.at[0], dx.at[0], out_recv.at[1]).wait()


def _chain(n_stage, n_inner, x, g, w1, w2):
    mb, rows, d = x.shape
    f = w1.shape[-1]
    rows = rows * MERGE
    m_all = mb * n_stage // MERGE
    early = EARLY
    nd, nf = d // LANES, f // LANES
    blk = SLABS * LANES
    groups = n_inner * early
    tokens = groups * rows
    tiles = SLABS * max(nd, groups)
    hbm = pl.BlockSpec(memory_space=pltpu.HBM)
    whole = (n_inner, m_all, nd, rows, LANES)
    late = jax.ShapeDtypeStruct((n_inner, m_all - early, nd, rows, LANES), BF16)
    dma = pltpu.SemaphoreType.DMA
    vmem = pltpu.VMEM
    return pl.pallas_call(
        functools.partial(_chain_kernel, n_stage, n_inner),
        out_shape=[
            jax.ShapeDtypeStruct(x.shape, BF16), jax.ShapeDtypeStruct(x.shape, BF16), late, late,
            jax.ShapeDtypeStruct((nf, d, LANES), BF16), jax.ShapeDtypeStruct((nf, d, LANES), BF16),
            jax.ShapeDtypeStruct((f // blk, SLABS * nd, LANES, LANES), F32),
            jax.ShapeDtypeStruct((f // blk, SLABS * nd, LANES, LANES), F32),
            jax.ShapeDtypeStruct((2 * f // blk, SLABS, tokens, LANES), BF16),
            jax.ShapeDtypeStruct((2 * f // blk, SLABS * groups, rows, LANES), F32),
        ],
        in_specs=[hbm] * 4,
        out_specs=[hbm] * 10,
        scratch_shapes=[
            vmem((nf, d, LANES), BF16), vmem((nd, f, LANES), BF16),
            vmem((nd, f, LANES), BF16), vmem((nf, d, LANES), BF16),
            vmem(whole, BF16), vmem(whole, BF16),
            vmem((m_all, nd, rows, LANES), BF16), vmem((m_all, nd, rows, LANES), BF16),
            vmem((m_all, nf, rows, LANES), F32), vmem((nf, rows, LANES), BF16),
            vmem((tokens // LANES, d, LANES), BF16),
            vmem((2, SLABS, tokens, LANES), BF16), vmem((2, tiles, LANES, LANES), F32),
            vmem((2, nd, rows // MERGE, LANES), BF16),
            dma((2,)), dma((2,)), dma((m_all,)), dma((m_all,)), dma((m_all,)), dma((m_all,)), dma((2,)),
            dma((2, m_all, 4)), dma((2, m_all, 4)), dma((2, 2)), dma((2, n_inner)), dma((2, 2)), dma((2,)), dma((2,)),
        ],
        compiler_params=pltpu.CompilerParams(
            collective_id=0, has_side_effects=True, vmem_limit_bytes=VMEM_LIMIT
        ),
        name="chain",
    )(x, g, w1, w2)


def _late_kernel(
    h, g, y_in, dx_in, w1, w2t, p1, p2, ap, sp, d1, d2, y, dx,
    hv, gv, w1v, w2v, p1v, p2v, av, sv, d1v, d2v, ht, ab, zb, yv, first_sem, load_sem, store_sem, pass_sem,
):
    groups, nd, rows, _ = h.shape
    units = w1.shape[0] // SLABS
    d, blk = d1v.shape[1:]

    def pre(j):
        return (lax.axis_index("stage") < PRE_LATE) & (j % 2 == 1)

    def weights(j):
        b, some = j % DEEP, pl.ds(j * SLABS, SLABS)
        return (pltpu.make_async_copy(w2t.at[some], w2v.at[b], load_sem.at[0, b]),)

    def own(j):
        b, some = j % DEEP, pl.ds(j * SLABS, SLABS)
        return (pltpu.make_async_copy(w1.at[some], w1v.at[b], load_sem.at[1, b]),)

    def ready(j):
        b = j % DEEP
        return (
            pltpu.make_async_copy(ap.at[units + j], av.at[b], load_sem.at[1, b]),
            pltpu.make_async_copy(sp.at[units + j], sv.at[b], load_sem.at[2, b]),
        )

    def parts(j):
        b = j % DEEP
        return (
            pltpu.make_async_copy(p1.at[j], p1v.at[b], load_sem.at[3, b]),
            pltpu.make_async_copy(p2.at[j], p2v.at[b], load_sem.at[4, b]),
        )

    def stores(j):
        b, some = j % 2, pl.ds(pl.multiple_of(j * blk, blk), blk)
        return (
            pltpu.make_async_copy(d1v.at[b], d1.at[:, some], store_sem.at[0, b]),
            pltpu.make_async_copy(d2v.at[b], d2.at[some, :], store_sem.at[1, b]),
        )

    def do(copies, how):
        for c in copies:
            getattr(c, how)()

    def inputs(j, how):
        @pl.when(pre(j))
        def _():
            do(ready(j), how)

        @pl.when(jnp.logical_not(pre(j)))
        def _():
            do(own(j), how)

        do(weights(j), how)

    firsts = (pltpu.make_async_copy(h, hv, first_sem.at[0]), pltpu.make_async_copy(g, gv, first_sem.at[1]))
    firsts[0].start()
    inputs(0, "start")
    firsts[1].start()
    do(parts(0), "start")
    into = [pltpu.make_async_copy(a, yv.at[n], pass_sem.at[n]) for n, a in enumerate((y_in, dx_in))]
    out_of = [pltpu.make_async_copy(yv.at[n], a, pass_sem.at[n]) for n, a in enumerate((y, dx))]
    do(into, "start")
    firsts[0].wait()
    _transposed_rows(lambda k, c: hv[k, c], groups, rows, nd, ht)
    do(into, "wait")
    do(out_of, "start")

    def unit(j, carry):
        b, n = j % 2, j % DEEP
        inputs(j, "wait")
        do(parts(j), "wait")

        @pl.when(j == 0)
        def _():
            firsts[1].wait()
            for e in range(1, DEEP - 1):
                inputs(e, "start")
                do(parts(e), "start")

        @pl.when(j + DEEP - 1 < units)
        def _():
            inputs(j + DEEP - 1, "start")
            do(parts(j + DEEP - 1), "start")

        @pl.when(j > 1)
        def _():
            do(stores(j), "wait")

        def put(v1, v2):
            for c in range(SLABS):
                for e in range(nd):
                    r, s = slice(e * LANES, (e + 1) * LANES), slice(c * LANES, (c + 1) * LANES)
                    d2v[b, s, r] = p2v[n, c * nd + e] + v2[s, r]
                    d1v[b, r, s] = p1v[n, c * nd + e] + v1[r, s]

        def block(ready):
            _dw_block(
                512, lambda k, c: hv[k, c], lambda k, c: gv[k, c], groups, rows, nd,
                lambda: _wide([w1v[n, c] for c in range(SLABS)]), lambda: _wide([w2v[n, c] for c in range(SLABS)]),
                ht, ab, zb, put, ready,
            )

        @pl.when(pre(j))
        def _():
            block((lambda c: av[n, c], lambda k, c: sv[n, c * groups + k]))

        @pl.when(jnp.logical_not(pre(j)))
        def _():
            block(None)

        do(stores(j), "start")
        return carry

    lax.fori_loop(0, units, unit, 0)
    do(stores(units - 2), "wait")
    do(stores(units - 1), "wait")
    do(out_of, "wait")


def _late(h, g, y, dx, w1, w2t, p1, p2, ap, sp):
    groups, nd, rows, _ = h.shape
    nf, d, _ = w1.shape
    f, blk, t = nf * LANES, SLABS * LANES, groups * rows
    hbm = pl.BlockSpec(memory_space=pltpu.HBM)
    vmem, dma = pltpu.VMEM, pltpu.SemaphoreType.DMA
    return pl.pallas_call(
        _late_kernel,
        in_specs=[hbm] * 10,
        out_specs=[hbm] * 4,
        out_shape=[
            jax.ShapeDtypeStruct((d, f), F32), jax.ShapeDtypeStruct((f, d), F32),
            jax.ShapeDtypeStruct(y.shape, BF16), jax.ShapeDtypeStruct(dx.shape, BF16),
        ],
        scratch_shapes=[
            vmem(h.shape, BF16), vmem(g.shape, BF16),
            vmem((DEEP, SLABS, d, LANES), BF16), vmem((DEEP, SLABS, d, LANES), BF16),
            vmem((DEEP, *p1.shape[1:]), F32), vmem((DEEP, *p2.shape[1:]), F32),
            vmem((DEEP, *ap.shape[1:]), BF16), vmem((DEEP, *sp.shape[1:]), F32),
            vmem((2, d, blk), F32), vmem((2, blk, d), F32),
            vmem((t // LANES, d, LANES), BF16), vmem((SLABS, t, LANES), BF16), vmem((SLABS, t, LANES), BF16),
            vmem((2, *y.shape), BF16),
            dma((2,)), dma((5, DEEP)), dma((2, 2)), dma((2,)),
        ],
        compiler_params=pltpu.CompilerParams(vmem_limit_bytes=VMEM_LIMIT),
        cost_estimate=pl.CostEstimate(flops=8 * t * d * f, bytes_accessed=20 * d * f, transcendentals=t * f),
        name="late",
    )(h, g, y, dx, w1, w2t, p1, p2, ap, sp)


def solution(mesh):
    n_stage, n_inner = mesh.shape["stage"], mesh.shape["inner"]

    def body(x, g, w1, w2):
        y, dx, h, gg, w1s, w2s, *parts = _chain(n_stage, n_inner, x, g, w1, w2)
        flat = (-1, *h.shape[2:])
        d1, d2, y, dx = _late(h.reshape(flat), gg.reshape(flat), y, dx, w1s, w2s, *parts)
        return y, dx, d1.reshape(w1.shape), d2.reshape(w2.shape)

    tok = P(("data", "stage"), "inner", None)
    wsp = P(None, "stage", None, None)
    dsp = P("data", "stage", None, None)
    return jax.shard_map(body, mesh=mesh, in_specs=(tok, tok, wsp, wsp), out_specs=(tok, tok, dsp, dsp), check_vma=False)
```

```python
import functools

import jax
import jax.numpy as jnp
from jax import lax
from jax.experimental import pallas as pl
from jax.experimental.pallas import tpu as pltpu
from jax.sharding import PartitionSpec as P

MESH = pl.DeviceIdType.MESH
F32, BF16 = jnp.float32, jnp.bfloat16
C0, C1 = 0.7978845608028654, 0.044715
LANES = 128
VMEM_LIMIT = 67043328
SLABS = 4
MERGE = 2
EARLY = 2
DEEP = 3
PRE_LATE = 2


def _gelu_and_slope(z):
    z2 = z * z
    half = 0.5 * jnp.tanh(z * (C0 + (C0 * C1) * z2)) + 0.5
    a = z * half
    return a, half + (a - a * half) * (2.0 * C0 + (6.0 * C0 * C1) * z2)


def _dot(a, b):
    return jnp.dot(a, b, preferred_element_type=F32)


def _wide(slabs):
    return jnp.concatenate(slabs, axis=1)


def _tall(parts):
    return jnp.concatenate(parts, axis=0)


def _cut(value, c):
    return value[:, c * LANES : (c + 1) * LANES]


def _rows_of(read, ks, n):
    return _tall([_wide([read(k, c) for c in range(n)]) for k in ks])


def _chunks(rows, groups, group_rows):
    step = max(1, rows // group_rows)
    for k in range(0, groups, step):
        ks = range(k, min(k + step, groups))
        yield ks, slice(k * group_rows, (k + len(ks)) * group_rows)


def _dw_block(
    rows, hg, gg, groups, group_rows, nd, w1_block, w2t_block, ht, ab, zb, put, ready=None
):
    for ks, s in _chunks(rows, groups, group_rows):
        if ready is None:
            z = _dot(_rows_of(hg, ks, nd), w1_block())
        da = _dot(_rows_of(gg, ks, nd), w2t_block())
        if ready is None:
            a, slope = _gelu_and_slope(z)
            a = a.astype(BF16)
            for c in range(SLABS):
                ab[c, s, :] = _cut(a, c)
        else:
            slope = _rows_of(ready[1], ks, SLABS)
        dz = (da * slope).astype(BF16)
        for c in range(SLABS):
            zb[c, s, :] = _cut(dz, c)
    a = _wide([ab[c] for c in range(SLABS)] if ready is None else [ready[0](c) for c in range(SLABS)])
    v2 = lax.dot_general(
        a, _rows_of(gg, range(groups), nd), (((0,), (0,)), ((), ())), preferred_element_type=F32
    )
    put(_dot(_wide([ht[t] for t in range(ht.shape[0])]), _wide([zb[c] for c in range(SLABS)])), v2)


def _transposed_rows(hg, groups, group_rows, nd, ht):
    per = LANES // group_rows
    for t in range(groups // per):
        ht[t] = _tall([_wide([hg(t * per + e, c) for c in range(nd)]) for e in range(per)]).T


def _chain_kernel(
    n_stage, n_inner, x, g, w1, w2, y, dx, h_late, g_late, w1_out, w2_out, d1_part, d2_part, a_pre, s_pre,
    w1v, w2v, w1t, w2t, hw, gw, ho, go, zs, act, ht, narrow, full, own_v,
    wsem, xsem, h_recv, g_recv, h_send, g_send, out_recv, ring_send, ring_recv, part_sem, late_sem, pre_sem, keep_sem, own_sem,
):
    p, i = lax.axis_index("stage"), lax.axis_index("inner")
    right, left = lax.rem(i + 1, n_inner), lax.rem(i + n_inner - 1, n_inner)
    _, m_all, nd, rows, _ = hw.shape
    nf = w1v.shape[0]
    units = nf // SLABS
    early = EARLY
    last = n_stage - 1
    half = nd // 2
    part = rows // MERGE
    mid = n_stage // 2
    groups = n_inner * early
    tokens = groups * rows
    ab, zb = narrow.at[0], narrow.at[1]

    def flat(ref, c):
        return ref.at[0, :, c * LANES : (c + 1) * LANES]

    mine = [
        pltpu.make_async_copy(flat(src, c), own_v.at[n, c], own_sem.at[n]) for n, src in enumerate((x, g)) for c in range(nd)
    ]
    for c in mine:
        c.start()

    barrier = pltpu.get_barrier_semaphore()
    for q in range(1, n_stage):
        pl.semaphore_signal(barrier, inc=1, device_id={"stage": lax.rem(p + q, n_stage)}, device_id_type=MESH)
    for q in (left, right):
        pl.semaphore_signal(barrier, inc=1, device_id={"inner": q}, device_id_type=MESH)

    loads = [
        pltpu.make_async_copy(w1.at[0, 0, :, c * LANES : (c + 1) * LANES], w1v.at[c], wsem.at[0]) for c in range(nf)
    ] + [pltpu.make_async_copy(w2.at[0, 0, :, c * LANES : (c + 1) * LANES], w2v.at[c], wsem.at[1]) for c in range(nd)]
    for c in loads:
        c.start()

    def to_stage(src, dst, send, recv, stage):
        return pltpu.make_async_remote_copy(
            src_ref=src, dst_ref=dst, send_sem=send, recv_sem=recv,
            device_id={"stage": stage}, device_id_type=MESH,
        )

    def to_inner(src, dst, send, recv, inner):
        return pltpu.make_async_remote_copy(
            src_ref=src, dst_ref=dst, send_sem=send, recv_sem=recv,
            device_id={"inner": inner}, device_id_type=MESH,
        )

    def piece(e):
        return pl.ds(pl.multiple_of(e * part, part), part)

    with jax.named_scope("barrier"):
        pl.semaphore_wait(barrier, n_stage + 1)
    for c in mine:
        c.wait()

    def own(mine_v, slots, recv, sem, stage):
        there = slots.at[i, p // MERGE, :, piece(p % MERGE)]

        @pl.when(p == stage)
        def _():
            pltpu.make_async_copy(mine_v, there, recv.at[p // MERGE]).start()

        @pl.when(p != stage)
        def _():
            to_stage(mine_v, there, sem, recv.at[p // MERGE], stage).start()

    own(own_v.at[0], hw, h_recv, xsem.at[0], 0)
    own(own_v.at[1], gw, g_recv, xsem.at[1], last)

    def ring_first(q, m, whole):
        a = whole.at[i, m]
        to_inner(a, a, ring_send.at[q, m, 0], ring_recv.at[q, m, 0], right).start()
        to_inner(a, a, ring_send.at[q, m, 1], ring_recv.at[q, m, 1], left).start()

    def forward_right(q, m, whole):
        a = whole.at[left, m]
        to_inner(a, a, ring_send.at[q, m, 0], ring_recv.at[q, m, 0], right).wait_recv()
        a = whole.at[left, m, pl.ds(0, half)]
        to_inner(a, a, ring_send.at[q, m, 2], ring_recv.at[q, m, 2], right).start()

    def forward_left(q, m, whole):
        b = whole.at[right, m]
        to_inner(b, b, ring_send.at[q, m, 1], ring_recv.at[q, m, 1], left).wait_recv()
        b = whole.at[right, m, pl.ds(half, half)]
        to_inner(b, b, ring_send.at[q, m, 3], ring_recv.at[q, m, 3], left).start()

    def ring_forward(q, m, whole):
        forward_right(q, m, whole)
        forward_left(q, m, whole)

    def ring_far(q, m, whole):
        far = lax.rem(i + 2, n_inner)
        a, b = whole.at[far, m, pl.ds(0, half)], whole.at[far, m, pl.ds(half, half)]
        return (
            to_inner(a, a, ring_send.at[q, m, 2], ring_recv.at[q, m, 2], right),
            to_inner(b, b, ring_send.at[q, m, 3], ring_recv.at[q, m, 3], left),
        )

    def ring_arrived(m, q):
        for c in ring_far(q, m, (hw, gw)[q]):
            c.wait_recv()

    def ring_sent(m):
        for q, whole in ((0, hw), (1, gw)):
            for c in ring_far(q, m, whole):
                c.wait_send()
            a = whole.at[i, m]
            to_inner(a, a, ring_send.at[q, m, 0], ring_recv.at[q, m, 0], right).wait_send()
            to_inner(a, a, ring_send.at[q, m, 1], ring_recv.at[q, m, 1], left).wait_send()

    def pass_on(m, lo, hi, src, slots, send, recv, end, nxt, out, out_sem):
        @pl.when(p != end)
        def _():
            some = pl.ds(lo, hi - lo)
            to_stage(src.at[m, some], slots.at[i, m, some], send.at[m], recv.at[m], nxt).start()

        if hi - lo < nd:
            return

        @pl.when(p == end)
        def _():
            for e in range(MERGE):
                home = m * MERGE + e

                @pl.when(p != home)
                def _():
                    for c in range(nd):
                        to_stage(src.at[m, c, piece(e)], flat(out, c), send.at[m], out_sem, home).start()

                @pl.when(p == home)
                def _():
                    for c in range(nd):
                        pltpu.make_async_copy(src.at[m, c, piece(e)], flat(out, c), out_sem).start()

    def project(m, split, res, w, src, *rest):
        whole = _wide([act[c] for c in range(nf)])
        count = half if split else nd
        for lo in range(0, nd, count):
            u = _dot(whole, _wide([w[lo + c] for c in range(count)]))
            out = (res[:, lo * LANES : (lo + count) * LANES].astype(F32) + u).astype(BF16)
            for c in range(count):
                src[m, lo + c] = _cut(out, c)
            pass_on(m, lo, lo + count, src, *rest)

    def forward(m, sloped, split):
        with jax.named_scope("wait_h"):
            pltpu.make_async_copy(hw.at[i, m], hw.at[i, m], h_recv.at[m]).wait()
        h = _wide([hw[i, m, c] for c in range(nd)])
        for b in range(0, nf, SLABS):
            z = _dot(h, _wide([w1v[b + c] for c in range(SLABS)]))
            a, slope = _gelu_and_slope(z)
            a, kept = a.astype(BF16), slope if sloped else z
            for c in range(SLABS):
                zs[m, b + c] = _cut(kept, c)
                act[b + c] = _cut(a, c)

        @pl.when((m == 0) & (p < n_stage // 2))
        def _():
            for c in loads[nf:]:
                c.wait()

        project(m, split, h, w2v, ho, hw, h_send, h_recv, last, jnp.minimum(p + 1, last), y, out_recv.at[0])

        @pl.when((p < mid) | (m < early))
        def _():
            ring_first(0, m, hw)

    def backward(m, split):
        @pl.when((p >= mid) & (p < n_stage - 2) & (m == early + 1))
        def _():
            ring_forward(1, early - 1, gw)

        @pl.when((p < mid) & (m == 1))
        def _():
            forward_right(1, 0, gw)

        with jax.named_scope("wait_g"):
            pltpu.make_async_copy(gw.at[i, m], gw.at[i, m], g_recv.at[m]).wait()

        @pl.when(m < early)
        def _():
            ring_first(1, m, gw)

        dh = _wide([gw[i, m, c] for c in range(nd)])
        for b in range(0, nf, SLABS):
            da = _dot(dh, _wide([w2t[b + c] for c in range(SLABS)]))
            dz = (da * _wide([zs[m, b + c] for c in range(SLABS)])).astype(BF16)
            for c in range(SLABS):
                act[b + c] = _cut(dz, c)
        project(m, split, dh, w1t, go, gw, g_send, g_recv, 0, jnp.maximum(p - 1, 0), dx, out_recv.at[1])

        @pl.when((p >= n_stage - 2) & (m == early))
        def _():
            ring_forward(0, 0, hw)

        @pl.when((p < mid) & (m > 1) & (m <= early))
        def _():
            forward_right(1, jnp.maximum(m - 1, 0), gw)

        @pl.when((p < mid) & (m > 0) & (m <= early))
        def _():
            forward_left(1, jnp.maximum(m - 1, 0), gw)

        @pl.when((p >= mid) & (p < n_stage - 2) & (m == early))
        def _():
            ring_forward(1, 0, gw)

    def transpose_weights():
        def some(c, carry):
            s = pl.ds(pl.multiple_of(c * LANES, LANES), LANES)
            for e in range(nd):
                w1t[e, s, :] = w1v[c, e * LANES : (e + 1) * LANES, :].T
                w2t[c, e * LANES : (e + 1) * LANES, :] = w2v[e, s, :].T
            return carry

        lax.fori_loop(0, nf, some, 0)

    def slopes():
        def some(t, carry):
            m, b = t // (nf // SLABS), t % (nf // SLABS) * SLABS
            for c in range(SLABS):
                zs[m, b + c] = _gelu_and_slope(zs[m, b + c])[1]
            return carry

        lax.fori_loop(0, m_all * (nf // SLABS), some, 0)

    def each(lo, hi, fn):
        lax.fori_loop(lo, hi, lambda m, c: (fn(m), c)[1], 0)

    def group(whole, part=0):
        return lambda k, c: whole[k // early, part * early + k % early, c]

    def pre_stores(j):
        b = j % 2
        return (
            pltpu.make_async_copy(narrow.at[b], a_pre.at[j], pre_sem.at[0, b]),
            pltpu.make_async_copy(full.at[b, pl.ds(0, SLABS * groups)], s_pre.at[j], pre_sem.at[1, b]),
        )

    def pre_loads(j):
        b = j % 2
        return (
            pltpu.make_async_copy(
                a_pre.at[j], w2v.at[pl.ds(b * SLABS, SLABS), pl.ds(0, tokens)], pre_sem.at[0, b]
            ),
            pltpu.make_async_copy(s_pre.at[j], zs.at[b, pl.ds(0, SLABS * groups)], pre_sem.at[1, b]),
        )

    def pre_unit(j):
        b = j % 2

        @pl.when(j > 1)
        def _():
            for c in pre_stores(j):
                c.wait()

        for ks, s in _chunks(256, groups, rows):
            z = _dot(_rows_of(group(hw, j // units), ks, nd), _wide([w1v[j % units * SLABS + c] for c in range(SLABS)]))
            a, slope = _gelu_and_slope(z)
            a = a.astype(BF16)
            for c in range(SLABS):
                narrow[b, c, s, :] = _cut(a, c)
                for n, k in enumerate(ks):
                    full[b, c * groups + k] = _cut(slope[n * rows : (n + 1) * rows], c)
        for c in pre_stores(j):
            c.start()

    formed = jnp.where(
        p < PRE_LATE, 2 * units,
        jnp.where(p < mid - 1, units, jnp.where(p == mid - 1, units * 3 // 4, jnp.where(p == mid, units // 2, 0))),
    )

    def part_copies(j):
        b, some = j % 2, pl.ds(0, SLABS * nd)
        return (
            pltpu.make_async_copy(full.at[b, some], d1_part.at[j], part_sem.at[0, b]),
            pltpu.make_async_copy(zs.at[m_all - 2 + b, some], d2_part.at[j], part_sem.at[1, b]),
        )

    def late_copies():
        return [
            pltpu.make_async_copy(whole.at[k, pl.ds(early, m_all - early)], out.at[k], late_sem.at[q, k])
            for q, (whole, out) in enumerate(((hw, h_late), (gw, g_late)))
            for k in range(n_inner)
        ]

    def sent(m):
        ring_sent(m)
        for src, slots, send, recv, end in ((ho, hw, h_send, h_recv, last), (go, gw, g_send, g_recv, 0)):
            for e in range(MERGE):
                a = src.at[m, :, piece(e)]

                @pl.when((p != end) | (p != m * MERGE + e))
                def _():
                    to_stage(a, a, send.at[m], recv.at[m], 0).wait_send()

        @pl.when((m == 0) & (p != 0))
        def _():
            to_stage(own_v.at[0], own_v.at[0], xsem.at[0], h_recv.at[0], 0).wait_send()

        @pl.when((m == 0) & (p != last))
        def _():
            to_stage(own_v.at[1], own_v.at[1], xsem.at[1], g_recv.at[0], last).wait_send()

    def unit(j):
        def forwards(m):
            @pl.when(p >= mid)
            def _():
                ring_forward(0, m, hw)

            ring_forward(1, m, gw)

        def firsts(m):
            @pl.when(p >= mid)
            def _():
                ring_first(0, m, hw)

            ring_first(1, m, gw)

        @pl.when(j == 0)
        def _():
            @pl.when(p >= n_stage - 2)
            def _():
                ring_forward(1, 0, gw)
                each(1, early, lambda e: (ring_forward(0, e, hw), ring_forward(1, e, gw)))


            @pl.when(formed > 0)
            def _():
                for c in pre_loads(0):
                    c.start()

            each(0, early, lambda m: ring_arrived(m, 1))

            @pl.when(formed == 0)
            def _():
                each(0, early, lambda m: ring_arrived(m, 0))

            each(early, m_all, firsts)

            @pl.when(formed == 0)
            def _():
                _transposed_rows(group(hw), groups, rows, nd, ht)

        for m in range(early, m_all):
            @pl.when(j == 2 * (m - early + 1) + jnp.where(p < mid, 0, 1))
            def _():
                forwards(m)

        @pl.when(j == units - 1)
        def _():
            each(early, m_all, lambda m: ring_arrived(m, 1))

            @pl.when(p >= PRE_LATE)
            def _():
                each(early, m_all, lambda m: ring_arrived(m, 0))

            for c in late_copies():
                c.start()
            each(0, m_all, sent)

        @pl.when(j > 1)
        def _():
            for c in part_copies(j):
                c.wait()

        def put(v1, v2):
            for c in range(SLABS):
                for e in range(nd):
                    zs[m_all - 2 + j % 2, c * nd + e] = _cut(v2[c * LANES : (c + 1) * LANES], e)
                    full[j % 2, c * nd + e] = _cut(v1[e * LANES : (e + 1) * LANES], c)

        def block(ready):
            _dw_block(
                512, group(hw), group(gw), groups, rows, nd,
                lambda: _wide([w1v[j * SLABS + c] for c in range(SLABS)]),
                lambda: _wide([w2t[j * SLABS + c] for c in range(SLABS)]),
                ht, ab, zb, put, ready,
            )

        @pl.when(j < formed)
        def _():
            b = j % 2
            for c in pre_loads(j):
                c.wait()

            @pl.when(j + 1 < jnp.minimum(formed, units))
            def _():
                for c in pre_loads(j + 1):
                    c.start()

            block((
                lambda c: w2v[b * SLABS + c, 0:tokens, :],
                lambda k, c: zs[b, c * groups + k],
            ))

        @pl.when(j >= formed)
        def _():
            block(None)

        for c in part_copies(j):
            c.start()

    kept = (
        pltpu.make_async_copy(w1v, w1_out, keep_sem.at[0]), pltpu.make_async_copy(w2t, w2_out, keep_sem.at[1])
    )
    with jax.named_scope("loads"):
        for c in loads[:nf]:
            c.wait()

    first = jnp.where(p == last, 1, m_all)
    rest = m_all - first
    turn = jnp.where(p < n_stage // 2, first, 0)

    def step(k, carry):
        j = k - first
        swap = j < 2 * rest
        is_u = k >= 2 * m_all
        is_f = (j < 0) | (swap & (j % 2 == 1))
        is_b = jnp.logical_not(is_f | is_u)
        m_f = jnp.where(j < 0, k, jnp.minimum(first + j // 2, m_all - 1))
        m_b = jnp.maximum(jnp.minimum(jnp.where(swap, j // 2, j - rest), m_all - 1), 0)
        u = jnp.maximum(k - 2 * m_all, 0)

        @pl.when(k == turn)
        def _():
            with jax.named_scope("transp"):
                @pl.when(p >= n_stage // 2)
                def _():
                    for c in loads[nf:]:
                        c.wait()

                transpose_weights()
                for c in kept:
                    c.start()

        @pl.when((k == first) & (p < n_stage - 2))
        def _():
            with jax.named_scope("slopes"):
                slopes()
            with jax.named_scope("hring"):
                each(0, jnp.where(p < mid, m_all, early), lambda m: ring_forward(0, m, hw))

        @pl.when((k == first) & (formed > 0))
        def _():
            with jax.named_scope("pre"):
                each(0, early, lambda m: ring_arrived(m, 0))

                @pl.when(p < PRE_LATE)
                def _():
                    each(early, m_all, lambda m: ring_arrived(m, 0))

                _transposed_rows(group(hw), groups, rows, nd, ht)
                each(0, formed, pre_unit)
                for c in (*pre_stores(0), *pre_stores(1)):
                    c.wait()

        early_f, odd = is_f & (p < n_stage - 2), p % 2 == 1
        for when, sloped, split in (
            (early_f & jnp.logical_not(odd), False, False),
            (early_f & odd, False, True),
            (is_f & (p >= n_stage - 2), True, False),
        ):
            @pl.when(when)
            def _():
                with jax.named_scope("fwd"):
                    forward(m_f, sloped, split)

        leaves = (p > 0) & jnp.logical_not(odd)
        for when, split in ((is_b & leaves, True), (is_b & jnp.logical_not(leaves), False)):
            @pl.when(when)
            def _():
                with jax.named_scope("bwd"):
                    backward(m_b, split)

        @pl.when(is_u)
        def _():
            with jax.named_scope("unit"):
                unit(u)

        return carry

    lax.fori_loop(0, 2 * m_all + units, step, 0)

    with jax.named_scope("finish"):
        for c in (*kept, *part_copies(units - 2), *part_copies(units - 1), *late_copies()):
            c.wait()
    with jax.named_scope("outwait"):
        pltpu.make_async_copy(y.at[0], y.at[0], out_recv.at[0]).wait()
        pltpu.make_async_copy(dx.at[0], dx.at[0], out_recv.at[1]).wait()


def _chain(n_stage, n_inner, x, g, w1, w2):
    mb, rows, d = x.shape
    f = w1.shape[-1]
    rows = rows * MERGE
    m_all = mb * n_stage // MERGE
    early = EARLY
    nd, nf = d // LANES, f // LANES
    blk = SLABS * LANES
    groups = n_inner * early
    tokens = groups * rows
    tiles = SLABS * max(nd, groups)
    hbm = pl.BlockSpec(memory_space=pltpu.HBM)
    whole = (n_inner, m_all, nd, rows, LANES)
    late = jax.ShapeDtypeStruct((n_inner, m_all - early, nd, rows, LANES), BF16)
    dma = pltpu.SemaphoreType.DMA
    vmem = pltpu.VMEM
    return pl.pallas_call(
        functools.partial(_chain_kernel, n_stage, n_inner),
        out_shape=[
            jax.ShapeDtypeStruct(x.shape, BF16), jax.ShapeDtypeStruct(x.shape, BF16), late, late,
            jax.ShapeDtypeStruct((nf, d, LANES), BF16), jax.ShapeDtypeStruct((nf, d, LANES), BF16),
            jax.ShapeDtypeStruct((f // blk, SLABS * nd, LANES, LANES), F32),
            jax.ShapeDtypeStruct((f // blk, SLABS * nd, LANES, LANES), F32),
            jax.ShapeDtypeStruct((2 * f // blk, SLABS, tokens, LANES), BF16),
            jax.ShapeDtypeStruct((2 * f // blk, SLABS * groups, rows, LANES), F32),
        ],
        in_specs=[hbm] * 4,
        out_specs=[hbm] * 10,
        scratch_shapes=[
            vmem((nf, d, LANES), BF16), vmem((nd, f, LANES), BF16),
            vmem((nd, f, LANES), BF16), vmem((nf, d, LANES), BF16),
            vmem(whole, BF16), vmem(whole, BF16),
            vmem((m_all, nd, rows, LANES), BF16), vmem((m_all, nd, rows, LANES), BF16),
            vmem((m_all, nf, rows, LANES), F32), vmem((nf, rows, LANES), BF16),
            vmem((tokens // LANES, d, LANES), BF16),
            vmem((2, SLABS, tokens, LANES), BF16), vmem((2, tiles, LANES, LANES), F32),
            vmem((2, nd, rows // MERGE, LANES), BF16),
            dma((2,)), dma((2,)), dma((m_all,)), dma((m_all,)), dma((m_all,)), dma((m_all,)), dma((2,)),
            dma((2, m_all, 4)), dma((2, m_all, 4)), dma((2, 2)), dma((2, n_inner)), dma((2, 2)), dma((2,)), dma((2,)),
        ],
        compiler_params=pltpu.CompilerParams(
            collective_id=0, has_side_effects=True, vmem_limit_bytes=VMEM_LIMIT
        ),
        name="chain",
    )(x, g, w1, w2)


def _late_kernel(
    h, g, y_in, dx_in, w1, w2t, p1, p2, ap, sp, d1, d2, y, dx,
    hv, gv, w1v, w2v, p1v, p2v, av, sv, d1v, d2v, ht, ab, zb, yv, first_sem, load_sem, store_sem, pass_sem,
):
    groups, nd, rows, _ = h.shape
    units = w1.shape[0] // SLABS
    d, blk = d1v.shape[1:]

    def pre(j):
        return (lax.axis_index("stage") < PRE_LATE) & (j % 2 == 1)

    def weights(j):
        b, some = j % DEEP, pl.ds(j * SLABS, SLABS)
        return (pltpu.make_async_copy(w2t.at[some], w2v.at[b], load_sem.at[0, b]),)

    def own(j):
        b, some = j % DEEP, pl.ds(j * SLABS, SLABS)
        return (pltpu.make_async_copy(w1.at[some], w1v.at[b], load_sem.at[1, b]),)

    def ready(j):
        b = j % DEEP
        return (
            pltpu.make_async_copy(ap.at[units + j], av.at[b], load_sem.at[1, b]),
            pltpu.make_async_copy(sp.at[units + j], sv.at[b], load_sem.at[2, b]),
        )

    def parts(j):
        b = j % DEEP
        return (
            pltpu.make_async_copy(p1.at[j], p1v.at[b], load_sem.at[3, b]),
            pltpu.make_async_copy(p2.at[j], p2v.at[b], load_sem.at[4, b]),
        )

    def stores(j):
        b, some = j % 2, pl.ds(pl.multiple_of(j * blk, blk), blk)
        return (
            pltpu.make_async_copy(d1v.at[b], d1.at[:, some], store_sem.at[0, b]),
            pltpu.make_async_copy(d2v.at[b], d2.at[some, :], store_sem.at[1, b]),
        )

    def do(copies, how):
        for c in copies:
            getattr(c, how)()

    def inputs(j, how):
        @pl.when(pre(j))
        def _():
            do(ready(j), how)

        @pl.when(jnp.logical_not(pre(j)))
        def _():
            do(own(j), how)

        do(weights(j), how)

    firsts = (pltpu.make_async_copy(h, hv, first_sem.at[0]), pltpu.make_async_copy(g, gv, first_sem.at[1]))
    firsts[0].start()
    inputs(0, "start")
    firsts[1].start()
    do(parts(0), "start")
    into = [pltpu.make_async_copy(a, yv.at[n], pass_sem.at[n]) for n, a in enumerate((y_in, dx_in))]
    out_of = [pltpu.make_async_copy(yv.at[n], a, pass_sem.at[n]) for n, a in enumerate((y, dx))]
    do(into, "start")
    firsts[0].wait()
    _transposed_rows(lambda k, c: hv[k, c], groups, rows, nd, ht)
    do(into, "wait")
    do(out_of, "start")

    def unit(j, carry):
        b, n = j % 2, j % DEEP
        inputs(j, "wait")
        do(parts(j), "wait")

        @pl.when(j == 0)
        def _():
            firsts[1].wait()
            for e in range(1, DEEP - 1):
                inputs(e, "start")
                do(parts(e), "start")

        @pl.when(j + DEEP - 1 < units)
        def _():
            inputs(j + DEEP - 1, "start")
            do(parts(j + DEEP - 1), "start")

        @pl.when(j > 1)
        def _():
            do(stores(j), "wait")

        def put(v1, v2):
            for c in range(SLABS):
                for e in range(nd):
                    r, s = slice(e * LANES, (e + 1) * LANES), slice(c * LANES, (c + 1) * LANES)
                    d2v[b, s, r] = p2v[n, c * nd + e] + v2[s, r]
                    d1v[b, r, s] = p1v[n, c * nd + e] + v1[r, s]

        def block(ready):
            _dw_block(
                512, lambda k, c: hv[k, c], lambda k, c: gv[k, c], groups, rows, nd,
                lambda: _wide([w1v[n, c] for c in range(SLABS)]), lambda: _wide([w2v[n, c] for c in range(SLABS)]),
                ht, ab, zb, put, ready,
            )

        @pl.when(pre(j))
        def _():
            block((lambda c: av[n, c], lambda k, c: sv[n, c * groups + k]))

        @pl.when(jnp.logical_not(pre(j)))
        def _():
            block(None)

        do(stores(j), "start")
        return carry

    lax.fori_loop(0, units, unit, 0)
    do(stores(units - 2), "wait")
    do(stores(units - 1), "wait")
    do(out_of, "wait")


def _late(h, g, y, dx, w1, w2t, p1, p2, ap, sp):
    groups, nd, rows, _ = h.shape
    nf, d, _ = w1.shape
    f, blk, t = nf * LANES, SLABS * LANES, groups * rows
    hbm = pl.BlockSpec(memory_space=pltpu.HBM)
    vmem, dma = pltpu.VMEM, pltpu.SemaphoreType.DMA
    return pl.pallas_call(
        _late_kernel,
        in_specs=[hbm] * 10,
        out_specs=[hbm] * 4,
        out_shape=[
            jax.ShapeDtypeStruct((d, f), F32), jax.ShapeDtypeStruct((f, d), F32),
            jax.ShapeDtypeStruct(y.shape, BF16), jax.ShapeDtypeStruct(dx.shape, BF16),
        ],
        scratch_shapes=[
            vmem(h.shape, BF16), vmem(g.shape, BF16),
            vmem((DEEP, SLABS, d, LANES), BF16), vmem((DEEP, SLABS, d, LANES), BF16),
            vmem((DEEP, *p1.shape[1:]), F32), vmem((DEEP, *p2.shape[1:]), F32),
            vmem((DEEP, *ap.shape[1:]), BF16), vmem((DEEP, *sp.shape[1:]), F32),
            vmem((2, d, blk), F32), vmem((2, blk, d), F32),
            vmem((t // LANES, d, LANES), BF16), vmem((SLABS, t, LANES), BF16), vmem((SLABS, t, LANES), BF16),
            vmem((2, *y.shape), BF16),
            dma((2,)), dma((5, DEEP)), dma((2, 2)), dma((2,)),
        ],
        compiler_params=pltpu.CompilerParams(vmem_limit_bytes=VMEM_LIMIT),
        cost_estimate=pl.CostEstimate(flops=8 * t * d * f, bytes_accessed=20 * d * f, transcendentals=t * f),
        name="late",
    )(h, g, y, dx, w1, w2t, p1, p2, ap, sp)


def solution(mesh):
    n_stage, n_inner = mesh.shape["stage"], mesh.shape["inner"]

    def body(x, g, w1, w2):
        y, dx, h, gg, w1s, w2s, *parts = _chain(n_stage, n_inner, x, g, w1, w2)
        flat = (-1, *h.shape[2:])
        d1, d2, y, dx = _late(h.reshape(flat), gg.reshape(flat), y, dx, w1s, w2s, *parts)
        return y, dx, d1.reshape(w1.shape), d2.reshape(w2.shape)

    tok = P(("data", "stage"), "inner", None)
    wsp = P(None, "stage", None, None)
    dsp = P("data", "stage", None, None)
    return jax.shard_map(body, mesh=mesh, in_specs=(tok, tok, wsp, wsp), out_specs=(tok, tok, dsp, dsp), check_vma=False)
```

```python
import functools

import jax
import jax.numpy as jnp
from jax import lax
from jax.experimental import pallas as pl
from jax.experimental.pallas import tpu as pltpu
from jax.sharding import PartitionSpec as P

MESH = pl.DeviceIdType.MESH
F32, BF16 = jnp.float32, jnp.bfloat16
C0, C1 = 0.7978845608028654, 0.044715
LANES = 128
VMEM_LIMIT = 67043328
SLABS = 4
MERGE = 2
EARLY = 2
DEEP = 3
PRE_LATE = 2


def _gelu_and_slope(z):
    z2 = z * z
    half = 0.5 * jnp.tanh(z * (C0 + (C0 * C1) * z2)) + 0.5
    a = z * half
    return a, half + (a - a * half) * (2.0 * C0 + (6.0 * C0 * C1) * z2)


def _dot(a, b):
    return jnp.dot(a, b, preferred_element_type=F32)


def _wide(slabs):
    return jnp.concatenate(slabs, axis=1)


def _tall(parts):
    return jnp.concatenate(parts, axis=0)


def _cut(value, c):
    return value[:, c * LANES : (c + 1) * LANES]


def _rows_of(read, ks, n):
    return _tall([_wide([read(k, c) for c in range(n)]) for k in ks])


def _chunks(rows, groups, group_rows):
    step = max(1, rows // group_rows)
    for k in range(0, groups, step):
        ks = range(k, min(k + step, groups))
        yield ks, slice(k * group_rows, (k + len(ks)) * group_rows)


def _dw_block(
    rows, hg, gg, groups, group_rows, nd, w1_block, w2t_block, ht, ab, zb, put, ready=None
):
    for ks, s in _chunks(rows, groups, group_rows):
        if ready is None:
            z = _dot(_rows_of(hg, ks, nd), w1_block())
        da = _dot(_rows_of(gg, ks, nd), w2t_block())
        if ready is None:
            a, slope = _gelu_and_slope(z)
            a = a.astype(BF16)
            for c in range(SLABS):
                ab[c, s, :] = _cut(a, c)
        else:
            slope = _rows_of(ready[1], ks, SLABS)
        dz = (da * slope).astype(BF16)
        for c in range(SLABS):
            zb[c, s, :] = _cut(dz, c)
    a = _wide([ab[c] for c in range(SLABS)] if ready is None else [ready[0](c) for c in range(SLABS)])
    v2 = lax.dot_general(
        a, _rows_of(gg, range(groups), nd), (((0,), (0,)), ((), ())), preferred_element_type=F32
    )
    put(_dot(_wide([ht[t] for t in range(ht.shape[0])]), _wide([zb[c] for c in range(SLABS)])), v2)


def _transposed_rows(hg, groups, group_rows, nd, ht):
    per = LANES // group_rows
    for t in range(groups // per):
        ht[t] = _tall([_wide([hg(t * per + e, c) for c in range(nd)]) for e in range(per)]).T


def _chain_kernel(
    n_stage, n_inner, x, g, w1, w2, y, dx, h_late, g_late, w1_out, w2_out, d1_part, d2_part, a_pre, s_pre,
    w1v, w2v, w1t, w2t, hw, gw, ho, go, zs, act, ht, narrow, full, own_v,
    wsem, xsem, h_recv, g_recv, h_send, g_send, out_recv, ring_send, ring_recv, part_sem, late_sem, pre_sem, keep_sem, own_sem,
):
    p, i = lax.axis_index("stage"), lax.axis_index("inner")
    right, left = lax.rem(i + 1, n_inner), lax.rem(i + n_inner - 1, n_inner)
    _, m_all, nd, rows, _ = hw.shape
    nf = w1v.shape[0]
    units = nf // SLABS
    early = EARLY
    last = n_stage - 1
    half = nd // 2
    part = rows // MERGE
    mid = n_stage // 2
    groups = n_inner * early
    tokens = groups * rows
    ab, zb = narrow.at[0], narrow.at[1]

    def flat(ref, c):
        return ref.at[0, :, c * LANES : (c + 1) * LANES]

    mine = [
        pltpu.make_async_copy(flat(src, c), own_v.at[n, c], own_sem.at[n]) for n, src in enumerate((x, g)) for c in range(nd)
    ]
    for c in mine:
        c.start()

    barrier = pltpu.get_barrier_semaphore()
    for q in range(1, n_stage):
        pl.semaphore_signal(barrier, inc=1, device_id={"stage": lax.rem(p + q, n_stage)}, device_id_type=MESH)
    for q in (left, right):
        pl.semaphore_signal(barrier, inc=1, device_id={"inner": q}, device_id_type=MESH)

    loads = [
        pltpu.make_async_copy(w1.at[0, 0, :, c * LANES : (c + 1) * LANES], w1v.at[c], wsem.at[0]) for c in range(nf)
    ] + [pltpu.make_async_copy(w2.at[0, 0, :, c * LANES : (c + 1) * LANES], w2v.at[c], wsem.at[1]) for c in range(nd)]
    for c in loads:
        c.start()

    def to_stage(src, dst, send, recv, stage):
        return pltpu.make_async_remote_copy(
            src_ref=src, dst_ref=dst, send_sem=send, recv_sem=recv,
            device_id={"stage": stage}, device_id_type=MESH,
        )

    def to_inner(src, dst, send, recv, inner):
        return pltpu.make_async_remote_copy(
            src_ref=src, dst_ref=dst, send_sem=send, recv_sem=recv,
            device_id={"inner": inner}, device_id_type=MESH,
        )

    def piece(e):
        return pl.ds(pl.multiple_of(e * part, part), part)

    with jax.named_scope("barrier"):
        pl.semaphore_wait(barrier, n_stage + 1)
    for c in mine:
        c.wait()

    def own(mine_v, slots, recv, sem, stage):
        there = slots.at[i, p // MERGE, :, piece(p % MERGE)]

        @pl.when(p == stage)
        def _():
            pltpu.make_async_copy(mine_v, there, recv.at[p // MERGE]).start()

        @pl.when(p != stage)
        def _():
            to_stage(mine_v, there, sem, recv.at[p // MERGE], stage).start()

    own(own_v.at[0], hw, h_recv, xsem.at[0], 0)
    own(own_v.at[1], gw, g_recv, xsem.at[1], last)

    def ring_first(q, m, whole):
        a = whole.at[i, m]
        to_inner(a, a, ring_send.at[q, m, 0], ring_recv.at[q, m, 0], right).start()
        to_inner(a, a, ring_send.at[q, m, 1], ring_recv.at[q, m, 1], left).start()

    def forward_right(q, m, whole):
        a = whole.at[left, m]
        to_inner(a, a, ring_send.at[q, m, 0], ring_recv.at[q, m, 0], right).wait_recv()
        a = whole.at[left, m, pl.ds(0, half)]
        to_inner(a, a, ring_send.at[q, m, 2], ring_recv.at[q, m, 2], right).start()

    def forward_left(q, m, whole):
        b = whole.at[right, m]
        to_inner(b, b, ring_send.at[q, m, 1], ring_recv.at[q, m, 1], left).wait_recv()
        b = whole.at[right, m, pl.ds(half, half)]
        to_inner(b, b, ring_send.at[q, m, 3], ring_recv.at[q, m, 3], left).start()

    def ring_forward(q, m, whole):
        forward_right(q, m, whole)
        forward_left(q, m, whole)

    def ring_far(q, m, whole):
        far = lax.rem(i + 2, n_inner)
        a, b = whole.at[far, m, pl.ds(0, half)], whole.at[far, m, pl.ds(half, half)]
        return (
            to_inner(a, a, ring_send.at[q, m, 2], ring_recv.at[q, m, 2], right),
            to_inner(b, b, ring_send.at[q, m, 3], ring_recv.at[q, m, 3], left),
        )

    def ring_arrived(m, q):
        for c in ring_far(q, m, (hw, gw)[q]):
            c.wait_recv()

    def ring_sent(m):
        for q, whole in ((0, hw), (1, gw)):
            for c in ring_far(q, m, whole):
                c.wait_send()
            a = whole.at[i, m]
            to_inner(a, a, ring_send.at[q, m, 0], ring_recv.at[q, m, 0], right).wait_send()
            to_inner(a, a, ring_send.at[q, m, 1], ring_recv.at[q, m, 1], left).wait_send()

    def pass_on(m, lo, hi, src, slots, send, recv, end, nxt, out, out_sem):
        @pl.when(p != end)
        def _():
            some = pl.ds(lo, hi - lo)
            to_stage(src.at[m, some], slots.at[i, m, some], send.at[m], recv.at[m], nxt).start()

        if hi - lo < nd:
            return

        @pl.when(p == end)
        def _():
            for e in range(MERGE):
                home = m * MERGE + e

                @pl.when(p != home)
                def _():
                    for c in range(nd):
                        to_stage(src.at[m, c, piece(e)], flat(out, c), send.at[m], out_sem, home).start()

                @pl.when(p == home)
                def _():
                    for c in range(nd):
                        pltpu.make_async_copy(src.at[m, c, piece(e)], flat(out, c), out_sem).start()

    def step_of(m, split, x_in, wa, activate, second, wb, src, *rest):
        blocks, k_half = nf // SLABS, nf // 2
        early_acts = blocks // 2 if second is None else blocks - 1
        zs_in = []

        def act_of(b):
            a = activate(b * SLABS, zs_in[b])
            for c in range(SLABS):
                act[b * SLABS + c] = _cut(a, c)

        def part_dot(lo, count, k):
            a = _wide([act[k + c] for c in range(k_half)])
            return _dot(a, _wide([wb[lo + c, k * LANES : (k + k_half) * LANES, :] for c in range(count)]))

        for b in range(blocks):
            zs_in.append(_dot(x_in, _wide([wa[b * SLABS + c] for c in range(SLABS)])))
            if 0 < b <= early_acts:
                act_of(b - 1)
        if second is not None:
            act_of(blocks - 1)
            second()
        count = half if split else nd
        for lo in range(0, nd, count):
            u = part_dot(lo, count, 0)
            if lo == 0 and second is None:
                for b in range(early_acts, blocks):
                    act_of(b)
            u = u + part_dot(lo, count, k_half)
            out = (x_in[:, lo * LANES : (lo + count) * LANES].astype(F32) + u).astype(BF16)
            for c in range(count):
                src[m, lo + c] = _cut(out, c)
            pass_on(m, lo, lo + count, src, *rest)

    def second_weights():
        for c in loads[nf:]:
            c.wait()

    def forward(m, sloped, split):
        @pl.when((m == 0) & (p > 0) & (p < mid))
        def _():
            second_weights()

        with jax.named_scope("wait_h"):
            pltpu.make_async_copy(hw.at[i, m], hw.at[i, m], h_recv.at[m]).wait()
        h = _wide([hw[i, m, c] for c in range(nd)])

        def activate(b, z):
            a, slope = _gelu_and_slope(z)
            for c in range(SLABS):
                zs[m, b + c] = _cut(slope if sloped else z, c)
            return a.astype(BF16)

        def second():
            @pl.when((m == 0) & (p == 0))
            def _():
                second_weights()

        step_of(
            m, split, h, w1v, activate, None if sloped or split else second, w2v,
            ho, hw, h_send, h_recv, last, jnp.minimum(p + 1, last), y, out_recv.at[0],
        )

        @pl.when((p < mid) | (m < early))
        def _():
            ring_first(0, m, hw)

    def backward(m, split):
        @pl.when((p >= mid) & (p < n_stage - 2) & (m == early + 1))
        def _():
            ring_forward(1, early - 1, gw)

        with jax.named_scope("wait_g"):
            pltpu.make_async_copy(gw.at[i, m], gw.at[i, m], g_recv.at[m]).wait()

        @pl.when(m < early)
        def _():
            ring_first(1, m, gw)

        dh = _wide([gw[i, m, c] for c in range(nd)])
        step_of(
            m, split, dh, w2t, lambda b, da: (da * _wide([zs[m, b + c] for c in range(SLABS)])).astype(BF16), None,
            w1t, go, gw, g_send, g_recv, 0, jnp.maximum(p - 1, 0), dx, out_recv.at[1],
        )

        @pl.when((p >= n_stage - 2) & (m == early))
        def _():
            ring_forward(0, 0, hw)

        @pl.when((p < mid) & (m > 0) & (m <= early))
        def _():
            ring_forward(1, jnp.maximum(m - 1, 0), gw)

        @pl.when((p >= mid) & (p < n_stage - 2) & (m == early))
        def _():
            ring_forward(1, 0, gw)

    def transpose_weights():
        def some(c, carry):
            s = pl.ds(pl.multiple_of(c * LANES, LANES), LANES)
            for e in range(nd):
                w1t[e, s, :] = w1v[c, e * LANES : (e + 1) * LANES, :].T
                w2t[c, e * LANES : (e + 1) * LANES, :] = w2v[e, s, :].T
            return carry

        lax.fori_loop(0, nf, some, 0)

    def slopes():
        def some(t, carry):
            m, b = t // (nf // SLABS), t % (nf // SLABS) * SLABS
            for c in range(SLABS):
                zs[m, b + c] = _gelu_and_slope(zs[m, b + c])[1]
            return carry

        lax.fori_loop(0, m_all * (nf // SLABS), some, 0)

    def each(lo, hi, fn):
        lax.fori_loop(lo, hi, lambda m, c: (fn(m), c)[1], 0)

    def group(whole, part=0):
        return lambda k, c: whole[k // early, part * early + k % early, c]

    def pre_stores(j):
        b = j % 2
        return (
            pltpu.make_async_copy(narrow.at[b], a_pre.at[j], pre_sem.at[0, b]),
            pltpu.make_async_copy(full.at[b, pl.ds(0, SLABS * groups)], s_pre.at[j], pre_sem.at[1, b]),
        )

    def pre_loads(j):
        b = j % 2
        return (
            pltpu.make_async_copy(
                a_pre.at[j], w2v.at[pl.ds(b * SLABS, SLABS), pl.ds(0, tokens)], pre_sem.at[0, b]
            ),
            pltpu.make_async_copy(s_pre.at[j], zs.at[b, pl.ds(0, SLABS * groups)], pre_sem.at[1, b]),
        )

    def pre_unit(j):
        b = j % 2

        @pl.when(j > 1)
        def _():
            for c in pre_stores(j):
                c.wait()

        for ks, s in _chunks(256, groups, rows):
            z = _dot(_rows_of(group(hw, j // units), ks, nd), _wide([w1v[j % units * SLABS + c] for c in range(SLABS)]))
            a, slope = _gelu_and_slope(z)
            a = a.astype(BF16)
            for c in range(SLABS):
                narrow[b, c, s, :] = _cut(a, c)
                for n, k in enumerate(ks):
                    full[b, c * groups + k] = _cut(slope[n * rows : (n + 1) * rows], c)
        for c in pre_stores(j):
            c.start()

    formed = jnp.where(
        p < PRE_LATE, 2 * units,
        jnp.where(p < mid - 1, units, jnp.where(p == mid - 1, units * 3 // 4, 0)),
    )

    def part_copies(j):
        b, some = j % 2, pl.ds(0, SLABS * nd)
        return (
            pltpu.make_async_copy(full.at[b, some], d1_part.at[j], part_sem.at[0, b]),
            pltpu.make_async_copy(zs.at[m_all - 2 + b, some], d2_part.at[j], part_sem.at[1, b]),
        )

    def late_copies():
        return [
            pltpu.make_async_copy(whole.at[k, pl.ds(early, m_all - early)], out.at[k], late_sem.at[q, k])
            for q, (whole, out) in enumerate(((hw, h_late), (gw, g_late)))
            for k in range(n_inner)
        ]

    def sent(m):
        ring_sent(m)
        for src, slots, send, recv, end in ((ho, hw, h_send, h_recv, last), (go, gw, g_send, g_recv, 0)):
            for e in range(MERGE):
                a = src.at[m, :, piece(e)]

                @pl.when((p != end) | (p != m * MERGE + e))
                def _():
                    to_stage(a, a, send.at[m], recv.at[m], 0).wait_send()

        @pl.when((m == 0) & (p != 0))
        def _():
            to_stage(own_v.at[0], own_v.at[0], xsem.at[0], h_recv.at[0], 0).wait_send()

        @pl.when((m == 0) & (p != last))
        def _():
            to_stage(own_v.at[1], own_v.at[1], xsem.at[1], g_recv.at[0], last).wait_send()

    def unit(j):
        def forwards(m):
            @pl.when(p >= mid)
            def _():
                ring_forward(0, m, hw)

            ring_forward(1, m, gw)

        def firsts(m):
            @pl.when(p >= mid)
            def _():
                ring_first(0, m, hw)

            ring_first(1, m, gw)

        @pl.when(j == 0)
        def _():
            @pl.when(p >= n_stage - 2)
            def _():
                ring_forward(1, 0, gw)
                each(1, early, lambda e: (ring_forward(0, e, hw), ring_forward(1, e, gw)))


            @pl.when(formed > 0)
            def _():
                for c in pre_loads(0):
                    c.start()

            each(0, early, lambda m: ring_arrived(m, 1))

            @pl.when(formed == 0)
            def _():
                each(0, early, lambda m: ring_arrived(m, 0))

            each(early, m_all, firsts)

            @pl.when(formed == 0)
            def _():
                _transposed_rows(group(hw), groups, rows, nd, ht)

        for m in range(early, m_all):
            @pl.when(j == 2 * (m - early + 1) + jnp.where(p < mid, 0, 1))
            def _():
                forwards(m)

        @pl.when(j == units - 1)
        def _():
            each(early, m_all, lambda m: ring_arrived(m, 1))

            @pl.when(p >= PRE_LATE)
            def _():
                each(early, m_all, lambda m: ring_arrived(m, 0))

            for c in late_copies():
                c.start()
            each(0, m_all, sent)

        @pl.when(j > 1)
        def _():
            for c in part_copies(j):
                c.wait()

        def put(v1, v2):
            for c in range(SLABS):
                for e in range(nd):
                    zs[m_all - 2 + j % 2, c * nd + e] = _cut(v2[c * LANES : (c + 1) * LANES], e)
                    full[j % 2, c * nd + e] = _cut(v1[e * LANES : (e + 1) * LANES], c)

        def block(ready):
            _dw_block(
                512, group(hw), group(gw), groups, rows, nd,
                lambda: _wide([w1v[j * SLABS + c] for c in range(SLABS)]),
                lambda: _wide([w2t[j * SLABS + c] for c in range(SLABS)]),
                ht, ab, zb, put, ready,
            )

        @pl.when(j < formed)
        def _():
            b = j % 2
            for c in pre_loads(j):
                c.wait()

            @pl.when(j + 1 < jnp.minimum(formed, units))
            def _():
                for c in pre_loads(j + 1):
                    c.start()

            block((
                lambda c: w2v[b * SLABS + c, 0:tokens, :],
                lambda k, c: zs[b, c * groups + k],
            ))

        @pl.when(j >= formed)
        def _():
            block(None)

        for c in part_copies(j):
            c.start()

    kept = (
        pltpu.make_async_copy(w1v, w1_out, keep_sem.at[0]), pltpu.make_async_copy(w2t, w2_out, keep_sem.at[1])
    )
    with jax.named_scope("loads"):
        for c in loads[:nf]:
            c.wait()

    first = jnp.where(p == last, 1, m_all)
    rest = m_all - first
    turn = jnp.where(p < n_stage // 2, first, 0)

    def step(k, carry):
        j = k - first
        swap = j < 2 * rest
        is_u = k >= 2 * m_all
        is_f = (j < 0) | (swap & (j % 2 == 1))
        is_b = jnp.logical_not(is_f | is_u)
        m_f = jnp.where(j < 0, k, jnp.minimum(first + j // 2, m_all - 1))
        m_b = jnp.maximum(jnp.minimum(jnp.where(swap, j // 2, j - rest), m_all - 1), 0)
        u = jnp.maximum(k - 2 * m_all, 0)

        @pl.when(k == turn)
        def _():
            with jax.named_scope("transp"):
                @pl.when(p >= n_stage // 2)
                def _():
                    for c in loads[nf:]:
                        c.wait()

                transpose_weights()
                for c in kept:
                    c.start()

        @pl.when((k == first) & (p < n_stage - 2))
        def _():
            with jax.named_scope("slopes"):
                slopes()
            with jax.named_scope("hring"):
                each(0, jnp.where(p < mid, m_all, early), lambda m: ring_forward(0, m, hw))

        @pl.when((k == first) & (formed > 0))
        def _():
            with jax.named_scope("pre"):
                each(0, early, lambda m: ring_arrived(m, 0))

                @pl.when(p < PRE_LATE)
                def _():
                    each(early, m_all, lambda m: ring_arrived(m, 0))

                _transposed_rows(group(hw), groups, rows, nd, ht)
                each(0, formed, pre_unit)
                for c in (*pre_stores(0), *pre_stores(1)):
                    c.wait()

        early_f, odd = is_f & (p < n_stage - 2), p % 2 == 1
        for when, sloped, split in (
            (early_f & jnp.logical_not(odd), False, False),
            (early_f & odd, False, True),
            (is_f & (p >= n_stage - 2), True, False),
        ):
            @pl.when(when)
            def _():
                with jax.named_scope("fwd"):
                    forward(m_f, sloped, split)

        leaves = (p > 0) & jnp.logical_not(odd)
        for when, split in ((is_b & leaves, True), (is_b & jnp.logical_not(leaves), False)):
            @pl.when(when)
            def _():
                with jax.named_scope("bwd"):
                    backward(m_b, split)

        @pl.when(is_u)
        def _():
            with jax.named_scope("unit"):
                unit(u)

        return carry

    lax.fori_loop(0, 2 * m_all + units, step, 0)

    with jax.named_scope("finish"):
        for c in (*kept, *part_copies(units - 2), *part_copies(units - 1), *late_copies()):
            c.wait()
    with jax.named_scope("outwait"):
        pltpu.make_async_copy(y.at[0], y.at[0], out_recv.at[0]).wait()
        pltpu.make_async_copy(dx.at[0], dx.at[0], out_recv.at[1]).wait()


def _chain(n_stage, n_inner, x, g, w1, w2):
    mb, rows, d = x.shape
    f = w1.shape[-1]
    rows = rows * MERGE
    m_all = mb * n_stage // MERGE
    early = EARLY
    nd, nf = d // LANES, f // LANES
    blk = SLABS * LANES
    groups = n_inner * early
    tokens = groups * rows
    tiles = SLABS * max(nd, groups)
    hbm = pl.BlockSpec(memory_space=pltpu.HBM)
    whole = (n_inner, m_all, nd, rows, LANES)
    late = jax.ShapeDtypeStruct((n_inner, m_all - early, nd, rows, LANES), BF16)
    dma = pltpu.SemaphoreType.DMA
    vmem = pltpu.VMEM
    return pl.pallas_call(
        functools.partial(_chain_kernel, n_stage, n_inner),
        out_shape=[
            jax.ShapeDtypeStruct(x.shape, BF16), jax.ShapeDtypeStruct(x.shape, BF16), late, late,
            jax.ShapeDtypeStruct((nf, d, LANES), BF16), jax.ShapeDtypeStruct((nf, d, LANES), BF16),
            jax.ShapeDtypeStruct((f // blk, SLABS * nd, LANES, LANES), F32),
            jax.ShapeDtypeStruct((f // blk, SLABS * nd, LANES, LANES), F32),
            jax.ShapeDtypeStruct((2 * f // blk, SLABS, tokens, LANES), BF16),
            jax.ShapeDtypeStruct((2 * f // blk, SLABS * groups, rows, LANES), F32),
        ],
        in_specs=[hbm] * 4,
        out_specs=[hbm] * 10,
        scratch_shapes=[
            vmem((nf, d, LANES), BF16), vmem((nd, f, LANES), BF16),
            vmem((nd, f, LANES), BF16), vmem((nf, d, LANES), BF16),
            vmem(whole, BF16), vmem(whole, BF16),
            vmem((m_all, nd, rows, LANES), BF16), vmem((m_all, nd, rows, LANES), BF16),
            vmem((m_all, nf, rows, LANES), F32), vmem((nf, rows, LANES), BF16),
            vmem((tokens // LANES, d, LANES), BF16),
            vmem((2, SLABS, tokens, LANES), BF16), vmem((2, tiles, LANES, LANES), F32),
            vmem((2, nd, rows // MERGE, LANES), BF16),
            dma((2,)), dma((2,)), dma((m_all,)), dma((m_all,)), dma((m_all,)), dma((m_all,)), dma((2,)),
            dma((2, m_all, 4)), dma((2, m_all, 4)), dma((2, 2)), dma((2, n_inner)), dma((2, 2)), dma((2,)), dma((2,)),
        ],
        compiler_params=pltpu.CompilerParams(
            collective_id=0, has_side_effects=True, vmem_limit_bytes=VMEM_LIMIT
        ),
        name="chain",
    )(x, g, w1, w2)


def _late_kernel(
    h, g, y_in, dx_in, w1, w2t, p1, p2, ap, sp, d1, d2, y, dx,
    hv, gv, w1v, w2v, p1v, p2v, av, sv, d1v, d2v, ht, ab, zb, yv, first_sem, load_sem, store_sem, pass_sem,
):
    groups, nd, rows, _ = h.shape
    units = w1.shape[0] // SLABS
    d, blk = d1v.shape[1:]

    def pre(j):
        return (lax.axis_index("stage") < PRE_LATE) & (j % 2 == 1)

    def weights(j):
        b, some = j % DEEP, pl.ds(j * SLABS, SLABS)
        return (pltpu.make_async_copy(w2t.at[some], w2v.at[b], load_sem.at[0, b]),)

    def own(j):
        b, some = j % DEEP, pl.ds(j * SLABS, SLABS)
        return (pltpu.make_async_copy(w1.at[some], w1v.at[b], load_sem.at[1, b]),)

    def ready(j):
        b = j % DEEP
        return (
            pltpu.make_async_copy(ap.at[units + j], av.at[b], load_sem.at[1, b]),
            pltpu.make_async_copy(sp.at[units + j], sv.at[b], load_sem.at[2, b]),
        )

    def parts(j):
        b = j % DEEP
        return (
            pltpu.make_async_copy(p1.at[j], p1v.at[b], load_sem.at[3, b]),
            pltpu.make_async_copy(p2.at[j], p2v.at[b], load_sem.at[4, b]),
        )

    def stores(j):
        b, some = j % 2, pl.ds(pl.multiple_of(j * blk, blk), blk)
        return (
            pltpu.make_async_copy(d1v.at[b], d1.at[:, some], store_sem.at[0, b]),
            pltpu.make_async_copy(d2v.at[b], d2.at[some, :], store_sem.at[1, b]),
        )

    def do(copies, how):
        for c in copies:
            getattr(c, how)()

    def inputs(j, how):
        @pl.when(pre(j))
        def _():
            do(ready(j), how)

        @pl.when(jnp.logical_not(pre(j)))
        def _():
            do(own(j), how)

        do(weights(j), how)

    firsts = (pltpu.make_async_copy(h, hv, first_sem.at[0]), pltpu.make_async_copy(g, gv, first_sem.at[1]))
    firsts[0].start()
    inputs(0, "start")
    firsts[1].start()
    do(parts(0), "start")
    into = [pltpu.make_async_copy(a, yv.at[n], pass_sem.at[n]) for n, a in enumerate((y_in, dx_in))]
    out_of = [pltpu.make_async_copy(yv.at[n], a, pass_sem.at[n]) for n, a in enumerate((y, dx))]
    do(into, "start")
    firsts[0].wait()
    _transposed_rows(lambda k, c: hv[k, c], groups, rows, nd, ht)
    do(into, "wait")
    do(out_of, "start")

    def unit(j, carry):
        b, n = j % 2, j % DEEP
        inputs(j, "wait")
        do(parts(j), "wait")

        @pl.when(j == 0)
        def _():
            firsts[1].wait()
            for e in range(1, DEEP - 1):
                inputs(e, "start")
                do(parts(e), "start")

        @pl.when(j + DEEP - 1 < units)
        def _():
            inputs(j + DEEP - 1, "start")
            do(parts(j + DEEP - 1), "start")

        @pl.when(j > 1)
        def _():
            do(stores(j), "wait")

        def put(v1, v2):
            for c in range(SLABS):
                for e in range(nd):
                    r, s = slice(e * LANES, (e + 1) * LANES), slice(c * LANES, (c + 1) * LANES)
                    d2v[b, s, r] = p2v[n, c * nd + e] + v2[s, r]
                    d1v[b, r, s] = p1v[n, c * nd + e] + v1[r, s]

        def block(ready):
            _dw_block(
                512, lambda k, c: hv[k, c], lambda k, c: gv[k, c], groups, rows, nd,
                lambda: _wide([w1v[n, c] for c in range(SLABS)]), lambda: _wide([w2v[n, c] for c in range(SLABS)]),
                ht, ab, zb, put, ready,
            )

        @pl.when(pre(j))
        def _():
            block((lambda c: av[n, c], lambda k, c: sv[n, c * groups + k]))

        @pl.when(jnp.logical_not(pre(j)))
        def _():
            block(None)

        do(stores(j), "start")
        return carry

    lax.fori_loop(0, units, unit, 0)
    do(stores(units - 2), "wait")
    do(stores(units - 1), "wait")
    do(out_of, "wait")


def _late(h, g, y, dx, w1, w2t, p1, p2, ap, sp):
    groups, nd, rows, _ = h.shape
    nf, d, _ = w1.shape
    f, blk, t = nf * LANES, SLABS * LANES, groups * rows
    hbm = pl.BlockSpec(memory_space=pltpu.HBM)
    vmem, dma = pltpu.VMEM, pltpu.SemaphoreType.DMA
    return pl.pallas_call(
        _late_kernel,
        in_specs=[hbm] * 10,
        out_specs=[hbm] * 4,
        out_shape=[
            jax.ShapeDtypeStruct((d, f), F32), jax.ShapeDtypeStruct((f, d), F32),
            jax.ShapeDtypeStruct(y.shape, BF16), jax.ShapeDtypeStruct(dx.shape, BF16),
        ],
        scratch_shapes=[
            vmem(h.shape, BF16), vmem(g.shape, BF16),
            vmem((DEEP, SLABS, d, LANES), BF16), vmem((DEEP, SLABS, d, LANES), BF16),
            vmem((DEEP, *p1.shape[1:]), F32), vmem((DEEP, *p2.shape[1:]), F32),
            vmem((DEEP, *ap.shape[1:]), BF16), vmem((DEEP, *sp.shape[1:]), F32),
            vmem((2, d, blk), F32), vmem((2, blk, d), F32),
            vmem((t // LANES, d, LANES), BF16), vmem((SLABS, t, LANES), BF16), vmem((SLABS, t, LANES), BF16),
            vmem((2, *y.shape), BF16),
            dma((2,)), dma((5, DEEP)), dma((2, 2)), dma((2,)),
        ],
        compiler_params=pltpu.CompilerParams(vmem_limit_bytes=VMEM_LIMIT),
        cost_estimate=pl.CostEstimate(flops=8 * t * d * f, bytes_accessed=20 * d * f, transcendentals=t * f),
        name="late",
    )(h, g, y, dx, w1, w2t, p1, p2, ap, sp)


def solution(mesh):
    n_stage, n_inner = mesh.shape["stage"], mesh.shape["inner"]

    def body(x, g, w1, w2):
        y, dx, h, gg, w1s, w2s, *parts = _chain(n_stage, n_inner, x, g, w1, w2)
        flat = (-1, *h.shape[2:])
        d1, d2, y, dx = _late(h.reshape(flat), gg.reshape(flat), y, dx, w1s, w2s, *parts)
        return y, dx, d1.reshape(w1.shape), d2.reshape(w2.shape)

    tok = P(("data", "stage"), "inner", None)
    wsp = P(None, "stage", None, None)
    dsp = P("data", "stage", None, None)
    return jax.shard_map(body, mesh=mesh, in_specs=(tok, tok, wsp, wsp), out_specs=(tok, tok, dsp, dsp), check_vma=False)
```

```python
import functools

import jax
import jax.numpy as jnp
from jax import lax
from jax.experimental import pallas as pl
from jax.experimental.pallas import tpu as pltpu
from jax.sharding import PartitionSpec as P

MESH = pl.DeviceIdType.MESH
F32, BF16 = jnp.float32, jnp.bfloat16
C0, C1 = 0.7978845608028654, 0.044715
LANES = 128
VMEM_LIMIT = 67043328
SLABS = 4
MERGE = 2
EARLY = 2
DEEP = 3
PRE_LATE = 2


def _gelu_and_slope(z):
    z2 = z * z
    half = 0.5 * jnp.tanh(z * (C0 + (C0 * C1) * z2)) + 0.5
    a = z * half
    return a, half + (a - a * half) * (2.0 * C0 + (6.0 * C0 * C1) * z2)


def _dot(a, b):
    return jnp.dot(a, b, preferred_element_type=F32)


def _wide(slabs):
    return jnp.concatenate(slabs, axis=1)


def _tall(parts):
    return jnp.concatenate(parts, axis=0)


def _cut(value, c):
    return value[:, c * LANES : (c + 1) * LANES]


def _rows_of(read, ks, n):
    return _tall([_wide([read(k, c) for c in range(n)]) for k in ks])


def _chunks(rows, groups, group_rows):
    step = max(1, rows // group_rows)
    for k in range(0, groups, step):
        ks = range(k, min(k + step, groups))
        yield ks, slice(k * group_rows, (k + len(ks)) * group_rows)


def _dw_block(
    rows, hg, gg, groups, group_rows, nd, w1_block, w2t_block, ht, ab, zb, put, ready=None
):
    for ks, s in _chunks(rows, groups, group_rows):
        if ready is None:
            z = _dot(_rows_of(hg, ks, nd), w1_block())
        da = _dot(_rows_of(gg, ks, nd), w2t_block())
        if ready is None:
            a, slope = _gelu_and_slope(z)
            a = a.astype(BF16)
            for c in range(SLABS):
                ab[c, s, :] = _cut(a, c)
        else:
            slope = _rows_of(ready[1], ks, SLABS)
        dz = (da * slope).astype(BF16)
        for c in range(SLABS):
            zb[c, s, :] = _cut(dz, c)
    a = _wide([ab[c] for c in range(SLABS)] if ready is None else [ready[0](c) for c in range(SLABS)])
    v2 = lax.dot_general(
        a, _rows_of(gg, range(groups), nd), (((0,), (0,)), ((), ())), preferred_element_type=F32
    )
    put(_dot(_wide([ht[t] for t in range(ht.shape[0])]), _wide([zb[c] for c in range(SLABS)])), v2)


def _transposed_rows(hg, groups, group_rows, nd, ht):
    per = LANES // group_rows
    for t in range(groups // per):
        ht[t] = _tall([_wide([hg(t * per + e, c) for c in range(nd)]) for e in range(per)]).T


def _chain_kernel(
    n_stage, n_inner, x, g, w1, w2, y, dx, h_late, g_late, w1_out, w2_out, d1_part, d2_part, a_pre, s_pre,
    w1v, w2v, w1t, w2t, hw, gw, ho, go, zs, act, ht, narrow, full, own_v,
    wsem, xsem, h_recv, g_recv, h_send, g_send, out_recv, ring_send, ring_recv, part_sem, late_sem, pre_sem, keep_sem, own_sem,
):
    p, i = lax.axis_index("stage"), lax.axis_index("inner")
    right, left = lax.rem(i + 1, n_inner), lax.rem(i + n_inner - 1, n_inner)
    _, m_all, nd, rows, _ = hw.shape
    nf = w1v.shape[0]
    units = nf // SLABS
    early = EARLY
    last = n_stage - 1
    half = nd // 2
    part = rows // MERGE
    mid = n_stage // 2
    groups = n_inner * early
    tokens = groups * rows
    ab, zb = narrow.at[0], narrow.at[1]

    def flat(ref, c):
        return ref.at[0, :, c * LANES : (c + 1) * LANES]

    mine = [
        pltpu.make_async_copy(flat(src, c), own_v.at[n, c], own_sem.at[n]) for n, src in enumerate((x, g)) for c in range(nd)
    ]
    for c in mine:
        c.start()

    barrier = pltpu.get_barrier_semaphore()
    for q in range(1, n_stage):
        pl.semaphore_signal(barrier, inc=1, device_id={"stage": lax.rem(p + q, n_stage)}, device_id_type=MESH)
    for q in (left, right):
        pl.semaphore_signal(barrier, inc=1, device_id={"inner": q}, device_id_type=MESH)

    loads = [
        pltpu.make_async_copy(w1.at[0, 0, :, c * LANES : (c + 1) * LANES], w1v.at[c], wsem.at[0]) for c in range(nf)
    ] + [pltpu.make_async_copy(w2.at[0, 0, :, c * LANES : (c + 1) * LANES], w2v.at[c], wsem.at[1]) for c in range(nd)]
    for c in loads:
        c.start()

    def to_stage(src, dst, send, recv, stage):
        return pltpu.make_async_remote_copy(
            src_ref=src, dst_ref=dst, send_sem=send, recv_sem=recv,
            device_id={"stage": stage}, device_id_type=MESH,
        )

    def to_inner(src, dst, send, recv, inner):
        return pltpu.make_async_remote_copy(
            src_ref=src, dst_ref=dst, send_sem=send, recv_sem=recv,
            device_id={"inner": inner}, device_id_type=MESH,
        )

    def piece(e):
        return pl.ds(pl.multiple_of(e * part, part), part)

    with jax.named_scope("barrier"):
        pl.semaphore_wait(barrier, n_stage + 1)
    for c in mine:
        c.wait()

    def own(mine_v, slots, recv, sem, stage):
        there = slots.at[i, p // MERGE, :, piece(p % MERGE)]

        @pl.when(p == stage)
        def _():
            pltpu.make_async_copy(mine_v, there, recv.at[p // MERGE]).start()

        @pl.when(p != stage)
        def _():
            to_stage(mine_v, there, sem, recv.at[p // MERGE], stage).start()

    own(own_v.at[0], hw, h_recv, xsem.at[0], 0)
    own(own_v.at[1], gw, g_recv, xsem.at[1], last)

    low, high = pl.ds(0, half), pl.ds(half, half)

    def ring_own(q, m, whole):
        kinds = ((0, low, right), (1, high, left), (4, high, right), (5, low, left))
        return [
            to_inner(
                whole.at[i, m, some], whole.at[i, m, some], ring_send.at[q, m, k], ring_recv.at[q, m, k], inner
            )
            for k, some, inner in kinds
        ]

    def ring_first(q, m, whole):
        for c in ring_own(q, m, whole):
            c.start()

    def ring_relay(q, m, whole, k):
        src, some, inner = (left, low, right) if k == 0 else (right, high, left)
        a = whole.at[src, m, some]
        return (
            to_inner(a, a, ring_send.at[q, m, k], ring_recv.at[q, m, k], inner),
            to_inner(a, a, ring_send.at[q, m, 2 + k], ring_recv.at[q, m, 2 + k], inner),
        )

    def ring_forward(q, m, whole):
        for k in (0, 1):
            arrival, onward = ring_relay(q, m, whole, k)
            arrival.wait_recv()
            onward.start()

    def ring_arrived(m, q):
        whole = (hw, gw)[q]
        far = lax.rem(i + 2, n_inner)
        for k, src, some in ((4, left, high), (5, right, low), (2, far, low), (3, far, high)):
            a = whole.at[src, m, some]
            to_inner(a, a, ring_send.at[q, m, k], ring_recv.at[q, m, k], right).wait_recv()

    def ring_sent(m):
        for q, whole in ((0, hw), (1, gw)):
            for c in ring_own(q, m, whole):
                c.wait_send()
            for k in (0, 1):
                ring_relay(q, m, whole, k)[1].wait_send()

    def pass_on(m, lo, hi, src, slots, send, recv, end, nxt, out, out_sem):
        @pl.when(p != end)
        def _():
            some = pl.ds(lo, hi - lo)
            to_stage(src.at[m, some], slots.at[i, m, some], send.at[m], recv.at[m], nxt).start()

        if hi - lo < nd:
            return

        @pl.when(p == end)
        def _():
            for e in range(MERGE):
                home = m * MERGE + e

                @pl.when(p != home)
                def _():
                    for c in range(nd):
                        to_stage(src.at[m, c, piece(e)], flat(out, c), send.at[m], out_sem, home).start()

                @pl.when(p == home)
                def _():
                    for c in range(nd):
                        pltpu.make_async_copy(src.at[m, c, piece(e)], flat(out, c), out_sem).start()

    def step_of(m, split, x_in, wa, activate, second, wb, src, *rest):
        blocks, k_half = nf // SLABS, nf // 2
        early_acts = blocks // 2 if second is None else blocks - 1
        zs_in = []

        def act_of(b):
            a = activate(b * SLABS, zs_in[b])
            for c in range(SLABS):
                act[b * SLABS + c] = _cut(a, c)

        def part_dot(lo, count, k):
            a = _wide([act[k + c] for c in range(k_half)])
            return _dot(a, _wide([wb[lo + c, k * LANES : (k + k_half) * LANES, :] for c in range(count)]))

        for b in range(blocks):
            zs_in.append(_dot(x_in, _wide([wa[b * SLABS + c] for c in range(SLABS)])))
            if 0 < b <= early_acts:
                act_of(b - 1)
        if second is not None:
            act_of(blocks - 1)
            second()
        count = half if split else nd
        for lo in range(0, nd, count):
            u = part_dot(lo, count, 0)
            if lo == 0 and second is None:
                for b in range(early_acts, blocks):
                    act_of(b)
            u = u + part_dot(lo, count, k_half)
            out = (x_in[:, lo * LANES : (lo + count) * LANES].astype(F32) + u).astype(BF16)
            for c in range(count):
                src[m, lo + c] = _cut(out, c)
            pass_on(m, lo, lo + count, src, *rest)

    def second_weights():
        for c in loads[nf:]:
            c.wait()

    def forward(m, sloped, split):
        @pl.when((m == 0) & (p > 0) & (p < mid))
        def _():
            second_weights()

        with jax.named_scope("wait_h"):
            pltpu.make_async_copy(hw.at[i, m], hw.at[i, m], h_recv.at[m]).wait()
        h = _wide([hw[i, m, c] for c in range(nd)])

        def activate(b, z):
            a, slope = _gelu_and_slope(z)
            for c in range(SLABS):
                zs[m, b + c] = _cut(slope if sloped else z, c)
            return a.astype(BF16)

        def second():
            @pl.when((m == 0) & (p == 0))
            def _():
                second_weights()

        step_of(
            m, split, h, w1v, activate, None if sloped or split else second, w2v,
            ho, hw, h_send, h_recv, last, jnp.minimum(p + 1, last), y, out_recv.at[0],
        )

        @pl.when((p < mid) | (m < early))
        def _():
            ring_first(0, m, hw)

    def backward(m, split):
        @pl.when((p >= mid) & (p < n_stage - 2) & (m == early + 1))
        def _():
            ring_forward(1, early - 1, gw)

        @pl.when((p < mid) & (m == 1))
        def _():
            ring_forward(1, 0, gw)

        with jax.named_scope("wait_g"):
            pltpu.make_async_copy(gw.at[i, m], gw.at[i, m], g_recv.at[m]).wait()

        @pl.when(m < early)
        def _():
            ring_first(1, m, gw)

        dh = _wide([gw[i, m, c] for c in range(nd)])
        step_of(
            m, split, dh, w2t, lambda b, da: (da * _wide([zs[m, b + c] for c in range(SLABS)])).astype(BF16), None,
            w1t, go, gw, g_send, g_recv, 0, jnp.maximum(p - 1, 0), dx, out_recv.at[1],
        )

        @pl.when((p >= n_stage - 2) & (m == early))
        def _():
            ring_forward(0, 0, hw)

        @pl.when((p < mid) & (m > 1) & (m <= early))
        def _():
            ring_forward(1, jnp.maximum(m - 1, 0), gw)

        @pl.when((p >= mid) & (p < n_stage - 2) & (m == early))
        def _():
            ring_forward(1, 0, gw)

    def transpose_weights():
        def some(c, carry):
            s = pl.ds(pl.multiple_of(c * LANES, LANES), LANES)
            for e in range(nd):
                w1t[e, s, :] = w1v[c, e * LANES : (e + 1) * LANES, :].T
                w2t[c, e * LANES : (e + 1) * LANES, :] = w2v[e, s, :].T
            return carry

        lax.fori_loop(0, nf, some, 0)

    def slopes():
        def some(t, carry):
            m, b = t // (nf // SLABS), t % (nf // SLABS) * SLABS
            for c in range(SLABS):
                zs[m, b + c] = _gelu_and_slope(zs[m, b + c])[1]
            return carry

        lax.fori_loop(0, m_all * (nf // SLABS), some, 0)

    def each(lo, hi, fn):
        lax.fori_loop(lo, hi, lambda m, c: (fn(m), c)[1], 0)

    def group(whole, part=0):
        return lambda k, c: whole[k // early, part * early + k % early, c]

    def pre_stores(j):
        b = j % 2
        return (
            pltpu.make_async_copy(narrow.at[b], a_pre.at[j], pre_sem.at[0, b]),
            pltpu.make_async_copy(full.at[b, pl.ds(0, SLABS * groups)], s_pre.at[j], pre_sem.at[1, b]),
        )

    def pre_loads(j):
        b = j % 2
        return (
            pltpu.make_async_copy(
                a_pre.at[j], w2v.at[pl.ds(b * SLABS, SLABS), pl.ds(0, tokens)], pre_sem.at[0, b]
            ),
            pltpu.make_async_copy(s_pre.at[j], zs.at[b, pl.ds(0, SLABS * groups)], pre_sem.at[1, b]),
        )

    def pre_unit(j):
        b = j % 2

        @pl.when(j > 1)
        def _():
            for c in pre_stores(j):
                c.wait()

        for ks, s in _chunks(256, groups, rows):
            z = _dot(_rows_of(group(hw, j // units), ks, nd), _wide([w1v[j % units * SLABS + c] for c in range(SLABS)]))
            a, slope = _gelu_and_slope(z)
            a = a.astype(BF16)
            for c in range(SLABS):
                narrow[b, c, s, :] = _cut(a, c)
                for n, k in enumerate(ks):
                    full[b, c * groups + k] = _cut(slope[n * rows : (n + 1) * rows], c)
        for c in pre_stores(j):
            c.start()

    formed = jnp.where(
        p < PRE_LATE, 2 * units,
        jnp.where(p < mid - 1, units, jnp.where(p == mid - 1, units * 3 // 4, 0)),
    )

    def part_copies(j):
        b, some = j % 2, pl.ds(0, SLABS * nd)
        return (
            pltpu.make_async_copy(full.at[b, some], d1_part.at[j], part_sem.at[0, b]),
            pltpu.make_async_copy(zs.at[m_all - 2 + b, some], d2_part.at[j], part_sem.at[1, b]),
        )

    def late_copies():
        return [
            pltpu.make_async_copy(whole.at[k, pl.ds(early, m_all - early)], out.at[k], late_sem.at[q, k])
            for q, (whole, out) in enumerate(((hw, h_late), (gw, g_late)))
            for k in range(n_inner)
        ]

    def sent(m):
        ring_sent(m)
        for src, slots, send, recv, end in ((ho, hw, h_send, h_recv, last), (go, gw, g_send, g_recv, 0)):
            for e in range(MERGE):
                a = src.at[m, :, piece(e)]

                @pl.when((p != end) | (p != m * MERGE + e))
                def _():
                    to_stage(a, a, send.at[m], recv.at[m], 0).wait_send()

        @pl.when((m == 0) & (p != 0))
        def _():
            to_stage(own_v.at[0], own_v.at[0], xsem.at[0], h_recv.at[0], 0).wait_send()

        @pl.when((m == 0) & (p != last))
        def _():
            to_stage(own_v.at[1], own_v.at[1], xsem.at[1], g_recv.at[0], last).wait_send()

    def unit(j):
        def forwards(m):
            @pl.when(p >= mid)
            def _():
                ring_forward(0, m, hw)

            ring_forward(1, m, gw)

        def firsts(m):
            @pl.when(p >= mid)
            def _():
                ring_first(0, m, hw)

            ring_first(1, m, gw)

        @pl.when(j == 0)
        def _():
            @pl.when(p >= n_stage - 2)
            def _():
                ring_forward(1, 0, gw)
                each(1, early, lambda e: (ring_forward(0, e, hw), ring_forward(1, e, gw)))


            @pl.when(formed > 0)
            def _():
                for c in pre_loads(0):
                    c.start()

            each(0, early, lambda m: ring_arrived(m, 1))

            @pl.when(formed == 0)
            def _():
                each(0, early, lambda m: ring_arrived(m, 0))

            each(early, m_all, firsts)

            @pl.when(formed == 0)
            def _():
                _transposed_rows(group(hw), groups, rows, nd, ht)

        for m in range(early, m_all):
            @pl.when(j == 2 * (m - early + 1) + jnp.where(p < mid, 0, 1))
            def _():
                forwards(m)

        @pl.when(j == units - 1)
        def _():
            each(early, m_all, lambda m: ring_arrived(m, 1))

            @pl.when(p >= PRE_LATE)
            def _():
                each(early, m_all, lambda m: ring_arrived(m, 0))

            for c in late_copies():
                c.start()

        @pl.when(j > 1)
        def _():
            for c in part_copies(j):
                c.wait()

        def put(v1, v2):
            for c in range(SLABS):
                for e in range(nd):
                    zs[m_all - 2 + j % 2, c * nd + e] = _cut(v2[c * LANES : (c + 1) * LANES], e)
                    full[j % 2, c * nd + e] = _cut(v1[e * LANES : (e + 1) * LANES], c)

        def block(ready):
            _dw_block(
                512, group(hw), group(gw), groups, rows, nd,
                lambda: _wide([w1v[j * SLABS + c] for c in range(SLABS)]),
                lambda: _wide([w2t[j * SLABS + c] for c in range(SLABS)]),
                ht, ab, zb, put, ready,
            )

        @pl.when(j < formed)
        def _():
            b = j % 2
            for c in pre_loads(j):
                c.wait()

            @pl.when(j + 1 < jnp.minimum(formed, units))
            def _():
                for c in pre_loads(j + 1):
                    c.start()

            block((
                lambda c: w2v[b * SLABS + c, 0:tokens, :],
                lambda k, c: zs[b, c * groups + k],
            ))

        @pl.when(j >= formed)
        def _():
            block(None)

        for c in part_copies(j):
            c.start()

    kept = (
        pltpu.make_async_copy(w1v, w1_out, keep_sem.at[0]), pltpu.make_async_copy(w2t, w2_out, keep_sem.at[1])
    )
    with jax.named_scope("loads"):
        for c in loads[:nf]:
            c.wait()

    first = jnp.where(p == last, 1, m_all)
    rest = m_all - first
    turn = jnp.where(p < n_stage // 2, first, 0)

    def step(k, carry):
        j = k - first
        swap = j < 2 * rest
        is_u = k >= 2 * m_all
        is_f = (j < 0) | (swap & (j % 2 == 1))
        is_b = jnp.logical_not(is_f | is_u)
        m_f = jnp.where(j < 0, k, jnp.minimum(first + j // 2, m_all - 1))
        m_b = jnp.maximum(jnp.minimum(jnp.where(swap, j // 2, j - rest), m_all - 1), 0)
        u = jnp.maximum(k - 2 * m_all, 0)

        @pl.when(k == turn)
        def _():
            with jax.named_scope("transp"):
                @pl.when(p >= n_stage // 2)
                def _():
                    for c in loads[nf:]:
                        c.wait()

                transpose_weights()
                for c in kept:
                    c.start()

        @pl.when((k == first) & (p < n_stage - 2))
        def _():
            with jax.named_scope("slopes"):
                slopes()
            with jax.named_scope("hring"):
                each(0, jnp.where(p < mid, m_all, early), lambda m: ring_forward(0, m, hw))

        @pl.when((k == first) & (formed > 0))
        def _():
            with jax.named_scope("pre"):
                each(0, early, lambda m: ring_arrived(m, 0))

                @pl.when(p < PRE_LATE)
                def _():
                    each(early, m_all, lambda m: ring_arrived(m, 0))

                _transposed_rows(group(hw), groups, rows, nd, ht)
                each(0, formed, pre_unit)
                for c in (*pre_stores(0), *pre_stores(1)):
                    c.wait()

        early_f, odd = is_f & (p < n_stage - 2), p % 2 == 1
        for when, sloped, split in (
            (early_f & jnp.logical_not(odd), False, False),
            (early_f & odd, False, True),
            (is_f & (p >= n_stage - 2), True, False),
        ):
            @pl.when(when)
            def _():
                with jax.named_scope("fwd"):
                    forward(m_f, sloped, split)

        leaves = (p > 0) & jnp.logical_not(odd)
        for when, split in ((is_b & leaves, True), (is_b & jnp.logical_not(leaves), False)):
            @pl.when(when)
            def _():
                with jax.named_scope("bwd"):
                    backward(m_b, split)

        @pl.when(is_u)
        def _():
            with jax.named_scope("unit"):
                unit(u)

        return carry

    lax.fori_loop(0, 2 * m_all + units, step, 0)

    with jax.named_scope("finish"):
        each(0, m_all, sent)
        for c in (*kept, *part_copies(units - 2), *part_copies(units - 1), *late_copies()):
            c.wait()
    with jax.named_scope("outwait"):
        pltpu.make_async_copy(y.at[0], y.at[0], out_recv.at[0]).wait()
        pltpu.make_async_copy(dx.at[0], dx.at[0], out_recv.at[1]).wait()


def _chain(n_stage, n_inner, x, g, w1, w2):
    mb, rows, d = x.shape
    f = w1.shape[-1]
    rows = rows * MERGE
    m_all = mb * n_stage // MERGE
    early = EARLY
    nd, nf = d // LANES, f // LANES
    blk = SLABS * LANES
    groups = n_inner * early
    tokens = groups * rows
    tiles = SLABS * max(nd, groups)
    hbm = pl.BlockSpec(memory_space=pltpu.HBM)
    whole = (n_inner, m_all, nd, rows, LANES)
    late = jax.ShapeDtypeStruct((n_inner, m_all - early, nd, rows, LANES), BF16)
    dma = pltpu.SemaphoreType.DMA
    vmem = pltpu.VMEM
    return pl.pallas_call(
        functools.partial(_chain_kernel, n_stage, n_inner),
        out_shape=[
            jax.ShapeDtypeStruct(x.shape, BF16), jax.ShapeDtypeStruct(x.shape, BF16), late, late,
            jax.ShapeDtypeStruct((nf, d, LANES), BF16), jax.ShapeDtypeStruct((nf, d, LANES), BF16),
            jax.ShapeDtypeStruct((f // blk, SLABS * nd, LANES, LANES), F32),
            jax.ShapeDtypeStruct((f // blk, SLABS * nd, LANES, LANES), F32),
            jax.ShapeDtypeStruct((2 * f // blk, SLABS, tokens, LANES), BF16),
            jax.ShapeDtypeStruct((2 * f // blk, SLABS * groups, rows, LANES), F32),
        ],
        in_specs=[hbm] * 4,
        out_specs=[hbm] * 10,
        scratch_shapes=[
            vmem((nf, d, LANES), BF16), vmem((nd, f, LANES), BF16),
            vmem((nd, f, LANES), BF16), vmem((nf, d, LANES), BF16),
            vmem(whole, BF16), vmem(whole, BF16),
            vmem((m_all, nd, rows, LANES), BF16), vmem((m_all, nd, rows, LANES), BF16),
            vmem((m_all, nf, rows, LANES), F32), vmem((nf, rows, LANES), BF16),
            vmem((tokens // LANES, d, LANES), BF16),
            vmem((2, SLABS, tokens, LANES), BF16), vmem((2, tiles, LANES, LANES), F32),
            vmem((2, nd, rows // MERGE, LANES), BF16),
            dma((2,)), dma((2,)), dma((m_all,)), dma((m_all,)), dma((m_all,)), dma((m_all,)), dma((2,)),
            dma((2, m_all, 6)), dma((2, m_all, 6)), dma((2, 2)), dma((2, n_inner)), dma((2, 2)), dma((2,)), dma((2,)),
        ],
        compiler_params=pltpu.CompilerParams(
            collective_id=0, has_side_effects=True, vmem_limit_bytes=VMEM_LIMIT
        ),
        name="chain",
    )(x, g, w1, w2)


def _late_kernel(
    h, g, y_in, dx_in, w1, w2t, p1, p2, ap, sp, d1, d2, y, dx,
    hv, gv, w1v, w2v, p1v, p2v, av, sv, d1v, d2v, ht, ab, zb, yv, first_sem, load_sem, store_sem, pass_sem,
):
    groups, nd, rows, _ = h.shape
    units = w1.shape[0] // SLABS
    d, blk = d1v.shape[1:]

    def pre(j):
        return (lax.axis_index("stage") < PRE_LATE) & (j % 2 == 1)

    def weights(j):
        b, some = j % DEEP, pl.ds(j * SLABS, SLABS)
        return (pltpu.make_async_copy(w2t.at[some], w2v.at[b], load_sem.at[0, b]),)

    def own(j):
        b, some = j % DEEP, pl.ds(j * SLABS, SLABS)
        return (pltpu.make_async_copy(w1.at[some], w1v.at[b], load_sem.at[1, b]),)

    def ready(j):
        b = j % DEEP
        return (
            pltpu.make_async_copy(ap.at[units + j], av.at[b], load_sem.at[1, b]),
            pltpu.make_async_copy(sp.at[units + j], sv.at[b], load_sem.at[2, b]),
        )

    def parts(j):
        b = j % DEEP
        return (
            pltpu.make_async_copy(p1.at[j], p1v.at[b], load_sem.at[3, b]),
            pltpu.make_async_copy(p2.at[j], p2v.at[b], load_sem.at[4, b]),
        )

    def stores(j):
        b, some = j % 2, pl.ds(pl.multiple_of(j * blk, blk), blk)
        return (
            pltpu.make_async_copy(d1v.at[b], d1.at[:, some], store_sem.at[0, b]),
            pltpu.make_async_copy(d2v.at[b], d2.at[some, :], store_sem.at[1, b]),
        )

    def do(copies, how):
        for c in copies:
            getattr(c, how)()

    def inputs(j, how):
        @pl.when(pre(j))
        def _():
            do(ready(j), how)

        @pl.when(jnp.logical_not(pre(j)))
        def _():
            do(own(j), how)

        do(weights(j), how)

    firsts = (pltpu.make_async_copy(h, hv, first_sem.at[0]), pltpu.make_async_copy(g, gv, first_sem.at[1]))
    firsts[0].start()
    inputs(0, "start")
    firsts[1].start()
    do(parts(0), "start")
    into = [pltpu.make_async_copy(a, yv.at[n], pass_sem.at[n]) for n, a in enumerate((y_in, dx_in))]
    out_of = [pltpu.make_async_copy(yv.at[n], a, pass_sem.at[n]) for n, a in enumerate((y, dx))]
    do(into, "start")
    firsts[0].wait()
    _transposed_rows(lambda k, c: hv[k, c], groups, rows, nd, ht)
    do(into, "wait")
    do(out_of, "start")

    def unit(j, carry):
        b, n = j % 2, j % DEEP
        inputs(j, "wait")
        do(parts(j), "wait")

        @pl.when(j == 0)
        def _():
            firsts[1].wait()
            for e in range(1, DEEP - 1):
                inputs(e, "start")
                do(parts(e), "start")

        @pl.when(j + DEEP - 1 < units)
        def _():
            inputs(j + DEEP - 1, "start")
            do(parts(j + DEEP - 1), "start")

        @pl.when(j > 1)
        def _():
            do(stores(j), "wait")

        def put(v1, v2):
            for c in range(SLABS):
                for e in range(nd):
                    r, s = slice(e * LANES, (e + 1) * LANES), slice(c * LANES, (c + 1) * LANES)
                    d2v[b, s, r] = p2v[n, c * nd + e] + v2[s, r]
                    d1v[b, r, s] = p1v[n, c * nd + e] + v1[r, s]

        def block(ready):
            _dw_block(
                512, lambda k, c: hv[k, c], lambda k, c: gv[k, c], groups, rows, nd,
                lambda: _wide([w1v[n, c] for c in range(SLABS)]), lambda: _wide([w2v[n, c] for c in range(SLABS)]),
                ht, ab, zb, put, ready,
            )

        @pl.when(pre(j))
        def _():
            block((lambda c: av[n, c], lambda k, c: sv[n, c * groups + k]))

        @pl.when(jnp.logical_not(pre(j)))
        def _():
            block(None)

        do(stores(j), "start")
        return carry

    lax.fori_loop(0, units, unit, 0)
    do(stores(units - 2), "wait")
    do(stores(units - 1), "wait")
    do(out_of, "wait")


def _late(h, g, y, dx, w1, w2t, p1, p2, ap, sp):
    groups, nd, rows, _ = h.shape
    nf, d, _ = w1.shape
    f, blk, t = nf * LANES, SLABS * LANES, groups * rows
    hbm = pl.BlockSpec(memory_space=pltpu.HBM)
    vmem, dma = pltpu.VMEM, pltpu.SemaphoreType.DMA
    return pl.pallas_call(
        _late_kernel,
        in_specs=[hbm] * 10,
        out_specs=[hbm] * 4,
        out_shape=[
            jax.ShapeDtypeStruct((d, f), F32), jax.ShapeDtypeStruct((f, d), F32),
            jax.ShapeDtypeStruct(y.shape, BF16), jax.ShapeDtypeStruct(dx.shape, BF16),
        ],
        scratch_shapes=[
            vmem(h.shape, BF16), vmem(g.shape, BF16),
            vmem((DEEP, SLABS, d, LANES), BF16), vmem((DEEP, SLABS, d, LANES), BF16),
            vmem((DEEP, *p1.shape[1:]), F32), vmem((DEEP, *p2.shape[1:]), F32),
            vmem((DEEP, *ap.shape[1:]), BF16), vmem((DEEP, *sp.shape[1:]), F32),
            vmem((2, d, blk), F32), vmem((2, blk, d), F32),
            vmem((t // LANES, d, LANES), BF16), vmem((SLABS, t, LANES), BF16), vmem((SLABS, t, LANES), BF16),
            vmem((2, *y.shape), BF16),
            dma((2,)), dma((5, DEEP)), dma((2, 2)), dma((2,)),
        ],
        compiler_params=pltpu.CompilerParams(vmem_limit_bytes=VMEM_LIMIT),
        cost_estimate=pl.CostEstimate(flops=8 * t * d * f, bytes_accessed=20 * d * f, transcendentals=t * f),
        name="late",
    )(h, g, y, dx, w1, w2t, p1, p2, ap, sp)


def solution(mesh):
    n_stage, n_inner = mesh.shape["stage"], mesh.shape["inner"]

    def body(x, g, w1, w2):
        y, dx, h, gg, w1s, w2s, *parts = _chain(n_stage, n_inner, x, g, w1, w2)
        flat = (-1, *h.shape[2:])
        d1, d2, y, dx = _late(h.reshape(flat), gg.reshape(flat), y, dx, w1s, w2s, *parts)
        return y, dx, d1.reshape(w1.shape), d2.reshape(w2.shape)

    tok = P(("data", "stage"), "inner", None)
    wsp = P(None, "stage", None, None)
    dsp = P("data", "stage", None, None)
    return jax.shard_map(body, mesh=mesh, in_specs=(tok, tok, wsp, wsp), out_specs=(tok, tok, dsp, dsp), check_vma=False)
```

```python
import functools

import jax
import jax.numpy as jnp
from jax import lax
from jax.experimental import pallas as pl
from jax.experimental.pallas import tpu as pltpu
from jax.sharding import PartitionSpec as P

MESH = pl.DeviceIdType.MESH
F32, BF16 = jnp.float32, jnp.bfloat16
C0, C1 = 0.7978845608028654, 0.044715
LANES = 128
VMEM_LIMIT = 67043328
SLABS = 4
MERGE = 2
EARLY = 2
DEEP = 3
PRE_LATE = 2


def _gelu_and_slope(z):
    z2 = z * z
    half = 0.5 * jnp.tanh(z * (C0 + (C0 * C1) * z2)) + 0.5
    a = z * half
    return a, half + (a - a * half) * (2.0 * C0 + (6.0 * C0 * C1) * z2)


def _dot(a, b):
    return jnp.dot(a, b, preferred_element_type=F32)


def _wide(slabs):
    return jnp.concatenate(slabs, axis=1)


def _tall(parts):
    return jnp.concatenate(parts, axis=0)


def _cut(value, c):
    return value[:, c * LANES : (c + 1) * LANES]


def _rows_of(read, ks, n):
    return _tall([_wide([read(k, c) for c in range(n)]) for k in ks])


def _chunks(rows, groups, group_rows):
    step = max(1, rows // group_rows)
    for k in range(0, groups, step):
        ks = range(k, min(k + step, groups))
        yield ks, slice(k * group_rows, (k + len(ks)) * group_rows)


def _dw_block(
    rows, hg, gg, groups, group_rows, nd, w1_block, w2t_block, ht, ab, zb, put, ready=None
):
    for ks, s in _chunks(rows, groups, group_rows):
        if ready is None:
            z = _dot(_rows_of(hg, ks, nd), w1_block())
        da = _dot(_rows_of(gg, ks, nd), w2t_block())
        if ready is None:
            a, slope = _gelu_and_slope(z)
            a = a.astype(BF16)
            for c in range(SLABS):
                ab[c, s, :] = _cut(a, c)
        else:
            slope = _rows_of(ready[1], ks, SLABS)
        dz = (da * slope).astype(BF16)
        for c in range(SLABS):
            zb[c, s, :] = _cut(dz, c)
    a = _wide([ab[c] for c in range(SLABS)] if ready is None else [ready[0](c) for c in range(SLABS)])
    v2 = lax.dot_general(
        a, _rows_of(gg, range(groups), nd), (((0,), (0,)), ((), ())), preferred_element_type=F32
    )
    put(_dot(_wide([ht[t] for t in range(ht.shape[0])]), _wide([zb[c] for c in range(SLABS)])), v2)


def _transposed_rows(hg, groups, group_rows, nd, ht):
    per = LANES // group_rows
    for t in range(groups // per):
        ht[t] = _tall([_wide([hg(t * per + e, c) for c in range(nd)]) for e in range(per)]).T


def _chain_kernel(
    n_stage, n_inner, x, g, w1, w2, y, dx, h_late, g_late, w1_out, w2_out, d1_part, d2_part, a_pre, s_pre,
    w1v, w2v, w1t, w2t, hw, gw, ho, go, zs, act, ht, narrow, full, own_v,
    wsem, xsem, h_recv, g_recv, h_send, g_send, out_recv, ring_send, ring_recv, part_sem, late_sem, pre_sem, keep_sem, own_sem,
):
    p, i = lax.axis_index("stage"), lax.axis_index("inner")
    right, left = lax.rem(i + 1, n_inner), lax.rem(i + n_inner - 1, n_inner)
    _, m_all, nd, rows, _ = hw.shape
    nf = w1v.shape[0]
    units = nf // SLABS
    early = EARLY
    last = n_stage - 1
    half = nd // 2
    part = rows // MERGE
    mid = n_stage // 2
    groups = n_inner * early
    tokens = groups * rows
    ab, zb = narrow.at[0], narrow.at[1]

    def flat(ref, c):
        return ref.at[0, :, c * LANES : (c + 1) * LANES]

    mine = [
        pltpu.make_async_copy(flat(src, c), own_v.at[n, c], own_sem.at[n]) for n, src in enumerate((x, g)) for c in range(nd)
    ]
    for c in mine:
        c.start()

    barrier = pltpu.get_barrier_semaphore()
    for q in range(1, n_stage):
        pl.semaphore_signal(barrier, inc=1, device_id={"stage": lax.rem(p + q, n_stage)}, device_id_type=MESH)
    for q in (left, right):
        pl.semaphore_signal(barrier, inc=1, device_id={"inner": q}, device_id_type=MESH)

    loads = [
        pltpu.make_async_copy(w1.at[0, 0, :, c * LANES : (c + 1) * LANES], w1v.at[c], wsem.at[0]) for c in range(nf)
    ] + [pltpu.make_async_copy(w2.at[0, 0, :, c * LANES : (c + 1) * LANES], w2v.at[c], wsem.at[1]) for c in range(nd)]
    for c in loads:
        c.start()

    def to_stage(src, dst, send, recv, stage):
        return pltpu.make_async_remote_copy(
            src_ref=src, dst_ref=dst, send_sem=send, recv_sem=recv,
            device_id={"stage": stage}, device_id_type=MESH,
        )

    def to_inner(src, dst, send, recv, inner):
        return pltpu.make_async_remote_copy(
            src_ref=src, dst_ref=dst, send_sem=send, recv_sem=recv,
            device_id={"inner": inner}, device_id_type=MESH,
        )

    def piece(e):
        return pl.ds(pl.multiple_of(e * part, part), part)

    with jax.named_scope("barrier"):
        pl.semaphore_wait(barrier, n_stage + 1)
    for c in mine:
        c.wait()

    def own(mine_v, slots, recv, sem, stage):
        there = slots.at[i, p // MERGE, :, piece(p % MERGE)]

        @pl.when(p == stage)
        def _():
            pltpu.make_async_copy(mine_v, there, recv.at[p // MERGE]).start()

        @pl.when(p != stage)
        def _():
            to_stage(mine_v, there, sem, recv.at[p // MERGE], stage).start()

    own(own_v.at[0], hw, h_recv, xsem.at[0], 0)
    own(own_v.at[1], gw, g_recv, xsem.at[1], last)

    def ring_first(q, m, whole):
        a = whole.at[i, m]
        to_inner(a, a, ring_send.at[q, m, 0], ring_recv.at[q, m, 0], right).start()
        to_inner(a, a, ring_send.at[q, m, 1], ring_recv.at[q, m, 1], left).start()

    def forward_right(q, m, whole):
        a = whole.at[left, m]
        to_inner(a, a, ring_send.at[q, m, 0], ring_recv.at[q, m, 0], right).wait_recv()
        a = whole.at[left, m, pl.ds(0, half)]
        to_inner(a, a, ring_send.at[q, m, 2], ring_recv.at[q, m, 2], right).start()

    def forward_left(q, m, whole):
        b = whole.at[right, m]
        to_inner(b, b, ring_send.at[q, m, 1], ring_recv.at[q, m, 1], left).wait_recv()
        b = whole.at[right, m, pl.ds(half, half)]
        to_inner(b, b, ring_send.at[q, m, 3], ring_recv.at[q, m, 3], left).start()

    def ring_forward(q, m, whole):
        forward_right(q, m, whole)
        forward_left(q, m, whole)

    def ring_far(q, m, whole):
        far = lax.rem(i + 2, n_inner)
        a, b = whole.at[far, m, pl.ds(0, half)], whole.at[far, m, pl.ds(half, half)]
        return (
            to_inner(a, a, ring_send.at[q, m, 2], ring_recv.at[q, m, 2], right),
            to_inner(b, b, ring_send.at[q, m, 3], ring_recv.at[q, m, 3], left),
        )

    def ring_arrived(m, q):
        for c in ring_far(q, m, (hw, gw)[q]):
            c.wait_recv()

    def ring_sent(m):
        for q, whole in ((0, hw), (1, gw)):
            for c in ring_far(q, m, whole):
                c.wait_send()
            a = whole.at[i, m]
            to_inner(a, a, ring_send.at[q, m, 0], ring_recv.at[q, m, 0], right).wait_send()
            to_inner(a, a, ring_send.at[q, m, 1], ring_recv.at[q, m, 1], left).wait_send()

    def pass_on(m, lo, hi, src, slots, send, recv, end, nxt, out, out_sem):
        @pl.when(p != end)
        def _():
            some = pl.ds(lo, hi - lo)
            to_stage(src.at[m, some], slots.at[i, m, some], send.at[m], recv.at[m], nxt).start()

        if hi - lo < nd:
            return

        @pl.when(p == end)
        def _():
            for e in range(MERGE):
                home = m * MERGE + e

                @pl.when(p != home)
                def _():
                    for c in range(nd):
                        to_stage(src.at[m, c, piece(e)], flat(out, c), send.at[m], out_sem, home).start()

                @pl.when(p == home)
                def _():
                    for c in range(nd):
                        pltpu.make_async_copy(src.at[m, c, piece(e)], flat(out, c), out_sem).start()

    def step_of(m, split, x_in, wa, activate, second, wb, src, *rest):
        blocks, k_half = nf // SLABS, nf // 2
        early_acts = blocks // 2 if second is None else blocks - 1
        zs_in = []

        def act_of(b):
            a = activate(b * SLABS, zs_in[b])
            for c in range(SLABS):
                act[b * SLABS + c] = _cut(a, c)

        def part_dot(lo, count, k):
            a = _wide([act[k + c] for c in range(k_half)])
            return _dot(a, _wide([wb[lo + c, k * LANES : (k + k_half) * LANES, :] for c in range(count)]))

        for b in range(blocks):
            zs_in.append(_dot(x_in, _wide([wa[b * SLABS + c] for c in range(SLABS)])))
            if 0 < b <= early_acts:
                act_of(b - 1)
        if second is not None:
            act_of(blocks - 1)
            second()
        count = half if split else nd
        for lo in range(0, nd, count):
            u = part_dot(lo, count, 0)
            if lo == 0 and second is None:
                for b in range(early_acts, blocks):
                    act_of(b)
            u = u + part_dot(lo, count, k_half)
            out = (x_in[:, lo * LANES : (lo + count) * LANES].astype(F32) + u).astype(BF16)
            for c in range(count):
                src[m, lo + c] = _cut(out, c)
            pass_on(m, lo, lo + count, src, *rest)

    def second_weights():
        for c in loads[nf:]:
            c.wait()

    def forward(m, sloped, split):
        @pl.when((m == 0) & (p > 0) & (p < mid))
        def _():
            second_weights()

        with jax.named_scope("wait_h"):
            pltpu.make_async_copy(hw.at[i, m], hw.at[i, m], h_recv.at[m]).wait()
        h = _wide([hw[i, m, c] for c in range(nd)])

        def activate(b, z):
            a, slope = _gelu_and_slope(z)
            for c in range(SLABS):
                zs[m, b + c] = _cut(slope if sloped else z, c)
            return a.astype(BF16)

        def second():
            @pl.when((m == 0) & (p == 0))
            def _():
                second_weights()

        step_of(
            m, split, h, w1v, activate, None if sloped or split else second, w2v,
            ho, hw, h_send, h_recv, last, jnp.minimum(p + 1, last), y, out_recv.at[0],
        )

        @pl.when((p < mid) | (m < early))
        def _():
            ring_first(0, m, hw)

    def backward(m, split):
        @pl.when((p >= mid) & (p < n_stage - 2) & (m == early + 1))
        def _():
            ring_forward(1, early - 1, gw)

        with jax.named_scope("wait_g"):
            pltpu.make_async_copy(gw.at[i, m], gw.at[i, m], g_recv.at[m]).wait()

        @pl.when(m < early)
        def _():
            ring_first(1, m, gw)

        dh = _wide([gw[i, m, c] for c in range(nd)])
        step_of(
            m, split, dh, w2t, lambda b, da: (da * _wide([zs[m, b + c] for c in range(SLABS)])).astype(BF16), None,
            w1t, go, gw, g_send, g_recv, 0, jnp.maximum(p - 1, 0), dx, out_recv.at[1],
        )

        @pl.when((p >= n_stage - 2) & (m == early))
        def _():
            ring_forward(0, 0, hw)

        @pl.when((p < mid) & (m > 0) & (m <= early))
        def _():
            ring_forward(1, jnp.maximum(m - 1, 0), gw)

        @pl.when((p >= mid) & (p < n_stage - 2) & (m == early))
        def _():
            ring_forward(1, 0, gw)

    def transpose_weights():
        def some(c, carry):
            s = pl.ds(pl.multiple_of(c * LANES, LANES), LANES)
            for e in range(nd):
                w1t[e, s, :] = w1v[c, e * LANES : (e + 1) * LANES, :].T
                w2t[c, e * LANES : (e + 1) * LANES, :] = w2v[e, s, :].T
            return carry

        lax.fori_loop(0, nf, some, 0)

    def slopes():
        def some(t, carry):
            m, b = t // (nf // SLABS), t % (nf // SLABS) * SLABS
            for c in range(SLABS):
                zs[m, b + c] = _gelu_and_slope(zs[m, b + c])[1]
            return carry

        lax.fori_loop(0, m_all * (nf // SLABS), some, 0)

    def each(lo, hi, fn):
        lax.fori_loop(lo, hi, lambda m, c: (fn(m), c)[1], 0)

    def group(whole, part=0):
        return lambda k, c: whole[k // early, part * early + k % early, c]

    def pre_stores(j):
        b = j % 2
        return (
            pltpu.make_async_copy(narrow.at[b], a_pre.at[j], pre_sem.at[0, b]),
            pltpu.make_async_copy(full.at[b, pl.ds(0, SLABS * groups)], s_pre.at[j], pre_sem.at[1, b]),
        )

    def pre_loads(j):
        b = j % 2
        return (
            pltpu.make_async_copy(
                a_pre.at[j], w2v.at[pl.ds(b * SLABS, SLABS), pl.ds(0, tokens)], pre_sem.at[0, b]
            ),
            pltpu.make_async_copy(s_pre.at[j], zs.at[b, pl.ds(0, SLABS * groups)], pre_sem.at[1, b]),
        )

    def pre_unit(j):
        b = j % 2

        @pl.when(j > 1)
        def _():
            for c in pre_stores(j):
                c.wait()

        for ks, s in _chunks(256, groups, rows):
            z = _dot(_rows_of(group(hw, j // units), ks, nd), _wide([w1v[j % units * SLABS + c] for c in range(SLABS)]))
            a, slope = _gelu_and_slope(z)
            a = a.astype(BF16)
            for c in range(SLABS):
                narrow[b, c, s, :] = _cut(a, c)
                for n, k in enumerate(ks):
                    full[b, c * groups + k] = _cut(slope[n * rows : (n + 1) * rows], c)
        for c in pre_stores(j):
            c.start()

    formed = jnp.where(
        p < PRE_LATE, 2 * units,
        jnp.where(p < mid - 1, units, jnp.where(p == mid - 1, units * 3 // 4, 0)),
    )

    def part_copies(j):
        b, some = j % 2, pl.ds(0, SLABS * nd)
        return (
            pltpu.make_async_copy(full.at[b, some], d1_part.at[j], part_sem.at[0, b]),
            pltpu.make_async_copy(zs.at[m_all - 2 + b, some], d2_part.at[j], part_sem.at[1, b]),
        )

    def late_copies():
        return [
            pltpu.make_async_copy(whole.at[k, pl.ds(early, m_all - early)], out.at[k], late_sem.at[q, k])
            for q, (whole, out) in enumerate(((hw, h_late), (gw, g_late)))
            for k in range(n_inner)
        ]

    def sent(m):
        ring_sent(m)
        for src, slots, send, recv, end in ((ho, hw, h_send, h_recv, last), (go, gw, g_send, g_recv, 0)):
            for e in range(MERGE):
                a = src.at[m, :, piece(e)]

                @pl.when((p != end) | (p != m * MERGE + e))
                def _():
                    to_stage(a, a, send.at[m], recv.at[m], 0).wait_send()

        @pl.when((m == 0) & (p != 0))
        def _():
            to_stage(own_v.at[0], own_v.at[0], xsem.at[0], h_recv.at[0], 0).wait_send()

        @pl.when((m == 0) & (p != last))
        def _():
            to_stage(own_v.at[1], own_v.at[1], xsem.at[1], g_recv.at[0], last).wait_send()

    def unit(j):
        def forwards(m):
            @pl.when(p >= mid)
            def _():
                ring_forward(0, m, hw)

            ring_forward(1, m, gw)

        def firsts(m):
            @pl.when(p >= mid)
            def _():
                ring_first(0, m, hw)

            ring_first(1, m, gw)

        @pl.when(j == 0)
        def _():
            @pl.when(p >= n_stage - 2)
            def _():
                ring_forward(1, 0, gw)
                each(1, early, lambda e: (ring_forward(0, e, hw), ring_forward(1, e, gw)))


            @pl.when(formed > 0)
            def _():
                for c in pre_loads(0):
                    c.start()

            each(0, early, lambda m: ring_arrived(m, 1))

            @pl.when(formed == 0)
            def _():
                each(0, early, lambda m: ring_arrived(m, 0))

            each(early, m_all, firsts)

            @pl.when(formed == 0)
            def _():
                _transposed_rows(group(hw), groups, rows, nd, ht)

        for m in range(early, m_all):
            @pl.when(j == 2 * (m - early + 1) + jnp.where(p < mid, 0, 1))
            def _():
                forwards(m)

        @pl.when(j == units - 1)
        def _():
            each(early, m_all, lambda m: ring_arrived(m, 1))

            @pl.when(p >= PRE_LATE)
            def _():
                each(early, m_all, lambda m: ring_arrived(m, 0))

            for c in late_copies():
                c.start()
            each(0, m_all, sent)

        @pl.when(j > 1)
        def _():
            for c in part_copies(j):
                c.wait()

        def put(v1, v2):
            for c in range(SLABS):
                for e in range(nd):
                    zs[m_all - 2 + j % 2, c * nd + e] = _cut(v2[c * LANES : (c + 1) * LANES], e)
                    full[j % 2, c * nd + e] = _cut(v1[e * LANES : (e + 1) * LANES], c)

        def block(ready):
            _dw_block(
                512, group(hw), group(gw), groups, rows, nd,
                lambda: _wide([w1v[j * SLABS + c] for c in range(SLABS)]),
                lambda: _wide([w2t[j * SLABS + c] for c in range(SLABS)]),
                ht, ab, zb, put, ready,
            )

        @pl.when(j < formed)
        def _():
            b = j % 2
            for c in pre_loads(j):
                c.wait()

            @pl.when(j + 1 < jnp.minimum(formed, units))
            def _():
                for c in pre_loads(j + 1):
                    c.start()

            block((
                lambda c: w2v[b * SLABS + c, 0:tokens, :],
                lambda k, c: zs[b, c * groups + k],
            ))

        @pl.when(j >= formed)
        def _():
            block(None)

        for c in part_copies(j):
            c.start()

    kept = (
        pltpu.make_async_copy(w1v, w1_out, keep_sem.at[0]), pltpu.make_async_copy(w2t, w2_out, keep_sem.at[1])
    )
    with jax.named_scope("loads"):
        for c in loads[:nf]:
            c.wait()

    first = jnp.where(p == last, 1, m_all)
    rest = m_all - first
    turn = jnp.where(p < n_stage // 2, first, 0)

    def step(k, carry):
        j = k - first
        swap = j < 2 * rest
        is_u = k >= 2 * m_all
        is_f = (j < 0) | (swap & (j % 2 == 1))
        is_b = jnp.logical_not(is_f | is_u)
        m_f = jnp.where(j < 0, k, jnp.minimum(first + j // 2, m_all - 1))
        m_b = jnp.maximum(jnp.minimum(jnp.where(swap, j // 2, j - rest), m_all - 1), 0)
        u = jnp.maximum(k - 2 * m_all, 0)

        @pl.when(k == turn)
        def _():
            with jax.named_scope("transp"):
                @pl.when(p >= n_stage // 2)
                def _():
                    for c in loads[nf:]:
                        c.wait()

                transpose_weights()
                for c in kept:
                    c.start()

        @pl.when((k == first) & (p < n_stage - 2))
        def _():
            with jax.named_scope("slopes"):
                slopes()
            with jax.named_scope("hring"):
                each(0, jnp.where(p < mid, m_all, early), lambda m: ring_forward(0, m, hw))

        @pl.when((k == first) & (formed > 0))
        def _():
            with jax.named_scope("pre"):
                each(0, early, lambda m: ring_arrived(m, 0))

                @pl.when(p < PRE_LATE)
                def _():
                    each(early, m_all, lambda m: ring_arrived(m, 0))

                _transposed_rows(group(hw), groups, rows, nd, ht)
                each(0, formed, pre_unit)
                for c in (*pre_stores(0), *pre_stores(1)):
                    c.wait()

        early_f, odd = is_f & (p < n_stage - 2), p % 2 == 1
        for when, sloped, split in (
            (early_f & jnp.logical_not(odd), False, False),
            (early_f & odd, False, True),
            (is_f & (p >= n_stage - 2), True, False),
        ):
            @pl.when(when)
            def _():
                with jax.named_scope("fwd"):
                    forward(m_f, sloped, split)

        leaves = (p > 0) & jnp.logical_not(odd)
        for when, split in ((is_b & leaves, True), (is_b & jnp.logical_not(leaves), False)):
            @pl.when(when)
            def _():
                with jax.named_scope("bwd"):
                    backward(m_b, split)

        @pl.when(is_u)
        def _():
            with jax.named_scope("unit"):
                unit(u)

        return carry

    lax.fori_loop(0, 2 * m_all + units, step, 0)

    with jax.named_scope("finish"):
        for c in (*kept, *part_copies(units - 2), *part_copies(units - 1), *late_copies()):
            c.wait()
    with jax.named_scope("outwait"):
        pltpu.make_async_copy(y.at[0], y.at[0], out_recv.at[0]).wait()
        pltpu.make_async_copy(dx.at[0], dx.at[0], out_recv.at[1]).wait()


def _chain(n_stage, n_inner, x, g, w1, w2):
    mb, rows, d = x.shape
    f = w1.shape[-1]
    rows = rows * MERGE
    m_all = mb * n_stage // MERGE
    early = EARLY
    nd, nf = d // LANES, f // LANES
    blk = SLABS * LANES
    groups = n_inner * early
    tokens = groups * rows
    tiles = SLABS * max(nd, groups)
    hbm = pl.BlockSpec(memory_space=pltpu.HBM)
    whole = (n_inner, m_all, nd, rows, LANES)
    late = jax.ShapeDtypeStruct((n_inner, m_all - early, nd, rows, LANES), BF16)
    dma = pltpu.SemaphoreType.DMA
    vmem = pltpu.VMEM
    return pl.pallas_call(
        functools.partial(_chain_kernel, n_stage, n_inner),
        out_shape=[
            jax.ShapeDtypeStruct(x.shape, BF16), jax.ShapeDtypeStruct(x.shape, BF16), late, late,
            jax.ShapeDtypeStruct((nf, d, LANES), BF16), jax.ShapeDtypeStruct((nf, d, LANES), BF16),
            jax.ShapeDtypeStruct((f // blk, SLABS * nd, LANES, LANES), F32),
            jax.ShapeDtypeStruct((f // blk, SLABS * nd, LANES, LANES), F32),
            jax.ShapeDtypeStruct((2 * f // blk, SLABS, tokens, LANES), BF16),
            jax.ShapeDtypeStruct((2 * f // blk, SLABS * groups, rows, LANES), F32),
        ],
        in_specs=[hbm] * 4,
        out_specs=[hbm] * 10,
        scratch_shapes=[
            vmem((nf, d, LANES), BF16), vmem((nd, f, LANES), BF16),
            vmem((nd, f, LANES), BF16), vmem((nf, d, LANES), BF16),
            vmem(whole, BF16), vmem(whole, BF16),
            vmem((m_all, nd, rows, LANES), BF16), vmem((m_all, nd, rows, LANES), BF16),
            vmem((m_all, nf, rows, LANES), F32), vmem((nf, rows, LANES), BF16),
            vmem((tokens // LANES, d, LANES), BF16),
            vmem((2, SLABS, tokens, LANES), BF16), vmem((2, tiles, LANES, LANES), F32),
            vmem((2, nd, rows // MERGE, LANES), BF16),
            dma((2,)), dma((2,)), dma((m_all,)), dma((m_all,)), dma((m_all,)), dma((m_all,)), dma((2,)),
            dma((2, m_all, 4)), dma((2, m_all, 4)), dma((2, 2)), dma((2, n_inner)), dma((2, 2)), dma((2,)), dma((2,)),
        ],
        compiler_params=pltpu.CompilerParams(
            collective_id=0, has_side_effects=True, vmem_limit_bytes=VMEM_LIMIT
        ),
        name="chain",
    )(x, g, w1, w2)


def _late_kernel(
    h, g, y_in, dx_in, w1, w2t, p1, p2, ap, sp, d1, d2, y, dx,
    hv, gv, w1v, w2v, p1v, p2v, av, sv, d1v, d2v, ht, ab, zb, yv, first_sem, load_sem, store_sem, pass_sem,
):
    groups, nd, rows, _ = h.shape
    units = w1.shape[0] // SLABS
    d, blk = d1v.shape[1:]

    def pre(j):
        return (lax.axis_index("stage") < PRE_LATE) & ((j % 2 == 1) | (j == units - 2))

    def weights(j):
        b, some = j % DEEP, pl.ds(j * SLABS, SLABS)
        return (pltpu.make_async_copy(w2t.at[some], w2v.at[b], load_sem.at[0, b]),)

    def own(j):
        b, some = j % DEEP, pl.ds(j * SLABS, SLABS)
        return (pltpu.make_async_copy(w1.at[some], w1v.at[b], load_sem.at[1, b]),)

    def ready(j):
        b = j % DEEP
        return (
            pltpu.make_async_copy(ap.at[units + j], av.at[b], load_sem.at[1, b]),
            pltpu.make_async_copy(sp.at[units + j], sv.at[b], load_sem.at[2, b]),
        )

    def parts(j):
        b = j % DEEP
        return (
            pltpu.make_async_copy(p1.at[j], p1v.at[b], load_sem.at[3, b]),
            pltpu.make_async_copy(p2.at[j], p2v.at[b], load_sem.at[4, b]),
        )

    def stores(j):
        b, some = j % 2, pl.ds(pl.multiple_of(j * blk, blk), blk)
        return (
            pltpu.make_async_copy(d1v.at[b], d1.at[:, some], store_sem.at[0, b]),
            pltpu.make_async_copy(d2v.at[b], d2.at[some, :], store_sem.at[1, b]),
        )

    def do(copies, how):
        for c in copies:
            getattr(c, how)()

    def inputs(j, how):
        @pl.when(pre(j))
        def _():
            do(ready(j), how)

        @pl.when(jnp.logical_not(pre(j)))
        def _():
            do(own(j), how)

        do(weights(j), how)

    firsts = (pltpu.make_async_copy(h, hv, first_sem.at[0]), pltpu.make_async_copy(g, gv, first_sem.at[1]))
    firsts[0].start()
    inputs(0, "start")
    firsts[1].start()
    do(parts(0), "start")
    into = [pltpu.make_async_copy(a, yv.at[n], pass_sem.at[n]) for n, a in enumerate((y_in, dx_in))]
    out_of = [pltpu.make_async_copy(yv.at[n], a, pass_sem.at[n]) for n, a in enumerate((y, dx))]
    do(into, "start")
    firsts[0].wait()
    _transposed_rows(lambda k, c: hv[k, c], groups, rows, nd, ht)
    do(into, "wait")
    do(out_of, "start")

    def unit(j, carry):
        b, n = j % 2, j % DEEP
        inputs(j, "wait")
        do(parts(j), "wait")

        @pl.when(j == 0)
        def _():
            firsts[1].wait()
            for e in range(1, DEEP - 1):
                inputs(e, "start")
                do(parts(e), "start")

        @pl.when(j + DEEP - 1 < units)
        def _():
            inputs(j + DEEP - 1, "start")
            do(parts(j + DEEP - 1), "start")

        @pl.when(j > 1)
        def _():
            do(stores(j), "wait")

        def put(v1, v2):
            for c in range(SLABS):
                for e in range(nd):
                    r, s = slice(e * LANES, (e + 1) * LANES), slice(c * LANES, (c + 1) * LANES)
                    d2v[b, s, r] = p2v[n, c * nd + e] + v2[s, r]
                    d1v[b, r, s] = p1v[n, c * nd + e] + v1[r, s]

        def block(ready):
            _dw_block(
                512, lambda k, c: hv[k, c], lambda k, c: gv[k, c], groups, rows, nd,
                lambda: _wide([w1v[n, c] for c in range(SLABS)]), lambda: _wide([w2v[n, c] for c in range(SLABS)]),
                ht, ab, zb, put, ready,
            )

        @pl.when(pre(j))
        def _():
            block((lambda c: av[n, c], lambda k, c: sv[n, c * groups + k]))

        @pl.when(jnp.logical_not(pre(j)))
        def _():
            block(None)

        do(stores(j), "start")
        return carry

    lax.fori_loop(0, units, unit, 0)
    do(stores(units - 2), "wait")
    do(stores(units - 1), "wait")
    do(out_of, "wait")


def _late(h, g, y, dx, w1, w2t, p1, p2, ap, sp):
    groups, nd, rows, _ = h.shape
    nf, d, _ = w1.shape
    f, blk, t = nf * LANES, SLABS * LANES, groups * rows
    hbm = pl.BlockSpec(memory_space=pltpu.HBM)
    vmem, dma = pltpu.VMEM, pltpu.SemaphoreType.DMA
    return pl.pallas_call(
        _late_kernel,
        in_specs=[hbm] * 10,
        out_specs=[hbm] * 4,
        out_shape=[
            jax.ShapeDtypeStruct((d, f), F32), jax.ShapeDtypeStruct((f, d), F32),
            jax.ShapeDtypeStruct(y.shape, BF16), jax.ShapeDtypeStruct(dx.shape, BF16),
        ],
        scratch_shapes=[
            vmem(h.shape, BF16), vmem(g.shape, BF16),
            vmem((DEEP, SLABS, d, LANES), BF16), vmem((DEEP, SLABS, d, LANES), BF16),
            vmem((DEEP, *p1.shape[1:]), F32), vmem((DEEP, *p2.shape[1:]), F32),
            vmem((DEEP, *ap.shape[1:]), BF16), vmem((DEEP, *sp.shape[1:]), F32),
            vmem((2, d, blk), F32), vmem((2, blk, d), F32),
            vmem((t // LANES, d, LANES), BF16), vmem((SLABS, t, LANES), BF16), vmem((SLABS, t, LANES), BF16),
            vmem((2, *y.shape), BF16),
            dma((2,)), dma((5, DEEP)), dma((2, 2)), dma((2,)),
        ],
        compiler_params=pltpu.CompilerParams(vmem_limit_bytes=VMEM_LIMIT),
        cost_estimate=pl.CostEstimate(flops=8 * t * d * f, bytes_accessed=20 * d * f, transcendentals=t * f),
        name="late",
    )(h, g, y, dx, w1, w2t, p1, p2, ap, sp)


def solution(mesh):
    n_stage, n_inner = mesh.shape["stage"], mesh.shape["inner"]

    def body(x, g, w1, w2):
        y, dx, h, gg, w1s, w2s, *parts = _chain(n_stage, n_inner, x, g, w1, w2)
        flat = (-1, *h.shape[2:])
        d1, d2, y, dx = _late(h.reshape(flat), gg.reshape(flat), y, dx, w1s, w2s, *parts)
        return y, dx, d1.reshape(w1.shape), d2.reshape(w2.shape)

    tok = P(("data", "stage"), "inner", None)
    wsp = P(None, "stage", None, None)
    dsp = P("data", "stage", None, None)
    return jax.shard_map(body, mesh=mesh, in_specs=(tok, tok, wsp, wsp), out_specs=(tok, tok, dsp, dsp), check_vma=False)
```
